128 devices in a mesh: fsdp: 32 (over z, y, x_hi), sp: 4 (over x_lo, core).
Axes of the slice: x: 4 (x_hi: 2, x_lo: 2; x = x_hi * 2 + x_lo), y: 4, z: 4, core: 2. Of those that a mesh axis runs over, the one named last changes fastest.
Arguments:
- tokens: bfloat16 [32, 512, 1536], P('fsdp', 'sp'), may hold values from -6 to 6
- modulation: float32 [32, 1, 6, 1536], P('fsdp'), may hold values from -4 to 4
- w_qkv: bfloat16 [1, 1536, 3, 1536], P(None, 'fsdp', None, 'sp'), may hold values from -0.15625 to 0.15625
- w_out: bfloat16 [1, 1536, 1536], P(None, 'sp', 'fsdp'), may hold values from -0.15625 to 0.15625
- w_in: bfloat16 [1, 1536, 6144], P(None, 'fsdp', 'sp'), may hold values from -0.15625 to 0.15625
- w_back: bfloat16 [1, 6144, 1536], P(None, 'sp', 'fsdp'), may hold values from -0.078125 to 0.078125
- out_grad: bfloat16 [32, 512, 1536], P('fsdp', 'sp'), may hold values from -6 to 6
Outputs:
- final_out: bfloat16 [32, 512, 1536], P('fsdp', 'sp')
- input_grad: float32 [32, 512, 1536], P('fsdp', 'sp')
- grad_qkv: float32 [1, 1536, 3, 1536], P(None, 'fsdp', None, 'sp')
- grad_out: float32 [1, 1536, 1536], P(None, 'sp', 'fsdp')
- grad_in: float32 [1, 1536, 6144], P(None, 'fsdp', 'sp')
- grad_back: float32 [1, 6144, 1536], P(None, 'sp', 'fsdp')
The draws below stay inside these ranges and needn't reach their ends.
All inputs are finite; a program needn't handle non-finite values.
Results may differ from the reference program's by a relative error of at most 0.03.
Values may be sent and summed in bfloat16 or wider, within the bound.
A program may use at most 128 MiB of HBM per device.

```python
import math
import jax
import jax.numpy as jnp
from jax import lax

D = 1536
HEAD_DIM = 128
FF = 6144
LAYERS = 1
SEQ = 512
BATCH = 32
N_FSDP = 32


def block_scale(rng, dims, shards, smallest, top_value):
    def one(axis_at, parts):
        heights = jax.random.uniform(jax.random.fold_in(jax.random.fold_in(rng, 6), axis_at), (parts,), jnp.float32, smallest / len(shards), top_value / len(shards))
        return jnp.repeat(jnp.exp(heights), dims[axis_at] // parts).reshape((-1,) + (1,) * (len(dims) - axis_at - 1))

    gain = one(*shards[0])
    for cut in shards[1:]:
        gain = gain * one(*cut)
    return gain


def bell_draw(stream_key, shape, spread, limit, cuts=(), dtype=jnp.bfloat16):
    drawn = spread * jax.random.normal(stream_key, shape, jnp.float32)
    if cuts:
        drawn = drawn * block_scale(stream_key, shape, cuts, -0.22, 0.18)
    return jnp.clip(drawn, -limit, limit).astype(dtype)


def setup_inputs(seed: int = 0) -> dict:
    keys = jax.random.split(jax.random.key(seed), 8)
    tokens = bell_draw(keys[0], (BATCH, SEQ, D), 1.0, 6.0, ((0, 32), (1, 4)))
    modulation = bell_draw(keys[1], (BATCH, LAYERS, 6, D), 1.0, 4.0, ((0, 32),), jnp.float32)
    w_qkv = bell_draw(keys[2], (LAYERS, D, 3, D), D ** -0.5, 0.15625, ((1, 32), (3, 4)))
    w_out = bell_draw(keys[3], (LAYERS, D, D), D ** -0.5, 0.15625, ((1, 4), (2, 32)))
    w_in = bell_draw(keys[4], (LAYERS, D, FF), D ** -0.5, 0.15625, ((1, 32), (2, 4)))
    w_back = bell_draw(keys[5], (LAYERS, FF, D), FF ** -0.5, 0.078125, ((1, 4), (2, 32)))
    out_grad = bell_draw(keys[6], (BATCH, SEQ, D), 1.0, 6.0, ((0, 32), (1, 4)))
    return dict(tokens=tokens, modulation=modulation, w_qkv=w_qkv, w_out=w_out, w_in=w_in, w_back=w_back, out_grad=out_grad)


ln_eps = 1e-06
temper = 2.5
block_limit = 512

def normalize(stream):
    mean_part = lax.optimization_barrier(jnp.mean(stream, axis=-1, keepdims=True))
    centred = stream - mean_part
    rstd = lax.rsqrt(lax.optimization_barrier(jnp.mean(centred * centred, axis=-1, keepdims=True)) + ln_eps)
    return (centred * rstd, rstd)

def norm_back(normed, rstd, incoming):
    first = lax.optimization_barrier(jnp.mean(incoming, axis=-1, keepdims=True))
    second = lax.optimization_barrier(jnp.mean(incoming * normed, axis=-1, keepdims=True))
    return rstd * (incoming - first - normed * second)

def gelu_tanh(hidden):
    return jax.nn.gelu(hidden, approximate=True)

def project(left, weight):
    flat_rows = left.reshape(-1, left.shape[-1])
    result = jnp.dot(flat_rows, weight, preferred_element_type=jnp.float32)
    return result.reshape(left.shape[:-1] + (weight.shape[1],))

def project_back(left, weight):
    flat_rows = left.reshape(-1, left.shape[-1])
    result = lax.dot_general(flat_rows, weight, (((1,), (1,)), ((), ())), preferred_element_type=jnp.float32)
    return result.reshape(left.shape[:-1] + (weight.shape[0],))

def group_grad(left, right, grad_scale):
    width_left = left.shape[-1]
    width_right = right.shape[-1]
    left_groups = left.reshape(N_FSDP, -1, width_left)
    right_groups = right.reshape(N_FSDP, -1, width_right)

    def add_group(total, pair):
        left_part, right_part = pair
        term = lax.dot_general(left_part, right_part, (((0,), (0,)), ((), ())), preferred_element_type=jnp.float32) * grad_scale
        rounded = lax.optimization_barrier(term.astype(jnp.bfloat16))
        return (total + rounded.astype(jnp.float32), None)
    total, unused = lax.scan(add_group, jnp.zeros((width_left, width_right), jnp.float32), (left_groups, right_groups))
    return total

def split_heads(packed, head_count):
    return packed.reshape(packed.shape[:-1] + (head_count, packed.shape[-1] // head_count))

def heads_major(tensor):
    videos, seq_len, head_count, head_width = tensor.shape
    return tensor.transpose(0, 2, 1, 3).reshape(videos * head_count, seq_len, head_width)

def heads_minor(tensor, videos):
    merged, seq_len, head_width = tensor.shape
    return tensor.reshape(videos, merged // videos, seq_len, head_width).transpose(0, 2, 1, 3)

def attend_head(triple):
    queries, key_rows, values = triple
    seq_len, head_width = queries.shape
    block_size = min(block_limit, seq_len)
    score_factor = temper / math.sqrt(head_width)
    values_wide = values.astype(jnp.float32)

    def one_block(query_rows):
        scores = jnp.dot(query_rows, key_rows.T, preferred_element_type=jnp.float32) * score_factor
        softmaxed = jax.nn.softmax(scores, axis=-1)
        return jnp.dot(softmaxed, values_wide, precision=lax.Precision.HIGHEST).astype(jnp.bfloat16)
    attended = lax.map(one_block, queries.reshape(seq_len // block_size, block_size, head_width))
    return attended.reshape(seq_len, head_width)

def attend_back(quadruple):
    queries, key_rows, values, upstream = quadruple
    seq_len, head_width = queries.shape
    block_size = min(block_limit, seq_len)
    score_factor = temper / math.sqrt(head_width)
    keys_wide = key_rows.astype(jnp.float32)

    def one_block(running, block_pair):
        query_rows, grad_rows = block_pair
        scores = jnp.dot(query_rows, key_rows.T, preferred_element_type=jnp.float32) * score_factor
        softmaxed = jax.nn.softmax(scores, axis=-1)
        dprobs = jnp.dot(grad_rows, values.T, preferred_element_type=jnp.float32)
        dscores = softmaxed * (dprobs - lax.optimization_barrier(jnp.sum(softmaxed * dprobs, axis=-1, keepdims=True))) * score_factor
        dquery = jnp.dot(dscores, keys_wide, precision=lax.Precision.HIGHEST)
        grad_keys = running[0] + jnp.dot(dscores.T, query_rows.astype(jnp.float32), precision=lax.Precision.HIGHEST)
        dvalues = running[1] + jnp.dot(softmaxed.T, grad_rows.astype(jnp.float32), precision=lax.Precision.HIGHEST)
        return ((grad_keys, dvalues), dquery)
    zero_rows = jnp.zeros((seq_len, head_width), jnp.float32)
    count = seq_len // block_size
    blocks = (queries.reshape(count, block_size, head_width), upstream.reshape(count, block_size, head_width))
    (grad_keys, dvalues), dquery = lax.scan(one_block, (zero_rows, zero_rows), blocks)
    return (dquery.reshape(seq_len, head_width).astype(jnp.bfloat16), grad_keys.astype(jnp.bfloat16), dvalues.astype(jnp.bfloat16))

def attend_all(queries, key_rows, values):
    attended = lax.map(attend_head, (heads_major(queries), heads_major(key_rows), heads_major(values)))
    return heads_minor(attended, queries.shape[0])

def attend_all_back(queries, key_rows, values, upstream):
    grad_heads = lax.map(attend_back, (heads_major(queries), heads_major(key_rows), heads_major(values), heads_major(upstream)))
    return tuple((heads_minor(grad_piece, queries.shape[0]) for grad_piece in grad_heads))

def reference(tokens, modulation, w_qkv, w_out, w_in, w_back, out_grad):
    videos, seq_len, model_width = tokens.shape
    layers = w_qkv.shape[0]
    head_count = model_width // HEAD_DIM
    grad_scale = 1.0 / math.sqrt(videos * seq_len)
    stream = tokens.astype(jnp.float32)
    stored = []
    for layer_index in range(layers):
        layer_mod = modulation[:, layer_index][:, :, None, :]
        joint = w_qkv[layer_index].reshape(model_width, 3 * model_width)
        normed_first, rstd_first = normalize(stream)
        input_first = (normed_first * (1.0 + layer_mod[:, 1]) + layer_mod[:, 0]).astype(jnp.bfloat16)
        packed = project(input_first, joint).astype(jnp.bfloat16)
        queries = split_heads(packed[..., :model_width], head_count)
        key_rows = split_heads(packed[..., model_width:2 * model_width], head_count)
        values = split_heads(packed[..., 2 * model_width:], head_count)
        attended = attend_all(queries, key_rows, values).reshape(videos, seq_len, model_width)
        middle = stream + layer_mod[:, 2] * project(attended, w_out[layer_index])
        normed_second, rstd_second = normalize(middle)
        input_second = (normed_second * (1.0 + layer_mod[:, 4]) + layer_mod[:, 3]).astype(jnp.bfloat16)
        hidden = project(input_second, w_in[layer_index])
        activated = gelu_tanh(hidden).astype(jnp.bfloat16)
        stream = middle + layer_mod[:, 5] * project(activated, w_back[layer_index])
        stored.append((normed_first, rstd_first, input_first, queries, key_rows, values, attended, normed_second, rstd_second, input_second, hidden, activated))
    final_out = stream.astype(jnp.bfloat16)
    stream_grad = out_grad.astype(jnp.float32)
    results = [None] * layers
    for layer_index in range(layers - 1, -1, -1):
        normed_first, rstd_first, input_first, queries, key_rows, values, attended, normed_second, rstd_second, input_second, hidden, activated = stored[layer_index]
        layer_mod = modulation[:, layer_index][:, :, None, :]
        joint = w_qkv[layer_index].reshape(model_width, 3 * model_width)
        down_grad = (layer_mod[:, 5] * stream_grad).astype(jnp.bfloat16)
        back_hidden = project_back(down_grad, w_back[layer_index])
        unused, pullback = jax.vjp(gelu_tanh, hidden)
        up_grad = pullback(back_hidden)[0].astype(jnp.bfloat16)
        back_second = project_back(up_grad, w_in[layer_index])
        stream_grad = stream_grad + norm_back(normed_second, rstd_second, back_second * (1.0 + layer_mod[:, 4]))
        attn_grad = (layer_mod[:, 2] * stream_grad).astype(jnp.bfloat16)
        mixed_grad = split_heads(project_back(attn_grad, w_out[layer_index]).astype(jnp.bfloat16), head_count)
        grad_query, grad_keys, grad_values = attend_all_back(queries, key_rows, values, mixed_grad)
        packed_grad = jnp.concatenate([grad_query.reshape(videos, seq_len, model_width), grad_keys.reshape(videos, seq_len, model_width), grad_values.reshape(videos, seq_len, model_width)], axis=-1)
        back_first = project_back(packed_grad, joint)
        stream_grad = stream_grad + norm_back(normed_first, rstd_first, back_first * (1.0 + layer_mod[:, 1]))
        results[layer_index] = (group_grad(input_first, packed_grad, grad_scale).reshape(model_width, 3, model_width), group_grad(attended, attn_grad, grad_scale), group_grad(input_second, up_grad, grad_scale), group_grad(activated, down_grad, grad_scale))
    grad_qkv = jnp.stack([results[index][0] for index in range(layers)])
    grad_out = jnp.stack([results[index][1] for index in range(layers)])
    grad_in = jnp.stack([results[index][2] for index in range(layers)])
    grad_back = jnp.stack([results[index][3] for index in range(layers)])
    return (final_out, stream_grad, grad_qkv, grad_out, grad_in, grad_back)
```

```python
import math

import jax
import jax.numpy as jnp
from jax import lax
from jax.sharding import PartitionSpec as P

HEAD_DIM = 128
LN_EPS = 1e-06
TEMPER = 2.5


def normalize(x):
    c = x - jnp.mean(x, axis=-1, keepdims=True)
    r = lax.rsqrt(jnp.mean(c * c, axis=-1, keepdims=True) + LN_EPS)
    return c * r, r


def norm_back(n, r, e):
    return r * (e - jnp.mean(e, axis=-1, keepdims=True) - n * jnp.mean(e * n, axis=-1, keepdims=True))


def dot(a, b, ca, cb):
    return lax.dot_general(a, b, (((ca,), (cb,)), ((), ())), preferred_element_type=jnp.float32)


def bf(x):
    return x.astype(jnp.bfloat16)


def body(tokens, modulation, w_qkv, w_out, w_in, w_back, out_grad):
    seq, width = tokens.shape[1:]
    own = w_qkv.shape[3]
    heads = own // HEAD_DIM
    ff = w_in.shape[2]
    c = TEMPER / math.sqrt(HEAD_DIM)
    q_s = 1.0 / math.sqrt(seq * lax.axis_size("fsdp") * lax.axis_size("sp"))
    mod = modulation[0, 0]
    m = [mod[i : i + 1] for i in range(6)]

    rows = w_qkv.shape[1]
    weights = [
        lax.all_gather(w, "fsdp", axis=0, tiled=True)
        for w in (w_qkv[0].reshape(rows, 3 * own), w_out[0].T, w_in[0], w_back[0].T)
    ]
    wq, wo, wi, wb = weights

    def gather(v):
        return lax.all_gather(v, "sp", axis=0, tiled=True)

    def scatter(v):
        return lax.psum_scatter(bf(v), "sp", scatter_dimension=0, tiled=True).astype(jnp.float32)

    x = tokens[0].astype(jnp.float32)
    dx = out_grad[0].astype(jnp.float32)
    n1, r1 = normalize(x)
    a1 = gather(bf(n1 * (1.0 + m[1]) + m[0]))
    dm = gather(bf(m[5] * dx))
    qkv = bf(dot(a1, wq, 1, 0))

    def attend(h):
        q, k, v = (qkv[:, i * own + h * HEAD_DIM : i * own + (h + 1) * HEAD_DIM] for i in range(3))
        p = jax.nn.softmax(dot(q, k, 1, 1) * c, axis=-1)
        return q, k, v, p

    o = jnp.concatenate([bf(dot(bf(p), v, 1, 0)) for q, k, v, p in map(attend, range(heads))], axis=1)
    mid = x + m[2] * scatter(dot(o, wo, 1, 1))
    n2, r2 = normalize(mid)
    a2 = gather(bf(n2 * (1.0 + m[4]) + m[3]))
    u = dot(a2, wi, 1, 0)
    act, pull = jax.vjp(lambda t: jax.nn.gelu(t, approximate=True), u)
    g = bf(act)
    final = bf(mid + m[5] * scatter(dot(g, wb, 1, 1)))

    du = bf(pull(dot(dm, wb, 1, 0))[0])
    dmid = dx + norm_back(n2, r2, scatter(dot(du, wi, 1, 1)) * (1.0 + m[4]))
    da = gather(bf(m[2] * dmid))
    do = bf(dot(da, wo, 1, 0))
    dq, dk, dv = [], [], []
    for h in range(heads):
        q, k, v, p = attend(h)
        doh = do[:, h * HEAD_DIM : (h + 1) * HEAD_DIM]
        dp = dot(doh, v, 1, 1)
        ds = bf(c * p * (dp - jnp.sum(p * dp, axis=-1, keepdims=True)))
        dq.append(bf(dot(ds, k, 1, 0)))
        dk.append(bf(dot(ds, q, 0, 0)))
        dv.append(bf(dot(bf(p), doh, 0, 0)))
    dqkv = jnp.concatenate(dq + dk + dv, axis=1)
    dxin = dmid + norm_back(n1, r1, scatter(dot(dqkv, wq, 1, 1)) * (1.0 + m[1]))

    def reduce(a, b):
        g = bf(dot(a, b, 0, 0) * q_s)
        return lax.psum_scatter(g, "fsdp", scatter_dimension=0, tiled=True).astype(jnp.float32)

    gb = reduce(dm, g)
    gi = reduce(a2, du)
    go = reduce(da, o)
    gq = reduce(a1, dqkv)
    return (
        final[None],
        dxin[None],
        gq.reshape(1, rows, 3, own),
        go.T[None],
        gi[None],
        gb.T[None],
    )


def solution(mesh):
    return jax.shard_map(
        body,
        mesh=mesh,
        in_specs=(
            P("fsdp", "sp", None),
            P("fsdp", None, None, None),
            P(None, "fsdp", None, "sp"),
            P(None, "sp", "fsdp"),
            P(None, "fsdp", "sp"),
            P(None, "sp", "fsdp"),
            P("fsdp", "sp", None),
        ),
        out_specs=(
            P("fsdp", "sp", None),
            P("fsdp", "sp", None),
            P(None, "fsdp", None, "sp"),
            P(None, "sp", "fsdp"),
            P(None, "fsdp", "sp"),
            P(None, "sp", "fsdp"),
        ),
        check_vma=False,
    )
```

```python
import functools
import math

import jax
import jax.numpy as jnp
from jax import lax
from jax.experimental import pallas as pl
from jax.experimental.pallas import tpu as pltpu
from jax.sharding import Mesh
from jax.sharding import PartitionSpec as P

HEAD_DIM = 128
LN_EPS = 1e-06
TEMPER = 2.5
BF = jnp.bfloat16
F32 = jnp.float32
AXES = ("z", "y", "h", "l", "c")


def bf(x):
    return x.astype(BF)


def f32(x):
    return x.astype(F32)


def dot(a, b, ca=1, cb=0):
    return lax.dot_general(a, b, (((ca,), (cb,)), ((), ())), preferred_element_type=F32)


def normalize(x):
    d = x - jnp.mean(x, axis=-1, keepdims=True)
    r = lax.rsqrt(jnp.mean(d * d, axis=-1, keepdims=True) + LN_EPS)
    return d * r, r


def norm_back(n, r, e):
    return r * (e - jnp.mean(e, axis=-1, keepdims=True) - n * jnp.mean(e * n, axis=-1, keepdims=True))


def gelu_pair(u):
    k0 = math.sqrt(2.0 / math.pi)
    s = u * u
    t = jnp.tanh(k0 * u * (1.0 + 0.044715 * s))
    g = 0.5 * u * (1.0 + t)
    d = 0.5 * (1.0 + t) + 0.5 * k0 * u * (1.0 - t * t) * (1.0 + 3.0 * 0.044715 * s)
    return g, d


def kernel(
    dims, tok, mod, wblk, og, fin, dxin, grads,
    W, G, R1A, R1B, R2A, R2B, A1, A2, DM, DA, GG, DU, QKV, DQKV, O, DO, PR, PS, RX, SX, MID, DX,
    own_sem, a1s, a1r, a2s, a2r, r1s, r1r, r2s, r2r, gs, gr, ss, sr,
):
    nz, ny, nh = dims
    z, y, h, l, c = (lax.axis_index(a) for a in AXES)
    ol, oc = 1 - l, 1 - c
    rows, width = wblk.shape[1:]
    half = width // 2
    seq = QKV.shape[0]
    pair = seq // 2
    own = QKV.shape[1] // 3
    heads = own // HEAD_DIM
    slab = ny * nh * rows
    scale = TEMPER / math.sqrt(HEAD_DIM)
    q_s = 1.0 / math.sqrt(seq * nz * ny * nh)
    cols = (pl.ds(0, half), pl.ds(half, half))

    def copy(src, dst, ssem, rsem, dev):
        return pltpu.make_async_remote_copy(
            src_ref=src, dst_ref=dst, send_sem=ssem, recv_sem=rsem,
            device_id=dev, device_id_type=pl.DeviceIdType.MESH,
        )

    def zz(k):
        return lax.rem(z + k + nz, nz)

    def yy(k):
        return lax.rem(y + k + ny, ny)

    def hh(k):
        return lax.rem(h + k + nh, nh)

    def at_rows(i):
        return pl.ds(pl.multiple_of(i * rows, 16), rows)

    group = (ny * nh, nz * nh)
    ring = (nz, ny)

    def far(color, j):
        d, dh = j // nh, j % nh
        return {"y": yy(d), "h": hh(dh)} if color == 0 else {"z": zz(d), "h": hh(dh)}

    def near(color, k):
        return {"z": zz(k)} if color == 0 else {"y": yy(k)}

    core_peer = {"c": oc}
    line_peer = {"l": ol}

    def own_block(s):
        return pltpu.make_async_copy(wblk.at[s], W.at[s, z, y, at_rows(h)], own_sem.at[s])

    def block_at(buf, s, color, j, sign):
        d, dh = j // nh, j % nh
        if color == 0:
            return buf.at[s, z, yy(sign * d), at_rows(hh(sign * dh)), cols[0]]
        return buf.at[s, zz(sign * d), y, at_rows(hh(sign * dh)), cols[1]]

    def slab_at(buf, s, color, k):
        if color == 0:
            return buf.at[s, zz(k), :, :, cols[0]]
        return buf.at[s, :, yy(k), :, cols[1]]

    def ag1(s, color, j, recv):
        piece = block_at(W, s, color, j if recv else 0, -1)
        return copy(piece, piece, a1s.at[s, color, j - 1], a1r.at[s, color, j - 1], far(color, j))

    def ag2(s, color, k, recv):
        piece = slab_at(W, s, color, -k if recv else 0)
        return copy(piece, piece, a2s.at[s, color, k - 1], a2r.at[s, color, k - 1], near(color, k))

    def ag1_start(s):
        for color in (0, 1):
            for j in range(1, group[color]):
                ag1(s, color, j, False).start()

    def ag2_start(s):
        for color in (0, 1):
            for j in range(1, group[color]):
                ag1(s, color, j, True).wait_recv()
            for k in range(1, ring[color]):
                ag2(s, color, k, False).start()

    def ag_wait(s):
        for color in (0, 1):
            for k in range(1, ring[color]):
                ag2(s, color, k, True).wait_recv()

    def ag_sent():
        for s in range(3):
            for color in (0, 1):
                for j in range(1, group[color]):
                    ag1(s, color, j, False).wait_send()
                for k in range(1, ring[color]):
                    ag2(s, color, k, False).wait_send()

    R1 = (R1A, R1B)
    R2 = (R2A, R2B)

    def rs1(s, g, color, k):
        return copy(
            slab_at(G, g, color, k), R1[color].at[g, k - 1],
            r1s.at[s, color, k - 1], r1r.at[s, color, k - 1], near(color, k),
        )

    def rs2(s, g, color, j):
        return copy(
            block_at(G, g, color, j, 1), R2[color].at[s, j - 1],
            r2s.at[s, color, j - 1], r2r.at[s, color, j - 1], far(color, j),
        )

    def rs1_start(s, g):
        for color in (0, 1):
            for k in range(1, ring[color]):
                rs1(s, g, color, k).start()

    def rs2_start(s, g):
        for color in (0, 1):
            for k in range(1, ring[color]):
                rs1(s, g, color, k).wait_recv()

            @pl.loop(0, group[color] // nh)
            def _(i):
                at = (g, z, i, slice(None), cols[0]) if color == 0 else (g, i, y, slice(None), cols[1])
                total = f32(G[at])
                for k in range(1, ring[color]):
                    total = total + f32(R1[color][g, k - 1, i])
                G[at] = bf(total)

        for color in (0, 1):
            for j in range(1, group[color]):
                rs2(s, g, color, j).start()

    def rs_finish(s, g):
        for color in (0, 1):
            for j in range(1, group[color]):
                rs2(s, g, color, j).wait_recv()
            total = f32(G[g, z, y, at_rows(h), cols[color]])
            for j in range(1, group[color]):
                total = total + f32(R2[color][s, j - 1])
            grads[s, :, cols[color]] = total

    def rs_sent(s, g):
        for color in (0, 1):
            for k in range(1, ring[color]):
                rs1(s, g, color, k).wait_send()
            for j in range(1, group[color]):
                rs2(s, g, color, j).wait_send()

    def g_copy(i, buf, step, recv):
        if step == 0:
            piece, dev = buf.at[l, oc if recv else c], core_peer
        elif step == 1:
            piece, dev = buf.at[ol if recv else l, c], line_peer
        else:
            piece, dev = buf.at[ol, oc if recv else c], core_peer
        return copy(piece, piece, gs.at[i, step], gr.at[i, step], dev)

    def gather_start(i, buf):
        g_copy(i, buf, 1, False).start()
        g_copy(i, buf, 0, False).start()

    def gather_relay(i, buf):
        g_copy(i, buf, 1, True).wait_recv()
        g_copy(i, buf, 2, False).start()

    def gather_wait(i, buf, step):
        g_copy(i, buf, step, True).wait_recv()

    def gather_sent(i, buf):
        for step in range(3):
            g_copy(i, buf, step, False).wait_send()

    def s_copy(i, step):
        src, dev = (
            (PS.at[ol, oc], core_peer),
            (SX, line_peer),
            (PS.at[l, oc], core_peer),
        )[step]
        return copy(src, RX.at[i % 2, step], ss.at[i, step], sr.at[i, step], dev)

    def scatter_far(i, compute):
        compute(ol)
        s_copy(i, 0).start()
        s_copy(i, 0).wait_recv()
        SX[...] = bf(f32(PS[ol, c]) + f32(RX[i % 2, 0]))
        s_copy(i, 1).start()

    def scatter_near(i, compute):
        compute(l)
        s_copy(i, 2).start()

    def scatter_result(i):
        s_copy(i, 2).wait_recv()
        s_copy(i, 1).wait_recv()
        total = f32(PS[l, c]) + f32(RX[i % 2, 2]) + f32(RX[i % 2, 1])
        for step in range(3):
            s_copy(i, step).wait_send()
        return total

    def pair_rows(i):
        return pl.ds(pl.multiple_of(i * pair, 128), pair)

    def back_product(left, s, lo, n):
        def compute(i):
            @pl.loop(0, nz)
            def _(b):
                w = W[s, b, :, :, pl.ds(lo, n)].reshape(slab, n)
                at = pl.ds(pl.multiple_of(b * slab, 128), slab)
                PS[i, :, :, at] = bf(dot(left(i), w, 1, 1)).reshape(2, pair // 2, slab)
        return compute

    def two(buf, i):
        return buf[i].reshape(pair, buf.shape[-1])

    def all_rows(buf, at):
        return buf[:, :, :, at].reshape(seq, -1)

    def grad_product(g, left, right, n, lo, tile):
        @pl.loop(0, nz)
        def _(b):
            a = all_rows(left, pl.ds(pl.multiple_of(b * slab, 128), slab)).T

            @pl.loop(0, n // tile)
            def _(t):
                at = pl.multiple_of(t * tile, 128)
                value = dot(a, right(pl.ds(at, tile))) * q_s
                G[g, b, :, :, pl.ds(lo + at, tile)] = bf(value).reshape(ny, nh * rows, tile)

    peers = [far(0, j) for j in range(1, group[0])]
    peers += [far(1, j) for j in range(1, group[1]) if j >= nh]
    peers += [{"c": oc}, {"l": ol}, {"l": ol, "c": oc}]
    barrier = pltpu.get_barrier_semaphore()
    for dev in peers:
        pl.semaphore_signal(barrier, inc=1, device_id=dev, device_id_type=pl.DeviceIdType.MESH)
    for s in range(3):
        own_block(s).start()
    m = [mod[i : i + 1, :] for i in range(6)]
    n1, r1 = normalize(f32(tok[...]))
    A1[l, c] = bf(n1 * (1.0 + m[1]) + m[0])
    DM[l, c] = bf(m[5] * f32(og[...]))
    for s in range(3):
        own_block(s).wait()
    pl.semaphore_wait(barrier, len(peers))

    ag1_start(0)
    gather_start(0, A1)
    ag1_start(1)
    ag1_start(2)
    ag2_start(0)
    gather_start(1, DM)
    gather_relay(0, A1)
    ag2_start(1)
    ag2_start(2)
    gather_relay(1, DM)
    gather_wait(0, A1, 0)
    gather_wait(0, A1, 2)

    ag_wait(0)

    @pl.loop(0, 3)
    def _(t):
        at = pl.ds(pl.multiple_of(t * own, 128), own)
        w = W[0, :, :, :, at].reshape(width, own)
        QKV[:, at] = bf(dot(A1[...].reshape(seq, width), w))

    def head(hd, i):
        return pl.ds(pl.multiple_of(i * own + hd * HEAD_DIM, 128), HEAD_DIM)

    @pl.loop(0, heads)
    def _(hd):
        s = dot(QKV[:, head(hd, 0)], QKV[:, head(hd, 1)], 1, 1) * scale
        e = jnp.exp(s - jnp.max(s, axis=-1, keepdims=True))
        p = bf(e * (1.0 / jnp.sum(e, axis=-1, keepdims=True)))
        PR[hd] = p
        O[:, head(hd, 0)] = bf(dot(p, QKV[:, head(hd, 2)]))

    out_product = back_product(lambda i: O[pair_rows(i), :], 0, 3 * own, own)
    scatter_far(0, out_product)
    scatter_near(0, out_product)
    mid = f32(tok[...]) + m[2] * scatter_result(0)
    MID[...] = mid
    n2, r2 = normalize(mid)
    A2[l, c] = bf(n2 * (1.0 + m[4]) + m[3])
    gather_start(2, A2)
    gather_wait(1, DM, 0)
    gather_wait(1, DM, 2)

    tile = 256

    def hidden(i):
        @pl.loop(0, width // tile)
        def _(t):
            at = pl.ds(pl.multiple_of(t * tile, 128), tile)
            g, d = gelu_pair(dot(two(A2, i), W[1, :, :, :, at].reshape(width, tile)))
            GG[i, :, :, at] = bf(g).reshape(2, pair // 2, tile)
            DU[i, :, :, at] = bf(d).reshape(2, pair // 2, tile)

    ag_wait(1)
    gather_wait(2, A2, 0)
    hidden(l)
    gather_relay(2, A2)
    gather_wait(2, A2, 2)
    hidden(ol)
    ag_wait(2)

    @pl.loop(0, width // tile)
    def _(t):
        at = pl.ds(pl.multiple_of(t * tile, 128), tile)
        dg = dot(DM[...].reshape(seq, width), W[2, :, :, :, at].reshape(width, tile))
        DU[:, :, :, at] = bf(f32(DU[:, :, :, at]) * dg.reshape(2, 2, pair // 2, tile))

    in_back = back_product(lambda i: two(DU, i), 1, 0, width)
    scatter_far(1, in_back)
    grad_product(0, DM, lambda at: all_rows(GG, at), width, 0, 2 * tile)
    rs1_start(2, 0)
    scatter_near(1, in_back)
    grad_product(1, A2, lambda at: all_rows(DU, at), width, 0, 2 * tile)
    rs1_start(1, 1)
    e2 = scatter_result(1) * (1.0 + m[4])
    n2, r2 = normalize(MID[...])
    dmid = f32(og[...]) + norm_back(n2, r2, e2)
    DX[...] = dmid
    DA[l, c] = bf(m[2] * dmid)
    gather_start(3, DA)

    ff_back = back_product(lambda i: two(GG, i), 2, 0, width)
    scatter_far(2, ff_back)
    scatter_near(2, ff_back)
    gather_relay(3, DA)
    gather_wait(3, DA, 0)
    gather_wait(3, DA, 2)

    DO[...] = bf(dot(DA[...].reshape(seq, width), W[0, :, :, :, pl.ds(3 * own, own)].reshape(width, own)))

    @pl.loop(0, heads)
    def _(hd):
        do = DO[:, head(hd, 0)]
        p = PR[hd]
        t = f32(p) * dot(do, QKV[:, head(hd, 2)], 1, 1)
        ds = bf(scale * (t - f32(p) * jnp.sum(t, axis=-1, keepdims=True)))
        DQKV[:, head(hd, 0)] = bf(dot(ds, QKV[:, head(hd, 1)]))
        DQKV[:, head(hd, 1)] = bf(dot(ds.T, QKV[:, head(hd, 0)]))
        DQKV[:, head(hd, 2)] = bf(dot(p.T, do))

    fin[...] = bf(MID[...] + m[5] * scatter_result(2))
    rs2_start(2, 0)
    qkv_back = back_product(lambda i: DQKV[pair_rows(i), :], 0, 0, 3 * own)
    scatter_far(3, qkv_back)
    rs_finish(2, 0)
    rs_sent(2, 0)
    grad_product(0, A1, lambda at: DQKV[:, at], 3 * own, 0, own)
    grad_product(0, DA, lambda at: O[:, at], own, 3 * own, own)
    rs1_start(0, 0)
    scatter_near(3, qkv_back)
    rs2_start(1, 1)
    e1 = scatter_result(3) * (1.0 + m[1])
    n1, r1 = normalize(f32(tok[...]))
    dxin[...] = DX[...] + norm_back(n1, r1, e1)
    rs2_start(0, 0)
    rs_finish(1, 1)
    rs_finish(0, 0)
    rs_sent(1, 1)
    rs_sent(0, 0)
    ag_sent()
    for i, buf in enumerate((A1, DM, A2, DA)):
        gather_sent(i, buf)


def step(dims, tokens, modulation, w_qkv, w_out, w_in, w_back, out_grad):
    nz, ny, nh = dims
    count, width = tokens.shape[1:]
    rows, own, ff = w_qkv.shape[1], w_qkv.shape[3], w_in.shape[2]
    assert ff == width and 4 * own == width
    seq = 4 * count
    heads = own // HEAD_DIM
    blocks = jnp.stack(
        [
            jnp.concatenate([w_qkv[0].reshape(rows, 3 * own), w_out[0].T], axis=1),
            w_in[0],
            w_back[0].T,
        ]
    )
    big = (nz, ny, nh * rows)
    half = width // 2
    vmem = pltpu.VMEM
    dma = pltpu.SemaphoreType.DMA
    tokens_buf = vmem((2, 2, count, width), BF)
    n1 = max(ny, nz) * nh - 1
    n2 = max(ny, nz) - 1
    scratch = [
        vmem((3, *big, width), BF),
        vmem((2, *big, width), BF),
        vmem((2, nz - 1, ny, nh * rows, half), BF),
        vmem((2, ny - 1, nz, nh * rows, half), BF),
        vmem((3, ny * nh - 1, rows, half), BF),
        vmem((3, nz * nh - 1, rows, half), BF),
        *[tokens_buf] * 6,
        vmem((seq, 3 * own), BF),
        vmem((seq, 3 * own), BF),
        vmem((seq, own), BF),
        vmem((seq, own), BF),
        vmem((heads, seq, seq), BF),
        tokens_buf,
        vmem((2, 3, count, width), BF),
        vmem((count, width), BF),
        vmem((count, width), F32),
        vmem((count, width), F32),
        dma((3,)),
        dma((3, 2, n1)), dma((3, 2, n1)),
        dma((3, 2, n2)), dma((3, 2, n2)),
        dma((3, 2, n2)), dma((3, 2, n2)),
        dma((3, 2, n1)), dma((3, 2, n1)),
        dma((4, 3)), dma((4, 3)),
        dma((4, 3)), dma((4, 3)),
    ]
    spec = pl.BlockSpec(memory_space=pltpu.VMEM)
    final, dx, grads = pl.pallas_call(
        functools.partial(kernel, dims),
        out_shape=(
            jax.ShapeDtypeStruct((count, width), BF),
            jax.ShapeDtypeStruct((count, width), F32),
            jax.ShapeDtypeStruct((3, rows, width), F32),
        ),
        in_specs=[spec, spec, pl.BlockSpec(memory_space=pl.ANY), spec],
        out_specs=(spec, spec, spec),
        scratch_shapes=scratch,
        compiler_params=pltpu.CompilerParams(
            collective_id=0, has_side_effects=True, vmem_limit_bytes=67043328
        ),
    )(tokens[0], modulation[0, 0], blocks, out_grad[0])
    return (
        final[None],
        dx[None],
        grads[0, :, : 3 * own].reshape(1, rows, 3, own),
        grads[0, :, 3 * own :].T[None],
        grads[1][None],
        grads[2].T[None],
    )


def solution(mesh):
    n = mesh.shape["fsdp"]
    nh = 2 if n > 4 else 1
    ny = int(round(math.sqrt(n // nh)))
    dims = (n // nh // ny, ny, nh)
    torus = Mesh(mesh.devices.reshape(*dims, 2, 2), AXES)
    fsdp, sp = AXES[:3], AXES[3:]
    placed = (
        P(fsdp, sp, None),
        P(fsdp, None, None, None),
        P(None, fsdp, None, sp),
        P(None, sp, fsdp),
        P(None, fsdp, sp),
        P(None, sp, fsdp),
        P(fsdp, sp, None),
    )
    return jax.shard_map(
        functools.partial(step, dims),
        mesh=torus,
        in_specs=placed,
        out_specs=(placed[0], *placed[:1], *placed[2:6]),
        check_vma=False,
    )
```

```python
import functools
import math

import jax
import jax.numpy as jnp
from jax import lax
from jax.experimental import pallas as pl
from jax.experimental.pallas import tpu as pltpu
from jax.sharding import Mesh
from jax.sharding import PartitionSpec as P

HEAD_DIM = 128
LN_EPS = 1e-06
TEMPER = 2.5
BF = jnp.bfloat16
F32 = jnp.float32
AXES = ("z", "y", "h", "l", "c")


def bf(x):
    return x.astype(BF)


def f32(x):
    return x.astype(F32)


def dot(a, b, ca=1, cb=0):
    return lax.dot_general(a, b, (((ca,), (cb,)), ((), ())), preferred_element_type=F32)


def normalize(x):
    d = x - jnp.mean(x, axis=-1, keepdims=True)
    r = lax.rsqrt(jnp.mean(d * d, axis=-1, keepdims=True) + LN_EPS)
    return d * r, r


def norm_back(n, r, e):
    return r * (e - jnp.mean(e, axis=-1, keepdims=True) - n * jnp.mean(e * n, axis=-1, keepdims=True))


def gelu_pair(u):
    k0 = math.sqrt(2.0 / math.pi)
    s = u * u
    t = jnp.tanh(k0 * u * (1.0 + 0.044715 * s))
    g = 0.5 * u * (1.0 + t)
    d = 0.5 * (1.0 + t) + 0.5 * k0 * u * (1.0 - t * t) * (1.0 + 3.0 * 0.044715 * s)
    return g, d


def kernel(
    dims, tok, mod, wblk, og, fin, dxin, grads,
    W, G, R1A, R1B, R2A, R2B, R3, A1, A2, DM, DA, GG, DU, QKV, DQKV, O, DO, PR, PS, RX, SX, MID, DX,
    own_sem, a1s, a1r, a2s, a2r, a3s, a3r, a4s, a4r, r1s, r1r, r2s, r2r, r3s, r3r, gs, gr, ss, sr,
):
    nz, ny, nh = dims
    z, y, h, l, c = (lax.axis_index(a) for a in AXES)
    ol, oc = 1 - l, 1 - c
    rows, width = wblk.shape[1:]
    half, quarter = width // 2, width // 4
    seq = QKV.shape[0]
    pair = seq // 2
    own = QKV.shape[1] // 3
    heads = own // HEAD_DIM
    slab = ny * nh * rows
    scale = TEMPER / math.sqrt(HEAD_DIM)
    q_s = 1.0 / math.sqrt(seq * nz * ny * nh)
    cols = (pl.ds(0, half), pl.ds(half, half))

    def copy(src, dst, ssem, rsem, dev):
        return pltpu.make_async_remote_copy(
            src_ref=src, dst_ref=dst, send_sem=ssem, recv_sem=rsem,
            device_id=dev, device_id_type=pl.DeviceIdType.MESH,
        )

    def zz(k):
        return lax.rem(z + k + nz, nz)

    def yy(k):
        return lax.rem(y + k + ny, ny)

    def hh(k):
        return lax.rem(h + k + nh, nh)

    def at_rows(i):
        return pl.ds(pl.multiple_of(i * rows, 16), rows)

    core_peer = {"c": oc}
    line_peer = {"l": ol}
    pair_peer = {"h": 1 - h}
    ring_cols = ((pl.ds(0, quarter), pl.ds(quarter, quarter)), (pl.ds(half, quarter), pl.ds(half + quarter, quarter)))
    local_cols = (pl.ds(0, quarter), pl.ds(quarter, quarter))

    def last(color, k):
        return {"z": zz(k)} if color == 0 else {"y": yy(k)}

    def mid_dev(color, k):
        return last(1 - color, k)

    def slab_at(buf, color, k, at):
        return buf.at[zz(k), :, :, at] if color == 0 else buf.at[:, yy(k), :, at]

    def line_at(buf, color, k):
        return buf.at[z, yy(k), :, cols[0]] if color == 0 else buf.at[zz(k), y, :, cols[1]]

    def own_block(s):
        return pltpu.make_async_copy(wblk.at[s], W.at[s, z, y, at_rows(h)], own_sem.at[s])

    def ag_pair(s, recv):
        piece = W.at[s, z, y, at_rows(1 - h if recv else h)]
        return copy(piece, piece, a1s.at[s], a1r.at[s], pair_peer)

    def ag_mid(s, color, k, recv):
        piece = line_at(W.at[s], color, -k if recv else 0)
        return copy(piece, piece, a2s.at[s, color, k - 1], a2r.at[s, color, k - 1], mid_dev(color, k))

    def ag_last(s, color, d, recv):
        k = 1 - 2 * d
        piece = slab_at(W.at[s], color, -k if recv else 0, cols[color])
        return copy(piece, piece, a3s.at[s, color, d], a3r.at[s, color, d], last(color, k))

    def ag_relay(s, color, d, recv):
        k = 1 - 2 * d
        piece = slab_at(W.at[s], color, 2 if recv else -k, ring_cols[color][d])
        return copy(piece, piece, a4s.at[s, color, d], a4r.at[s, color, d], last(color, k))

    def ag_mid_start(s):
        ag_pair(s, True).wait_recv()
        for color in (0, 1):
            for k in range(1, 4):
                ag_mid(s, color, k, False).start()

    def ag_last_start(s):
        for color in (0, 1):
            for k in range(1, 4):
                ag_mid(s, color, k, True).wait_recv()
            for d in (0, 1):
                ag_last(s, color, d, False).start()

    def ag_relay_start(s):
        for color in (0, 1):
            for d in (0, 1):
                ag_last(s, color, d, True).wait_recv()
                ag_relay(s, color, d, False).start()

    def ag_wait(s):
        for color in (0, 1):
            for d in (0, 1):
                ag_relay(s, color, d, True).wait_recv()

    def ag_sent(s):
        ag_pair(s, False).wait_send()
        for color in (0, 1):
            for k in range(1, 4):
                ag_mid(s, color, k, False).wait_send()
            for d in (0, 1):
                ag_last(s, color, d, False).wait_send()
                ag_relay(s, color, d, False).wait_send()

    R1 = (R1A, R1B)
    R2 = (R2A, R2B)
    parts = (W.at[1], G.at[1], G.at[0])

    def rs_ring(s, color, d, kind):
        k = 1 - 2 * d
        q = 1 - d if kind == 1 else d
        src = slab_at(parts[s], color, 2 if kind == 0 else k, ring_cols[color][q])
        dst = R1[color].at[s, 2 if kind == 0 else d, :, :, local_cols[q]]
        return copy(src, dst, r1s.at[s, color, d, kind], r1r.at[s, color, d, kind], last(color, k))

    def rs_mid(s, color, k):
        return copy(
            line_at(parts[s], color, k), R2[color].at[s, k - 1],
            r2s.at[s, color, k - 1], r2r.at[s, color, k - 1], mid_dev(color, k),
        )

    def rs_pair(s):
        return copy(parts[s].at[z, y, at_rows(1 - h)], R3.at[s], r3s.at[s], r3r.at[s], pair_peer)

    def rs_start(s):
        for kind in (0, 1):
            for color in (0, 1):
                for d in (0, 1):
                    rs_ring(s, color, d, kind).start()

    def rs_combine(s):
        for color in (0, 1):
            for d in (0, 1):
                rs_ring(s, color, d, 0).wait_recv()
                k = 1 - 2 * d

                @pl.loop(0, 4)
                def _(i):
                    at = (zz(k), i) if color == 0 else (i, yy(k))
                    at = (*at, slice(None), ring_cols[color][d])
                    parts[s][at] = bf(f32(parts[s][at]) + f32(R1[color][s, 2, i, :, local_cols[d]]))

                rs_ring(s, color, d, 2).start()

    def rs_mid_start(s):
        for color in (0, 1):
            for d in (0, 1):
                for kind in (1, 2):
                    rs_ring(s, color, d, kind).wait_recv()

            @pl.loop(0, 4)
            def _(i):
                at = (z, i) if color == 0 else (i, y)
                at = (*at, slice(None), cols[color])
                parts[s][at] = bf(f32(parts[s][at]) + f32(R1[color][s, 0, i]) + f32(R1[color][s, 1, i]))

            for k in range(1, 4):
                rs_mid(s, color, k).start()

    def rs_pair_start(s):
        for color in (0, 1):
            for k in range(1, 4):
                rs_mid(s, color, k).wait_recv()
            at = (z, y, slice(None), cols[color])
            total = f32(parts[s][at])
            for k in range(3):
                total = total + f32(R2[color][s, k])
            parts[s][at] = bf(total)
        rs_pair(s).start()

    def rs_finish(s):
        rs_pair(s).wait_recv()
        grads[s] = f32(parts[s][z, y, at_rows(h), :]) + f32(R3[s])

    def rs_sent(s):
        for color in (0, 1):
            for d in (0, 1):
                for kind in (0, 1, 2):
                    rs_ring(s, color, d, kind).wait_send()
            for k in range(1, 4):
                rs_mid(s, color, k).wait_send()
        rs_pair(s).wait_send()

    def g_copy(i, buf, step, recv):
        if step == 0:
            piece, dev = buf.at[l, oc if recv else c], core_peer
        elif step == 1:
            piece, dev = buf.at[ol if recv else l, c], line_peer
        else:
            piece, dev = buf.at[ol, oc if recv else c], core_peer
        return copy(piece, piece, gs.at[i, step], gr.at[i, step], dev)

    def gather_start(i, buf):
        g_copy(i, buf, 1, False).start()
        g_copy(i, buf, 0, False).start()

    def gather_relay(i, buf):
        g_copy(i, buf, 1, True).wait_recv()
        g_copy(i, buf, 2, False).start()

    def gather_wait(i, buf, step):
        g_copy(i, buf, step, True).wait_recv()

    def gather_sent(i, buf):
        for step in range(3):
            g_copy(i, buf, step, False).wait_send()

    def s_copy(i, step):
        src, dev = (
            (PS.at[ol, oc], core_peer),
            (SX, line_peer),
            (PS.at[l, oc], core_peer),
        )[step]
        return copy(src, RX.at[i % 2, step], ss.at[i, step], sr.at[i, step], dev)

    def scatter_far(i, compute):
        compute(ol)
        s_copy(i, 0).start()
        s_copy(i, 0).wait_recv()
        SX[...] = bf(f32(PS[ol, c]) + f32(RX[i % 2, 0]))
        s_copy(i, 1).start()

    def scatter_near(i, compute):
        compute(l)
        s_copy(i, 2).start()

    def scatter_result(i):
        s_copy(i, 2).wait_recv()
        s_copy(i, 1).wait_recv()
        total = f32(PS[l, c]) + f32(RX[i % 2, 2]) + f32(RX[i % 2, 1])
        for step in range(3):
            s_copy(i, step).wait_send()
        return total

    def pair_rows(i):
        return pl.ds(pl.multiple_of(i * pair, 128), pair)

    def back_product(left, s, lo, n):
        def compute(i):
            @pl.loop(0, nz)
            def _(b):
                w = W[s, b, :, :, pl.ds(lo, n)].reshape(slab, n)
                at = pl.ds(pl.multiple_of(b * slab, 128), slab)
                PS[i, :, :, at] = bf(dot(left(i), w, 1, 1)).reshape(2, pair // 2, slab)
        return compute

    def two(buf, i):
        return buf[i].reshape(pair, buf.shape[-1])

    def all_rows(buf, at):
        return buf[:, :, :, at].reshape(seq, -1)

    def grad_product(s, left, right, n, lo, tile):
        @pl.loop(0, nz)
        def _(b):
            a = all_rows(left, pl.ds(pl.multiple_of(b * slab, 128), slab)).T

            @pl.loop(0, n // tile)
            def _(t):
                at = pl.multiple_of(t * tile, 128)
                value = dot(a, right(pl.ds(at, tile))) * q_s
                parts[s][b, :, :, pl.ds(lo + at, tile)] = bf(value).reshape(ny, nh * rows, tile)

    peers = [{"z": zz(k)} for k in range(1, 4)] + [{"y": yy(k)} for k in range(1, 4)]
    peers += [pair_peer, core_peer, line_peer, {"l": ol, "c": oc}]
    barrier = pltpu.get_barrier_semaphore()
    for dev in peers:
        pl.semaphore_signal(barrier, inc=1, device_id=dev, device_id_type=pl.DeviceIdType.MESH)
    for s in range(3):
        own_block(s).start()
    m = [mod[i : i + 1, :] for i in range(6)]
    n1, r1 = normalize(f32(tok[...]))
    A1[l, c] = bf(n1 * (1.0 + m[1]) + m[0])
    DM[l, c] = bf(m[5] * f32(og[...]))
    for s in range(3):
        own_block(s).wait()
    pl.semaphore_wait(barrier, len(peers))

    ag_pair(0, False).start()
    gather_start(0, A1)
    ag_pair(1, False).start()
    ag_pair(2, False).start()
    ag_mid_start(0)
    ag_last_start(0)
    ag_mid_start(1)
    gather_relay(0, A1)
    gather_start(1, DM)
    ag_relay_start(0)
    ag_mid_start(2)
    ag_last_start(1)
    gather_relay(1, DM)
    gather_wait(0, A1, 0)
    gather_wait(0, A1, 2)

    ag_wait(0)

    @pl.loop(0, 3)
    def _(t):
        at = pl.ds(pl.multiple_of(t * own, 128), own)
        w = W[0, :, :, :, at].reshape(width, own)
        QKV[:, at] = bf(dot(A1[...].reshape(seq, width), w))

    def head(hd, i):
        return pl.ds(pl.multiple_of(i * own + hd * HEAD_DIM, 128), HEAD_DIM)

    @pl.loop(0, heads)
    def _(hd):
        s = dot(QKV[:, head(hd, 0)], QKV[:, head(hd, 1)], 1, 1) * scale
        e = jnp.exp(s - jnp.max(s, axis=-1, keepdims=True))
        p = bf(e * (1.0 / jnp.sum(e, axis=-1, keepdims=True)))
        PR[hd] = p
        O[:, head(hd, 0)] = bf(dot(p, QKV[:, head(hd, 2)]))

    out_product = back_product(lambda i: O[pair_rows(i), :], 0, 3 * own, own)
    scatter_far(0, out_product)
    scatter_near(0, out_product)
    ag_last_start(2)
    ag_relay_start(1)
    mid = f32(tok[...]) + m[2] * scatter_result(0)
    MID[...] = mid
    n2, r2 = normalize(mid)
    A2[l, c] = bf(n2 * (1.0 + m[4]) + m[3])
    gather_start(2, A2)
    gather_wait(1, DM, 0)
    gather_wait(1, DM, 2)

    tile = 256

    def hidden(i):
        @pl.loop(0, width // tile)
        def _(t):
            at = pl.ds(pl.multiple_of(t * tile, 128), tile)
            g, d = gelu_pair(dot(two(A2, i), W[1, :, :, :, at].reshape(width, tile)))
            GG[i, :, :, at] = bf(g).reshape(2, pair // 2, tile)
            DU[i, :, :, at] = bf(d).reshape(2, pair // 2, tile)

    ag_wait(1)
    gather_wait(2, A2, 0)
    hidden(l)
    gather_relay(2, A2)
    gather_wait(2, A2, 2)
    hidden(ol)
    ag_relay_start(2)
    ag_wait(2)

    @pl.loop(0, width // tile)
    def _(t):
        at = pl.ds(pl.multiple_of(t * tile, 128), tile)
        dg = dot(DM[...].reshape(seq, width), W[2, :, :, :, at].reshape(width, tile))
        DU[:, :, :, at] = bf(f32(DU[:, :, :, at]) * dg.reshape(2, 2, pair // 2, tile))

    in_back = back_product(lambda i: two(DU, i), 1, 0, width)
    scatter_far(1, in_back)
    grad_product(2, DM, lambda at: all_rows(GG, at), width, 0, 2 * tile)
    rs_start(2)
    scatter_near(1, in_back)
    grad_product(1, A2, lambda at: all_rows(DU, at), width, 0, 2 * tile)
    rs_start(1)
    rs_combine(2)
    e2 = scatter_result(1) * (1.0 + m[4])
    n2, r2 = normalize(MID[...])
    dmid = f32(og[...]) + norm_back(n2, r2, e2)
    DX[...] = dmid
    DA[l, c] = bf(m[2] * dmid)
    gather_start(3, DA)

    ff_back = back_product(lambda i: two(GG, i), 2, 0, width)
    scatter_far(2, ff_back)
    scatter_near(2, ff_back)
    rs_combine(1)
    gather_relay(3, DA)
    gather_wait(3, DA, 0)
    gather_wait(3, DA, 2)

    DO[...] = bf(dot(DA[...].reshape(seq, width), W[0, :, :, :, pl.ds(3 * own, own)].reshape(width, own)))

    @pl.loop(0, heads)
    def _(hd):
        do = DO[:, head(hd, 0)]
        p = PR[hd]
        t = f32(p) * dot(do, QKV[:, head(hd, 2)], 1, 1)
        ds = bf(scale * (t - f32(p) * jnp.sum(t, axis=-1, keepdims=True)))
        DQKV[:, head(hd, 0)] = bf(dot(ds, QKV[:, head(hd, 1)]))
        DQKV[:, head(hd, 1)] = bf(dot(ds.T, QKV[:, head(hd, 0)]))
        DQKV[:, head(hd, 2)] = bf(dot(p.T, do))

    ag_sent(1)
    grad_product(0, A1, lambda at: DQKV[:, at], 3 * own, 0, own)
    grad_product(0, DA, lambda at: O[:, at], own, 3 * own, own)
    rs_start(0)
    fin[...] = bf(MID[...] + m[5] * scatter_result(2))
    qkv_back = back_product(lambda i: DQKV[pair_rows(i), :], 0, 0, 3 * own)
    scatter_far(3, qkv_back)
    scatter_near(3, qkv_back)
    rs_mid_start(2)
    rs_combine(0)
    e1 = scatter_result(3) * (1.0 + m[1])
    n1, r1 = normalize(f32(tok[...]))
    dxin[...] = DX[...] + norm_back(n1, r1, e1)
    rs_mid_start(1)
    rs_pair_start(2)
    rs_mid_start(0)
    rs_pair_start(1)
    rs_finish(2)
    rs_pair_start(0)
    rs_finish(1)
    rs_finish(0)
    for s in range(3):
        rs_sent(s)
    ag_sent(0)
    ag_sent(2)
    for i, buf in enumerate((A1, DM, A2, DA)):
        gather_sent(i, buf)


def step(dims, tokens, modulation, w_qkv, w_out, w_in, w_back, out_grad):
    nz, ny, nh = dims
    count, width = tokens.shape[1:]
    rows, own, ff = w_qkv.shape[1], w_qkv.shape[3], w_in.shape[2]
    assert ff == width and 4 * own == width
    seq = 4 * count
    heads = own // HEAD_DIM
    blocks = jnp.stack(
        [
            jnp.concatenate([w_qkv[0].reshape(rows, 3 * own), w_out[0].T], axis=1),
            w_in[0],
            w_back[0].T,
        ]
    )
    big = (nz, ny, nh * rows)
    half = width // 2
    vmem = pltpu.VMEM
    dma = pltpu.SemaphoreType.DMA
    tokens_buf = vmem((2, 2, count, width), BF)
    scratch = [
        vmem((3, *big, width), BF),
        vmem((2, *big, width), BF),
        vmem((3, 3, 4, nh * rows, half), BF),
        vmem((3, 3, 4, nh * rows, half), BF),
        vmem((3, 3, nh * rows, half), BF),
        vmem((3, 3, nh * rows, half), BF),
        vmem((3, rows, width), BF),
        *[tokens_buf] * 6,
        vmem((seq, 3 * own), BF),
        vmem((seq, 3 * own), BF),
        vmem((seq, own), BF),
        vmem((seq, own), BF),
        vmem((heads, seq, seq), BF),
        tokens_buf,
        vmem((2, 3, count, width), BF),
        vmem((count, width), BF),
        vmem((count, width), F32),
        vmem((count, width), F32),
        dma((3,)),
        dma((3,)), dma((3,)),
        dma((3, 2, 3)), dma((3, 2, 3)),
        dma((3, 2, 2)), dma((3, 2, 2)),
        dma((3, 2, 2)), dma((3, 2, 2)),
        dma((3, 2, 2, 3)), dma((3, 2, 2, 3)),
        dma((3, 2, 3)), dma((3, 2, 3)),
        dma((3,)), dma((3,)),
        dma((4, 3)), dma((4, 3)),
        dma((4, 3)), dma((4, 3)),
    ]
    spec = pl.BlockSpec(memory_space=pltpu.VMEM)
    final, dx, grads = pl.pallas_call(
        functools.partial(kernel, dims),
        out_shape=(
            jax.ShapeDtypeStruct((count, width), BF),
            jax.ShapeDtypeStruct((count, width), F32),
            jax.ShapeDtypeStruct((3, rows, width), F32),
        ),
        in_specs=[spec, spec, pl.BlockSpec(memory_space=pl.ANY), spec],
        out_specs=(spec, spec, spec),
        scratch_shapes=scratch,
        compiler_params=pltpu.CompilerParams(
            collective_id=0, has_side_effects=True, vmem_limit_bytes=67043328
        ),
    )(tokens[0], modulation[0, 0], blocks, out_grad[0])
    return (
        final[None],
        dx[None],
        grads[0, :, : 3 * own].reshape(1, rows, 3, own),
        grads[0, :, 3 * own :].T[None],
        grads[1][None],
        grads[2].T[None],
    )


def solution(mesh):
    dims = (4, 4, 2)
    assert mesh.shape["fsdp"] == 32 and mesh.shape["sp"] == 4
    torus = Mesh(mesh.devices.reshape(*dims, 2, 2), AXES)
    fsdp, sp = AXES[:3], AXES[3:]
    placed = (
        P(fsdp, sp, None),
        P(fsdp, None, None, None),
        P(None, fsdp, None, sp),
        P(None, sp, fsdp),
        P(None, fsdp, sp),
        P(None, sp, fsdp),
        P(fsdp, sp, None),
    )
    return jax.shard_map(
        functools.partial(step, dims),
        mesh=torus,
        in_specs=placed,
        out_specs=(placed[0], *placed[:1], *placed[2:6]),
        check_vma=False,
    )
```

```python
import functools
import math

import jax
import jax.numpy as jnp
from jax import lax
from jax.experimental import pallas as pl
from jax.experimental.pallas import tpu as pltpu
from jax.sharding import Mesh
from jax.sharding import PartitionSpec as P

HEAD_DIM = 128
LN_EPS = 1e-06
TEMPER = 2.5
BF = jnp.bfloat16
F32 = jnp.float32
AXES = ("z", "y", "h", "l", "c")


def bf(x):
    return x.astype(BF)


def f32(x):
    return x.astype(F32)


def dot(a, b, ca=1, cb=0):
    return lax.dot_general(a, b, (((ca,), (cb,)), ((), ())), preferred_element_type=F32)


def normalize(x):
    d = x - jnp.mean(x, axis=-1, keepdims=True)
    r = lax.rsqrt(jnp.mean(d * d, axis=-1, keepdims=True) + LN_EPS)
    return d * r, r


def norm_back(n, r, e):
    return r * (e - jnp.mean(e, axis=-1, keepdims=True) - n * jnp.mean(e * n, axis=-1, keepdims=True))


def gelu_pair(u):
    k0 = math.sqrt(2.0 / math.pi)
    s = u * u
    t = jnp.tanh(k0 * u * (1.0 + 0.044715 * s))
    g = 0.5 * u * (1.0 + t)
    d = 0.5 * (1.0 + t) + 0.5 * k0 * u * (1.0 - t * t) * (1.0 + 3.0 * 0.044715 * s)
    return g, d


def kernel(
    dims, tok_in, mod_in, wq_in, wo_in, wi_in, wb_in, og_in, fin, dxin, grads,
    W, G, R1A, R1B, R2A, R2B, R3, A1, A2, DM, DA, GG, DU, QKV, DQKV, O, DO, PR, PS, RX, SX, MID, DX,
    tok, mod, og, in_sem, a1s, a1r, a2s, a2r, a3s, a3r, a4s, a4r, r1s, r1r, r2s, r2r, r3s, r3r, gs, gr, ss, sr,
):
    nz, ny, nh = dims
    z, y, h, l, c = (lax.axis_index(a) for a in AXES)
    ol, oc = 1 - l, 1 - c
    rows, width = wi_in.shape
    half = width // 2
    seq = QKV.shape[0]
    pair = seq // 2
    own = QKV.shape[1] // 3
    heads = own // HEAD_DIM
    slab = ny * nh * rows
    scale = TEMPER / math.sqrt(HEAD_DIM)
    q_s = 1.0 / math.sqrt(seq * nz * ny * nh)
    cols = (pl.ds(0, half), pl.ds(half, half))

    def copy(src, dst, ssem, rsem, dev):
        return pltpu.make_async_remote_copy(
            src_ref=src, dst_ref=dst, send_sem=ssem, recv_sem=rsem,
            device_id=dev, device_id_type=pl.DeviceIdType.MESH,
        )

    def zz(k):
        return lax.rem(z + k + nz, nz)

    def yy(k):
        return lax.rem(y + k + ny, ny)

    def hh(k):
        return lax.rem(h + k + nh, nh)

    def at_rows(i):
        return pl.ds(pl.multiple_of(i * rows, 16), rows)

    core_peer = {"c": oc}
    line_peer = {"l": ol}
    pair_peer = {"h": 1 - h}
    halves = (pl.ds(0, 2), pl.ds(2, 2))

    def last(color, k):
        return {"z": zz(k)} if color == 0 else {"y": yy(k)}

    def mid_dev(color, k):
        return last(1 - color, k)

    def slab_at(buf, color, k, at, part=slice(None)):
        return buf.at[zz(k), part, :, at] if color == 0 else buf.at[part, yy(k), :, at]

    def line_at(buf, color, k, at, part=slice(None)):
        return buf.at[z, yy(k), part, at] if color == 0 else buf.at[zz(k), y, part, at]

    def ag_pair(s, recv):
        piece = W.at[s, z, y, at_rows(1 - h if recv else h)]
        return copy(piece, piece, a1s.at[s], a1r.at[s], pair_peer)

    def ag_mid(s, color, k, which, recv):
        piece = line_at(W.at[s], color, -k if recv else 0, cols[color], at_rows(h if which == 0 else 1 - h))
        return copy(piece, piece, a2s.at[s, color, k - 1, which], a2r.at[s, color, k - 1, which], mid_dev(color, k))

    def ag_last(s, color, d, recv):
        k = 1 - 2 * d
        piece = slab_at(W.at[s], color, -k if recv else 0, cols[color])
        return copy(piece, piece, a3s.at[s, color, d], a3r.at[s, color, d], last(color, k))

    def ag_relay(s, color, d, recv):
        k = 1 - 2 * d
        piece = slab_at(W.at[s], color, 2 if recv else -k, cols[color], halves[d])
        return copy(piece, piece, a4s.at[s, color, d], a4r.at[s, color, d], last(color, k))

    def ag_mid_start(s, which):
        if which:
            ag_pair(s, True).wait_recv()
        for k in (1, 3, 2):
            for color in (0, 1):
                ag_mid(s, color, k, which, False).start()

    def ag_last_start(s):
        for color in (0, 1):
            for which in (0, 1):
                for k in range(1, 4):
                    ag_mid(s, color, k, which, True).wait_recv()
            for d in (0, 1):
                ag_last(s, color, d, False).start()

    def ag_relay_start(s):
        for color in (0, 1):
            for d in (0, 1):
                ag_last(s, color, d, True).wait_recv()
                ag_relay(s, color, d, False).start()

    def ag_wait(s):
        for color in (0, 1):
            for d in (0, 1):
                ag_relay(s, color, d, True).wait_recv()

    def ag_sent(s):
        ag_pair(s, False).wait_send()
        for color in (0, 1):
            for which in (0, 1):
                for k in range(1, 4):
                    ag_mid(s, color, k, which, False).wait_send()
            for d in (0, 1):
                ag_last(s, color, d, False).wait_send()
                ag_relay(s, color, d, False).wait_send()

    R1 = (R1A, R1B)
    R2 = (R2A, R2B)
    parts = (G.at[0], G.at[1], W.at[1], W.at[1])
    slots = (2, 1, 0, 0)
    full = 3 * own
    local_cols = (
        (pl.ds(0, half), pl.ds(0, half)),
        (pl.ds(0, half), pl.ds(0, half)),
        (pl.ds(half - 256, 256), pl.ds(half - 128, 128)),
        (pl.ds(0, half - 256), pl.ds(0, half - 128)),
    )
    grad_cols = (
        (cols[0], cols[1]),
        (cols[0], cols[1]),
        (pl.ds(full, 256), pl.ds(full + 256, 128)),
        (pl.ds(0, half - 256), pl.ds(half - 256, half - 128)),
    )
    pair_cols = (pl.ds(0, width), pl.ds(0, width), pl.ds(full, own), pl.ds(0, full))

    def rs_ring(s, color, d, kind):
        k = 1 - 2 * d
        part = halves[1 - d if kind == 1 else d]
        src = slab_at(parts[s], color, 2 if kind == 0 else k, grad_cols[s][color], part)
        dst = R1[color].at[slots[s], 2 if kind == 0 else d, part, :, local_cols[s][color]]
        return copy(src, dst, r1s.at[s, color, d, kind], r1r.at[s, color, d, kind], last(color, k))

    def rs_mid(s, color, k):
        return copy(
            line_at(parts[s], color, k, grad_cols[s][color]),
            R2[color].at[slots[s], k - 1, :, local_cols[s][color]],
            r2s.at[s, color, k - 1], r2r.at[s, color, k - 1], mid_dev(color, k),
        )

    def rs_pair(s):
        return copy(
            parts[s].at[z, y, at_rows(1 - h), pair_cols[s]], R3.at[slots[s], :, pair_cols[s]],
            r3s.at[s], r3r.at[s], pair_peer,
        )

    def rs_start(s):
        for kind in (0, 1):
            for color in (0, 1):
                for d in (0, 1):
                    rs_ring(s, color, d, kind).start()

    def rs_combine(s):
        for color in (0, 1):
            for d in (0, 1):
                rs_ring(s, color, d, 0).wait_recv()
                k = 1 - 2 * d

                @pl.loop(2 * d, 2 * d + 2)
                def _(i):
                    at = (zz(k), i) if color == 0 else (i, yy(k))
                    at = (*at, slice(None), grad_cols[s][color])
                    came = R1[color][slots[s], 2, i, :, local_cols[s][color]]
                    parts[s][at] = bf(f32(parts[s][at]) + f32(came))

                rs_ring(s, color, d, 2).start()

    def rs_mid_start(s):
        for color in (0, 1):
            for d in (0, 1):
                for kind in (1, 2):
                    rs_ring(s, color, d, kind).wait_recv()

            @pl.loop(0, 4)
            def _(i):
                at = (z, i) if color == 0 else (i, y)
                at = (*at, slice(None), grad_cols[s][color])
                total = f32(parts[s][at])
                for d in (0, 1):
                    total = total + f32(R1[color][slots[s], d, i, :, local_cols[s][color]])
                parts[s][at] = bf(total)

            for k in (1, 3, 2):
                rs_mid(s, color, k).start()

    def rs_pair_start(s):
        for color in (0, 1):
            for k in range(1, 4):
                rs_mid(s, color, k).wait_recv()
            at = (z, y, slice(None), grad_cols[s][color])
            total = f32(parts[s][at])
            for k in range(3):
                total = total + f32(R2[color][slots[s], k, :, local_cols[s][color]])
            parts[s][at] = bf(total)
        rs_pair(s).start()

    def rs_finish(s):
        rs_pair(s).wait_recv()
        at = pair_cols[s]
        grads[slots[s], :, at] = f32(parts[s][z, y, at_rows(h), at]) + f32(R3[slots[s], :, at])

    def rs_sent(s):
        for color in (0, 1):
            for d in (0, 1):
                for kind in (0, 1, 2):
                    rs_ring(s, color, d, kind).wait_send()
            for k in range(1, 4):
                rs_mid(s, color, k).wait_send()
        rs_pair(s).wait_send()

    def g_copy(i, buf, step, recv):
        if step == 0:
            piece, dev = buf.at[l, oc if recv else c], core_peer
        elif step == 1:
            piece, dev = buf.at[ol if recv else l, c], line_peer
        else:
            piece, dev = buf.at[ol, oc if recv else c], core_peer
        return copy(piece, piece, gs.at[i, step], gr.at[i, step], dev)

    def gather_start(i, buf):
        g_copy(i, buf, 1, False).start()
        g_copy(i, buf, 0, False).start()

    def gather_relay(i, buf):
        g_copy(i, buf, 1, True).wait_recv()
        g_copy(i, buf, 2, False).start()

    def gather_wait(i, buf, step):
        g_copy(i, buf, step, True).wait_recv()

    def gather_sent(i, buf):
        for step in range(3):
            g_copy(i, buf, step, False).wait_send()

    def s_copy(i, step):
        src, dev = (
            (PS.at[ol, oc], core_peer),
            (SX, line_peer),
            (PS.at[l, oc], core_peer),
        )[step]
        return copy(src, RX.at[i % 2, step], ss.at[i, step], sr.at[i, step], dev)

    def scatter_far(i, compute):
        compute(ol)
        s_copy(i, 0).start()
        s_copy(i, 0).wait_recv()
        SX[...] = bf(f32(PS[ol, c]) + f32(RX[i % 2, 0]))
        s_copy(i, 1).start()

    def scatter_near(i, compute):
        compute(l)
        s_copy(i, 2).start()

    def scatter_result(i):
        s_copy(i, 2).wait_recv()
        s_copy(i, 1).wait_recv()
        total = f32(PS[l, c]) + f32(RX[i % 2, 2]) + f32(RX[i % 2, 1])
        for step in range(3):
            s_copy(i, step).wait_send()
        return total

    def pair_rows(i):
        return pl.ds(pl.multiple_of(i * pair, 128), pair)

    def back_product(left, s, lo, n):
        def compute(i):
            @pl.loop(0, nz)
            def _(b):
                w = W[s, b, :, :, pl.ds(lo, n)].reshape(slab, n)
                at = pl.ds(pl.multiple_of(b * slab, 128), slab)
                PS[i, :, :, at] = bf(dot(left(i), w, 1, 1)).reshape(2, pair // 2, slab)
        return compute

    def two(buf, i):
        return buf[i].reshape(pair, buf.shape[-1])

    def all_rows(buf, at):
        return buf[:, :, :, at].reshape(seq, -1)

    def grad_product(s, left, right, n, lo, tile):
        @pl.loop(0, nz)
        def _(b):
            a = all_rows(left, pl.ds(pl.multiple_of(b * slab, 128), slab)).T

            @pl.loop(0, n // tile)
            def _(t):
                at = pl.multiple_of(t * tile, 128)
                value = dot(a, right(pl.ds(at, tile))) * q_s
                parts[s][b, :, :, pl.ds(lo + at, tile)] = bf(value).reshape(ny, nh * rows, tile)

    peers = [{"z": zz(k)} for k in range(1, 4)] + [{"y": yy(k)} for k in range(1, 4)]
    peers += [pair_peer, core_peer, line_peer, {"l": ol, "c": oc}]
    barrier = pltpu.get_barrier_semaphore()
    for dev in peers:
        pl.semaphore_signal(barrier, inc=1, device_id=dev, device_id_type=pl.DeviceIdType.MESH)
    mine = at_rows(h)
    moves = [(wq_in.at[i], W.at[0, z, y, mine, pl.ds(i * own, own)]) for i in range(3)]
    moves += [(wo_in, W.at[0, z, y, mine, pl.ds(3 * own, own)])]
    moves += [(wi_in, W.at[1, z, y, mine]), (wb_in, W.at[2, z, y, mine])]
    moves += [(tok_in, tok), (og_in, og), (mod_in, mod)]
    loads = [pltpu.make_async_copy(src, dst, in_sem.at[i]) for i, (src, dst) in enumerate(moves)]
    for load in loads:
        load.start()
    for load in loads:
        load.wait()
    m = [mod[i] for i in range(6)]
    n1, r1 = normalize(f32(tok[...]))
    A1[l, c] = bf(n1 * (1.0 + m[1]) + m[0])
    DM[l, c] = bf(m[5] * f32(og[...]))
    pl.semaphore_wait(barrier, len(peers))

    for s in range(3):
        ag_pair(s, False).start()
        ag_mid_start(s, 0)
    gather_start(0, A1)
    ag_mid_start(0, 1)
    ag_mid_start(1, 1)
    ag_last_start(0)
    ag_mid_start(2, 1)
    gather_relay(0, A1)
    gather_start(1, DM)
    ag_relay_start(0)
    ag_last_start(1)
    gather_wait(0, A1, 0)
    gather_wait(0, A1, 2)
    gather_relay(1, DM)

    ag_wait(0)

    @pl.loop(0, 3)
    def _(t):
        at = pl.ds(pl.multiple_of(t * own, 128), own)
        w = W[0, :, :, :, at].reshape(width, own)
        QKV[:, at] = bf(dot(A1[...].reshape(seq, width), w))

    def head(hd, i):
        return pl.ds(pl.multiple_of(i * own + hd * HEAD_DIM, 128), HEAD_DIM)

    @pl.loop(0, heads)
    def _(hd):
        s = dot(QKV[:, head(hd, 0)], QKV[:, head(hd, 1)], 1, 1) * scale
        e = jnp.exp(s - jnp.max(s, axis=-1, keepdims=True))
        p = bf(e * (1.0 / jnp.sum(e, axis=-1, keepdims=True)))
        PR[hd] = p
        O[:, head(hd, 0)] = bf(dot(p, QKV[:, head(hd, 2)]))

    out_product = back_product(lambda i: O[pair_rows(i), :], 0, 3 * own, own)
    ag_last_start(2)
    scatter_far(0, out_product)
    scatter_near(0, out_product)
    ag_relay_start(1)
    mid = f32(tok[...]) + m[2] * scatter_result(0)
    MID[...] = mid
    n2, r2 = normalize(mid)
    A2[l, c] = bf(n2 * (1.0 + m[4]) + m[3])
    gather_start(2, A2)
    gather_wait(1, DM, 0)
    gather_wait(1, DM, 2)

    tile = 256

    def hidden(i):
        @pl.loop(0, width // tile)
        def _(t):
            at = pl.ds(pl.multiple_of(t * tile, 128), tile)
            g, d = gelu_pair(dot(two(A2, i), W[1, :, :, :, at].reshape(width, tile)))
            GG[i, :, :, at] = bf(g).reshape(2, pair // 2, tile)
            DU[i, :, :, at] = bf(d).reshape(2, pair // 2, tile)

    ag_relay_start(2)
    gather_relay(2, A2)
    gather_wait(2, A2, 0)
    ag_wait(1)
    hidden(l)
    gather_wait(2, A2, 2)
    hidden(ol)
    grad_product(0, DM, lambda at: all_rows(GG, at), width, 0, 2 * tile)
    rs_start(0)
    ag_wait(2)

    @pl.loop(0, width // tile)
    def _(t):
        at = pl.ds(pl.multiple_of(t * tile, 128), tile)
        dg = dot(DM[...].reshape(seq, width), W[2, :, :, :, at].reshape(width, tile))
        DU[:, :, :, at] = bf(f32(DU[:, :, :, at]) * dg.reshape(2, 2, pair // 2, tile))

    in_back = back_product(lambda i: two(DU, i), 1, 0, width)
    scatter_far(1, in_back)
    grad_product(1, A2, lambda at: all_rows(DU, at), width, 0, 2 * tile)
    rs_start(1)
    scatter_near(1, in_back)
    rs_combine(0)
    e2 = scatter_result(1) * (1.0 + m[4])
    n2, r2 = normalize(MID[...])
    dmid = f32(og[...]) + norm_back(n2, r2, e2)
    DX[...] = dmid
    DA[l, c] = bf(m[2] * dmid)
    gather_start(3, DA)

    ff_back = back_product(lambda i: two(GG, i), 2, 0, width)
    scatter_far(2, ff_back)
    scatter_near(2, ff_back)
    rs_combine(1)
    gather_relay(3, DA)
    gather_wait(3, DA, 0)
    gather_wait(3, DA, 2)

    DO[...] = bf(dot(DA[...].reshape(seq, width), W[0, :, :, :, pl.ds(3 * own, own)].reshape(width, own)))
    ag_sent(1)
    grad_product(2, DA, lambda at: O[:, at], own, 3 * own, own)
    rs_start(2)

    @pl.loop(0, heads)
    def _(hd):
        do = DO[:, head(hd, 0)]
        p = PR[hd]
        t = f32(p) * dot(do, QKV[:, head(hd, 2)], 1, 1)
        ds = bf(scale * (t - f32(p) * jnp.sum(t, axis=-1, keepdims=True)))
        DQKV[:, head(hd, 0)] = bf(dot(ds, QKV[:, head(hd, 1)]))
        DQKV[:, head(hd, 1)] = bf(dot(ds.T, QKV[:, head(hd, 0)]))
        DQKV[:, head(hd, 2)] = bf(dot(p.T, do))

    grad_product(3, A1, lambda at: DQKV[:, at], 3 * own, 0, own)
    rs_start(3)
    fin[...] = bf(MID[...] + m[5] * scatter_result(2))
    qkv_back = back_product(lambda i: DQKV[pair_rows(i), :], 0, 0, 3 * own)
    scatter_far(3, qkv_back)
    scatter_near(3, qkv_back)
    rs_mid_start(0)
    rs_combine(2)
    rs_combine(3)
    e1 = scatter_result(3) * (1.0 + m[1])
    n1, r1 = normalize(f32(tok[...]))
    dxin[...] = DX[...] + norm_back(n1, r1, e1)
    rs_mid_start(1)
    rs_pair_start(0)
    rs_mid_start(2)
    rs_mid_start(3)
    rs_pair_start(1)
    rs_finish(0)
    rs_pair_start(2)
    rs_pair_start(3)
    rs_finish(1)
    rs_finish(2)
    rs_finish(3)
    for s in range(4):
        rs_sent(s)
    ag_sent(0)
    ag_sent(2)
    for i, buf in enumerate((A1, DM, A2, DA)):
        gather_sent(i, buf)


def place(fin, dx, grads, o_fin, o_dx, o_qkv, o_out, o_in, o_back):
    own = o_out.shape[1]
    o_fin[0] = fin[...]
    o_dx[0] = dx[...]
    for i in range(3):
        o_qkv[i] = grads[0, :, i * own : (i + 1) * own]
    o_out[...] = grads[0, :, 3 * own :]
    o_in[0] = grads[1]
    o_back[...] = grads[2]


def step(dims, tokens, modulation, w_qkv, w_out, w_in, w_back, out_grad):
    nz, ny, nh = dims
    count, width = tokens.shape[1:]
    rows, own, ff = w_qkv.shape[1], w_qkv.shape[3], w_in.shape[2]
    assert ff == width and 4 * own == width
    seq = 4 * count
    heads = own // HEAD_DIM
    big = (nz, ny, nh * rows)
    half = width // 2
    vmem = pltpu.VMEM
    dma = pltpu.SemaphoreType.DMA
    tokens_buf = vmem((2, 2, count, width), BF)
    scratch = [
        vmem((3, *big, width), BF),
        vmem((2, *big, width), BF),
        vmem((3, 3, 4, nh * rows, half), BF),
        vmem((3, 3, 4, nh * rows, half), BF),
        vmem((3, 3, nh * rows, half), BF),
        vmem((3, 3, nh * rows, half), BF),
        vmem((3, rows, width), BF),
        *[tokens_buf] * 6,
        vmem((seq, 3 * own), BF),
        vmem((seq, 3 * own), BF),
        vmem((seq, own), BF),
        vmem((seq, own), BF),
        vmem((heads, seq, seq), BF),
        tokens_buf,
        vmem((2, 3, count, width), BF),
        vmem((count, width), BF),
        vmem((count, width), F32),
        vmem((count, width), F32),
        vmem((count, width), BF),
        vmem((6, 1, width), F32),
        vmem((count, width), BF),
        dma((9,)),
        dma((3,)), dma((3,)),
        dma((3, 2, 3, 2)), dma((3, 2, 3, 2)),
        dma((3, 2, 2)), dma((3, 2, 2)),
        dma((3, 2, 2)), dma((3, 2, 2)),
        dma((4, 2, 2, 3)), dma((4, 2, 2, 3)),
        dma((4, 2, 3)), dma((4, 2, 3)),
        dma((4,)), dma((4,)),
        dma((4, 3)), dma((4, 3)),
        dma((4, 3)), dma((4, 3)),
    ]
    spec = pl.BlockSpec(memory_space=pltpu.VMEM)
    final, dx, grads = pl.pallas_call(
        functools.partial(kernel, dims),
        out_shape=(
            jax.ShapeDtypeStruct((count, width), BF),
            jax.ShapeDtypeStruct((count, width), F32),
            jax.ShapeDtypeStruct((3, rows, width), F32),
        ),
        in_specs=[pl.BlockSpec(memory_space=pl.ANY)] * 7,
        out_specs=(spec, spec, spec),
        scratch_shapes=scratch,
        compiler_params=pltpu.CompilerParams(
            collective_id=0, has_side_effects=True, vmem_limit_bytes=67043328
        ),
    )(
        tokens[0], modulation[0].transpose(1, 0, 2), w_qkv[0].transpose(1, 0, 2), w_out[0].T,
        w_in[0], w_back[0].T, out_grad[0],
    )
    final, dx, qkv, out, inner, back = pl.pallas_call(
        place,
        out_shape=(
            jax.ShapeDtypeStruct((1, count, width), BF),
            jax.ShapeDtypeStruct((1, count, width), F32),
            jax.ShapeDtypeStruct((3, rows, own), F32),
            jax.ShapeDtypeStruct((rows, own), F32),
            jax.ShapeDtypeStruct((1, rows, width), F32),
            jax.ShapeDtypeStruct((rows, width), F32),
        ),
        in_specs=[spec] * 3,
        out_specs=(spec,) * 6,
    )(final, dx, grads)
    return final, dx, qkv.transpose(1, 0, 2)[None], out.T[None], inner, back.T[None]


def solution(mesh):
    dims = (4, 4, 2)
    assert mesh.shape["fsdp"] == 32 and mesh.shape["sp"] == 4
    torus = Mesh(mesh.devices.reshape(*dims, 2, 2), AXES)
    fsdp, sp = AXES[:3], AXES[3:]
    placed = (
        P(fsdp, sp, None),
        P(fsdp, None, None, None),
        P(None, fsdp, None, sp),
        P(None, sp, fsdp),
        P(None, fsdp, sp),
        P(None, sp, fsdp),
        P(fsdp, sp, None),
    )
    return jax.shard_map(
        functools.partial(step, dims),
        mesh=torus,
        in_specs=placed,
        out_specs=(placed[0], *placed[:1], *placed[2:6]),
        check_vma=False,
    )
```

```python
import functools
import math

import jax
import jax.numpy as jnp
from jax import lax
from jax.experimental import pallas as pl
from jax.experimental.pallas import tpu as pltpu
from jax.sharding import Mesh
from jax.sharding import PartitionSpec as P

HEAD_DIM = 128
LN_EPS = 1e-06
TEMPER = 2.5
BF = jnp.bfloat16
F32 = jnp.float32
AXES = ("z", "y", "h", "l", "c")


def bf(x):
    return x.astype(BF)


def f32(x):
    return x.astype(F32)


def dot(a, b, ca=1, cb=0):
    return lax.dot_general(a, b, (((ca,), (cb,)), ((), ())), preferred_element_type=F32)


def normalize(x):
    d = x - jnp.mean(x, axis=-1, keepdims=True)
    r = lax.rsqrt(jnp.mean(d * d, axis=-1, keepdims=True) + LN_EPS)
    return d * r, r


def norm_back(n, r, e):
    return r * (e - jnp.mean(e, axis=-1, keepdims=True) - n * jnp.mean(e * n, axis=-1, keepdims=True))


def gelu_pair(u):
    k0 = math.sqrt(2.0 / math.pi)
    s = u * u
    t = jnp.tanh(k0 * u * (1.0 + 0.044715 * s))
    g = 0.5 * u * (1.0 + t)
    d = 0.5 * (1.0 + t) + 0.5 * k0 * u * (1.0 - t * t) * (1.0 + 3.0 * 0.044715 * s)
    return g, d


def kernel(
    dims, tok_in, mod_in, wq_in, wo_in, wi_in, wb_in, og_in, fin, dxin, grads,
    W, G, R1A, R1B, R2A, R2B, R3, A1, A2, DM, DA, GG, DU, QKV, DQKV, O, DO, PR, PS, RX, SX, MID, DX, AT,
    tok, mod, og, in_sem, a1s, a1r, a2s, a2r, a3s, a3r, a4s, a4r, r1s, r1r, r2s, r2r, r3s, r3r, gs, gr, ss, sr,
):
    nz, ny, nh = dims
    z, y, h, l, c = (lax.axis_index(a) for a in AXES)
    ol, oc = 1 - l, 1 - c
    rows, width = wi_in.shape
    half = width // 2
    seq = QKV.shape[0]
    pair = seq // 2
    own = QKV.shape[1] // 3
    heads = own // HEAD_DIM
    slab = ny * nh * rows
    scale = TEMPER / math.sqrt(HEAD_DIM)
    q_s = 1.0 / math.sqrt(seq * nz * ny * nh)
    cols = (pl.ds(0, half), pl.ds(half, half))

    def copy(src, dst, ssem, rsem, dev):
        return pltpu.make_async_remote_copy(
            src_ref=src, dst_ref=dst, send_sem=ssem, recv_sem=rsem,
            device_id=dev, device_id_type=pl.DeviceIdType.MESH,
        )

    def zz(k):
        return lax.rem(z + k + nz, nz)

    def yy(k):
        return lax.rem(y + k + ny, ny)

    def hh(k):
        return lax.rem(h + k + nh, nh)

    def at_rows(i):
        return pl.ds(pl.multiple_of(i * rows, 16), rows)

    core_peer = {"c": oc}
    line_peer = {"l": ol}
    pair_peer = {"h": 1 - h}
    halves = (pl.ds(0, 2), pl.ds(2, 2))

    def last(color, k):
        return {"z": zz(k)} if color == 0 else {"y": yy(k)}

    def mid_dev(color, k):
        return last(1 - color, k)

    def slab_at(buf, color, k, at, part=slice(None)):
        return buf.at[zz(k), part, :, at] if color == 0 else buf.at[part, yy(k), :, at]

    def line_at(buf, color, k, at, part=slice(None)):
        return buf.at[z, yy(k), part, at] if color == 0 else buf.at[zz(k), y, part, at]

    def ag_pair(s, recv):
        piece = W.at[s, z, y, at_rows(1 - h if recv else h)]
        return copy(piece, piece, a1s.at[s], a1r.at[s], pair_peer)

    def ag_mid(s, color, k, which, recv):
        piece = line_at(W.at[s], color, -k if recv else 0, cols[color], at_rows(h if which == 0 else 1 - h))
        return copy(piece, piece, a2s.at[s, color, k - 1, which], a2r.at[s, color, k - 1, which], mid_dev(color, k))

    def ag_last(s, color, d, recv):
        k = 1 - 2 * d
        piece = slab_at(W.at[s], color, -k if recv else 0, cols[color])
        return copy(piece, piece, a3s.at[s, color, d], a3r.at[s, color, d], last(color, k))

    def ag_relay(s, color, d, recv):
        k = 1 - 2 * d
        piece = slab_at(W.at[s], color, 2 if recv else -k, cols[color], halves[d])
        return copy(piece, piece, a4s.at[s, color, d], a4r.at[s, color, d], last(color, k))

    def ag_mid_start(s, which):
        if which:
            ag_pair(s, True).wait_recv()
        for k in (1, 3, 2):
            for color in (0, 1):
                ag_mid(s, color, k, which, False).start()

    def ag_last_start(s):
        for color in (0, 1):
            for which in (0, 1):
                for k in range(1, 4):
                    ag_mid(s, color, k, which, True).wait_recv()
            for d in (0, 1):
                ag_last(s, color, d, False).start()

    def ag_relay_start(s):
        for color in (0, 1):
            for d in (0, 1):
                ag_last(s, color, d, True).wait_recv()
                ag_relay(s, color, d, False).start()

    def ag_wait(s):
        for color in (0, 1):
            for d in (0, 1):
                ag_relay(s, color, d, True).wait_recv()

    def ag_sent(s):
        ag_pair(s, False).wait_send()
        for color in (0, 1):
            for which in (0, 1):
                for k in range(1, 4):
                    ag_mid(s, color, k, which, False).wait_send()
            for d in (0, 1):
                ag_last(s, color, d, False).wait_send()
                ag_relay(s, color, d, False).wait_send()

    R1 = (R1A, R1B)
    R2 = (R2A, R2B)
    full = 3 * own
    sections = 3 + heads
    parts = (G.at[0], G.at[1]) + (W.at[1],) * (1 + heads)
    slots = (2, 1) + (0,) * (1 + heads)
    local_cols = [cols[:1] * 2] * 2
    grad_cols = [cols] * 2
    pair_cols = [pl.ds(0, width)] * 2
    at0 = [0, 0]
    for i, base in enumerate([full] + [hd * own for hd in range(heads)]):
        first = 256 if i % 2 == 0 else 128
        second = own - first
        local_cols.append((pl.ds(at0[0], first), pl.ds(at0[1], second)))
        grad_cols.append((pl.ds(base, first), pl.ds(base + first, second)))
        pair_cols.append(pl.ds(base, own))
        at0 = [at0[0] + first, at0[1] + second]

    def rs_ring(s, color, d, kind):
        k = 1 - 2 * d
        part = halves[1 - d if kind == 1 else d]
        src = slab_at(parts[s], color, 2 if kind == 0 else k, grad_cols[s][color], part)
        dst = R1[color].at[slots[s], 2 if kind == 0 else d, part, :, local_cols[s][color]]
        return copy(src, dst, r1s.at[s, color, d, kind], r1r.at[s, color, d, kind], last(color, k))

    def rs_mid(s, color, k):
        return copy(
            line_at(parts[s], color, k, grad_cols[s][color]),
            R2[color].at[slots[s], k - 1, :, local_cols[s][color]],
            r2s.at[s, color, k - 1], r2r.at[s, color, k - 1], mid_dev(color, k),
        )

    def rs_pair(s):
        return copy(
            parts[s].at[z, y, at_rows(1 - h), pair_cols[s]], R3.at[slots[s], :, pair_cols[s]],
            r3s.at[s], r3r.at[s], pair_peer,
        )

    def rs_start(s, colors=(0, 1)):
        for kind in (0, 1):
            for color in colors:
                for d in (0, 1):
                    rs_ring(s, color, d, kind).start()

    def rs_combine(s):
        for color in (0, 1):
            for d in (0, 1):
                rs_ring(s, color, d, 0).wait_recv()
                k = 1 - 2 * d

                @pl.loop(2 * d, 2 * d + 2)
                def _(i):
                    at = (zz(k), i) if color == 0 else (i, yy(k))
                    at = (*at, slice(None), grad_cols[s][color])
                    came = R1[color][slots[s], 2, i, :, local_cols[s][color]]
                    parts[s][at] = bf(f32(parts[s][at]) + f32(came))

                rs_ring(s, color, d, 2).start()

    def rs_mid_start(s):
        for color in (0, 1):
            for d in (0, 1):
                for kind in (1, 2):
                    rs_ring(s, color, d, kind).wait_recv()

            @pl.loop(0, 4)
            def _(i):
                at = (z, i) if color == 0 else (i, y)
                at = (*at, slice(None), grad_cols[s][color])
                total = f32(parts[s][at])
                for d in (0, 1):
                    total = total + f32(R1[color][slots[s], d, i, :, local_cols[s][color]])
                parts[s][at] = bf(total)

            for k in (1, 3, 2):
                rs_mid(s, color, k).start()

    def rs_pair_start(s):
        for color in (0, 1):
            for k in range(1, 4):
                rs_mid(s, color, k).wait_recv()
            at = (z, y, slice(None), grad_cols[s][color])
            total = f32(parts[s][at])
            for k in range(3):
                total = total + f32(R2[color][slots[s], k, :, local_cols[s][color]])
            parts[s][at] = bf(total)
        rs_pair(s).start()

    def rs_finish(s):
        rs_pair(s).wait_recv()
        at = pair_cols[s]
        grads[slots[s], :, at] = f32(parts[s][z, y, at_rows(h), at]) + f32(R3[slots[s], :, at])

    def rs_sent(s):
        for color in (0, 1):
            for d in (0, 1):
                for kind in (0, 1, 2):
                    rs_ring(s, color, d, kind).wait_send()
            for k in range(1, 4):
                rs_mid(s, color, k).wait_send()
        rs_pair(s).wait_send()

    def g_copy(i, buf, step, recv):
        if step == 0:
            piece, dev = buf.at[l, oc if recv else c], core_peer
        elif step == 1:
            piece, dev = buf.at[ol if recv else l, c], line_peer
        else:
            piece, dev = buf.at[ol, oc if recv else c], core_peer
        return copy(piece, piece, gs.at[i, step], gr.at[i, step], dev)

    def gather_start(i, buf):
        g_copy(i, buf, 1, False).start()
        g_copy(i, buf, 0, False).start()

    def gather_relay(i, buf):
        g_copy(i, buf, 1, True).wait_recv()
        g_copy(i, buf, 2, False).start()

    def gather_wait(i, buf, step):
        g_copy(i, buf, step, True).wait_recv()

    def gather_sent(i, buf):
        for step in range(3):
            g_copy(i, buf, step, False).wait_send()

    def s_copy(i, step):
        src, dev = (
            (PS.at[ol, oc], core_peer),
            (SX, line_peer),
            (PS.at[l, oc], core_peer),
        )[step]
        return copy(src, RX.at[i % 2, step], ss.at[i, step], sr.at[i, step], dev)

    def scatter_far(i, compute):
        compute(ol)
        s_copy(i, 0).start()
        s_copy(i, 0).wait_recv()
        SX[...] = bf(f32(PS[ol, c]) + f32(RX[i % 2, 0]))
        s_copy(i, 1).start()

    def scatter_near(i, compute):
        compute(l)
        s_copy(i, 2).start()

    def scatter_result(i):
        s_copy(i, 2).wait_recv()
        s_copy(i, 1).wait_recv()
        total = f32(PS[l, c]) + f32(RX[i % 2, 2]) + f32(RX[i % 2, 1])
        for step in range(3):
            s_copy(i, step).wait_send()
        return total

    def pair_rows(i):
        return pl.ds(pl.multiple_of(i * pair, 128), pair)

    def back_product(left, s, lo, n):
        def compute(i):
            @pl.loop(0, nz)
            def _(b):
                w = W[s, b, :, :, pl.ds(lo, n)].reshape(slab, n)
                at = pl.ds(pl.multiple_of(b * slab, 128), slab)
                PS[i, :, :, at] = bf(dot(left(i), w, 1, 1)).reshape(2, pair // 2, slab)
        return compute

    def two(buf, i):
        return buf[i].reshape(pair, buf.shape[-1])

    def all_rows(buf, at):
        return buf[:, :, :, at].reshape(seq, -1)

    def turn(buf):
        @pl.loop(0, nz)
        def _(b):
            AT[b] = all_rows(buf, pl.ds(pl.multiple_of(b * slab, 128), slab)).T

    def grad_turned(s, right, start, stop, tile):
        @pl.loop(0, (stop - start) // tile)
        def _(t):
            at = pl.ds(pl.multiple_of(start + t * tile, 128), tile)
            value = dot(AT[...].reshape(width, seq), right(at)) * q_s
            parts[s][:, :, :, at] = bf(value).reshape(nz, ny, nh * rows, tile)

    def grad_product(s, left, right, n, lo):
        @pl.loop(0, nz)
        def _(b):
            a = all_rows(left, pl.ds(pl.multiple_of(b * slab, 128), slab)).T
            value = dot(a, right) * q_s
            parts[s][b, :, :, pl.ds(lo, n)] = bf(value).reshape(ny, nh * rows, n)

    peers = [{"z": zz(k)} for k in range(1, 4)] + [{"y": yy(k)} for k in range(1, 4)]
    peers += [pair_peer, core_peer, line_peer, {"l": ol, "c": oc}]
    barrier = pltpu.get_barrier_semaphore()
    for dev in peers:
        pl.semaphore_signal(barrier, inc=1, device_id=dev, device_id_type=pl.DeviceIdType.MESH)
    mine = at_rows(h)
    moves = [
        (wq_in.at[i, :, pl.ds(hd * HEAD_DIM, HEAD_DIM)], W.at[0, z, y, mine, pl.ds((3 * hd + i) * HEAD_DIM, HEAD_DIM)])
        for i in range(3) for hd in range(heads)
    ]
    moves += [(wo_in, W.at[0, z, y, mine, pl.ds(3 * own, own)])]
    moves += [(wi_in, W.at[1, z, y, mine]), (wb_in, W.at[2, z, y, mine])]
    moves += [(tok_in, tok), (og_in, og), (mod_in, mod)]
    loads = [pltpu.make_async_copy(src, dst, in_sem.at[i]) for i, (src, dst) in enumerate(moves)]
    for load in loads:
        load.start()
    for load in loads:
        load.wait()
    m = [mod[i] for i in range(6)]
    n1, r1 = normalize(f32(tok[...]))
    A1[l, c] = bf(n1 * (1.0 + m[1]) + m[0])
    DM[l, c] = bf(m[5] * f32(og[...]))
    pl.semaphore_wait(barrier, len(peers))

    for s in range(3):
        ag_pair(s, False).start()
        ag_mid_start(s, 0)
    gather_start(0, A1)
    ag_mid_start(0, 1)
    ag_mid_start(1, 1)
    ag_last_start(0)
    ag_mid_start(2, 1)
    gather_relay(0, A1)
    gather_start(1, DM)
    ag_relay_start(0)
    ag_last_start(1)
    gather_wait(0, A1, 0)
    gather_wait(0, A1, 2)
    gather_relay(1, DM)
    gather_wait(1, DM, 0)
    gather_wait(1, DM, 2)
    turn(DM)

    ag_wait(0)

    @pl.loop(0, 3)
    def _(t):
        at = pl.ds(pl.multiple_of(t * own, 128), own)
        w = W[0, :, :, :, at].reshape(width, own)
        QKV[:, at] = bf(dot(A1[...].reshape(seq, width), w))

    def head(hd, i):
        return pl.ds(pl.multiple_of((3 * hd + i) * HEAD_DIM, 128), HEAD_DIM)

    def wide(hd):
        return pl.ds(pl.multiple_of(hd * HEAD_DIM, 128), HEAD_DIM)

    @pl.loop(0, heads)
    def _(hd):
        s = dot(QKV[:, head(hd, 0)], QKV[:, head(hd, 1)], 1, 1) * scale
        e = jnp.exp(s - jnp.max(s, axis=-1, keepdims=True))
        p = bf(e * (1.0 / jnp.sum(e, axis=-1, keepdims=True)))
        PR[hd] = p
        O[:, wide(hd)] = bf(dot(p, QKV[:, head(hd, 2)]))

    out_product = back_product(lambda i: O[pair_rows(i), :], 0, 3 * own, own)
    ag_last_start(2)
    scatter_far(0, out_product)
    scatter_near(0, out_product)
    ag_relay_start(1)
    mid = f32(tok[...]) + m[2] * scatter_result(0)
    MID[...] = mid
    n2, r2 = normalize(mid)
    A2[l, c] = bf(n2 * (1.0 + m[4]) + m[3])
    gather_start(2, A2)

    tile = 256

    def hidden(i):
        @pl.loop(0, width // tile)
        def _(t):
            at = pl.ds(pl.multiple_of(t * tile, 128), tile)
            g, d = gelu_pair(dot(two(A2, i), W[1, :, :, :, at].reshape(width, tile)))
            GG[i, :, :, at] = bf(g).reshape(2, pair // 2, tile)
            DU[i, :, :, at] = bf(d).reshape(2, pair // 2, tile)

    ag_relay_start(2)
    gather_relay(2, A2)
    gather_wait(2, A2, 0)
    ag_wait(1)
    hidden(l)
    gather_wait(2, A2, 2)
    hidden(ol)
    for color in (0, 1):
        grad_turned(0, lambda at: all_rows(GG, at), color * half, (color + 1) * half, tile)
        rs_start(0, (color,))
    ag_wait(2)

    @pl.loop(0, width // tile)
    def _(t):
        at = pl.ds(pl.multiple_of(t * tile, 128), tile)
        dg = dot(DM[...].reshape(seq, width), W[2, :, :, :, at].reshape(width, tile))
        DU[:, :, :, at] = bf(f32(DU[:, :, :, at]) * dg.reshape(2, 2, pair // 2, tile))

    in_back = back_product(lambda i: two(DU, i), 1, 0, width)
    scatter_far(1, in_back)
    turn(A2)
    grad_turned(1, lambda at: all_rows(DU, at), 0, half, tile)
    rs_combine(0)
    rs_start(1, (0,))
    grad_turned(1, lambda at: all_rows(DU, at), half, width, tile)
    rs_start(1, (1,))
    scatter_near(1, in_back)
    e2 = scatter_result(1) * (1.0 + m[4])
    n2, r2 = normalize(MID[...])
    dmid = f32(og[...]) + norm_back(n2, r2, e2)
    DX[...] = dmid
    DA[l, c] = bf(m[2] * dmid)
    gather_start(3, DA)

    ff_back = back_product(lambda i: two(GG, i), 2, 0, width)
    scatter_far(2, ff_back)
    scatter_near(2, ff_back)
    turn(A1)
    rs_combine(1)
    rs_mid_start(0)
    gather_relay(3, DA)
    gather_wait(3, DA, 0)
    gather_wait(3, DA, 2)

    DO[...] = bf(dot(DA[...].reshape(seq, width), W[0, :, :, :, pl.ds(3 * own, own)].reshape(width, own)))
    ag_sent(1)
    grad_product(2, DA, O[...], own, full)
    rs_start(2)

    for hd in range(heads):
        do = DO[:, wide(hd)]
        p = PR[hd]
        t = f32(p) * dot(do, QKV[:, head(hd, 2)], 1, 1)
        ds = bf(scale * (t - f32(p) * jnp.sum(t, axis=-1, keepdims=True)))
        DQKV[:, head(hd, 0)] = bf(dot(ds, QKV[:, head(hd, 1)]))
        DQKV[:, head(hd, 1)] = bf(dot(ds.T, QKV[:, head(hd, 0)]))
        DQKV[:, head(hd, 2)] = bf(dot(p.T, do))
        grad_turned(3 + hd, lambda at: DQKV[:, at], hd * own, (hd + 1) * own, own)
        if hd == 1:
            rs_mid_start(1)
        rs_start(3 + hd)

    qkv_back = back_product(lambda i: DQKV[pair_rows(i), :], 0, 0, 3 * own)
    fin[...] = bf(MID[...] + m[5] * scatter_result(2))
    scatter_far(3, qkv_back)
    rs_combine(2)
    rs_combine(3)
    scatter_near(3, qkv_back)
    rs_pair_start(0)
    rs_combine(4)
    rs_mid_start(2)
    rs_combine(5)
    rs_mid_start(3)
    e1 = scatter_result(3) * (1.0 + m[1])
    n1, r1 = normalize(f32(tok[...]))
    dxin[...] = DX[...] + norm_back(n1, r1, e1)
    rs_pair_start(1)
    rs_finish(0)
    rs_mid_start(4)
    rs_pair_start(2)
    rs_mid_start(5)
    rs_pair_start(3)
    rs_finish(1)
    rs_pair_start(4)
    rs_pair_start(5)
    for s in range(2, sections):
        rs_finish(s)
    for s in range(sections):
        rs_sent(s)
    ag_sent(0)
    ag_sent(2)
    for i, buf in enumerate((A1, DM, A2, DA)):
        gather_sent(i, buf)


def place(fin, dx, grads, o_fin, o_dx, o_qkv, o_out, o_in, o_back):
    own = o_out.shape[1]
    o_fin[0] = fin[...]
    o_dx[0] = dx[...]
    for i in range(3):
        for hd in range(own // HEAD_DIM):
            at = (3 * hd + i) * HEAD_DIM
            o_qkv[i, :, hd * HEAD_DIM : (hd + 1) * HEAD_DIM] = grads[0, :, at : at + HEAD_DIM]
    o_out[...] = grads[0, :, 3 * own :]
    o_in[0] = grads[1]
    o_back[...] = grads[2]


def step(dims, tokens, modulation, w_qkv, w_out, w_in, w_back, out_grad):
    nz, ny, nh = dims
    count, width = tokens.shape[1:]
    rows, own, ff = w_qkv.shape[1], w_qkv.shape[3], w_in.shape[2]
    assert ff == width and 4 * own == width
    seq = 4 * count
    heads = own // HEAD_DIM
    big = (nz, ny, nh * rows)
    half = width // 2
    vmem = pltpu.VMEM
    dma = pltpu.SemaphoreType.DMA
    tokens_buf = vmem((2, 2, count, width), BF)
    scratch = [
        vmem((3, *big, width), BF),
        vmem((2, *big, width), BF),
        vmem((3, 3, 4, nh * rows, half), BF),
        vmem((3, 3, 4, nh * rows, half), BF),
        vmem((3, 3, nh * rows, half), BF),
        vmem((3, 3, nh * rows, half), BF),
        vmem((3, rows, width), BF),
        *[tokens_buf] * 6,
        vmem((seq, 3 * own), BF),
        vmem((seq, 3 * own), BF),
        vmem((seq, own), BF),
        vmem((seq, own), BF),
        vmem((heads, seq, seq), BF),
        tokens_buf,
        vmem((2, 3, count, width), BF),
        vmem((count, width), BF),
        vmem((count, width), F32),
        vmem((count, width), F32),
        vmem((nz, ny * nh * rows, seq), BF),
        vmem((count, width), BF),
        vmem((6, 1, width), F32),
        vmem((count, width), BF),
        dma((6 + 3 * heads,)),
        dma((3,)), dma((3,)),
        dma((3, 2, 3, 2)), dma((3, 2, 3, 2)),
        dma((3, 2, 2)), dma((3, 2, 2)),
        dma((3, 2, 2)), dma((3, 2, 2)),
        dma((3 + heads, 2, 2, 3)), dma((3 + heads, 2, 2, 3)),
        dma((3 + heads, 2, 3)), dma((3 + heads, 2, 3)),
        dma((3 + heads,)), dma((3 + heads,)),
        dma((4, 3)), dma((4, 3)),
        dma((4, 3)), dma((4, 3)),
    ]
    spec = pl.BlockSpec(memory_space=pltpu.VMEM)
    final, dx, grads = pl.pallas_call(
        functools.partial(kernel, dims),
        out_shape=(
            jax.ShapeDtypeStruct((count, width), BF),
            jax.ShapeDtypeStruct((count, width), F32),
            jax.ShapeDtypeStruct((3, rows, width), F32),
        ),
        in_specs=[pl.BlockSpec(memory_space=pl.ANY)] * 7,
        out_specs=(spec, spec, spec),
        scratch_shapes=scratch,
        compiler_params=pltpu.CompilerParams(
            collective_id=0, has_side_effects=True, vmem_limit_bytes=67043328
        ),
    )(
        tokens[0], modulation[0].transpose(1, 0, 2), w_qkv[0].transpose(1, 0, 2), w_out[0].T,
        w_in[0], w_back[0].T, out_grad[0],
    )
    final, dx, qkv, out, inner, back = pl.pallas_call(
        place,
        out_shape=(
            jax.ShapeDtypeStruct((1, count, width), BF),
            jax.ShapeDtypeStruct((1, count, width), F32),
            jax.ShapeDtypeStruct((3, rows, own), F32),
            jax.ShapeDtypeStruct((rows, own), F32),
            jax.ShapeDtypeStruct((1, rows, width), F32),
            jax.ShapeDtypeStruct((rows, width), F32),
        ),
        in_specs=[spec] * 3,
        out_specs=(spec,) * 6,
    )(final, dx, grads)
    return final, dx, qkv.transpose(1, 0, 2)[None], out.T[None], inner, back.T[None]


def solution(mesh):
    dims = (4, 4, 2)
    assert mesh.shape["fsdp"] == 32 and mesh.shape["sp"] == 4
    torus = Mesh(mesh.devices.reshape(*dims, 2, 2), AXES)
    fsdp, sp = AXES[:3], AXES[3:]
    placed = (
        P(fsdp, sp, None),
        P(fsdp, None, None, None),
        P(None, fsdp, None, sp),
        P(None, sp, fsdp),
        P(None, fsdp, sp),
        P(None, sp, fsdp),
        P(fsdp, sp, None),
    )
    return jax.shard_map(
        functools.partial(step, dims),
        mesh=torus,
        in_specs=placed,
        out_specs=(placed[0], *placed[:1], *placed[2:6]),
        check_vma=False,
    )
```

```python
import functools
import math

import jax
import jax.numpy as jnp
from jax import lax
from jax.experimental import pallas as pl
from jax.experimental.pallas import tpu as pltpu
from jax.sharding import Mesh
from jax.sharding import PartitionSpec as P

HEAD_DIM = 128
LN_EPS = 1e-06
TEMPER = 2.5
BF = jnp.bfloat16
F32 = jnp.float32
AXES = ("z", "y", "h", "l", "c")


def bf(x):
    return x.astype(BF)


def f32(x):
    return x.astype(F32)


def dot(a, b, ca=1, cb=0):
    return lax.dot_general(a, b, (((ca,), (cb,)), ((), ())), preferred_element_type=F32)


def normalize(x):
    d = x - jnp.mean(x, axis=-1, keepdims=True)
    r = lax.rsqrt(jnp.mean(d * d, axis=-1, keepdims=True) + LN_EPS)
    return d * r, r


def norm_back(n, r, e):
    return r * (e - jnp.mean(e, axis=-1, keepdims=True) - n * jnp.mean(e * n, axis=-1, keepdims=True))


def gelu_pair(u):
    k0 = math.sqrt(2.0 / math.pi)
    s = u * u
    t = jnp.tanh(k0 * u * (1.0 + 0.044715 * s))
    g = 0.5 * u * (1.0 + t)
    d = 0.5 * (1.0 + t) + 0.5 * k0 * u * (1.0 - t * t) * (1.0 + 3.0 * 0.044715 * s)
    return g, d


def kernel(
    dims, tok_in, mod_in, wq_in, wo_in, wi_in, wb_in, og_in, fin, dxin, grads,
    W, G, R1A, R1B, R2A, R2B, R3, R1C, R2C, R4, R4H, A1, A2, DM, DA, GG, DU, QKV, DQKV, O, DO, PR, PS, RX, SX, MID, DX, AT,
    tok, mod, og, in_sem, a1s, a1r, a2s, a2r, a3s, a3r, a4s, a4r, r1s, r1r, r2s, r2r, r3s, r3r, r4s, r4r, gs, gr, ss, sr,
):
    nz, ny, nh = dims
    z, y, h, l, c = (lax.axis_index(a) for a in AXES)
    ol, oc = 1 - l, 1 - c
    rows, width = wi_in.shape
    half = width // 2
    seq = QKV.shape[0]
    pair = seq // 2
    own = QKV.shape[1] // 3
    heads = own // HEAD_DIM
    slab = ny * nh * rows
    scale = TEMPER / math.sqrt(HEAD_DIM)
    q_s = 1.0 / math.sqrt(seq * nz * ny * nh)
    cols = (pl.ds(0, half), pl.ds(half, half))

    def copy(src, dst, ssem, rsem, dev):
        return pltpu.make_async_remote_copy(
            src_ref=src, dst_ref=dst, send_sem=ssem, recv_sem=rsem,
            device_id=dev, device_id_type=pl.DeviceIdType.MESH,
        )

    def zz(k):
        return lax.rem(z + k + nz, nz)

    def yy(k):
        return lax.rem(y + k + ny, ny)

    def hh(k):
        return lax.rem(h + k + nh, nh)

    def at_rows(i):
        return pl.ds(pl.multiple_of(i * rows, 16), rows)

    core_peer = {"c": oc}
    line_peer = {"l": ol}
    pair_peer = {"h": 1 - h}
    halves = (pl.ds(0, 2), pl.ds(2, 2))

    def last(color, k):
        return {"z": zz(k)} if color == 0 else {"y": yy(k)}

    def mid_dev(color, k):
        return last(1 - color, k)

    strip = 256
    side = (width - strip) // 2
    ag_cols = ((pl.ds(0, side), pl.ds(side, side), pl.ds(2 * side, strip)),) * 2 + (cols,)
    every = slice(None)

    def slab_at(buf, color, k, at, part=every, row=every):
        return buf.at[zz(k), part, row, at] if color == 0 else buf.at[part, yy(k), row, at]

    def line_at(buf, color, k, at, row=every):
        return buf.at[z, yy(k), row, at] if color == 0 else buf.at[zz(k), y, row, at]

    def line_of(s, color):
        return color if color < 2 else s % 2

    def row_of(color):
        return every if color < 2 else at_rows(h)

    def ag_pair(s, recv):
        piece = W.at[s, z, y, at_rows(1 - h if recv else h), pl.ds(0, 2 * side if s < 2 else width)]
        return copy(piece, piece, a1s.at[s, 0], a1r.at[s, 0], pair_peer)

    def ag_final(s, recv):
        piece = W.at[s, :, :, at_rows(1 - h if recv else h), ag_cols[s][2]]
        return copy(piece, piece, a1s.at[s, 1], a1r.at[s, 1], pair_peer)

    def ag_mid(s, color, k, which, recv):
        line = line_of(s, color)
        piece = line_at(W.at[s], line, -k if recv else 0, ag_cols[s][color], at_rows(h if which == 0 else 1 - h))
        return copy(piece, piece, a2s.at[s, color, k - 1, which], a2r.at[s, color, k - 1, which], mid_dev(line, k))

    def ag_last(s, color, d, recv):
        k, line = 1 - 2 * d, line_of(s, color)
        piece = slab_at(W.at[s], line, -k if recv else 0, ag_cols[s][color], row=row_of(color))
        return copy(piece, piece, a3s.at[s, color, d], a3r.at[s, color, d], last(line, k))

    def ag_relay(s, color, d, recv):
        k, line = 1 - 2 * d, line_of(s, color)
        piece = slab_at(W.at[s], line, 2 if recv else -k, ag_cols[s][color], halves[d], row_of(color))
        return copy(piece, piece, a4s.at[s, color, d], a4r.at[s, color, d], last(line, k))

    def ag_mid_start(s, which, colors=(0, 1)):
        if which:
            ag_pair(s, True).wait_recv()
        for k in (1, 3, 2):
            for color in colors:
                ag_mid(s, color, k, which, False).start()

    def ag_last_start(s, colors=(0, 1)):
        for color in colors:
            for which in (0, 1) if color < 2 else (0,):
                for k in range(1, 4):
                    ag_mid(s, color, k, which, True).wait_recv()
            for d in (0, 1):
                ag_last(s, color, d, False).start()

    def ag_relay_start(s, colors=(0, 1)):
        for color in colors:
            for d in (0, 1):
                ag_last(s, color, d, True).wait_recv()
                ag_relay(s, color, d, False).start()

    def ag_final_start(s):
        for d in (0, 1):
            ag_relay(s, 2, d, True).wait_recv()
        ag_final(s, False).start()

    def ag_wait(s):
        for color in (0, 1):
            for d in (0, 1):
                ag_relay(s, color, d, True).wait_recv()

    def ag_sent(s):
        ag_pair(s, False).wait_send()
        if s < 2:
            ag_final(s, False).wait_send()
        for color in (0, 1, 2) if s < 2 else (0, 1):
            for which in (0, 1) if color < 2 else (0,):
                for k in range(1, 4):
                    ag_mid(s, color, k, which, False).wait_send()
            for d in (0, 1):
                ag_last(s, color, d, False).wait_send()
                ag_relay(s, color, d, False).wait_send()

    R1 = (R1A, R1B)
    R2 = (R2A, R2B)
    full = 3 * own
    sections = 3 + heads
    parts = (G.at[0], G.at[1]) + (W.at[1],) * (1 + heads)
    slots = (2, 1) + (0,) * (1 + heads)
    lead = pl.ds(0, side)
    local_cols = [(lead, lead), (cols[0], cols[0])]
    grad_cols = [ag_cols[0], cols]
    pair_cols = [pl.ds(0, 2 * side), pl.ds(0, width)]
    third = own // 3
    for i, start in enumerate([full] + [hd * own for hd in range(heads)]):
        at = pl.ds(i * third, third)
        local_cols.append((at, at, pl.ds((4 + i // 2) * third, third)))
        grad_cols.append(tuple(pl.ds(start + j * third, third) for j in range(3)))
        pair_cols.append(pl.ds(start, 2 * third))

    def r1_at(s, color):
        if color < 2:
            return R1[color].at[slots[s], :, :, :, local_cols[s][color]]
        return R1C if s == 0 else R1[s % 2].at[0, :, :, pl.ds(0, rows), local_cols[s][2]]

    def r2_at(s, color):
        if color < 2:
            return R2[color].at[slots[s], :, :, local_cols[s][color]]
        return R2C if s == 0 else R2[s % 2].at[0, :, pl.ds(0, rows), local_cols[s][2]]

    def r4_at(s):
        return R4 if s == 0 else R4H.at[s - 2]

    def rs_first(s):
        src = parts[s].at[:, :, at_rows(1 - h), grad_cols[s][2]]
        return copy(src, r4_at(s), r4s.at[s], r4r.at[s], pair_peer)

    def rs_ring(s, color, d, kind):
        k, line = 1 - 2 * d, line_of(s, color)
        part = halves[1 - d if kind == 1 else d]
        src = slab_at(parts[s], line, 2 if kind == 0 else k, grad_cols[s][color], part, row_of(color))
        dst = r1_at(s, color).at[2 if kind == 0 else d, part]
        return copy(src, dst, r1s.at[s, color, d, kind], r1r.at[s, color, d, kind], last(line, k))

    def rs_mid(s, color, k):
        line = line_of(s, color)
        return copy(
            line_at(parts[s], line, k, grad_cols[s][color], row_of(color)), r2_at(s, color).at[k - 1],
            r2s.at[s, color, k - 1], r2r.at[s, color, k - 1], mid_dev(line, k),
        )

    def rs_pair(s):
        return copy(
            parts[s].at[z, y, at_rows(1 - h), pair_cols[s]], R3.at[slots[s], :, pair_cols[s]],
            r3s.at[s], r3r.at[s], pair_peer,
        )

    def rs_second(s):
        rs_first(s).wait_recv()

        @pl.loop(0, nz)
        def _(i):
            at = (i, every, at_rows(h), grad_cols[s][2])
            parts[s][at] = bf(f32(parts[s][at]) + f32(r4_at(s)[i]))

        rs_start(s, (2,))

    def rs_start(s, colors=(0, 1)):
        for kind in (0, 1):
            for color in colors:
                for d in (0, 1):
                    rs_ring(s, color, d, kind).start()

    def rs_combine(s, colors=(0, 1)):
        for color in colors:
            line = line_of(s, color)
            for d in (0, 1):
                rs_ring(s, color, d, 0).wait_recv()
                k = 1 - 2 * d

                @pl.loop(2 * d, 2 * d + 2)
                def _(i):
                    at = (zz(k), i) if line == 0 else (i, yy(k))
                    at = (*at, row_of(color), grad_cols[s][color])
                    parts[s][at] = bf(f32(parts[s][at]) + f32(r1_at(s, color)[2, i]))

                rs_ring(s, color, d, 2).start()

    def rs_mid_start(s, colors=(0, 1)):
        for color in colors:
            line = line_of(s, color)
            for d in (0, 1):
                for kind in (1, 2):
                    rs_ring(s, color, d, kind).wait_recv()

            @pl.loop(0, 4)
            def _(i):
                at = (z, i) if line == 0 else (i, y)
                at = (*at, row_of(color), grad_cols[s][color])
                total = f32(parts[s][at])
                for d in (0, 1):
                    total = total + f32(r1_at(s, color)[d, i])
                parts[s][at] = bf(total)

            for k in (1, 3, 2):
                rs_mid(s, color, k).start()

    def rs_total(s, color):
        for k in range(1, 4):
            rs_mid(s, color, k).wait_recv()
        total = f32(parts[s][z, y, row_of(color), grad_cols[s][color]])
        for k in range(3):
            total = total + f32(r2_at(s, color)[k])
        return total

    def rs_pair_start(s):
        for color in (0, 1):
            parts[s][z, y, every, grad_cols[s][color]] = bf(rs_total(s, color))
        rs_pair(s).start()

    def rs_finish(s):
        rs_pair(s).wait_recv()
        at = pair_cols[s]
        grads[slots[s], :, at] = f32(parts[s][z, y, at_rows(h), at]) + f32(R3[slots[s], :, at])

    def rs_finish_third(s):
        grads[slots[s], :, grad_cols[s][2]] = rs_total(s, 2)

    def rs_sent(s):
        for color in (0, 1) if s == 1 else (0, 1, 2):
            for d in (0, 1):
                for kind in (0, 1, 2):
                    rs_ring(s, color, d, kind).wait_send()
            for k in range(1, 4):
                rs_mid(s, color, k).wait_send()
        if s != 1:
            rs_first(s).wait_send()
        rs_pair(s).wait_send()

    def g_copy(i, buf, step, recv):
        if step == 0:
            piece, dev = buf.at[l, oc if recv else c], core_peer
        elif step == 1:
            piece, dev = buf.at[ol if recv else l, c], line_peer
        else:
            piece, dev = buf.at[ol, oc if recv else c], core_peer
        return copy(piece, piece, gs.at[i, step], gr.at[i, step], dev)

    def gather_start(i, buf):
        g_copy(i, buf, 1, False).start()
        g_copy(i, buf, 0, False).start()

    def gather_relay(i, buf):
        g_copy(i, buf, 1, True).wait_recv()
        g_copy(i, buf, 2, False).start()

    def gather_wait(i, buf, step):
        g_copy(i, buf, step, True).wait_recv()

    def gather_sent(i, buf):
        for step in range(3):
            g_copy(i, buf, step, False).wait_send()

    def s_copy(i, step):
        src, dev = (
            (PS.at[ol, oc], core_peer),
            (SX, line_peer),
            (PS.at[l, oc], core_peer),
        )[step]
        return copy(src, RX.at[i % 2, step], ss.at[i, step], sr.at[i, step], dev)

    def scatter_far(i, compute):
        compute(ol)
        s_copy(i, 0).start()
        s_copy(i, 0).wait_recv()
        SX[...] = bf(f32(PS[ol, c]) + f32(RX[i % 2, 0]))
        s_copy(i, 1).start()

    def scatter_near(i, compute):
        compute(l)
        s_copy(i, 2).start()

    def scatter_result(i):
        s_copy(i, 2).wait_recv()
        s_copy(i, 1).wait_recv()
        total = f32(PS[l, c]) + f32(RX[i % 2, 2]) + f32(RX[i % 2, 1])
        for step in range(3):
            s_copy(i, step).wait_send()
        return total

    def pair_rows(i):
        return pl.ds(pl.multiple_of(i * pair, 128), pair)

    def back_product(left, s, lo, n):
        def compute(i):
            @pl.loop(0, nz)
            def _(b):
                w = W[s, b, :, :, pl.ds(lo, n)].reshape(slab, n)
                at = pl.ds(pl.multiple_of(b * slab, 128), slab)
                PS[i, :, :, at] = bf(dot(left(i), w, 1, 1)).reshape(2, pair // 2, slab)
        return compute

    def two(buf, i):
        return buf[i].reshape(pair, buf.shape[-1])

    def all_rows(buf, at):
        return buf[:, :, :, at].reshape(seq, -1)

    def turn(buf):
        @pl.loop(0, nz)
        def _(b):
            AT[b] = all_rows(buf, pl.ds(pl.multiple_of(b * slab, 128), slab)).T

    def grad_turned(s, right, start, stop, tile):
        @pl.loop(0, (stop - start) // tile)
        def _(t):
            at = pl.ds(pl.multiple_of(start + t * tile, 128), tile)
            value = dot(AT[...].reshape(width, seq), right(at)) * q_s
            parts[s][:, :, :, at] = bf(value).reshape(nz, ny, nh * rows, tile)

    def grad_product(s, left, right, n, lo):
        @pl.loop(0, nz)
        def _(b):
            a = all_rows(left, pl.ds(pl.multiple_of(b * slab, 128), slab)).T
            value = dot(a, right) * q_s
            parts[s][b, :, :, pl.ds(lo, n)] = bf(value).reshape(ny, nh * rows, n)

    peers = [{"z": zz(k)} for k in range(1, 4)] + [{"y": yy(k)} for k in range(1, 4)]
    peers += [pair_peer, core_peer, line_peer, {"l": ol, "c": oc}]
    barrier = pltpu.get_barrier_semaphore()
    for dev in peers:
        pl.semaphore_signal(barrier, inc=1, device_id=dev, device_id_type=pl.DeviceIdType.MESH)
    mine = at_rows(h)
    moves = [
        (wq_in.at[i, :, pl.ds(hd * HEAD_DIM, HEAD_DIM)], W.at[0, z, y, mine, pl.ds((3 * hd + i) * HEAD_DIM, HEAD_DIM)])
        for i in range(3) for hd in range(heads)
    ]
    moves += [(wo_in, W.at[0, z, y, mine, pl.ds(3 * own, own)])]
    moves += [(wi_in, W.at[1, z, y, mine]), (wb_in, W.at[2, z, y, mine])]
    moves += [(tok_in, tok), (og_in, og), (mod_in, mod)]
    loads = [pltpu.make_async_copy(src, dst, in_sem.at[i]) for i, (src, dst) in enumerate(moves)]
    for load in loads:
        load.start()
    for load in loads:
        load.wait()
    m = [mod[i] for i in range(6)]
    n1, r1 = normalize(f32(tok[...]))
    A1[l, c] = bf(n1 * (1.0 + m[1]) + m[0])
    DM[l, c] = bf(m[5] * f32(og[...]))
    pl.semaphore_wait(barrier, len(peers))

    for s in range(3):
        ag_pair(s, False).start()
    for s in (0, 1):
        ag_mid_start(s, 0, (2,))
        ag_mid_start(s, 0)
    gather_start(0, A1)
    ag_last_start(0, (2,))
    ag_mid_start(0, 1)
    ag_mid_start(1, 1)
    ag_last_start(1, (2,))
    ag_relay_start(0, (2,))
    ag_last_start(0)
    ag_relay_start(1, (2,))
    ag_mid_start(2, 0)
    ag_mid_start(2, 1)
    ag_final_start(0)
    gather_relay(0, A1)
    ag_relay_start(0)
    ag_last_start(1)
    ag_final_start(1)
    gather_start(1, DM)
    gather_wait(0, A1, 0)
    gather_wait(0, A1, 2)

    ag_wait(0)

    @pl.loop(0, 3)
    def _(t):
        at = pl.ds(pl.multiple_of(t * own, 128), own)
        w = W[0, :, :, :, at].reshape(width, own)
        QKV[:, at] = bf(dot(A1[...].reshape(seq, width), w))

    def head(hd, i):
        return pl.ds(pl.multiple_of((3 * hd + i) * HEAD_DIM, 128), HEAD_DIM)

    def wide(hd):
        return pl.ds(pl.multiple_of(hd * HEAD_DIM, 128), HEAD_DIM)

    @pl.loop(0, heads)
    def _(hd):
        s = dot(QKV[:, head(hd, 0)], QKV[:, head(hd, 1)], 1, 1) * scale
        e = jnp.exp(s - jnp.max(s, axis=-1, keepdims=True))
        p = bf(e * (1.0 / jnp.sum(e, axis=-1, keepdims=True)))
        PR[hd] = p
        O[:, wide(hd)] = bf(dot(p, QKV[:, head(hd, 2)]))

    out_product = back_product(lambda i: O[pair_rows(i), :], 0, 3 * own, own)
    ag_last_start(2)
    ag_final(0, True).wait_recv()
    scatter_far(0, out_product)
    scatter_near(0, out_product)
    ag_relay_start(1)
    mid = f32(tok[...]) + m[2] * scatter_result(0)
    MID[...] = mid
    n2, r2 = normalize(mid)
    A2[l, c] = bf(n2 * (1.0 + m[4]) + m[3])
    gather_start(2, A2)

    tile = 256

    def hidden(i):
        @pl.loop(0, width // tile)
        def _(t):
            at = pl.ds(pl.multiple_of(t * tile, 128), tile)
            g, d = gelu_pair(dot(two(A2, i), W[1, :, :, :, at].reshape(width, tile)))
            GG[i, :, :, at] = bf(g).reshape(2, pair // 2, tile)
            DU[i, :, :, at] = bf(d).reshape(2, pair // 2, tile)

    gather_relay(1, DM)
    gather_wait(1, DM, 0)
    gather_wait(1, DM, 2)
    turn(DM)
    ag_relay_start(2)
    gather_relay(2, A2)
    gather_wait(2, A2, 0)
    ag_wait(1)
    ag_final(1, True).wait_recv()
    hidden(l)
    gather_wait(2, A2, 2)
    hidden(ol)
    for lo, hi in ((2 * side, width), (0, half), (half, 2 * side)):
        grad_turned(0, lambda at: all_rows(GG, at), lo, hi, tile)
        if lo == 2 * side:
            rs_first(0).start()
        else:
            rs_start(0, (0,) if lo == 0 else (1,))
    ag_wait(2)

    @pl.loop(0, width // tile)
    def _(t):
        at = pl.ds(pl.multiple_of(t * tile, 128), tile)
        dg = dot(DM[...].reshape(seq, width), W[2, :, :, :, at].reshape(width, tile))
        DU[:, :, :, at] = bf(f32(DU[:, :, :, at]) * dg.reshape(2, 2, pair // 2, tile))

    in_back = back_product(lambda i: two(DU, i), 1, 0, width)
    scatter_far(1, in_back)
    turn(A2)
    grad_turned(1, lambda at: all_rows(DU, at), 0, half, tile)
    rs_combine(0)
    rs_second(0)
    rs_start(1, (0,))
    grad_turned(1, lambda at: all_rows(DU, at), half, width, tile)
    rs_start(1, (1,))
    scatter_near(1, in_back)
    e2 = scatter_result(1) * (1.0 + m[4])
    n2, r2 = normalize(MID[...])
    dmid = f32(og[...]) + norm_back(n2, r2, e2)
    DX[...] = dmid
    DA[l, c] = bf(m[2] * dmid)
    gather_start(3, DA)

    ff_back = back_product(lambda i: two(GG, i), 2, 0, width)
    scatter_far(2, ff_back)
    scatter_near(2, ff_back)
    turn(A1)
    rs_combine(0, (2,))
    rs_combine(1)
    rs_mid_start(0)
    gather_relay(3, DA)
    gather_wait(3, DA, 0)
    gather_wait(3, DA, 2)

    DO[...] = bf(dot(DA[...].reshape(seq, width), W[0, :, :, :, pl.ds(3 * own, own)].reshape(width, own)))
    ag_sent(1)
    grad_product(2, DA, O[...], own, full)
    rs_first(2).start()
    rs_start(2)

    for hd in range(heads):
        do = DO[:, wide(hd)]
        p = PR[hd]
        t = f32(p) * dot(do, QKV[:, head(hd, 2)], 1, 1)
        ds = bf(scale * (t - f32(p) * jnp.sum(t, axis=-1, keepdims=True)))
        DQKV[:, head(hd, 0)] = bf(dot(ds, QKV[:, head(hd, 1)]))
        DQKV[:, head(hd, 1)] = bf(dot(ds.T, QKV[:, head(hd, 0)]))
        DQKV[:, head(hd, 2)] = bf(dot(p.T, do))
        grad_turned(3 + hd, lambda at: DQKV[:, at], hd * own, (hd + 1) * own, own)
        rs_first(3 + hd).start()
        rs_start(3 + hd)

    qkv_back = back_product(lambda i: DQKV[pair_rows(i), :], 0, 0, 3 * own)
    fin[...] = bf(MID[...] + m[5] * scatter_result(2))
    scatter_far(3, qkv_back)
    rs_second(2)
    rs_combine(2)
    rs_mid_start(1)
    scatter_near(3, qkv_back)
    rs_combine(3)
    rs_second(3)
    rs_mid_start(0, (2,))
    rs_combine(4)
    rs_combine(2, (2,))
    rs_second(4)
    rs_pair_start(0)
    rs_combine(5)
    rs_mid_start(2)
    rs_second(5)
    rs_combine(3, (2,))
    rs_mid_start(3)
    rs_finish_third(0)
    rs_mid_start(2, (2,))
    rs_combine(4, (2,))
    e1 = scatter_result(3) * (1.0 + m[1])
    n1, r1 = normalize(f32(tok[...]))
    dxin[...] = DX[...] + norm_back(n1, r1, e1)
    rs_mid_start(4)
    rs_mid_start(3, (2,))
    rs_combine(5, (2,))
    rs_mid_start(5)
    rs_pair_start(1)
    rs_finish(0)
    rs_pair_start(2)
    rs_mid_start(4, (2,))
    rs_pair_start(3)
    rs_mid_start(5, (2,))
    rs_pair_start(4)
    rs_finish(1)
    rs_pair_start(5)
    for s in range(2, sections):
        rs_finish_third(s)
    for s in range(2, sections):
        rs_finish(s)
    for s in range(sections):
        rs_sent(s)
    ag_sent(0)
    ag_sent(2)
    for i, buf in enumerate((A1, DM, A2, DA)):
        gather_sent(i, buf)


def place(fin, dx, grads, o_fin, o_dx, o_qkv, o_out, o_in, o_back):
    own = o_out.shape[1]
    o_fin[0] = fin[...]
    o_dx[0] = dx[...]
    for i in range(3):
        for hd in range(own // HEAD_DIM):
            at = (3 * hd + i) * HEAD_DIM
            o_qkv[i, :, hd * HEAD_DIM : (hd + 1) * HEAD_DIM] = grads[0, :, at : at + HEAD_DIM]
    o_out[...] = grads[0, :, 3 * own :]
    o_in[0] = grads[1]
    o_back[...] = grads[2]


def step(dims, tokens, modulation, w_qkv, w_out, w_in, w_back, out_grad):
    nz, ny, nh = dims
    count, width = tokens.shape[1:]
    rows, own, ff = w_qkv.shape[1], w_qkv.shape[3], w_in.shape[2]
    assert ff == width and 4 * own == width
    seq = 4 * count
    heads = own // HEAD_DIM
    big = (nz, ny, nh * rows)
    half = width // 2
    vmem = pltpu.VMEM
    dma = pltpu.SemaphoreType.DMA
    tokens_buf = vmem((2, 2, count, width), BF)
    scratch = [
        vmem((3, *big, width), BF),
        vmem((2, *big, width), BF),
        vmem((3, 3, 4, nh * rows, half), BF),
        vmem((3, 3, 4, nh * rows, half), BF),
        vmem((3, 3, nh * rows, half), BF),
        vmem((3, 3, nh * rows, half), BF),
        vmem((3, rows, width), BF),
        vmem((3, 4, rows, 256), BF),
        vmem((3, rows, 256), BF),
        vmem((nz, ny, rows, 256), BF),
        vmem((1 + heads, nz, ny, rows, own // 3), BF),
        *[tokens_buf] * 6,
        vmem((seq, 3 * own), BF),
        vmem((seq, 3 * own), BF),
        vmem((seq, own), BF),
        vmem((seq, own), BF),
        vmem((heads, seq, seq), BF),
        tokens_buf,
        vmem((2, 3, count, width), BF),
        vmem((count, width), BF),
        vmem((count, width), F32),
        vmem((count, width), F32),
        vmem((nz, ny * nh * rows, seq), BF),
        vmem((count, width), BF),
        vmem((6, 1, width), F32),
        vmem((count, width), BF),
        dma((6 + 3 * heads,)),
        dma((3, 2)), dma((3, 2)),
        dma((3, 3, 3, 2)), dma((3, 3, 3, 2)),
        dma((3, 3, 2)), dma((3, 3, 2)),
        dma((3, 3, 2)), dma((3, 3, 2)),
        dma((3 + heads, 3, 2, 3)), dma((3 + heads, 3, 2, 3)),
        dma((3 + heads, 3, 3)), dma((3 + heads, 3, 3)),
        dma((3 + heads,)), dma((3 + heads,)),
        dma((3 + heads,)), dma((3 + heads,)),
        dma((4, 3)), dma((4, 3)),
        dma((4, 3)), dma((4, 3)),
    ]
    spec = pl.BlockSpec(memory_space=pltpu.VMEM)
    final, dx, grads = pl.pallas_call(
        functools.partial(kernel, dims),
        out_shape=(
            jax.ShapeDtypeStruct((count, width), BF),
            jax.ShapeDtypeStruct((count, width), F32),
            jax.ShapeDtypeStruct((3, rows, width), F32),
        ),
        in_specs=[pl.BlockSpec(memory_space=pl.ANY)] * 7,
        out_specs=(spec, spec, spec),
        scratch_shapes=scratch,
        compiler_params=pltpu.CompilerParams(
            collective_id=0, has_side_effects=True, vmem_limit_bytes=67043328
        ),
    )(
        tokens[0], modulation[0].transpose(1, 0, 2), w_qkv[0].transpose(1, 0, 2), w_out[0].T,
        w_in[0], w_back[0].T, out_grad[0],
    )
    final, dx, qkv, out, inner, back = pl.pallas_call(
        place,
        out_shape=(
            jax.ShapeDtypeStruct((1, count, width), BF),
            jax.ShapeDtypeStruct((1, count, width), F32),
            jax.ShapeDtypeStruct((3, rows, own), F32),
            jax.ShapeDtypeStruct((rows, own), F32),
            jax.ShapeDtypeStruct((1, rows, width), F32),
            jax.ShapeDtypeStruct((rows, width), F32),
        ),
        in_specs=[spec] * 3,
        out_specs=(spec,) * 6,
    )(final, dx, grads)
    return final, dx, qkv.transpose(1, 0, 2)[None], out.T[None], inner, back.T[None]


def solution(mesh):
    dims = (4, 4, 2)
    assert mesh.shape["fsdp"] == 32 and mesh.shape["sp"] == 4
    torus = Mesh(mesh.devices.reshape(*dims, 2, 2), AXES)
    fsdp, sp = AXES[:3], AXES[3:]
    placed = (
        P(fsdp, sp, None),
        P(fsdp, None, None, None),
        P(None, fsdp, None, sp),
        P(None, sp, fsdp),
        P(None, fsdp, sp),
        P(None, sp, fsdp),
        P(fsdp, sp, None),
    )
    return jax.shard_map(
        functools.partial(step, dims),
        mesh=torus,
        in_specs=placed,
        out_specs=(placed[0], *placed[:1], *placed[2:6]),
        check_vma=False,
    )
```

```python
import functools
import math

import jax
import jax.numpy as jnp
from jax import lax
from jax.experimental import pallas as pl
from jax.experimental.pallas import tpu as pltpu
from jax.sharding import Mesh
from jax.sharding import PartitionSpec as P

HEAD_DIM = 128
LN_EPS = 1e-06
TEMPER = 2.5
BF = jnp.bfloat16
F32 = jnp.float32
AXES = ("z", "y", "h", "l", "c")


def bf(x):
    return x.astype(BF)


def f32(x):
    return x.astype(F32)


def dot(a, b, ca=1, cb=0):
    return lax.dot_general(a, b, (((ca,), (cb,)), ((), ())), preferred_element_type=F32)


def normalize(x):
    d = x - jnp.mean(x, axis=-1, keepdims=True)
    r = lax.rsqrt(jnp.mean(d * d, axis=-1, keepdims=True) + LN_EPS)
    return d * r, r


def norm_back(n, r, e):
    return r * (e - jnp.mean(e, axis=-1, keepdims=True) - n * jnp.mean(e * n, axis=-1, keepdims=True))


def gelu_pair(u):
    k0 = math.sqrt(2.0 / math.pi)
    s = u * u
    t = jnp.tanh(k0 * u * (1.0 + 0.044715 * s))
    g = 0.5 * u * (1.0 + t)
    d = 0.5 * (1.0 + t) + 0.5 * k0 * u * (1.0 - t * t) * (1.0 + 3.0 * 0.044715 * s)
    return g, d


def kernel(
    dims, tok_in, mod_in, wq_in, wo_in, wi_in, wb_in, og_in, fin, dxin, grads,
    W, G, R1A, R1B, R2A, R2B, R3, R1C, R2C, R4, R4H, A1, A2, DM, DA, GG, DU, QKV, DQKV, O, DO, PR, PS, RX, SX, MID, DX, AT,
    tok, mod, og, in_sem, a1s, a1r, a2s, a2r, a3s, a3r, a4s, a4r, r1s, r1r, r2s, r2r, r3s, r3r, r4s, r4r, gs, gr, ss, sr,
):
    nz, ny, nh = dims
    z, y, h, l, c = (lax.axis_index(a) for a in AXES)
    ol, oc = 1 - l, 1 - c
    rows, width = wi_in.shape
    half = width // 2
    seq = QKV.shape[0]
    pair = seq // 2
    own = QKV.shape[1] // 3
    heads = own // HEAD_DIM
    slab = ny * nh * rows
    scale = TEMPER / math.sqrt(HEAD_DIM)
    q_s = 1.0 / math.sqrt(seq * nz * ny * nh)
    cols = (pl.ds(0, half), pl.ds(half, half))

    def copy(src, dst, ssem, rsem, dev):
        return pltpu.make_async_remote_copy(
            src_ref=src, dst_ref=dst, send_sem=ssem, recv_sem=rsem,
            device_id=dev, device_id_type=pl.DeviceIdType.MESH,
        )

    def zz(k):
        return lax.rem(z + k + nz, nz)

    def yy(k):
        return lax.rem(y + k + ny, ny)

    def hh(k):
        return lax.rem(h + k + nh, nh)

    def at_rows(i):
        return pl.ds(pl.multiple_of(i * rows, 16), rows)

    core_peer = {"c": oc}
    line_peer = {"l": ol}
    pair_peer = {"h": 1 - h}
    halves = (pl.ds(0, 2), pl.ds(2, 2))

    def last(color, k):
        return {"z": zz(k)} if color == 0 else {"y": yy(k)}

    def mid_dev(color, k):
        return last(1 - color, k)

    strip = 256
    side = (width - strip) // 2
    ag_cols = ((pl.ds(0, side), pl.ds(side, side), pl.ds(2 * side, strip)),) * 2 + (cols,)
    every = slice(None)

    def slab_at(buf, color, k, at, part=every, row=every):
        return buf.at[zz(k), part, row, at] if color == 0 else buf.at[part, yy(k), row, at]

    def line_at(buf, color, k, at, row=every):
        return buf.at[z, yy(k), row, at] if color == 0 else buf.at[zz(k), y, row, at]

    def line_of(s, color):
        return color if color < 2 else s % 2

    def row_of(color):
        return every if color < 2 else at_rows(h)

    def ag_pair(s, recv):
        piece = W.at[s, z, y, at_rows(1 - h if recv else h), pl.ds(0, 2 * side if s < 2 else width)]
        return copy(piece, piece, a1s.at[s, 0], a1r.at[s, 0], pair_peer)

    def ag_final(s, recv):
        piece = W.at[s, :, :, at_rows(1 - h if recv else h), ag_cols[s][2]]
        return copy(piece, piece, a1s.at[s, 1], a1r.at[s, 1], pair_peer)

    def ag_mid(s, color, k, which, recv):
        line = line_of(s, color)
        piece = line_at(W.at[s], line, -k if recv else 0, ag_cols[s][color], at_rows(h if which == 0 else 1 - h))
        return copy(piece, piece, a2s.at[s, color, k - 1, which], a2r.at[s, color, k - 1, which], mid_dev(line, k))

    def ag_last(s, color, d, j, recv):
        k, line = 1 - 2 * d, line_of(s, color)
        part = halves[d if j == 0 else 1 - d]
        piece = slab_at(W.at[s], line, -k if recv else 0, ag_cols[s][color], part, row_of(color))
        return copy(piece, piece, a3s.at[s, color, d, j], a3r.at[s, color, d, j], last(line, k))

    def ag_relay(s, color, d, recv):
        k, line = 1 - 2 * d, line_of(s, color)
        piece = slab_at(W.at[s], line, 2 if recv else -k, ag_cols[s][color], halves[d], row_of(color))
        return copy(piece, piece, a4s.at[s, color, d], a4r.at[s, color, d], last(line, k))

    def ag_mid_start(s, which, colors=(0, 1)):
        if which:
            ag_pair(s, True).wait_recv()
        for k in (1, 3, 2):
            for color in colors:
                ag_mid(s, color, k, which, False).start()

    def ag_last_start(s, colors=(0, 1)):
        for color in colors:
            for which in (0, 1) if color < 2 else (0,):
                for k in range(1, 4):
                    ag_mid(s, color, k, which, True).wait_recv()
        for j in (0, 1):
            for color in colors:
                for d in (0, 1):
                    ag_last(s, color, d, j, False).start()

    def ag_relay_start(s, colors=(0, 1)):
        for color in colors:
            for d in (0, 1):
                ag_last(s, color, d, 0, True).wait_recv()
                ag_relay(s, color, d, False).start()

    def ag_final_start(s):
        for d in (0, 1):
            ag_last(s, 2, d, 1, True).wait_recv()
            ag_relay(s, 2, d, True).wait_recv()
        ag_final(s, False).start()

    def ag_wait(s):
        for color in (0, 1):
            for d in (0, 1):
                ag_last(s, color, d, 1, True).wait_recv()
                ag_relay(s, color, d, True).wait_recv()

    def ag_sent(s):
        ag_pair(s, False).wait_send()
        if s < 2:
            ag_final(s, False).wait_send()
        for color in (0, 1, 2) if s < 2 else (0, 1):
            for which in (0, 1) if color < 2 else (0,):
                for k in range(1, 4):
                    ag_mid(s, color, k, which, False).wait_send()
            for d in (0, 1):
                for j in (0, 1):
                    ag_last(s, color, d, j, False).wait_send()
                ag_relay(s, color, d, False).wait_send()

    R1 = (R1A, R1B)
    R2 = (R2A, R2B)
    full = 3 * own
    sections = 3 + heads
    parts = (G.at[0], G.at[1]) + (W.at[1],) * (1 + heads)
    slots = (2, 1) + (0,) * (1 + heads)
    lead = pl.ds(0, side)
    local_cols = [(lead, lead), (cols[0], cols[0])]
    grad_cols = [ag_cols[0], cols]
    pair_cols = [pl.ds(0, 2 * side), pl.ds(0, width)]
    third = own // 3
    for i, start in enumerate([full] + [hd * own for hd in range(heads)]):
        at = pl.ds(i * third, third)
        local_cols.append((at, at, pl.ds((4 + i // 2) * third, third)))
        grad_cols.append(tuple(pl.ds(start + j * third, third) for j in range(3)))
        pair_cols.append(pl.ds(start, 2 * third))

    def r1_at(s, color):
        if color < 2:
            return R1[color].at[slots[s], :, :, :, local_cols[s][color]]
        return R1C if s == 0 else R1[s % 2].at[0, :, :, pl.ds(0, rows), local_cols[s][2]]

    def r2_at(s, color):
        if color < 2:
            return R2[color].at[slots[s], :, :, local_cols[s][color]]
        return R2C if s == 0 else R2[s % 2].at[0, :, pl.ds(0, rows), local_cols[s][2]]

    def r4_at(s):
        return R4 if s == 0 else R4H.at[s - 2]

    def rs_first(s):
        src = parts[s].at[:, :, at_rows(1 - h), grad_cols[s][2]]
        return copy(src, r4_at(s), r4s.at[s], r4r.at[s], pair_peer)

    def rs_ring(s, color, d, kind):
        k, line = 1 - 2 * d, line_of(s, color)
        part = halves[1 - d if kind == 1 else d]
        src = slab_at(parts[s], line, 2 if kind == 0 else k, grad_cols[s][color], part, row_of(color))
        dst = r1_at(s, color).at[2 if kind == 0 else d, part]
        return copy(src, dst, r1s.at[s, color, d, kind], r1r.at[s, color, d, kind], last(line, k))

    def rs_mid(s, color, k):
        line = line_of(s, color)
        return copy(
            line_at(parts[s], line, k, grad_cols[s][color], row_of(color)), r2_at(s, color).at[k - 1],
            r2s.at[s, color, k - 1], r2r.at[s, color, k - 1], mid_dev(line, k),
        )

    def rs_pair(s):
        return copy(
            parts[s].at[z, y, at_rows(1 - h), pair_cols[s]], R3.at[slots[s], :, pair_cols[s]],
            r3s.at[s], r3r.at[s], pair_peer,
        )

    def rs_second(s):
        rs_first(s).wait_recv()

        @pl.loop(0, nz)
        def _(i):
            at = (i, every, at_rows(h), grad_cols[s][2])
            parts[s][at] = bf(f32(parts[s][at]) + f32(r4_at(s)[i]))

        rs_start(s, (2,))

    def rs_start(s, colors=(0, 1)):
        for kind in (0, 1):
            for color in colors:
                for d in (0, 1):
                    rs_ring(s, color, d, kind).start()

    def rs_combine(s, colors=(0, 1)):
        for color in colors:
            line = line_of(s, color)
            for d in (0, 1):
                rs_ring(s, color, d, 0).wait_recv()
                k = 1 - 2 * d

                @pl.loop(2 * d, 2 * d + 2)
                def _(i):
                    at = (zz(k), i) if line == 0 else (i, yy(k))
                    at = (*at, row_of(color), grad_cols[s][color])
                    parts[s][at] = bf(f32(parts[s][at]) + f32(r1_at(s, color)[2, i]))

                rs_ring(s, color, d, 2).start()

    def rs_mid_start(s, colors=(0, 1)):
        for color in colors:
            line = line_of(s, color)
            for d in (0, 1):
                for kind in (1, 2):
                    rs_ring(s, color, d, kind).wait_recv()

            @pl.loop(0, 4)
            def _(i):
                at = (z, i) if line == 0 else (i, y)
                at = (*at, row_of(color), grad_cols[s][color])
                total = f32(parts[s][at])
                for d in (0, 1):
                    total = total + f32(r1_at(s, color)[d, i])
                parts[s][at] = bf(total)

            for k in (1, 3, 2):
                rs_mid(s, color, k).start()

    def rs_total(s, color):
        for k in range(1, 4):
            rs_mid(s, color, k).wait_recv()
        total = f32(parts[s][z, y, row_of(color), grad_cols[s][color]])
        for k in range(3):
            total = total + f32(r2_at(s, color)[k])
        return total

    def rs_pair_start(s):
        for color in (0, 1):
            parts[s][z, y, every, grad_cols[s][color]] = bf(rs_total(s, color))
        rs_pair(s).start()

    def rs_finish(s):
        rs_pair(s).wait_recv()
        at = pair_cols[s]
        grads[slots[s], :, at] = f32(parts[s][z, y, at_rows(h), at]) + f32(R3[slots[s], :, at])

    def rs_finish_third(s):
        grads[slots[s], :, grad_cols[s][2]] = rs_total(s, 2)

    def rs_sent(s):
        for color in (0, 1) if s == 1 else (0, 1, 2):
            for d in (0, 1):
                for kind in (0, 1, 2):
                    rs_ring(s, color, d, kind).wait_send()
            for k in range(1, 4):
                rs_mid(s, color, k).wait_send()
        if s != 1:
            rs_first(s).wait_send()
        rs_pair(s).wait_send()

    def g_copy(i, buf, step, recv):
        if step == 0:
            piece, dev = buf.at[l, oc if recv else c], core_peer
        elif step == 1:
            piece, dev = buf.at[ol if recv else l, c], line_peer
        else:
            piece, dev = buf.at[ol, oc if recv else c], core_peer
        return copy(piece, piece, gs.at[i, step], gr.at[i, step], dev)

    def gather_start(i, buf):
        g_copy(i, buf, 1, False).start()
        g_copy(i, buf, 0, False).start()

    def gather_relay(i, buf):
        g_copy(i, buf, 1, True).wait_recv()
        g_copy(i, buf, 2, False).start()

    def gather_wait(i, buf, step):
        g_copy(i, buf, step, True).wait_recv()

    def gather_sent(i, buf):
        for step in range(3):
            g_copy(i, buf, step, False).wait_send()

    def s_copy(i, step):
        src, dev = (
            (PS.at[ol, oc], core_peer),
            (SX, line_peer),
            (PS.at[l, oc], core_peer),
        )[step]
        return copy(src, RX.at[i % 2, step], ss.at[i, step], sr.at[i, step], dev)

    def scatter_far(i, compute):
        compute(ol)
        s_copy(i, 0).start()
        s_copy(i, 0).wait_recv()
        SX[...] = bf(f32(PS[ol, c]) + f32(RX[i % 2, 0]))
        s_copy(i, 1).start()

    def scatter_near(i, compute):
        compute(l)
        s_copy(i, 2).start()

    def scatter_result(i):
        s_copy(i, 2).wait_recv()
        s_copy(i, 1).wait_recv()
        total = f32(PS[l, c]) + f32(RX[i % 2, 2]) + f32(RX[i % 2, 1])
        for step in range(3):
            s_copy(i, step).wait_send()
        return total

    def pair_rows(i):
        return pl.ds(pl.multiple_of(i * pair, 128), pair)

    def back_product(left, s, lo, n):
        def compute(i):
            @pl.loop(0, nz)
            def _(b):
                w = W[s, b, :, :, pl.ds(lo, n)].reshape(slab, n)
                at = pl.ds(pl.multiple_of(b * slab, 128), slab)
                PS[i, :, :, at] = bf(dot(left(i), w, 1, 1)).reshape(2, pair // 2, slab)
        return compute

    def two(buf, i):
        return buf[i].reshape(pair, buf.shape[-1])

    def all_rows(buf, at):
        return buf[:, :, :, at].reshape(seq, -1)

    def turn(buf):
        @pl.loop(0, nz)
        def _(b):
            AT[b] = all_rows(buf, pl.ds(pl.multiple_of(b * slab, 128), slab)).T

    def grad_turned(s, right, start, stop, tile):
        @pl.loop(0, (stop - start) // tile)
        def _(t):
            at = pl.ds(pl.multiple_of(start + t * tile, 128), tile)
            value = dot(AT[...].reshape(width, seq), right(at)) * q_s
            parts[s][:, :, :, at] = bf(value).reshape(nz, ny, nh * rows, tile)

    def grad_product(s, left, right, n, lo):
        @pl.loop(0, nz)
        def _(b):
            a = all_rows(left, pl.ds(pl.multiple_of(b * slab, 128), slab)).T
            value = dot(a, right) * q_s
            parts[s][b, :, :, pl.ds(lo, n)] = bf(value).reshape(ny, nh * rows, n)

    peers = [{"z": zz(k)} for k in range(1, 4)] + [{"y": yy(k)} for k in range(1, 4)]
    peers += [pair_peer, core_peer, line_peer, {"l": ol, "c": oc}]
    barrier = pltpu.get_barrier_semaphore()
    for dev in peers:
        pl.semaphore_signal(barrier, inc=1, device_id=dev, device_id_type=pl.DeviceIdType.MESH)
    mine = at_rows(h)
    moves = [
        (wq_in.at[i, :, pl.ds(hd * HEAD_DIM, HEAD_DIM)], W.at[0, z, y, mine, pl.ds((3 * hd + i) * HEAD_DIM, HEAD_DIM)])
        for i in range(3) for hd in range(heads)
    ]
    moves += [(wo_in, W.at[0, z, y, mine, pl.ds(3 * own, own)])]
    moves += [(wi_in, W.at[1, z, y, mine]), (wb_in, W.at[2, z, y, mine])]
    moves += [(tok_in, tok), (og_in, og), (mod_in, mod)]
    loads = [pltpu.make_async_copy(src, dst, in_sem.at[i]) for i, (src, dst) in enumerate(moves)]
    for load in loads:
        load.start()
    for load in loads:
        load.wait()
    m = [mod[i] for i in range(6)]
    n1, r1 = normalize(f32(tok[...]))
    A1[l, c] = bf(n1 * (1.0 + m[1]) + m[0])
    DM[l, c] = bf(m[5] * f32(og[...]))
    pl.semaphore_wait(barrier, len(peers))

    for s in range(3):
        ag_pair(s, False).start()
    for s in (0, 1):
        ag_mid_start(s, 0, (2,))
        ag_mid_start(s, 0)
    gather_start(0, A1)
    ag_last_start(0, (2,))
    ag_mid_start(0, 1)
    ag_mid_start(1, 1)
    ag_last_start(1, (2,))
    ag_relay_start(0, (2,))
    ag_last_start(0)
    ag_relay_start(1, (2,))
    ag_final_start(0)
    gather_relay(0, A1)
    ag_relay_start(0)
    ag_last_start(1)
    ag_mid_start(2, 0)
    ag_mid_start(2, 1)
    ag_final_start(1)
    gather_start(1, DM)
    gather_wait(0, A1, 0)
    gather_wait(0, A1, 2)

    ag_wait(0)

    @pl.loop(0, 3)
    def _(t):
        at = pl.ds(pl.multiple_of(t * own, 128), own)
        w = W[0, :, :, :, at].reshape(width, own)
        QKV[:, at] = bf(dot(A1[...].reshape(seq, width), w))

    def head(hd, i):
        return pl.ds(pl.multiple_of((3 * hd + i) * HEAD_DIM, 128), HEAD_DIM)

    def wide(hd):
        return pl.ds(pl.multiple_of(hd * HEAD_DIM, 128), HEAD_DIM)

    @pl.loop(0, heads)
    def _(hd):
        s = dot(QKV[:, head(hd, 0)], QKV[:, head(hd, 1)], 1, 1) * scale
        e = jnp.exp(s - jnp.max(s, axis=-1, keepdims=True))
        p = bf(e * (1.0 / jnp.sum(e, axis=-1, keepdims=True)))
        PR[hd] = p
        O[:, wide(hd)] = bf(dot(p, QKV[:, head(hd, 2)]))

    out_product = back_product(lambda i: O[pair_rows(i), :], 0, 3 * own, own)
    ag_final(0, True).wait_recv()
    scatter_far(0, out_product)
    scatter_near(0, out_product)
    ag_relay_start(1)
    ag_last_start(2)
    mid = f32(tok[...]) + m[2] * scatter_result(0)
    MID[...] = mid
    n2, r2 = normalize(mid)
    A2[l, c] = bf(n2 * (1.0 + m[4]) + m[3])
    gather_start(2, A2)

    tile = 256

    def hidden(i):
        @pl.loop(0, width // tile)
        def _(t):
            at = pl.ds(pl.multiple_of(t * tile, 128), tile)
            g, d = gelu_pair(dot(two(A2, i), W[1, :, :, :, at].reshape(width, tile)))
            GG[i, :, :, at] = bf(g).reshape(2, pair // 2, tile)
            DU[i, :, :, at] = bf(d).reshape(2, pair // 2, tile)

    gather_relay(1, DM)
    gather_wait(1, DM, 0)
    gather_wait(1, DM, 2)
    turn(DM)
    ag_wait(1)
    ag_final(1, True).wait_recv()
    gather_wait(2, A2, 0)
    hidden(l)
    ag_relay_start(2)
    gather_relay(2, A2)
    gather_wait(2, A2, 2)
    hidden(ol)
    for lo, hi in ((2 * side, width), (0, half), (half, 2 * side)):
        grad_turned(0, lambda at: all_rows(GG, at), lo, hi, tile)
        if lo == 2 * side:
            rs_first(0).start()
        else:
            rs_start(0, (0,) if lo == 0 else (1,))
    ag_wait(2)

    @pl.loop(0, width // tile)
    def _(t):
        at = pl.ds(pl.multiple_of(t * tile, 128), tile)
        dg = dot(DM[...].reshape(seq, width), W[2, :, :, :, at].reshape(width, tile))
        DU[:, :, :, at] = bf(f32(DU[:, :, :, at]) * dg.reshape(2, 2, pair // 2, tile))

    in_back = back_product(lambda i: two(DU, i), 1, 0, width)
    scatter_far(1, in_back)
    turn(A2)
    grad_turned(1, lambda at: all_rows(DU, at), 0, half, tile)
    rs_combine(0)
    rs_second(0)
    rs_start(1, (0,))
    grad_turned(1, lambda at: all_rows(DU, at), half, width, tile)
    rs_start(1, (1,))
    scatter_near(1, in_back)
    e2 = scatter_result(1) * (1.0 + m[4])
    n2, r2 = normalize(MID[...])
    dmid = f32(og[...]) + norm_back(n2, r2, e2)
    DX[...] = dmid
    DA[l, c] = bf(m[2] * dmid)
    gather_start(3, DA)

    ff_back = back_product(lambda i: two(GG, i), 2, 0, width)
    scatter_far(2, ff_back)
    scatter_near(2, ff_back)
    turn(A1)
    rs_combine(0, (2,))
    rs_combine(1)
    rs_mid_start(0)
    gather_relay(3, DA)
    gather_wait(3, DA, 0)
    gather_wait(3, DA, 2)

    DO[...] = bf(dot(DA[...].reshape(seq, width), W[0, :, :, :, pl.ds(3 * own, own)].reshape(width, own)))
    ag_sent(1)
    grad_product(2, DA, O[...], own, full)
    rs_first(2).start()
    rs_start(2)

    for hd in range(heads):
        do = DO[:, wide(hd)]
        p = PR[hd]
        t = f32(p) * dot(do, QKV[:, head(hd, 2)], 1, 1)
        ds = bf(scale * (t - f32(p) * jnp.sum(t, axis=-1, keepdims=True)))
        DQKV[:, head(hd, 0)] = bf(dot(ds, QKV[:, head(hd, 1)]))
        DQKV[:, head(hd, 1)] = bf(dot(ds.T, QKV[:, head(hd, 0)]))
        DQKV[:, head(hd, 2)] = bf(dot(p.T, do))
        grad_turned(3 + hd, lambda at: DQKV[:, at], hd * own, (hd + 1) * own, own)
        rs_first(3 + hd).start()
        rs_start(3 + hd)

    qkv_back = back_product(lambda i: DQKV[pair_rows(i), :], 0, 0, 3 * own)
    fin[...] = bf(MID[...] + m[5] * scatter_result(2))
    scatter_far(3, qkv_back)
    rs_second(2)
    rs_combine(2)
    rs_mid_start(1)
    scatter_near(3, qkv_back)
    rs_combine(3)
    rs_second(3)
    rs_mid_start(0, (2,))
    rs_combine(4)
    rs_combine(2, (2,))
    rs_second(4)
    rs_pair_start(0)
    rs_combine(5)
    rs_mid_start(2)
    rs_second(5)
    rs_combine(3, (2,))
    rs_mid_start(3)
    rs_finish_third(0)
    rs_mid_start(2, (2,))
    rs_combine(4, (2,))
    e1 = scatter_result(3) * (1.0 + m[1])
    n1, r1 = normalize(f32(tok[...]))
    dxin[...] = DX[...] + norm_back(n1, r1, e1)
    rs_mid_start(4)
    rs_mid_start(3, (2,))
    rs_combine(5, (2,))
    rs_mid_start(5)
    rs_pair_start(1)
    rs_finish(0)
    rs_pair_start(2)
    rs_mid_start(4, (2,))
    rs_pair_start(3)
    rs_mid_start(5, (2,))
    rs_pair_start(4)
    rs_finish(1)
    rs_pair_start(5)
    for s in range(2, sections):
        rs_finish_third(s)
    for s in range(2, sections):
        rs_finish(s)
    for s in range(sections):
        rs_sent(s)
    ag_sent(0)
    ag_sent(2)
    for i, buf in enumerate((A1, DM, A2, DA)):
        gather_sent(i, buf)


def place(fin, dx, grads, o_fin, o_dx, o_qkv, o_out, o_in, o_back):
    own = o_out.shape[1]
    o_fin[0] = fin[...]
    o_dx[0] = dx[...]
    for i in range(3):
        for hd in range(own // HEAD_DIM):
            at = (3 * hd + i) * HEAD_DIM
            o_qkv[i, :, hd * HEAD_DIM : (hd + 1) * HEAD_DIM] = grads[0, :, at : at + HEAD_DIM]
    o_out[...] = grads[0, :, 3 * own :]
    o_in[0] = grads[1]
    o_back[...] = grads[2]


def step(dims, tokens, modulation, w_qkv, w_out, w_in, w_back, out_grad):
    nz, ny, nh = dims
    count, width = tokens.shape[1:]
    rows, own, ff = w_qkv.shape[1], w_qkv.shape[3], w_in.shape[2]
    assert ff == width and 4 * own == width
    seq = 4 * count
    heads = own // HEAD_DIM
    big = (nz, ny, nh * rows)
    half = width // 2
    vmem = pltpu.VMEM
    dma = pltpu.SemaphoreType.DMA
    tokens_buf = vmem((2, 2, count, width), BF)
    scratch = [
        vmem((3, *big, width), BF),
        vmem((2, *big, width), BF),
        vmem((3, 3, 4, nh * rows, half), BF),
        vmem((3, 3, 4, nh * rows, half), BF),
        vmem((3, 3, nh * rows, half), BF),
        vmem((3, 3, nh * rows, half), BF),
        vmem((3, rows, width), BF),
        vmem((3, 4, rows, 256), BF),
        vmem((3, rows, 256), BF),
        vmem((nz, ny, rows, 256), BF),
        vmem((1 + heads, nz, ny, rows, own // 3), BF),
        *[tokens_buf] * 6,
        vmem((seq, 3 * own), BF),
        vmem((seq, 3 * own), BF),
        vmem((seq, own), BF),
        vmem((seq, own), BF),
        vmem((heads, seq, seq), BF),
        tokens_buf,
        vmem((2, 3, count, width), BF),
        vmem((count, width), BF),
        vmem((count, width), F32),
        vmem((count, width), F32),
        vmem((nz, ny * nh * rows, seq), BF),
        vmem((count, width), BF),
        vmem((6, 1, width), F32),
        vmem((count, width), BF),
        dma((6 + 3 * heads,)),
        dma((3, 2)), dma((3, 2)),
        dma((3, 3, 3, 2)), dma((3, 3, 3, 2)),
        dma((3, 3, 2, 2)), dma((3, 3, 2, 2)),
        dma((3, 3, 2)), dma((3, 3, 2)),
        dma((3 + heads, 3, 2, 3)), dma((3 + heads, 3, 2, 3)),
        dma((3 + heads, 3, 3)), dma((3 + heads, 3, 3)),
        dma((3 + heads,)), dma((3 + heads,)),
        dma((3 + heads,)), dma((3 + heads,)),
        dma((4, 3)), dma((4, 3)),
        dma((4, 3)), dma((4, 3)),
    ]
    spec = pl.BlockSpec(memory_space=pltpu.VMEM)
    final, dx, grads = pl.pallas_call(
        functools.partial(kernel, dims),
        out_shape=(
            jax.ShapeDtypeStruct((count, width), BF),
            jax.ShapeDtypeStruct((count, width), F32),
            jax.ShapeDtypeStruct((3, rows, width), F32),
        ),
        in_specs=[pl.BlockSpec(memory_space=pl.ANY)] * 7,
        out_specs=(spec, spec, spec),
        scratch_shapes=scratch,
        compiler_params=pltpu.CompilerParams(
            collective_id=0, has_side_effects=True, vmem_limit_bytes=67043328
        ),
    )(
        tokens[0], modulation[0].transpose(1, 0, 2), w_qkv[0].transpose(1, 0, 2), w_out[0].T,
        w_in[0], w_back[0].T, out_grad[0],
    )
    final, dx, qkv, out, inner, back = pl.pallas_call(
        place,
        out_shape=(
            jax.ShapeDtypeStruct((1, count, width), BF),
            jax.ShapeDtypeStruct((1, count, width), F32),
            jax.ShapeDtypeStruct((3, rows, own), F32),
            jax.ShapeDtypeStruct((rows, own), F32),
            jax.ShapeDtypeStruct((1, rows, width), F32),
            jax.ShapeDtypeStruct((rows, width), F32),
        ),
        in_specs=[spec] * 3,
        out_specs=(spec,) * 6,
    )(final, dx, grads)
    return final, dx, qkv.transpose(1, 0, 2)[None], out.T[None], inner, back.T[None]


def solution(mesh):
    dims = (4, 4, 2)
    assert mesh.shape["fsdp"] == 32 and mesh.shape["sp"] == 4
    torus = Mesh(mesh.devices.reshape(*dims, 2, 2), AXES)
    fsdp, sp = AXES[:3], AXES[3:]
    placed = (
        P(fsdp, sp, None),
        P(fsdp, None, None, None),
        P(None, fsdp, None, sp),
        P(None, sp, fsdp),
        P(None, fsdp, sp),
        P(None, sp, fsdp),
        P(fsdp, sp, None),
    )
    return jax.shard_map(
        functools.partial(step, dims),
        mesh=torus,
        in_specs=placed,
        out_specs=(placed[0], *placed[:1], *placed[2:6]),
        check_vma=False,
    )
```

```python
import functools
import math

import jax
import jax.numpy as jnp
from jax import lax
from jax.experimental import pallas as pl
from jax.experimental.pallas import tpu as pltpu
from jax.sharding import Mesh
from jax.sharding import PartitionSpec as P

HEAD_DIM = 128
LN_EPS = 1e-06
TEMPER = 2.5
BF = jnp.bfloat16
F32 = jnp.float32
AXES = ("z", "y", "h", "l", "c")


def bf(x):
    return x.astype(BF)


def f32(x):
    return x.astype(F32)


def dot(a, b, ca=1, cb=0):
    return lax.dot_general(a, b, (((ca,), (cb,)), ((), ())), preferred_element_type=F32)


def normalize(x):
    d = x - jnp.mean(x, axis=-1, keepdims=True)
    r = lax.rsqrt(jnp.mean(d * d, axis=-1, keepdims=True) + LN_EPS)
    return d * r, r


def norm_back(n, r, e):
    return r * (e - jnp.mean(e, axis=-1, keepdims=True) - n * jnp.mean(e * n, axis=-1, keepdims=True))


def gelu_pair(u):
    k0 = math.sqrt(2.0 / math.pi)
    s = u * u
    t = jnp.tanh(k0 * u * (1.0 + 0.044715 * s))
    g = 0.5 * u * (1.0 + t)
    d = 0.5 * (1.0 + t) + 0.5 * k0 * u * (1.0 - t * t) * (1.0 + 3.0 * 0.044715 * s)
    return g, d


def kernel(
    dims, tok_in, mod_in, wq_in, wo_in, wi_in, wb_in, og_in, fin, dxin, grads,
    W, G, R1A, R1B, R2A, R2B, R3, R1C, R2C, R4, R4H, A1, A2, DM, DA, GG, DU, QKV, DQKV, O, DO, PR, PS, RX, SX, MID, DX, AT,
    tok, mod, og, in_sem, a1s, a1r, a2s, a2r, a3s, a3r, a4s, a4r, a5s, a5r, r1s, r1r, r2s, r2r, r3s, r3r, r4s, r4r, r5s, r5r, gs, gr, ss, sr,
):
    nz, ny, nh = dims
    z, y, h, l, c = (lax.axis_index(a) for a in AXES)
    ol, oc = 1 - l, 1 - c
    rows, width = wi_in.shape
    half = width // 2
    seq = QKV.shape[0]
    pair = seq // 2
    own = QKV.shape[1] // 3
    heads = own // HEAD_DIM
    slab = ny * nh * rows
    scale = TEMPER / math.sqrt(HEAD_DIM)
    q_s = 1.0 / math.sqrt(seq * nz * ny * nh)
    cols = (pl.ds(0, half), pl.ds(half, half))

    def copy(src, dst, ssem, rsem, dev):
        return pltpu.make_async_remote_copy(
            src_ref=src, dst_ref=dst, send_sem=ssem, recv_sem=rsem,
            device_id=dev, device_id_type=pl.DeviceIdType.MESH,
        )

    def zz(k):
        return lax.rem(z + k + nz, nz)

    def yy(k):
        return lax.rem(y + k + ny, ny)

    def hh(k):
        return lax.rem(h + k + nh, nh)

    def at_rows(i):
        return pl.ds(pl.multiple_of(i * rows, 16), rows)

    core_peer = {"c": oc}
    line_peer = {"l": ol}
    pair_peer = {"h": 1 - h}
    halves = (pl.ds(0, 2), pl.ds(2, 2))

    def last(color, k):
        return {"z": zz(k)} if color == 0 else {"y": yy(k)}

    def mid_dev(color, k):
        return last(1 - color, k)

    strip = 256
    side = (width - strip) // 2
    ag_cols = ((pl.ds(0, side), pl.ds(side, side), pl.ds(2 * side, strip)),) * 2 + (cols,)
    every = slice(None)

    def slab_at(buf, color, k, at, part=every, row=every):
        return buf.at[zz(k), part, row, at] if color == 0 else buf.at[part, yy(k), row, at]

    def line_at(buf, color, k, at, row=every):
        return buf.at[z, yy(k), row, at] if color == 0 else buf.at[zz(k), y, row, at]

    def line_of(s, color):
        return color if color < 2 else s % 2

    def row_of(color):
        return every if color < 2 else at_rows(h)

    def ag_pair(s, recv):
        piece = W.at[s, z, y, at_rows(1 - h if recv else h), pl.ds(0, 2 * side if s < 2 else width)]
        return copy(piece, piece, a1s.at[s, 0], a1r.at[s, 0], pair_peer)

    def ag_final(s, recv):
        piece = W.at[s, :, :, at_rows(1 - h if recv else h), ag_cols[s][2]]
        return copy(piece, piece, a1s.at[s, 1], a1r.at[s, 1], pair_peer)

    def ag_mid(s, color, k, which, recv):
        line = line_of(s, color)
        piece = line_at(W.at[s], line, -k if recv else 0, ag_cols[s][color], at_rows(h if which == 0 else 1 - h))
        return copy(piece, piece, a2s.at[s, color, k - 1, which], a2r.at[s, color, k - 1, which], mid_dev(line, k))

    def ag_hop(s, color, d, recv):
        k = 1 - 2 * d
        piece = line_at(W.at[s], color, 2 if recv else -k, ag_cols[s][color], at_rows(d))
        return copy(piece, piece, a5s.at[s, color, d], a5r.at[s, color, d], mid_dev(color, k))

    def ag_last(s, color, d, j, recv):
        k, line = 1 - 2 * d, line_of(s, color)
        part = halves[d if j == 0 else 1 - d]
        piece = slab_at(W.at[s], line, -k if recv else 0, ag_cols[s][color], part, row_of(color))
        return copy(piece, piece, a3s.at[s, color, d, j], a3r.at[s, color, d, j], last(line, k))

    def ag_relay(s, color, d, recv):
        k, line = 1 - 2 * d, line_of(s, color)
        piece = slab_at(W.at[s], line, 2 if recv else -k, ag_cols[s][color], halves[d], row_of(color))
        return copy(piece, piece, a4s.at[s, color, d], a4r.at[s, color, d], last(line, k))

    def ag_mid_start(s, which, colors=(0, 1)):
        if which:
            ag_pair(s, True).wait_recv()
        for k in (1, 3, 2) if direct(s, colors[0]) else (1, 3):
            for color in colors:
                ag_mid(s, color, k, which, False).start()

    def direct(s, color):
        return s != 1 or color == 2

    def ag_hop_start(s):
        for color in (0, 1):
            for d in (0, 1):
                for which in (0, 1):
                    ag_mid(s, color, 1 + 2 * d, which, True).wait_recv()
                ag_hop(s, color, d, False).start()

    def ag_last_start(s, colors=(0, 1)):
        for color in colors:
            if direct(s, color):
                for which in (0, 1) if color < 2 else (0,):
                    for k in range(1, 4):
                        ag_mid(s, color, k, which, True).wait_recv()
            else:
                for d in (0, 1):
                    ag_hop(s, color, d, True).wait_recv()
        for j in (0, 1):
            for color in colors:
                for d in (0, 1):
                    ag_last(s, color, d, j, False).start()

    def ag_relay_start(s, colors=(0, 1)):
        for color in colors:
            for d in (0, 1):
                ag_last(s, color, d, 0, True).wait_recv()
                ag_relay(s, color, d, False).start()

    def ag_final_start(s):
        for d in (0, 1):
            ag_last(s, 2, d, 1, True).wait_recv()
            ag_relay(s, 2, d, True).wait_recv()
        ag_final(s, False).start()

    def ag_wait(s):
        for color in (0, 1):
            for d in (0, 1):
                ag_last(s, color, d, 1, True).wait_recv()
                ag_relay(s, color, d, True).wait_recv()

    def ag_sent(s):
        ag_pair(s, False).wait_send()
        if s < 2:
            ag_final(s, False).wait_send()
        for color in (0, 1, 2) if s < 2 else (0, 1):
            for which in (0, 1) if color < 2 else (0,):
                for k in (1, 2, 3) if direct(s, color) else (1, 3):
                    ag_mid(s, color, k, which, False).wait_send()
            if not direct(s, color):
                for d in (0, 1):
                    ag_hop(s, color, d, False).wait_send()
            for d in (0, 1):
                for j in (0, 1):
                    ag_last(s, color, d, j, False).wait_send()
                ag_relay(s, color, d, False).wait_send()

    R1 = (R1A, R1B)
    R2 = (R2A, R2B)
    full = 3 * own
    sections = 3 + heads
    parts = (G.at[0], G.at[1]) + (W.at[1],) * (1 + heads)
    slots = (2, 1) + (0,) * (1 + heads)
    lead = pl.ds(0, side)
    local_cols = [(lead, lead), (cols[0], cols[0])]
    grad_cols = [ag_cols[0], cols]
    pair_cols = [pl.ds(0, 2 * side), pl.ds(0, width)]
    third = own // 3
    for i, start in enumerate([full] + [hd * own for hd in range(heads)]):
        at = pl.ds(i * third, third)
        local_cols.append((at, at, pl.ds((4 + i // 2) * third, third)))
        grad_cols.append(tuple(pl.ds(start + j * third, third) for j in range(3)))
        pair_cols.append(pl.ds(start, 2 * third))

    def r1_at(s, color):
        if color < 2:
            return R1[color].at[slots[s], :, :, :, local_cols[s][color]]
        return R1C if s == 0 else R1[s % 2].at[0, :, :, pl.ds(0, rows), local_cols[s][2]]

    def r2_at(s, color):
        if color < 2:
            return R2[color].at[slots[s], :, :, local_cols[s][color]]
        return R2C if s == 0 else R2[s % 2].at[0, :, pl.ds(0, rows), local_cols[s][2]]

    def r4_at(s):
        return R4 if s == 0 else R4H.at[s - 2]

    def rs_first(s):
        src = parts[s].at[:, :, at_rows(1 - h), grad_cols[s][2]]
        return copy(src, r4_at(s), r4s.at[s], r4r.at[s], pair_peer)

    def rs_ring(s, color, d, kind):
        k, line = 1 - 2 * d, line_of(s, color)
        part = halves[1 - d if kind == 1 else d]
        src = slab_at(parts[s], line, 2 if kind == 0 else k, grad_cols[s][color], part, row_of(color))
        dst = r1_at(s, color).at[2 if kind == 0 else d, part]
        return copy(src, dst, r1s.at[s, color, d, kind], r1r.at[s, color, d, kind], last(line, k))

    def rs_mid(s, color, k):
        line = line_of(s, color)
        return copy(
            line_at(parts[s], line, k, grad_cols[s][color], row_of(color)), r2_at(s, color).at[k - 1],
            r2s.at[s, color, k - 1], r2r.at[s, color, k - 1], mid_dev(line, k),
        )

    def ringed(s, color):
        return s < 2 and color < 2

    def rs_hop(s, color, d, kind):
        k = 1 - 2 * d
        row = at_rows(1 - d if kind == 1 else d)
        src = line_at(parts[s], color, 2 if kind == 0 else k, grad_cols[s][color], row)
        dst = r2_at(s, color).at[2 if kind == 0 else d, row]
        return copy(src, dst, r5s.at[s, color, d, kind], r5r.at[s, color, d, kind], mid_dev(color, k))

    def rs_hop_combine(s):
        for color in (0, 1):
            for d in (0, 1):
                rs_hop(s, color, d, 0).wait_recv()
                k = 1 - 2 * d
                at = (z, yy(k)) if color == 0 else (zz(k), y)
                at = (*at, at_rows(d), grad_cols[s][color])
                parts[s][at] = bf(f32(parts[s][at]) + f32(r2_at(s, color)[2, d * rows : (d + 1) * rows]))
                rs_hop(s, color, d, 2).start()

    def rs_pair(s):
        return copy(
            parts[s].at[z, y, at_rows(1 - h), pair_cols[s]], R3.at[slots[s], :, pair_cols[s]],
            r3s.at[s], r3r.at[s], pair_peer,
        )

    def rs_second(s):
        rs_first(s).wait_recv()

        @pl.loop(0, nz)
        def _(i):
            at = (i, every, at_rows(h), grad_cols[s][2])
            parts[s][at] = bf(f32(parts[s][at]) + f32(r4_at(s)[i]))

        rs_start(s, (2,))

    def rs_start(s, colors=(0, 1)):
        for kind in (0, 1):
            for color in colors:
                for d in (0, 1):
                    rs_ring(s, color, d, kind).start()

    def rs_combine(s, colors=(0, 1)):
        for color in colors:
            line = line_of(s, color)
            for d in (0, 1):
                rs_ring(s, color, d, 0).wait_recv()
                k = 1 - 2 * d

                @pl.loop(2 * d, 2 * d + 2)
                def _(i):
                    at = (zz(k), i) if line == 0 else (i, yy(k))
                    at = (*at, row_of(color), grad_cols[s][color])
                    parts[s][at] = bf(f32(parts[s][at]) + f32(r1_at(s, color)[2, i]))

                rs_ring(s, color, d, 2).start()

    def rs_mid_start(s, colors=(0, 1)):
        for color in colors:
            line = line_of(s, color)
            for d in (0, 1):
                for kind in (1, 2):
                    rs_ring(s, color, d, kind).wait_recv()

            @pl.loop(0, 4)
            def _(i):
                at = (z, i) if line == 0 else (i, y)
                at = (*at, row_of(color), grad_cols[s][color])
                total = f32(parts[s][at])
                for d in (0, 1):
                    total = total + f32(r1_at(s, color)[d, i])
                parts[s][at] = bf(total)

            if ringed(s, color):
                for kind in (0, 1):
                    for d in (0, 1):
                        rs_hop(s, color, d, kind).start()
            else:
                for k in (1, 3, 2):
                    rs_mid(s, color, k).start()

    def rs_total(s, color):
        if ringed(s, color):
            for d in (0, 1):
                for kind in (1, 2):
                    rs_hop(s, color, d, kind).wait_recv()
        else:
            for k in range(1, 4):
                rs_mid(s, color, k).wait_recv()
        total = f32(parts[s][z, y, row_of(color), grad_cols[s][color]])
        for k in range(2 if ringed(s, color) else 3):
            total = total + f32(r2_at(s, color)[k])
        return total

    def rs_pair_start(s):
        for color in (0, 1):
            parts[s][z, y, every, grad_cols[s][color]] = bf(rs_total(s, color))
        rs_pair(s).start()

    def rs_finish(s):
        rs_pair(s).wait_recv()
        at = pair_cols[s]
        grads[slots[s], :, at] = f32(parts[s][z, y, at_rows(h), at]) + f32(R3[slots[s], :, at])

    def rs_finish_third(s):
        grads[slots[s], :, grad_cols[s][2]] = rs_total(s, 2)

    def rs_sent(s):
        for color in (0, 1) if s == 1 else (0, 1, 2):
            for d in (0, 1):
                for kind in (0, 1, 2):
                    rs_ring(s, color, d, kind).wait_send()
            if ringed(s, color):
                for d in (0, 1):
                    for kind in (0, 1, 2):
                        rs_hop(s, color, d, kind).wait_send()
            else:
                for k in range(1, 4):
                    rs_mid(s, color, k).wait_send()
        if s != 1:
            rs_first(s).wait_send()
        rs_pair(s).wait_send()

    def g_copy(i, buf, step, recv):
        if step == 0:
            piece, dev = buf.at[l, oc if recv else c], core_peer
        elif step == 1:
            piece, dev = buf.at[ol if recv else l, c], line_peer
        else:
            piece, dev = buf.at[ol, oc if recv else c], core_peer
        return copy(piece, piece, gs.at[i, step], gr.at[i, step], dev)

    def gather_start(i, buf):
        g_copy(i, buf, 1, False).start()
        g_copy(i, buf, 0, False).start()

    def gather_relay(i, buf):
        g_copy(i, buf, 1, True).wait_recv()
        g_copy(i, buf, 2, False).start()

    def gather_wait(i, buf, step):
        g_copy(i, buf, step, True).wait_recv()

    def gather_sent(i, buf):
        for step in range(3):
            g_copy(i, buf, step, False).wait_send()

    def s_copy(i, step):
        src, dev = (
            (PS.at[ol, oc], core_peer),
            (SX, line_peer),
            (PS.at[l, oc], core_peer),
        )[step]
        return copy(src, RX.at[i % 2, step], ss.at[i, step], sr.at[i, step], dev)

    def scatter_far(i, compute):
        compute(ol)
        s_copy(i, 0).start()
        s_copy(i, 0).wait_recv()
        SX[...] = bf(f32(PS[ol, c]) + f32(RX[i % 2, 0]))
        s_copy(i, 1).start()

    def scatter_near(i, compute):
        compute(l)
        s_copy(i, 2).start()

    def scatter_result(i):
        s_copy(i, 2).wait_recv()
        s_copy(i, 1).wait_recv()
        total = f32(PS[l, c]) + f32(RX[i % 2, 2]) + f32(RX[i % 2, 1])
        for step in range(3):
            s_copy(i, step).wait_send()
        return total

    def pair_rows(i):
        return pl.ds(pl.multiple_of(i * pair, 128), pair)

    def back_product(left, s, lo, n):
        def compute(i):
            @pl.loop(0, nz)
            def _(b):
                w = W[s, b, :, :, pl.ds(lo, n)].reshape(slab, n)
                at = pl.ds(pl.multiple_of(b * slab, 128), slab)
                PS[i, :, :, at] = bf(dot(left(i), w, 1, 1)).reshape(2, pair // 2, slab)
        return compute

    def two(buf, i):
        return buf[i].reshape(pair, buf.shape[-1])

    def all_rows(buf, at):
        return buf[:, :, :, at].reshape(seq, -1)

    def turn(buf):
        @pl.loop(0, nz)
        def _(b):
            AT[b] = all_rows(buf, pl.ds(pl.multiple_of(b * slab, 128), slab)).T

    def grad_turned(s, right, start, stop, tile):
        @pl.loop(0, (stop - start) // tile)
        def _(t):
            at = pl.ds(pl.multiple_of(start + t * tile, 128), tile)
            value = dot(AT[...].reshape(width, seq), right(at)) * q_s
            parts[s][:, :, :, at] = bf(value).reshape(nz, ny, nh * rows, tile)

    def grad_product(s, left, right, n, lo):
        @pl.loop(0, nz)
        def _(b):
            a = all_rows(left, pl.ds(pl.multiple_of(b * slab, 128), slab)).T
            value = dot(a, right) * q_s
            parts[s][b, :, :, pl.ds(lo, n)] = bf(value).reshape(ny, nh * rows, n)

    peers = [{"z": zz(k)} for k in range(1, 4)] + [{"y": yy(k)} for k in range(1, 4)]
    peers += [pair_peer, core_peer, line_peer, {"l": ol, "c": oc}]
    barrier = pltpu.get_barrier_semaphore()
    for dev in peers:
        pl.semaphore_signal(barrier, inc=1, device_id=dev, device_id_type=pl.DeviceIdType.MESH)
    mine = at_rows(h)
    moves = [
        (wq_in.at[i, :, pl.ds(hd * HEAD_DIM, HEAD_DIM)], W.at[0, z, y, mine, pl.ds((3 * hd + i) * HEAD_DIM, HEAD_DIM)])
        for i in range(3) for hd in range(heads)
    ]
    moves += [(wo_in, W.at[0, z, y, mine, pl.ds(3 * own, own)])]
    moves += [(wi_in, W.at[1, z, y, mine]), (wb_in, W.at[2, z, y, mine])]
    moves += [(tok_in, tok), (og_in, og), (mod_in, mod)]
    loads = [pltpu.make_async_copy(src, dst, in_sem.at[i]) for i, (src, dst) in enumerate(moves)]
    for load in loads:
        load.start()
    for load in loads:
        load.wait()
    m = [mod[i] for i in range(6)]
    n1, r1 = normalize(f32(tok[...]))
    A1[l, c] = bf(n1 * (1.0 + m[1]) + m[0])
    DM[l, c] = bf(m[5] * f32(og[...]))
    pl.semaphore_wait(barrier, len(peers))

    for s in range(3):
        ag_pair(s, False).start()
    for s in (0, 1):
        ag_mid_start(s, 0, (2,))
        ag_mid_start(s, 0)
    gather_start(0, A1)
    ag_last_start(0, (2,))
    ag_mid_start(0, 1)
    ag_mid_start(1, 1)
    ag_last_start(1, (2,))
    ag_relay_start(0, (2,))
    ag_hop_start(1)
    ag_last_start(0)
    ag_relay_start(1, (2,))
    ag_final_start(0)
    gather_relay(0, A1)
    gather_start(1, DM)
    ag_relay_start(0)
    ag_mid_start(2, 0)
    ag_mid_start(2, 1)
    ag_last_start(1)
    ag_final_start(1)
    gather_wait(0, A1, 0)
    gather_wait(0, A1, 2)

    ag_wait(0)

    @pl.loop(0, 3)
    def _(t):
        at = pl.ds(pl.multiple_of(t * own, 128), own)
        w = W[0, :, :, :, at].reshape(width, own)
        QKV[:, at] = bf(dot(A1[...].reshape(seq, width), w))

    def head(hd, i):
        return pl.ds(pl.multiple_of((3 * hd + i) * HEAD_DIM, 128), HEAD_DIM)

    def wide(hd):
        return pl.ds(pl.multiple_of(hd * HEAD_DIM, 128), HEAD_DIM)

    @pl.loop(0, heads)
    def _(hd):
        s = dot(QKV[:, head(hd, 0)], QKV[:, head(hd, 1)], 1, 1) * scale
        e = jnp.exp(s - jnp.max(s, axis=-1, keepdims=True))
        p = bf(e * (1.0 / jnp.sum(e, axis=-1, keepdims=True)))
        PR[hd] = p
        O[:, wide(hd)] = bf(dot(p, QKV[:, head(hd, 2)]))

    out_product = back_product(lambda i: O[pair_rows(i), :], 0, 3 * own, own)
    ag_final(0, True).wait_recv()
    scatter_far(0, out_product)
    scatter_near(0, out_product)
    ag_relay_start(1)
    ag_last_start(2)
    mid = f32(tok[...]) + m[2] * scatter_result(0)
    MID[...] = mid
    n2, r2 = normalize(mid)
    A2[l, c] = bf(n2 * (1.0 + m[4]) + m[3])
    gather_start(2, A2)

    tile = 256

    def hidden(i):
        @pl.loop(0, width // tile)
        def _(t):
            at = pl.ds(pl.multiple_of(t * tile, 128), tile)
            g, d = gelu_pair(dot(two(A2, i), W[1, :, :, :, at].reshape(width, tile)))
            GG[i, :, :, at] = bf(g).reshape(2, pair // 2, tile)
            DU[i, :, :, at] = bf(d).reshape(2, pair // 2, tile)

    gather_relay(1, DM)
    gather_wait(1, DM, 0)
    gather_wait(1, DM, 2)
    turn(DM)
    ag_wait(1)
    ag_final(1, True).wait_recv()
    gather_wait(2, A2, 0)
    hidden(l)
    ag_relay_start(2)
    gather_relay(2, A2)
    gather_wait(2, A2, 2)
    hidden(ol)
    for lo, hi in ((2 * side, width), (0, half), (half, 2 * side)):
        grad_turned(0, lambda at: all_rows(GG, at), lo, hi, tile)
        if lo == 2 * side:
            rs_first(0).start()
        else:
            rs_start(0, (0,) if lo == 0 else (1,))
    ag_wait(2)

    @pl.loop(0, width // tile)
    def _(t):
        at = pl.ds(pl.multiple_of(t * tile, 128), tile)
        dg = dot(DM[...].reshape(seq, width), W[2, :, :, :, at].reshape(width, tile))
        DU[:, :, :, at] = bf(f32(DU[:, :, :, at]) * dg.reshape(2, 2, pair // 2, tile))

    in_back = back_product(lambda i: two(DU, i), 1, 0, width)
    scatter_far(1, in_back)
    turn(A2)
    grad_turned(1, lambda at: all_rows(DU, at), 0, half, tile)
    rs_combine(0)
    rs_second(0)
    rs_start(1, (0,))
    grad_turned(1, lambda at: all_rows(DU, at), half, width, tile)
    rs_start(1, (1,))
    scatter_near(1, in_back)
    e2 = scatter_result(1) * (1.0 + m[4])
    n2, r2 = normalize(MID[...])
    dmid = f32(og[...]) + norm_back(n2, r2, e2)
    DX[...] = dmid
    DA[l, c] = bf(m[2] * dmid)
    gather_start(3, DA)

    ff_back = back_product(lambda i: two(GG, i), 2, 0, width)
    scatter_far(2, ff_back)
    scatter_near(2, ff_back)
    turn(A1)
    rs_combine(0, (2,))
    rs_combine(1)
    rs_mid_start(0)
    gather_relay(3, DA)
    gather_wait(3, DA, 0)
    gather_wait(3, DA, 2)

    DO[...] = bf(dot(DA[...].reshape(seq, width), W[0, :, :, :, pl.ds(3 * own, own)].reshape(width, own)))
    ag_sent(1)
    grad_product(2, DA, O[...], own, full)
    rs_first(2).start()
    rs_start(2)

    for hd in range(heads):
        do = DO[:, wide(hd)]
        p = PR[hd]
        t = f32(p) * dot(do, QKV[:, head(hd, 2)], 1, 1)
        ds = bf(scale * (t - f32(p) * jnp.sum(t, axis=-1, keepdims=True)))
        DQKV[:, head(hd, 0)] = bf(dot(ds, QKV[:, head(hd, 1)]))
        DQKV[:, head(hd, 1)] = bf(dot(ds.T, QKV[:, head(hd, 0)]))
        DQKV[:, head(hd, 2)] = bf(dot(p.T, do))
        grad_turned(3 + hd, lambda at: DQKV[:, at], hd * own, (hd + 1) * own, own)
        rs_first(3 + hd).start()
        rs_start(3 + hd)

    qkv_back = back_product(lambda i: DQKV[pair_rows(i), :], 0, 0, 3 * own)
    fin[...] = bf(MID[...] + m[5] * scatter_result(2))
    scatter_far(3, qkv_back)
    rs_hop_combine(0)
    rs_second(2)
    rs_combine(2)
    rs_mid_start(1)
    scatter_near(3, qkv_back)
    rs_combine(3)
    rs_second(3)
    rs_mid_start(0, (2,))
    rs_combine(4)
    rs_combine(2, (2,))
    rs_second(4)
    rs_combine(5)
    rs_mid_start(2)
    rs_pair_start(0)
    rs_second(5)
    rs_hop_combine(1)
    rs_combine(3, (2,))
    rs_mid_start(3)
    rs_finish_third(0)
    rs_mid_start(2, (2,))
    rs_combine(4, (2,))
    rs_mid_start(4)
    rs_mid_start(3, (2,))
    e1 = scatter_result(3) * (1.0 + m[1])
    n1, r1 = normalize(f32(tok[...]))
    dxin[...] = DX[...] + norm_back(n1, r1, e1)
    rs_pair_start(1)
    rs_combine(5, (2,))
    rs_mid_start(5)
    rs_finish(0)
    rs_pair_start(2)
    rs_mid_start(4, (2,))
    rs_pair_start(3)
    rs_mid_start(5, (2,))
    rs_pair_start(4)
    rs_pair_start(5)
    rs_finish(1)
    for s in range(2, sections):
        rs_finish_third(s)
    for s in range(2, sections):
        rs_finish(s)
    for s in range(sections):
        rs_sent(s)
    ag_sent(0)
    ag_sent(2)
    for i, buf in enumerate((A1, DM, A2, DA)):
        gather_sent(i, buf)


def place(fin, dx, grads, o_fin, o_dx, o_qkv, o_out, o_in, o_back):
    own = o_out.shape[1]
    o_fin[0] = fin[...]
    o_dx[0] = dx[...]
    for i in range(3):
        for hd in range(own // HEAD_DIM):
            at = (3 * hd + i) * HEAD_DIM
            o_qkv[i, :, hd * HEAD_DIM : (hd + 1) * HEAD_DIM] = grads[0, :, at : at + HEAD_DIM]
    o_out[...] = grads[0, :, 3 * own :]
    o_in[0] = grads[1]
    o_back[...] = grads[2]


def step(dims, tokens, modulation, w_qkv, w_out, w_in, w_back, out_grad):
    nz, ny, nh = dims
    count, width = tokens.shape[1:]
    rows, own, ff = w_qkv.shape[1], w_qkv.shape[3], w_in.shape[2]
    assert ff == width and 4 * own == width
    seq = 4 * count
    heads = own // HEAD_DIM
    big = (nz, ny, nh * rows)
    half = width // 2
    vmem = pltpu.VMEM
    dma = pltpu.SemaphoreType.DMA
    tokens_buf = vmem((2, 2, count, width), BF)
    scratch = [
        vmem((3, *big, width), BF),
        vmem((2, *big, width), BF),
        vmem((3, 3, 4, nh * rows, half), BF),
        vmem((3, 3, 4, nh * rows, half), BF),
        vmem((3, 3, nh * rows, half), BF),
        vmem((3, 3, nh * rows, half), BF),
        vmem((3, rows, width), BF),
        vmem((3, 4, rows, 256), BF),
        vmem((3, rows, 256), BF),
        vmem((nz, ny, rows, 256), BF),
        vmem((1 + heads, nz, ny, rows, own // 3), BF),
        *[tokens_buf] * 6,
        vmem((seq, 3 * own), BF),
        vmem((seq, 3 * own), BF),
        vmem((seq, own), BF),
        vmem((seq, own), BF),
        vmem((heads, seq, seq), BF),
        tokens_buf,
        vmem((2, 3, count, width), BF),
        vmem((count, width), BF),
        vmem((count, width), F32),
        vmem((count, width), F32),
        vmem((nz, ny * nh * rows, seq), BF),
        vmem((count, width), BF),
        vmem((6, 1, width), F32),
        vmem((count, width), BF),
        dma((6 + 3 * heads,)),
        dma((3, 2)), dma((3, 2)),
        dma((3, 3, 3, 2)), dma((3, 3, 3, 2)),
        dma((3, 3, 2, 2)), dma((3, 3, 2, 2)),
        dma((3, 3, 2)), dma((3, 3, 2)),
        dma((3, 2, 2)), dma((3, 2, 2)),
        dma((3 + heads, 3, 2, 3)), dma((3 + heads, 3, 2, 3)),
        dma((3 + heads, 3, 3)), dma((3 + heads, 3, 3)),
        dma((3 + heads,)), dma((3 + heads,)),
        dma((3 + heads,)), dma((3 + heads,)),
        dma((2, 2, 2, 3)), dma((2, 2, 2, 3)),
        dma((4, 3)), dma((4, 3)),
        dma((4, 3)), dma((4, 3)),
    ]
    spec = pl.BlockSpec(memory_space=pltpu.VMEM)
    final, dx, grads = pl.pallas_call(
        functools.partial(kernel, dims),
        out_shape=(
            jax.ShapeDtypeStruct((count, width), BF),
            jax.ShapeDtypeStruct((count, width), F32),
            jax.ShapeDtypeStruct((3, rows, width), F32),
        ),
        in_specs=[pl.BlockSpec(memory_space=pl.ANY)] * 7,
        out_specs=(spec, spec, spec),
        scratch_shapes=scratch,
        compiler_params=pltpu.CompilerParams(
            collective_id=0, has_side_effects=True, vmem_limit_bytes=67043328
        ),
    )(
        tokens[0], modulation[0].transpose(1, 0, 2), w_qkv[0].transpose(1, 0, 2), w_out[0].T,
        w_in[0], w_back[0].T, out_grad[0],
    )
    final, dx, qkv, out, inner, back = pl.pallas_call(
        place,
        out_shape=(
            jax.ShapeDtypeStruct((1, count, width), BF),
            jax.ShapeDtypeStruct((1, count, width), F32),
            jax.ShapeDtypeStruct((3, rows, own), F32),
            jax.ShapeDtypeStruct((rows, own), F32),
            jax.ShapeDtypeStruct((1, rows, width), F32),
            jax.ShapeDtypeStruct((rows, width), F32),
        ),
        in_specs=[spec] * 3,
        out_specs=(spec,) * 6,
    )(final, dx, grads)
    return final, dx, qkv.transpose(1, 0, 2)[None], out.T[None], inner, back.T[None]


def solution(mesh):
    dims = (4, 4, 2)
    assert mesh.shape["fsdp"] == 32 and mesh.shape["sp"] == 4
    torus = Mesh(mesh.devices.reshape(*dims, 2, 2), AXES)
    fsdp, sp = AXES[:3], AXES[3:]
    placed = (
        P(fsdp, sp, None),
        P(fsdp, None, None, None),
        P(None, fsdp, None, sp),
        P(None, sp, fsdp),
        P(None, fsdp, sp),
        P(None, sp, fsdp),
        P(fsdp, sp, None),
    )
    return jax.shard_map(
        functools.partial(step, dims),
        mesh=torus,
        in_specs=placed,
        out_specs=(placed[0], *placed[:1], *placed[2:6]),
        check_vma=False,
    )
```

```python
import functools
import math

import jax
import jax.numpy as jnp
from jax import lax
from jax.experimental import pallas as pl
from jax.experimental.pallas import tpu as pltpu
from jax.sharding import Mesh
from jax.sharding import PartitionSpec as P

HEAD_DIM = 128
LN_EPS = 1e-06
TEMPER = 2.5
BF = jnp.bfloat16
F32 = jnp.float32
AXES = ("z", "y", "h", "l", "c")


def bf(x):
    return x.astype(BF)


def f32(x):
    return x.astype(F32)


def dot(a, b, ca=1, cb=0):
    return lax.dot_general(a, b, (((ca,), (cb,)), ((), ())), preferred_element_type=F32)


def normalize(x):
    d = x - jnp.mean(x, axis=-1, keepdims=True)
    r = lax.rsqrt(jnp.mean(d * d, axis=-1, keepdims=True) + LN_EPS)
    return d * r, r


def norm_back(n, r, e):
    return r * (e - jnp.mean(e, axis=-1, keepdims=True) - n * jnp.mean(e * n, axis=-1, keepdims=True))


def gelu_pair(u):
    k0 = math.sqrt(2.0 / math.pi)
    s = u * u
    t = jnp.tanh(k0 * u * (1.0 + 0.044715 * s))
    g = 0.5 * u * (1.0 + t)
    d = 0.5 * (1.0 + t) + 0.5 * k0 * u * (1.0 - t * t) * (1.0 + 3.0 * 0.044715 * s)
    return g, d


class copy:
    def __init__(self, src, dst, ssem, rsem, dev):
        self.src, self.rest = src, (dst, ssem, rsem, dev)

    def made(self):
        dst, ssem, rsem, dev = self.rest
        return pltpu.make_async_remote_copy(
            src_ref=self.src, dst_ref=dst, send_sem=ssem, recv_sem=rsem,
            device_id=dev, device_id_type=pl.DeviceIdType.MESH,
        )

    def start(self):
        self.made().start()

    def wait_send(self):
        self.made().wait_send()

    def wait_recv(self):
        self.made().wait_recv()


def kernel(
    dims, tok_in, mod_in, wq_in, wo_in, wi_in, wb_in, og_in, fin_out, dx_out, grads_out,
    W, G, R1A, R1B, R2A, R2B, R3, R1C, R2C, R4, R4H, A1, A2, DM, DA, GG, DU, QKV, DQKV, O, DO, PR, PS, RX, SX, MID, DX, AT,
    tok, mod, og, fin, dxin, grads, in_sem, out_sem, ags, a1r, a2r, a3r, a4r, a5r, rss, r1r, r2r, r3r, r4r, r5r, gs, gr, ss, sr,
):
    nz, ny, nh = dims
    z, y, h, l, c = (lax.axis_index(a) for a in AXES)
    ol, oc = 1 - l, 1 - c
    rows, width = wi_in.shape
    half = width // 2
    seq = QKV.shape[0]
    pair = seq // 2
    own = QKV.shape[1] // 3
    heads = own // HEAD_DIM
    slab = ny * nh * rows
    scale = TEMPER / math.sqrt(HEAD_DIM)
    q_s = 1.0 / math.sqrt(seq * nz * ny * nh)
    cols = (pl.ds(0, half), pl.ds(half, half))

    def drain(sem, moves):
        units = sum(math.prod(move.src.shape) for move in moves) // (rows * 128)
        for height in (rows, nh * rows):
            for i in range(1, nz + 1):
                for j in range(1, ny + 1):
                    n, rest = divmod(units * rows, height * i * j)
                    if rest == 0 and n <= width // 128:
                        view = W.at[0, pl.ds(0, i), pl.ds(0, j), pl.ds(0, height), pl.ds(0, n * 128)]
                        pltpu.make_async_copy(view, view, sem).wait()
                        return
        raise ValueError(units)

    def zz(k):
        return lax.rem(z + k + nz, nz)

    def yy(k):
        return lax.rem(y + k + ny, ny)

    def hh(k):
        return lax.rem(h + k + nh, nh)

    def at_rows(i):
        return pl.ds(pl.multiple_of(i * rows, 16), rows)

    core_peer = {"c": oc}
    line_peer = {"l": ol}
    pair_peer = {"h": 1 - h}
    halves = (pl.ds(0, 2), pl.ds(2, 2))

    def last(color, k):
        return {"z": zz(k)} if color == 0 else {"y": yy(k)}

    def mid_dev(color, k):
        return last(1 - color, k)

    strip = 256
    side = (width - strip) // 2
    ag_cols = ((pl.ds(0, side), pl.ds(side, side), pl.ds(2 * side, strip)),) * 2 + (cols,)
    every = slice(None)

    def slab_at(buf, color, k, at, part=every, row=every):
        return buf.at[zz(k), part, row, at] if color == 0 else buf.at[part, yy(k), row, at]

    def line_at(buf, color, k, at, row=every):
        return buf.at[z, yy(k), row, at] if color == 0 else buf.at[zz(k), y, row, at]

    def line_of(s, color):
        return color if color < 2 else s % 2

    def row_of(color):
        return every if color < 2 else at_rows(h)

    def direct(s, color):
        return s == 0 or color == 2

    def ag_pair(s, recv):
        piece = W.at[s, z, y, at_rows(1 - h if recv else h), pl.ds(0, 2 * side if s < 2 else width)]
        return copy(piece, piece, ags.at[s, 0], a1r.at[s, 0], pair_peer)

    def ag_final(s, recv):
        piece = W.at[s, :, :, at_rows(1 - h if recv else h), ag_cols[s][2]]
        return copy(piece, piece, ags.at[s, 1], a1r.at[s, 1], pair_peer)

    def ag_mid(s, color, k, which, recv):
        line = line_of(s, color)
        piece = line_at(W.at[s], line, -k if recv else 0, ag_cols[s][color], at_rows(h if which == 0 else 1 - h))
        side_of = 0 if direct(s, color) else (k - 1) // 2
        return copy(piece, piece, ags.at[s, 2 + 2 * (color // 2)], a2r.at[s, color, side_of], mid_dev(line, k))

    def ag_hop(s, color, d, recv):
        k = 1 - 2 * d
        piece = line_at(W.at[s], color, 2 if recv else -k, ag_cols[s][color], at_rows(d))
        return copy(piece, piece, ags.at[s, 2], a5r.at[s, color], mid_dev(color, k))

    def ag_last(s, color, d, j, recv):
        k, line = 1 - 2 * d, line_of(s, color)
        part = halves[d if j == 0 else 1 - d]
        piece = slab_at(W.at[s], line, -k if recv else 0, ag_cols[s][color], part, row_of(color))
        arrived = a3r.at[s, color, d] if j == 0 else a4r.at[s, color // 2]
        return copy(piece, piece, ags.at[s, 3 + color // 2], arrived, last(line, k))

    def ag_relay(s, color, d, recv):
        k, line = 1 - 2 * d, line_of(s, color)
        piece = slab_at(W.at[s], line, 2 if recv else -k, ag_cols[s][color], halves[d], row_of(color))
        return copy(piece, piece, ags.at[s, 3 + color // 2], a4r.at[s, color // 2], last(line, k))

    def ag_mid_start(s, which, colors=(0, 1)):
        if which:
            ag_pair(s, True).wait_recv()
        for k in (1, 3, 2) if direct(s, colors[0]) else (1, 3):
            for color in colors:
                ag_mid(s, color, k, which, False).start()

    def ag_hop_start(s):
        for color in (0, 1):
            for d in (0, 1):
                drain(a2r.at[s, color, d], [ag_mid(s, color, 1 + 2 * d, which, True) for which in (0, 1)])
                ag_hop(s, color, d, False).start()

    def ag_last_start(s, colors=(0, 1)):
        for color in colors:
            if direct(s, color):
                sides = (0, 1) if color < 2 else (0,)
                drain(a2r.at[s, color, 0], [ag_mid(s, color, k, which, True) for which in sides for k in (1, 2, 3)])
            else:
                drain(a5r.at[s, color], [ag_hop(s, color, d, True) for d in (0, 1)])
        for j in (0, 1):
            for color in colors:
                for d in (0, 1):
                    ag_last(s, color, d, j, False).start()

    def ag_relay_start(s, colors=(0, 1)):
        for color in colors:
            for d in (0, 1):
                ag_last(s, color, d, 0, True).wait_recv()
                ag_relay(s, color, d, False).start()

    def late(s, colors):
        return [move for color in colors for d in (0, 1)
                for move in (ag_last(s, color, d, 1, True), ag_relay(s, color, d, True))]

    def ag_final_start(s):
        drain(a4r.at[s, 1], late(s, (2,)))
        ag_final(s, False).start()

    def ag_wait(s):
        drain(a4r.at[s, 0], late(s, (0, 1)))

    def ag_sent(s):
        ag_pair(s, False).wait_send()
        middle = [ag_mid(s, color, k, which, False) for color in (0, 1) for which in (0, 1)
                  for k in ((1, 2, 3) if direct(s, 0) else (1, 3))]
        if not direct(s, 0):
            middle += [ag_hop(s, color, d, False) for color in (0, 1) for d in (0, 1)]
        drain(ags.at[s, 2], middle)

        def ends(colors):
            return [ag_last(s, color, d, j, False) for color in colors for d in (0, 1) for j in (0, 1)] + [
                ag_relay(s, color, d, False) for color in colors for d in (0, 1)]

        drain(ags.at[s, 3], ends((0, 1)))
        if s < 2:
            ag_final(s, False).wait_send()
            drain(ags.at[s, 4], [ag_mid(s, 2, k, 0, False) for k in (1, 2, 3)] + ends((2,)))

    R1 = (R1A, R1B)
    R2 = (R2A, R2B)
    full = 3 * own
    sections = 3 + heads
    parts = (G.at[0], G.at[1]) + (W.at[1],) * (1 + heads)
    slots = (2, 1) + (0,) * (1 + heads)
    lead = pl.ds(0, side)
    local_cols = [(lead, lead), (cols[0], cols[0])]
    grad_cols = [ag_cols[0], cols]
    pair_cols = [pl.ds(0, 2 * side), pl.ds(0, width)]
    third = own // 3
    for i, start in enumerate([full] + [hd * own for hd in range(heads)]):
        at = pl.ds(i * third, third)
        local_cols.append((at, at))
        grad_cols.append(tuple(pl.ds(start + j * third, third) for j in range(3)))
        pair_cols.append(pl.ds(start, 2 * third))

    spare = {2: (1, 4), 3: (1, 5), 4: (0, 4), 5: (0, 5)}

    def rs_line(s, color):
        return color if color < 2 else (0, None, 1, 1, 0, 1)[s]

    def spare_at(s):
        return pl.ds(spare[s][1] * third, third)

    def r1_at(s, color):
        if color < 2:
            return R1[color].at[slots[s], :, :, :, local_cols[s][color]]
        return R1C if s == 0 else R1[spare[s][0]].at[0, :, :, pl.ds(0, rows), spare_at(s)]

    def r2_at(s, color):
        if color < 2:
            return R2[color].at[slots[s], :, :, local_cols[s][color]]
        return R2C if s == 0 else R2[spare[s][0]].at[0, :, pl.ds(0, rows), spare_at(s)]

    def r4_at(s):
        return R4 if s == 0 else R4H.at[s - 2]

    def rs_first(s):
        src = parts[s].at[:, :, at_rows(1 - h), grad_cols[s][2]]
        return copy(src, r4_at(s), rss.at[s, 5], r4r.at[s], pair_peer)

    def rs_ring(s, color, d, kind):
        k, line = 1 - 2 * d, rs_line(s, color)
        part = halves[1 - d if kind == 1 else d]
        src = slab_at(parts[s], line, 2 if kind == 0 else k, grad_cols[s][color], part, row_of(color))
        dst = r1_at(s, color).at[2 if kind == 0 else d, part]
        arrived = r1r.at[s, color, d if kind == 0 else 2]
        return copy(src, dst, rss.at[s, color // 2], arrived, last(line, k))

    def rs_mid(s, color, k):
        line = rs_line(s, color)
        return copy(
            line_at(parts[s], line, k, grad_cols[s][color], row_of(color)), r2_at(s, color).at[k - 1],
            rss.at[s, 2 + color // 2], r2r.at[s, color], mid_dev(line, k),
        )

    def ringed(s, color):
        return s < 2 and color < 2

    def rs_hop(s, color, d, kind):
        k = 1 - 2 * d
        row = at_rows(1 - d if kind == 1 else d)
        src = line_at(parts[s], color, 2 if kind == 0 else k, grad_cols[s][color], row)
        dst = r2_at(s, color).at[2 if kind == 0 else d, row]
        arrived = r5r.at[s, color, d if kind == 0 else 2]
        return copy(src, dst, rss.at[s, 2], arrived, mid_dev(color, k))

    def rs_hop_combine(s):
        for color in (0, 1):
            for d in (0, 1):
                rs_hop(s, color, d, 0).wait_recv()
                k = 1 - 2 * d
                at = (z, yy(k)) if color == 0 else (zz(k), y)
                at = (*at, at_rows(d), grad_cols[s][color])
                parts[s][at] = bf(f32(parts[s][at]) + f32(r2_at(s, color)[2, d * rows : (d + 1) * rows]))
                rs_hop(s, color, d, 2).start()

    def rs_pair(s):
        return copy(
            parts[s].at[z, y, at_rows(1 - h), pair_cols[s]], R3.at[slots[s], :, pair_cols[s]],
            rss.at[s, 4], r3r.at[s], pair_peer,
        )

    def rs_second(s):
        rs_first(s).wait_recv()

        @pl.loop(0, nz)
        def _(i):
            at = (i, every, at_rows(h), grad_cols[s][2])
            parts[s][at] = bf(f32(parts[s][at]) + f32(r4_at(s)[i]))

        rs_start(s, (2,))

    def rs_start(s, colors=(0, 1)):
        for kind in (0, 1):
            for color in colors:
                for d in (0, 1):
                    rs_ring(s, color, d, kind).start()

    def rs_combine(s, colors=(0, 1)):
        for color in colors:
            line = rs_line(s, color)
            for d in (0, 1):
                rs_ring(s, color, d, 0).wait_recv()
                k = 1 - 2 * d

                @pl.loop(2 * d, 2 * d + 2)
                def _(i):
                    at = (zz(k), i) if line == 0 else (i, yy(k))
                    at = (*at, row_of(color), grad_cols[s][color])
                    parts[s][at] = bf(f32(parts[s][at]) + f32(r1_at(s, color)[2, i]))

                rs_ring(s, color, d, 2).start()

    def rs_mid_start(s, colors=(0, 1)):
        for color in colors:
            line = rs_line(s, color)
            drain(r1r.at[s, color, 2], [rs_ring(s, color, d, kind) for d in (0, 1) for kind in (1, 2)])

            @pl.loop(0, 4)
            def _(i):
                at = (z, i) if line == 0 else (i, y)
                at = (*at, row_of(color), grad_cols[s][color])
                total = f32(parts[s][at])
                for d in (0, 1):
                    total = total + f32(r1_at(s, color)[d, i])
                parts[s][at] = bf(total)

            if ringed(s, color):
                for kind in (0, 1):
                    for d in (0, 1):
                        rs_hop(s, color, d, kind).start()
            else:
                for k in (1, 3, 2):
                    rs_mid(s, color, k).start()

    def rs_total(s, color):
        if ringed(s, color):
            drain(r5r.at[s, color, 2], [rs_hop(s, color, d, kind) for d in (0, 1) for kind in (1, 2)])
        else:
            drain(r2r.at[s, color], [rs_mid(s, color, k) for k in (1, 2, 3)])
        total = f32(parts[s][z, y, row_of(color), grad_cols[s][color]])
        for k in range(2 if ringed(s, color) else 3):
            total = total + f32(r2_at(s, color)[k])
        return total

    def rs_pair_start(s):
        for color in (0, 1):
            parts[s][z, y, every, grad_cols[s][color]] = bf(rs_total(s, color))
        rs_pair(s).start()

    def rs_finish(s):
        rs_pair(s).wait_recv()
        at = pair_cols[s]
        grads[slots[s], :, at] = f32(parts[s][z, y, at_rows(h), at]) + f32(R3[slots[s], :, at])

    def rs_finish_third(s):
        grads[slots[s], :, grad_cols[s][2]] = rs_total(s, 2)

    def rs_sent(s):
        for colors in ((0, 1),) if s == 1 else ((0, 1), (2,)):
            rings = [rs_ring(s, color, d, kind) for color in colors for d in (0, 1) for kind in (0, 1, 2)]
            drain(rss.at[s, colors[0] // 2], rings)
            if ringed(s, colors[0]):
                middle = [rs_hop(s, color, d, kind) for color in colors for d in (0, 1) for kind in (0, 1, 2)]
            else:
                middle = [rs_mid(s, color, k) for color in colors for k in (1, 2, 3)]
            drain(rss.at[s, 2 + colors[0] // 2], middle)
        if s != 1:
            rs_first(s).wait_send()
        rs_pair(s).wait_send()

    def g_copy(i, buf, step, recv):
        if step == 0:
            piece, dev = buf.at[l, oc if recv else c], core_peer
        elif step == 1:
            piece, dev = buf.at[ol if recv else l, c], line_peer
        else:
            piece, dev = buf.at[ol, oc if recv else c], core_peer
        return copy(piece, piece, gs.at[i], gr.at[i, step], dev)

    def gather_start(i, buf):
        g_copy(i, buf, 1, False).start()
        g_copy(i, buf, 0, False).start()

    def gather_relay(i, buf):
        g_copy(i, buf, 1, True).wait_recv()
        g_copy(i, buf, 2, False).start()

    def gather_wait(i, buf, step):
        g_copy(i, buf, step, True).wait_recv()

    def gather_sent(i, buf):
        drain(gs.at[i], [g_copy(i, buf, step, False) for step in range(3)])

    def s_copy(i, step):
        src, dev = (
            (PS.at[ol, oc], core_peer),
            (SX, line_peer),
            (PS.at[l, oc], core_peer),
        )[step]
        return copy(src, RX.at[i % 2, step], ss.at[i], sr.at[i, step], dev)

    def scatter_far(i, compute):
        compute(ol)
        s_copy(i, 0).start()
        s_copy(i, 0).wait_recv()
        SX[...] = bf(f32(PS[ol, c]) + f32(RX[i % 2, 0]))
        s_copy(i, 1).start()

    def scatter_near(i, compute):
        compute(l)
        s_copy(i, 2).start()

    def scatter_result(i):
        s_copy(i, 2).wait_recv()
        s_copy(i, 1).wait_recv()
        total = f32(PS[l, c]) + f32(RX[i % 2, 2]) + f32(RX[i % 2, 1])
        drain(ss.at[i], [s_copy(i, step) for step in range(3)])
        return total

    def pair_rows(i):
        return pl.ds(pl.multiple_of(i * pair, 128), pair)

    def back_product(left, s, lo, n):
        def compute(i):
            @pl.loop(0, nz)
            def _(b):
                w = W[s, b, :, :, pl.ds(lo, n)].reshape(slab, n)
                at = pl.ds(pl.multiple_of(b * slab, 128), slab)
                PS[i, :, :, at] = bf(dot(left(i), w, 1, 1)).reshape(2, pair // 2, slab)
        return compute

    def two(buf, i):
        return buf[i].reshape(pair, buf.shape[-1])

    def all_rows(buf, at):
        return buf[:, :, :, at].reshape(seq, -1)

    def turn(buf):
        @pl.loop(0, nz)
        def _(b):
            AT[b] = all_rows(buf, pl.ds(pl.multiple_of(b * slab, 128), slab)).T

    def grad_turned(s, right, start, stop, tile):
        @pl.loop(0, (stop - start) // tile)
        def _(t):
            at = pl.ds(pl.multiple_of(start + t * tile, 128), tile)
            value = dot(AT[...].reshape(width, seq), right(at)) * q_s
            parts[s][:, :, :, at] = bf(value).reshape(nz, ny, nh * rows, tile)

    def grad_product(s, left, right, n, lo):
        @pl.loop(0, nz)
        def _(b):
            a = all_rows(left, pl.ds(pl.multiple_of(b * slab, 128), slab)).T
            value = dot(a, right) * q_s
            parts[s][b, :, :, pl.ds(lo, n)] = bf(value).reshape(ny, nh * rows, n)

    peers = [{"z": zz(k)} for k in range(1, 4)] + [{"y": yy(k)} for k in range(1, 4)]
    peers += [pair_peer, core_peer, line_peer, {"l": ol, "c": oc}]
    barrier = pltpu.get_barrier_semaphore()
    for dev in peers:
        pl.semaphore_signal(barrier, inc=1, device_id=dev, device_id_type=pl.DeviceIdType.MESH)
    outs = [(fin, fin_out), (dxin, dx_out)] + [(grads.at[i], grads_out.at[i]) for i in range(3)]
    results = [pltpu.make_async_copy(src, dst, out_sem.at[i]) for i, (src, dst) in enumerate(outs)]
    mine = at_rows(h)
    moves = [
        (wq_in.at[i, :, pl.ds(hd * HEAD_DIM, HEAD_DIM)], W.at[0, z, y, mine, pl.ds((3 * hd + i) * HEAD_DIM, HEAD_DIM)])
        for i in range(3) for hd in range(heads)
    ]
    moves += [(wo_in, W.at[0, z, y, mine, pl.ds(3 * own, own)])]
    moves += [(wi_in, W.at[1, z, y, mine]), (wb_in, W.at[2, z, y, mine])]
    moves += [(tok_in, tok), (og_in, og), (mod_in, mod)]
    loads = [pltpu.make_async_copy(src, dst, in_sem.at[i]) for i, (src, dst) in enumerate(moves)]
    for load in loads:
        load.start()
    for load in loads:
        load.wait()
    m = [mod[i] for i in range(6)]
    n1, r1 = normalize(f32(tok[...]))
    A1[l, c] = bf(n1 * (1.0 + m[1]) + m[0])
    DM[l, c] = bf(m[5] * f32(og[...]))
    pl.semaphore_wait(barrier, len(peers))

    for s in range(3):
        ag_pair(s, False).start()
    for s in (0, 1):
        ag_mid_start(s, 0, (2,))
        ag_mid_start(s, 0)
    ag_mid_start(2, 0)
    gather_start(0, A1)
    ag_last_start(0, (2,))
    ag_mid_start(0, 1)
    ag_mid_start(1, 1)
    ag_last_start(1, (2,))
    ag_relay_start(0, (2,))
    ag_hop_start(1)
    ag_last_start(0)
    ag_relay_start(1, (2,))
    ag_final_start(0)
    gather_relay(0, A1)
    gather_start(1, DM)
    ag_relay_start(0)
    ag_mid_start(2, 1)
    ag_last_start(1)
    ag_final_start(1)
    gather_wait(0, A1, 0)
    gather_wait(0, A1, 2)

    ag_wait(0)

    @pl.loop(0, 3)
    def _(t):
        at = pl.ds(pl.multiple_of(t * own, 128), own)
        w = W[0, :, :, :, at].reshape(width, own)
        QKV[:, at] = bf(dot(A1[...].reshape(seq, width), w))

    ag_hop_start(2)

    def head(hd, i):
        return pl.ds(pl.multiple_of((3 * hd + i) * HEAD_DIM, 128), HEAD_DIM)

    def wide(hd):
        return pl.ds(pl.multiple_of(hd * HEAD_DIM, 128), HEAD_DIM)

    @pl.loop(0, heads)
    def _(hd):
        s = dot(QKV[:, head(hd, 0)], QKV[:, head(hd, 1)], 1, 1) * scale
        e = jnp.exp(s - jnp.max(s, axis=-1, keepdims=True))
        p = bf(e * (1.0 / jnp.sum(e, axis=-1, keepdims=True)))
        PR[hd] = p
        O[:, wide(hd)] = bf(dot(p, QKV[:, head(hd, 2)]))

    out_product = back_product(lambda i: O[pair_rows(i), :], 0, 3 * own, own)
    ag_final(0, True).wait_recv()
    scatter_far(0, out_product)
    scatter_near(0, out_product)
    ag_relay_start(1)
    ag_last_start(2)
    mid = f32(tok[...]) + m[2] * scatter_result(0)
    MID[...] = mid
    n2, r2 = normalize(mid)
    A2[l, c] = bf(n2 * (1.0 + m[4]) + m[3])
    gather_start(2, A2)

    tile = 256

    def hidden(i):
        @pl.loop(0, width // tile)
        def _(t):
            at = pl.ds(pl.multiple_of(t * tile, 128), tile)
            g, d = gelu_pair(dot(two(A2, i), W[1, :, :, :, at].reshape(width, tile)))
            GG[i, :, :, at] = bf(g).reshape(2, pair // 2, tile)
            DU[i, :, :, at] = bf(d).reshape(2, pair // 2, tile)

    gather_relay(1, DM)
    gather_wait(1, DM, 0)
    gather_wait(1, DM, 2)
    turn(DM)
    ag_wait(1)
    ag_final(1, True).wait_recv()
    gather_wait(2, A2, 0)
    hidden(l)
    ag_relay_start(2)
    gather_relay(2, A2)
    gather_wait(2, A2, 2)
    hidden(ol)
    for lo, hi in ((2 * side, width), (0, half), (half, 2 * side)):
        grad_turned(0, lambda at: all_rows(GG, at), lo, hi, tile)
        if lo == 2 * side:
            rs_first(0).start()
        else:
            rs_start(0, (0,) if lo == 0 else (1,))
    ag_wait(2)

    @pl.loop(0, width // tile)
    def _(t):
        at = pl.ds(pl.multiple_of(t * tile, 128), tile)
        dg = dot(DM[...].reshape(seq, width), W[2, :, :, :, at].reshape(width, tile))
        DU[:, :, :, at] = bf(f32(DU[:, :, :, at]) * dg.reshape(2, 2, pair // 2, tile))

    in_back = back_product(lambda i: two(DU, i), 1, 0, width)
    scatter_far(1, in_back)
    turn(A2)
    grad_turned(1, lambda at: all_rows(DU, at), 0, half, tile)
    rs_combine(0)
    rs_second(0)
    rs_start(1, (0,))
    grad_turned(1, lambda at: all_rows(DU, at), half, width, tile)
    rs_start(1, (1,))
    scatter_near(1, in_back)
    e2 = scatter_result(1) * (1.0 + m[4])
    n2, r2 = normalize(MID[...])
    dmid = f32(og[...]) + norm_back(n2, r2, e2)
    DX[...] = dmid
    DA[l, c] = bf(m[2] * dmid)
    gather_start(3, DA)

    ff_back = back_product(lambda i: two(GG, i), 2, 0, width)
    scatter_far(2, ff_back)
    scatter_near(2, ff_back)
    turn(A1)
    rs_combine(0, (2,))
    rs_combine(1)
    rs_mid_start(0)
    gather_relay(3, DA)
    gather_wait(3, DA, 0)
    gather_wait(3, DA, 2)

    DO[...] = bf(dot(DA[...].reshape(seq, width), W[0, :, :, :, pl.ds(3 * own, own)].reshape(width, own)))
    ag_sent(1)
    grad_product(2, DA, O[...], own, full)
    rs_first(2).start()
    rs_start(2)

    for hd in range(heads):
        do = DO[:, wide(hd)]
        p = PR[hd]
        t = f32(p) * dot(do, QKV[:, head(hd, 2)], 1, 1)
        ds = bf(scale * (t - f32(p) * jnp.sum(t, axis=-1, keepdims=True)))
        DQKV[:, head(hd, 0)] = bf(dot(ds, QKV[:, head(hd, 1)]))
        DQKV[:, head(hd, 1)] = bf(dot(ds.T, QKV[:, head(hd, 0)]))
        DQKV[:, head(hd, 2)] = bf(dot(p.T, do))
        grad_turned(3 + hd, lambda at: DQKV[:, at], hd * own, (hd + 1) * own, own)
        rs_first(3 + hd).start()
        rs_start(3 + hd)

    qkv_back = back_product(lambda i: DQKV[pair_rows(i), :], 0, 0, 3 * own)
    fin[...] = bf(MID[...] + m[5] * scatter_result(2))
    results[0].start()
    scatter_far(3, qkv_back)
    rs_hop_combine(0)
    rs_second(2)
    rs_combine(2)
    rs_mid_start(1)
    scatter_near(3, qkv_back)
    rs_combine(3)
    rs_second(3)
    rs_mid_start(0, (2,))
    rs_combine(4)
    rs_combine(2, (2,))
    rs_second(4)
    rs_combine(5)
    rs_mid_start(2)
    rs_pair_start(0)
    rs_second(5)
    rs_hop_combine(1)
    rs_combine(3, (2,))
    rs_mid_start(3)
    rs_finish_third(0)
    rs_mid_start(2, (2,))
    rs_combine(4, (2,))
    rs_mid_start(4)
    rs_mid_start(3, (2,))
    e1 = scatter_result(3) * (1.0 + m[1])
    n1, r1 = normalize(f32(tok[...]))
    dxin[...] = DX[...] + norm_back(n1, r1, e1)
    results[1].start()
    rs_pair_start(1)
    rs_combine(5, (2,))
    rs_mid_start(5)
    rs_finish(0)
    results[4].start()
    rs_pair_start(2)
    rs_mid_start(4, (2,))
    rs_pair_start(3)
    rs_mid_start(5, (2,))
    rs_pair_start(4)
    rs_pair_start(5)
    rs_finish(1)
    results[3].start()
    for s in range(2, sections):
        rs_finish_third(s)
    for s in range(2, sections):
        rs_finish(s)
    results[2].start()
    for s in range(sections):
        rs_sent(s)
    ag_sent(0)
    ag_sent(2)
    for i, buf in enumerate((A1, DM, A2, DA)):
        gather_sent(i, buf)
    for result in results:
        result.wait()


def place(fin, dx, grads, o_fin, o_dx, o_qkv, o_out, o_in, o_back, v_fin, v_dx, v_grads, sem_in, sem_out):
    own = o_out.shape[1]
    heads = own // HEAD_DIM
    sources = (
        (dx, v_dx), (grads.at[2], v_grads.at[2]), (grads.at[1], v_grads.at[1]),
        (fin, v_fin), (grads.at[0], v_grads.at[0]),
    )
    pieces = [
        (v_grads.at[0, :, pl.ds((3 * hd + i) * HEAD_DIM, HEAD_DIM)], o_qkv.at[i, :, pl.ds(hd * HEAD_DIM, HEAD_DIM)])
        for i in range(3) for hd in range(heads)
    ]
    pieces.append((v_grads.at[0, :, pl.ds(3 * own, own)], o_out))
    targets = (
        [(v_dx, o_dx.at[0])], [(v_grads.at[2], o_back)], [(v_grads.at[1], o_in.at[0])],
        [(v_fin, o_fin.at[0])], pieces,
    )
    loads = [pltpu.make_async_copy(a, b, sem_in.at[i]) for i, (a, b) in enumerate(sources)]
    for load in loads:
        load.start()
    stores = []
    for load, pairs in zip(loads, targets):
        load.wait()
        for a, b in pairs:
            store = pltpu.make_async_copy(a, b, sem_out.at[len(stores)])
            store.start()
            stores.append(store)
    for store in stores:
        store.wait()


def step(dims, tokens, modulation, w_qkv, w_out, w_in, w_back, out_grad):
    nz, ny, nh = dims
    count, width = tokens.shape[1:]
    rows, own, ff = w_qkv.shape[1], w_qkv.shape[3], w_in.shape[2]
    assert ff == width and 4 * own == width
    seq = 4 * count
    heads = own // HEAD_DIM
    big = (nz, ny, nh * rows)
    half = width // 2
    vmem = pltpu.VMEM
    dma = pltpu.SemaphoreType.DMA
    tokens_buf = vmem((2, 2, count, width), BF)
    scratch = [
        vmem((3, *big, width), BF),
        vmem((2, *big, width), BF),
        vmem((3, 3, 4, nh * rows, half), BF),
        vmem((3, 3, 4, nh * rows, half), BF),
        vmem((3, 3, nh * rows, half), BF),
        vmem((3, 3, nh * rows, half), BF),
        vmem((3, rows, width), BF),
        vmem((3, 4, rows, 256), BF),
        vmem((3, rows, 256), BF),
        vmem((nz, ny, rows, 256), BF),
        vmem((1 + heads, nz, ny, rows, own // 3), BF),
        *[tokens_buf] * 6,
        vmem((seq, 3 * own), BF),
        vmem((seq, 3 * own), BF),
        vmem((seq, own), BF),
        vmem((seq, own), BF),
        vmem((heads, seq, seq), BF),
        tokens_buf,
        vmem((2, 3, count, width), BF),
        vmem((count, width), BF),
        vmem((count, width), F32),
        vmem((count, width), F32),
        vmem((nz, ny * nh * rows, seq), BF),
        vmem((count, width), BF),
        vmem((6, 1, width), F32),
        vmem((count, width), BF),
        vmem((count, width), BF),
        vmem((count, width), F32),
        vmem((3, rows, width), F32),
        dma((6 + 3 * heads,)),
        dma((5,)),
        dma((3, 5)), dma((3, 2)), dma((3, 3, 2)), dma((3, 3, 2)), dma((3, 2)), dma((3, 2)),
        dma((3 + heads, 6)), dma((3 + heads, 3, 3)), dma((3 + heads, 3)), dma((3 + heads,)), dma((3 + heads,)),
        dma((2, 2, 3)),
        dma((4,)), dma((4, 3)), dma((4,)), dma((4, 3)),
    ]
    whole = pl.BlockSpec(memory_space=pl.ANY)
    final, dx, grads = pl.pallas_call(
        functools.partial(kernel, dims),
        out_shape=(
            jax.ShapeDtypeStruct((count, width), BF),
            jax.ShapeDtypeStruct((count, width), F32),
            jax.ShapeDtypeStruct((3, rows, width), F32),
        ),
        in_specs=[whole] * 7,
        out_specs=(whole,) * 3,
        scratch_shapes=scratch,
        compiler_params=pltpu.CompilerParams(
            collective_id=0, has_side_effects=True, vmem_limit_bytes=67043328
        ),
    )(
        tokens[0], modulation[0].transpose(1, 0, 2), w_qkv[0].transpose(1, 0, 2), w_out[0].T,
        w_in[0], w_back[0].T, out_grad[0],
    )
    final, dx, qkv, out, inner, back = pl.pallas_call(
        place,
        out_shape=(
            jax.ShapeDtypeStruct((1, count, width), BF),
            jax.ShapeDtypeStruct((1, count, width), F32),
            jax.ShapeDtypeStruct((3, rows, own), F32),
            jax.ShapeDtypeStruct((rows, own), F32),
            jax.ShapeDtypeStruct((1, rows, width), F32),
            jax.ShapeDtypeStruct((rows, width), F32),
        ),
        in_specs=[whole] * 3,
        out_specs=(whole,) * 6,
        scratch_shapes=[
            vmem((count, width), BF), vmem((count, width), F32), vmem((3, rows, width), F32),
            dma((5,)), dma((5 + 3 * heads,)),
        ],
    )(final, dx, grads)
    return final, dx, qkv.transpose(1, 0, 2)[None], out.T[None], inner, back.T[None]


def solution(mesh):
    dims = (4, 4, 2)
    assert mesh.shape["fsdp"] == 32 and mesh.shape["sp"] == 4
    torus = Mesh(mesh.devices.reshape(*dims, 2, 2), AXES)
    fsdp, sp = AXES[:3], AXES[3:]
    placed = (
        P(fsdp, sp, None),
        P(fsdp, None, None, None),
        P(None, fsdp, None, sp),
        P(None, sp, fsdp),
        P(None, fsdp, sp),
        P(None, sp, fsdp),
        P(fsdp, sp, None),
    )
    return jax.shard_map(
        functools.partial(step, dims),
        mesh=torus,
        in_specs=placed,
        out_specs=(placed[0], *placed[:1], *placed[2:6]),
        check_vma=False,
    )
```

```python
import functools
import math

import jax
import jax.numpy as jnp
from jax import lax
from jax.experimental import pallas as pl
from jax.experimental.pallas import tpu as pltpu
from jax.sharding import Mesh
from jax.sharding import PartitionSpec as P

HEAD_DIM = 128
LN_EPS = 1e-06
TEMPER = 2.5
BF = jnp.bfloat16
F32 = jnp.float32
AXES = ("z", "y", "h", "l", "c")


def bf(x):
    return x.astype(BF)


def f32(x):
    return x.astype(F32)


def dot(a, b, ca=1, cb=0):
    return lax.dot_general(a, b, (((ca,), (cb,)), ((), ())), preferred_element_type=F32)


def normalize(x):
    d = x - jnp.mean(x, axis=-1, keepdims=True)
    r = lax.rsqrt(jnp.mean(d * d, axis=-1, keepdims=True) + LN_EPS)
    return d * r, r


def norm_back(n, r, e):
    return r * (e - jnp.mean(e, axis=-1, keepdims=True) - n * jnp.mean(e * n, axis=-1, keepdims=True))


def gelu_pair(u):
    k0 = math.sqrt(2.0 / math.pi)
    s = u * u
    t = jnp.tanh(k0 * u * (1.0 + 0.044715 * s))
    g = 0.5 * u * (1.0 + t)
    d = 0.5 * (1.0 + t) + 0.5 * k0 * u * (1.0 - t * t) * (1.0 + 3.0 * 0.044715 * s)
    return g, d


class copy:
    def __init__(self, src, dst, ssem, rsem, dev):
        self.src, self.rest = src, (dst, ssem, rsem, dev)

    def made(self):
        dst, ssem, rsem, dev = self.rest
        return pltpu.make_async_remote_copy(
            src_ref=self.src, dst_ref=dst, send_sem=ssem, recv_sem=rsem,
            device_id=dev, device_id_type=pl.DeviceIdType.MESH,
        )

    def start(self):
        self.made().start()

    def wait_send(self):
        self.made().wait_send()

    def wait_recv(self):
        self.made().wait_recv()


def kernel(
    dims, tok_in, mod_in, wq_in, wo_in, wi_in, wb_in, og_in, fin_out, dx_out, grads_out,
    W, G, R1A, R1B, R2A, R2B, R3, R1C, R2C, R4, R4H, A1, A2, DM, DA, GG, DU, QKV, DQKV, O, DO, PR, PS, RX, SX, MID, DX, AT,
    tok, mod, og, fin, dxin, grads, in_sem, out_sem, ags, a1r, a2r, a3r, a4r, a5r, rss, r1r, r2r, r3r, r4r, r5r, gs, gr, ss, sr,
):
    nz, ny, nh = dims
    z, y, h, l, c = (lax.axis_index(a) for a in AXES)
    ol, oc = 1 - l, 1 - c
    rows, width = wi_in.shape
    half = width // 2
    seq = QKV.shape[0]
    pair = seq // 2
    own = QKV.shape[1] // 3
    heads = own // HEAD_DIM
    slab = ny * nh * rows
    scale = TEMPER / math.sqrt(HEAD_DIM)
    q_s = 1.0 / math.sqrt(seq * nz * ny * nh)
    cols = (pl.ds(0, half), pl.ds(half, half))

    def drain(sem, moves):
        units = sum(math.prod(move.src.shape) for move in moves) // (rows * 128)
        for height in (rows, nh * rows):
            for i in range(1, nz + 1):
                for j in range(1, ny + 1):
                    n, rest = divmod(units * rows, height * i * j)
                    if rest == 0 and n <= width // 128:
                        view = W.at[0, pl.ds(0, i), pl.ds(0, j), pl.ds(0, height), pl.ds(0, n * 128)]
                        pltpu.make_async_copy(view, view, sem).wait()
                        return
        raise ValueError(units)

    def zz(k):
        return lax.rem(z + k + nz, nz)

    def yy(k):
        return lax.rem(y + k + ny, ny)

    def hh(k):
        return lax.rem(h + k + nh, nh)

    def at_rows(i):
        return pl.ds(pl.multiple_of(i * rows, 16), rows)

    core_peer = {"c": oc}
    line_peer = {"l": ol}
    pair_peer = {"h": 1 - h}
    halves = (pl.ds(0, 2), pl.ds(2, 2))

    def last(color, k):
        return {"z": zz(k)} if color == 0 else {"y": yy(k)}

    def mid_dev(color, k):
        return last(1 - color, k)

    strip = 256
    side = (width - strip) // 2
    ag_cols = ((pl.ds(0, side), pl.ds(side, side), pl.ds(2 * side, strip)),) * 2 + (cols,)
    every = slice(None)

    def slab_at(buf, color, k, at, part=every, row=every):
        return buf.at[zz(k), part, row, at] if color == 0 else buf.at[part, yy(k), row, at]

    def line_at(buf, color, k, at, row=every):
        return buf.at[z, yy(k), row, at] if color == 0 else buf.at[zz(k), y, row, at]

    def line_of(s, color):
        return color if color < 2 else s % 2

    def row_of(color):
        return every if color < 2 else at_rows(h)

    def direct(s, color):
        return s == 0 or color == 2

    def ag_pair(s, recv):
        piece = W.at[s, z, y, at_rows(1 - h if recv else h), pl.ds(0, 2 * side if s < 2 else width)]
        return copy(piece, piece, ags.at[s, 0], a1r.at[s, 0], pair_peer)

    def ag_final(s, recv):
        piece = W.at[s, :, :, at_rows(1 - h if recv else h), ag_cols[s][2]]
        return copy(piece, piece, ags.at[s, 1], a1r.at[s, 1], pair_peer)

    def ag_mid(s, color, k, which, recv):
        line = line_of(s, color)
        piece = line_at(W.at[s], line, -k if recv else 0, ag_cols[s][color], at_rows(h if which == 0 else 1 - h))
        side_of = 0 if direct(s, color) else (k - 1) // 2
        return copy(piece, piece, ags.at[s, 2 + 2 * (color // 2)], a2r.at[s, color, side_of], mid_dev(line, k))

    def ag_hop(s, color, d, recv):
        k = 1 - 2 * d
        piece = line_at(W.at[s], color, 2 if recv else -k, ag_cols[s][color], at_rows(d))
        return copy(piece, piece, ags.at[s, 2], a5r.at[s, color], mid_dev(color, k))

    def ag_last(s, color, d, j, recv):
        k, line = 1 - 2 * d, line_of(s, color)
        part = halves[d if j == 0 else 1 - d]
        piece = slab_at(W.at[s], line, -k if recv else 0, ag_cols[s][color], part, row_of(color))
        arrived = a3r.at[s, color, d] if j == 0 else a4r.at[s, color // 2]
        return copy(piece, piece, ags.at[s, 3 + color // 2], arrived, last(line, k))

    def ag_relay(s, color, d, recv):
        k, line = 1 - 2 * d, line_of(s, color)
        piece = slab_at(W.at[s], line, 2 if recv else -k, ag_cols[s][color], halves[d], row_of(color))
        return copy(piece, piece, ags.at[s, 3 + color // 2], a4r.at[s, color // 2], last(line, k))

    def ag_mid_start(s, which, colors=(0, 1)):
        if which:
            ag_pair(s, True).wait_recv()
        for k in (1, 3, 2) if direct(s, colors[0]) else (1, 3):
            for color in colors:
                ag_mid(s, color, k, which, False).start()

    def ag_hop_start(s):
        for color in (0, 1):
            for d in (0, 1):
                drain(a2r.at[s, color, d], [ag_mid(s, color, 1 + 2 * d, which, True) for which in (0, 1)])
                ag_hop(s, color, d, False).start()

    def ag_last_start(s, colors=(0, 1)):
        for color in colors:
            if direct(s, color):
                sides = (0, 1) if color < 2 else (0,)
                drain(a2r.at[s, color, 0], [ag_mid(s, color, k, which, True) for which in sides for k in (1, 2, 3)])
            else:
                drain(a5r.at[s, color], [ag_hop(s, color, d, True) for d in (0, 1)])
        for j in (0, 1):
            for color in colors:
                for d in (0, 1):
                    ag_last(s, color, d, j, False).start()

    def ag_relay_start(s, colors=(0, 1)):
        for color in colors:
            for d in (0, 1):
                ag_last(s, color, d, 0, True).wait_recv()
                ag_relay(s, color, d, False).start()

    def late(s, colors):
        return [move for color in colors for d in (0, 1)
                for move in (ag_last(s, color, d, 1, True), ag_relay(s, color, d, True))]

    def ag_final_start(s):
        drain(a4r.at[s, 1], late(s, (2,)))
        ag_final(s, False).start()

    def ag_wait(s):
        drain(a4r.at[s, 0], late(s, (0, 1)))

    def ag_sent(s):
        ag_pair(s, False).wait_send()
        middle = [ag_mid(s, color, k, which, False) for color in (0, 1) for which in (0, 1)
                  for k in ((1, 2, 3) if direct(s, 0) else (1, 3))]
        if not direct(s, 0):
            middle += [ag_hop(s, color, d, False) for color in (0, 1) for d in (0, 1)]
        drain(ags.at[s, 2], middle)

        def ends(colors):
            return [ag_last(s, color, d, j, False) for color in colors for d in (0, 1) for j in (0, 1)] + [
                ag_relay(s, color, d, False) for color in colors for d in (0, 1)]

        drain(ags.at[s, 3], ends((0, 1)))
        if s < 2:
            ag_final(s, False).wait_send()
            drain(ags.at[s, 4], [ag_mid(s, 2, k, 0, False) for k in (1, 2, 3)] + ends((2,)))

    R1 = (R1A, R1B)
    R2 = (R2A, R2B)
    full = 3 * own
    sections = 3 + heads
    parts = (G.at[0], G.at[1]) + (W.at[1],) * (1 + heads)
    slots = (2, 1) + (0,) * (1 + heads)
    lead = pl.ds(0, side)
    local_cols = [(lead, lead), (cols[0], cols[0])]
    grad_cols = [ag_cols[0], cols]
    pair_cols = [pl.ds(0, 2 * side), pl.ds(0, width)]
    third = own // 3
    for i, start in enumerate([full] + [hd * own for hd in range(heads)]):
        at = pl.ds(i * third, third)
        local_cols.append((at, at))
        grad_cols.append(tuple(pl.ds(start + j * third, third) for j in range(3)))
        pair_cols.append(pl.ds(start, 2 * third))

    spare = {2: (1, 4), 3: (1, 5), 4: (0, 4), 5: (0, 5)}

    def rs_line(s, color):
        return color if color < 2 else (0, None, 1, 1, 0, 1)[s]

    def spare_at(s):
        return pl.ds(spare[s][1] * third, third)

    def r1_at(s, color):
        if color < 2:
            return R1[color].at[slots[s], :, :, :, local_cols[s][color]]
        return R1C if s == 0 else R1[spare[s][0]].at[0, :, :, pl.ds(0, rows), spare_at(s)]

    def r2_at(s, color):
        if color < 2:
            return R2[color].at[slots[s], :, :, local_cols[s][color]]
        return R2C if s == 0 else R2[spare[s][0]].at[0, :, pl.ds(0, rows), spare_at(s)]

    def r4_at(s):
        return R4 if s == 0 else R4H.at[s - 2]

    def rs_first(s):
        src = parts[s].at[:, :, at_rows(1 - h), grad_cols[s][2]]
        return copy(src, r4_at(s), rss.at[s, 5], r4r.at[s], pair_peer)

    def rs_ring(s, color, d, kind):
        k, line = 1 - 2 * d, rs_line(s, color)
        part = halves[1 - d if kind == 1 else d]
        src = slab_at(parts[s], line, 2 if kind == 0 else k, grad_cols[s][color], part, row_of(color))
        dst = r1_at(s, color).at[2 if kind == 0 else d, part]
        arrived = r1r.at[s, color, d if kind == 0 else 2]
        return copy(src, dst, rss.at[s, color // 2], arrived, last(line, k))

    def rs_mid(s, color, k):
        line = rs_line(s, color)
        return copy(
            line_at(parts[s], line, k, grad_cols[s][color], row_of(color)), r2_at(s, color).at[k - 1],
            rss.at[s, 2 + color // 2], r2r.at[s, color], mid_dev(line, k),
        )

    def ringed(s, color):
        return s < 2 and color < 2

    def rs_hop(s, color, d, kind):
        k = 1 - 2 * d
        row = at_rows(1 - d if kind == 1 else d)
        src = line_at(parts[s], color, 2 if kind == 0 else k, grad_cols[s][color], row)
        dst = r2_at(s, color).at[2 if kind == 0 else d, row]
        arrived = r5r.at[s, color, d if kind == 0 else 2]
        return copy(src, dst, rss.at[s, 2], arrived, mid_dev(color, k))

    def rs_hop_combine(s):
        for color in (0, 1):
            for d in (0, 1):
                rs_hop(s, color, d, 0).wait_recv()
                k = 1 - 2 * d
                at = (z, yy(k)) if color == 0 else (zz(k), y)
                at = (*at, at_rows(d), grad_cols[s][color])
                parts[s][at] = bf(f32(parts[s][at]) + f32(r2_at(s, color)[2, d * rows : (d + 1) * rows]))
                rs_hop(s, color, d, 2).start()

    def rs_pair(s):
        return copy(
            parts[s].at[z, y, at_rows(1 - h), pair_cols[s]], R3.at[slots[s], :, pair_cols[s]],
            rss.at[s, 4], r3r.at[s], pair_peer,
        )

    def rs_second(s):
        rs_first(s).wait_recv()

        @pl.loop(0, nz)
        def _(i):
            at = (i, every, at_rows(h), grad_cols[s][2])
            parts[s][at] = bf(f32(parts[s][at]) + f32(r4_at(s)[i]))

        rs_start(s, (2,))

    def rs_start(s, colors=(0, 1)):
        for kind in (0, 1):
            for color in colors:
                for d in (0, 1):
                    rs_ring(s, color, d, kind).start()

    def rs_combine(s, colors=(0, 1)):
        for color in colors:
            line = rs_line(s, color)
            for d in (0, 1):
                rs_ring(s, color, d, 0).wait_recv()
                k = 1 - 2 * d

                @pl.loop(2 * d, 2 * d + 2)
                def _(i):
                    at = (zz(k), i) if line == 0 else (i, yy(k))
                    at = (*at, row_of(color), grad_cols[s][color])
                    parts[s][at] = bf(f32(parts[s][at]) + f32(r1_at(s, color)[2, i]))

                rs_ring(s, color, d, 2).start()

    def rs_mid_start(s, colors=(0, 1)):
        for color in colors:
            line = rs_line(s, color)
            drain(r1r.at[s, color, 2], [rs_ring(s, color, d, kind) for d in (0, 1) for kind in (1, 2)])

            @pl.loop(0, 4)
            def _(i):
                at = (z, i) if line == 0 else (i, y)
                at = (*at, row_of(color), grad_cols[s][color])
                total = f32(parts[s][at])
                for d in (0, 1):
                    total = total + f32(r1_at(s, color)[d, i])
                parts[s][at] = bf(total)

            if ringed(s, color):
                for kind in (0, 1):
                    for d in (0, 1):
                        rs_hop(s, color, d, kind).start()
            else:
                for k in (1, 3, 2):
                    rs_mid(s, color, k).start()

    def rs_total(s, color):
        if ringed(s, color):
            drain(r5r.at[s, color, 2], [rs_hop(s, color, d, kind) for d in (0, 1) for kind in (1, 2)])
        else:
            drain(r2r.at[s, color], [rs_mid(s, color, k) for k in (1, 2, 3)])
        total = f32(parts[s][z, y, row_of(color), grad_cols[s][color]])
        for k in range(2 if ringed(s, color) else 3):
            total = total + f32(r2_at(s, color)[k])
        return total

    def rs_pair_start(s):
        for color in (0, 1):
            parts[s][z, y, every, grad_cols[s][color]] = bf(rs_total(s, color))
        rs_pair(s).start()

    def rs_finish(s):
        rs_pair(s).wait_recv()
        at = pair_cols[s]
        grads[slots[s], :, at] = f32(parts[s][z, y, at_rows(h), at]) + f32(R3[slots[s], :, at])

    def rs_finish_third(s):
        grads[slots[s], :, grad_cols[s][2]] = rs_total(s, 2)

    def rs_sent(s):
        for colors in ((0, 1),) if s == 1 else ((0, 1), (2,)):
            rings = [rs_ring(s, color, d, kind) for color in colors for d in (0, 1) for kind in (0, 1, 2)]
            drain(rss.at[s, colors[0] // 2], rings)
            if ringed(s, colors[0]):
                middle = [rs_hop(s, color, d, kind) for color in colors for d in (0, 1) for kind in (0, 1, 2)]
            else:
                middle = [rs_mid(s, color, k) for color in colors for k in (1, 2, 3)]
            drain(rss.at[s, 2 + colors[0] // 2], middle)
        if s != 1:
            rs_first(s).wait_send()
        rs_pair(s).wait_send()

    def g_copy(i, buf, step, recv):
        if step == 0:
            piece, dev = buf.at[l, oc if recv else c], core_peer
        elif step == 1:
            piece, dev = buf.at[ol if recv else l, c], line_peer
        else:
            piece, dev = buf.at[ol, oc if recv else c], core_peer
        return copy(piece, piece, gs.at[i], gr.at[i, step], dev)

    def gather_start(i, buf):
        g_copy(i, buf, 1, False).start()
        g_copy(i, buf, 0, False).start()

    def gather_relay(i, buf):
        g_copy(i, buf, 1, True).wait_recv()
        g_copy(i, buf, 2, False).start()

    def gather_wait(i, buf, step):
        g_copy(i, buf, step, True).wait_recv()

    def gather_sent(i, buf):
        drain(gs.at[i], [g_copy(i, buf, step, False) for step in range(3)])

    def s_copy(i, step):
        src, dev = (
            (PS.at[ol, oc], core_peer),
            (SX, line_peer),
            (PS.at[l, oc], core_peer),
        )[step]
        return copy(src, RX.at[i % 2, step], ss.at[i], sr.at[i, step], dev)

    def scatter_far(i, compute):
        compute(ol)
        s_copy(i, 0).start()
        s_copy(i, 0).wait_recv()
        SX[...] = bf(f32(PS[ol, c]) + f32(RX[i % 2, 0]))
        s_copy(i, 1).start()

    def scatter_near(i, compute):
        compute(l)
        s_copy(i, 2).start()

    def scatter_result(i):
        s_copy(i, 2).wait_recv()
        s_copy(i, 1).wait_recv()
        total = f32(PS[l, c]) + f32(RX[i % 2, 2]) + f32(RX[i % 2, 1])
        drain(ss.at[i], [s_copy(i, step) for step in range(3)])
        return total

    def pair_rows(i):
        return pl.ds(pl.multiple_of(i * pair, 128), pair)

    def back_product(left, s, lo, n):
        def compute(i):
            @pl.loop(0, nz)
            def _(b):
                w = W[s, b, :, :, pl.ds(lo, n)].reshape(slab, n)
                at = pl.ds(pl.multiple_of(b * slab, 128), slab)
                PS[i, :, :, at] = bf(dot(left(i), w, 1, 1)).reshape(2, pair // 2, slab)
        return compute

    def two(buf, i):
        return buf[i].reshape(pair, buf.shape[-1])

    def all_rows(buf, at):
        return buf[:, :, :, at].reshape(seq, -1)

    def turn(buf):
        @pl.loop(0, nz)
        def _(b):
            AT[b] = all_rows(buf, pl.ds(pl.multiple_of(b * slab, 128), slab)).T

    def grad_turned(s, right, start, stop, tile):
        @pl.loop(0, (stop - start) // tile)
        def _(t):
            at = pl.ds(pl.multiple_of(start + t * tile, 128), tile)
            value = dot(AT[...].reshape(width, seq), right(at)) * q_s
            parts[s][:, :, :, at] = bf(value).reshape(nz, ny, nh * rows, tile)

    def grad_product(s, left, right, n, lo):
        @pl.loop(0, nz)
        def _(b):
            a = all_rows(left, pl.ds(pl.multiple_of(b * slab, 128), slab)).T
            value = dot(a, right) * q_s
            parts[s][b, :, :, pl.ds(lo, n)] = bf(value).reshape(ny, nh * rows, n)

    peers = [{"z": zz(k)} for k in range(1, 4)] + [{"y": yy(k)} for k in range(1, 4)]
    peers += [pair_peer, core_peer, line_peer, {"l": ol, "c": oc}]
    barrier = pltpu.get_barrier_semaphore()
    for dev in peers:
        pl.semaphore_signal(barrier, inc=1, device_id=dev, device_id_type=pl.DeviceIdType.MESH)
    outs = [(fin, fin_out), (dxin, dx_out)] + [(grads.at[i], grads_out.at[i]) for i in range(3)]
    results = [pltpu.make_async_copy(src, dst, out_sem.at[i]) for i, (src, dst) in enumerate(outs)]
    mine = at_rows(h)
    moves = [
        (wq_in.at[i, :, pl.ds(hd * HEAD_DIM, HEAD_DIM)], W.at[0, z, y, mine, pl.ds((3 * hd + i) * HEAD_DIM, HEAD_DIM)])
        for i in range(3) for hd in range(heads)
    ]
    moves += [(wo_in, W.at[0, z, y, mine, pl.ds(3 * own, own)])]
    moves += [(wi_in, W.at[1, z, y, mine]), (wb_in, W.at[2, z, y, mine])]
    moves += [(tok_in, tok), (og_in, og), (mod_in, mod)]
    loads = [pltpu.make_async_copy(src, dst, in_sem.at[i]) for i, (src, dst) in enumerate(moves)]
    for load in loads:
        load.start()
    for load in loads:
        load.wait()
    m = [mod[i] for i in range(6)]
    n1, r1 = normalize(f32(tok[...]))
    A1[l, c] = bf(n1 * (1.0 + m[1]) + m[0])
    DM[l, c] = bf(m[5] * f32(og[...]))
    pl.semaphore_wait(barrier, len(peers))

    for s in range(3):
        ag_pair(s, False).start()
    for s in (0, 1):
        ag_mid_start(s, 0, (2,))
        ag_mid_start(s, 0)
    gather_start(0, A1)
    ag_last_start(0, (2,))
    ag_mid_start(0, 1)
    ag_mid_start(1, 1)
    ag_last_start(1, (2,))
    ag_relay_start(0, (2,))
    ag_hop_start(1)
    ag_last_start(0)
    ag_relay_start(1, (2,))
    ag_final_start(0)
    gather_relay(0, A1)
    gather_start(1, DM)
    ag_relay_start(0)
    ag_mid_start(2, 0)
    ag_mid_start(2, 1)
    ag_last_start(1)
    ag_final_start(1)
    gather_wait(0, A1, 0)
    gather_wait(0, A1, 2)

    ag_wait(0)

    @pl.loop(0, 3)
    def _(t):
        at = pl.ds(pl.multiple_of(t * own, 128), own)
        w = W[0, :, :, :, at].reshape(width, own)
        QKV[:, at] = bf(dot(A1[...].reshape(seq, width), w))

    ag_hop_start(2)

    def head(hd, i):
        return pl.ds(pl.multiple_of((3 * hd + i) * HEAD_DIM, 128), HEAD_DIM)

    def wide(hd):
        return pl.ds(pl.multiple_of(hd * HEAD_DIM, 128), HEAD_DIM)

    @pl.loop(0, heads)
    def _(hd):
        s = dot(QKV[:, head(hd, 0)], QKV[:, head(hd, 1)], 1, 1) * scale
        e = jnp.exp(s - jnp.max(s, axis=-1, keepdims=True))
        p = bf(e * (1.0 / jnp.sum(e, axis=-1, keepdims=True)))
        PR[hd] = p
        O[:, wide(hd)] = bf(dot(p, QKV[:, head(hd, 2)]))

    out_product = back_product(lambda i: O[pair_rows(i), :], 0, 3 * own, own)
    ag_final(0, True).wait_recv()
    scatter_far(0, out_product)
    scatter_near(0, out_product)
    ag_relay_start(1)
    ag_last_start(2)
    mid = f32(tok[...]) + m[2] * scatter_result(0)
    MID[...] = mid
    n2, r2 = normalize(mid)
    A2[l, c] = bf(n2 * (1.0 + m[4]) + m[3])
    gather_start(2, A2)

    tile = 256

    def hidden(i):
        @pl.loop(0, width // (2 * tile))
        def _(t):
            for j in (0, 1):
                at = pl.ds(pl.multiple_of((2 * t + j) * tile, 128), tile)
                g, d = gelu_pair(dot(two(A2, i), W[1, :, :, :, at].reshape(width, tile)))
                GG[i, :, :, at] = bf(g).reshape(2, pair // 2, tile)
                DU[i, :, :, at] = bf(d).reshape(2, pair // 2, tile)

    gather_relay(1, DM)
    gather_wait(1, DM, 0)
    gather_wait(1, DM, 2)
    turn(DM)
    ag_wait(1)
    ag_final(1, True).wait_recv()
    gather_wait(2, A2, 0)
    hidden(l)
    ag_relay_start(2)
    gather_relay(2, A2)
    gather_wait(2, A2, 2)
    hidden(ol)
    for lo, hi in ((2 * side, width), (0, half), (half, 2 * side)):
        grad_turned(0, lambda at: all_rows(GG, at), lo, hi, tile)
        if lo == 2 * side:
            rs_first(0).start()
        else:
            rs_start(0, (0,) if lo == 0 else (1,))
    ag_wait(2)

    @pl.loop(0, width // tile)
    def _(t):
        at = pl.ds(pl.multiple_of(t * tile, 128), tile)
        dg = dot(DM[...].reshape(seq, width), W[2, :, :, :, at].reshape(width, tile))
        DU[:, :, :, at] = bf(f32(DU[:, :, :, at]) * dg.reshape(2, 2, pair // 2, tile))

    in_back = back_product(lambda i: two(DU, i), 1, 0, width)
    scatter_far(1, in_back)
    turn(A2)
    grad_turned(1, lambda at: all_rows(DU, at), 0, half, tile)
    rs_combine(0)
    rs_second(0)
    rs_start(1, (0,))
    grad_turned(1, lambda at: all_rows(DU, at), half, width, tile)
    rs_start(1, (1,))
    scatter_near(1, in_back)
    e2 = scatter_result(1) * (1.0 + m[4])
    n2, r2 = normalize(MID[...])
    dmid = f32(og[...]) + norm_back(n2, r2, e2)
    DX[...] = dmid
    DA[l, c] = bf(m[2] * dmid)
    gather_start(3, DA)

    ff_back = back_product(lambda i: two(GG, i), 2, 0, width)
    scatter_far(2, ff_back)
    scatter_near(2, ff_back)
    turn(A1)
    rs_combine(0, (2,))
    rs_combine(1)
    rs_mid_start(0)
    gather_relay(3, DA)
    gather_wait(3, DA, 0)
    gather_wait(3, DA, 2)

    DO[...] = bf(dot(DA[...].reshape(seq, width), W[0, :, :, :, pl.ds(3 * own, own)].reshape(width, own)))
    ag_sent(1)
    grad_product(2, DA, O[...], own, full)
    rs_first(2).start()
    rs_start(2)

    for hd in range(heads):
        do = DO[:, wide(hd)]
        p = PR[hd]
        t = f32(p) * dot(do, QKV[:, head(hd, 2)], 1, 1)
        ds = bf(scale * (t - f32(p) * jnp.sum(t, axis=-1, keepdims=True)))
        DQKV[:, head(hd, 0)] = bf(dot(ds, QKV[:, head(hd, 1)]))
        DQKV[:, head(hd, 1)] = bf(dot(ds.T, QKV[:, head(hd, 0)]))
        DQKV[:, head(hd, 2)] = bf(dot(p.T, do))
        grad_turned(3 + hd, lambda at: DQKV[:, at], hd * own, (hd + 1) * own, own)
        rs_first(3 + hd).start()
        rs_start(3 + hd)

    qkv_back = back_product(lambda i: DQKV[pair_rows(i), :], 0, 0, 3 * own)
    fin[...] = bf(MID[...] + m[5] * scatter_result(2))
    results[0].start()
    rs_hop_combine(0)
    rs_combine(2)
    rs_mid_start(1)
    rs_combine(3)
    qkv_back = back_product(lambda i: DQKV[pair_rows(i), :], 0, 0, 3 * own)
    scatter_far(3, qkv_back)
    rs_second(2)
    rs_combine(4)
    scatter_near(3, qkv_back)
    rs_second(3)
    rs_mid_start(0, (2,))
    rs_pair_start(0)
    rs_combine(5)
    rs_mid_start(2)
    rs_combine(2, (2,))
    rs_second(4)
    rs_mid_start(3)
    rs_combine(3, (2,))
    rs_hop_combine(1)
    rs_mid_start(4)
    rs_mid_start(2, (2,))
    rs_second(5)
    rs_combine(4, (2,))
    rs_mid_start(3, (2,))
    rs_mid_start(5)
    rs_pair_start(2)
    rs_pair_start(1)
    rs_finish_third(0)
    rs_combine(5, (2,))
    rs_mid_start(4, (2,))
    rs_pair_start(3)
    rs_finish(0)
    results[4].start()
    e1 = scatter_result(3) * (1.0 + m[1])
    n1, r1 = normalize(f32(tok[...]))
    dxin[...] = DX[...] + norm_back(n1, r1, e1)
    results[1].start()
    rs_pair_start(4)
    rs_mid_start(5, (2,))
    rs_pair_start(5)
    rs_finish(1)
    results[3].start()
    for s in range(2, sections):
        rs_finish_third(s)
    for s in range(2, sections):
        rs_finish(s)
    results[2].start()
    for s in range(sections):
        rs_sent(s)
    ag_sent(0)
    ag_sent(2)
    for i, buf in enumerate((A1, DM, A2, DA)):
        gather_sent(i, buf)
    for result in results:
        result.wait()


def place(fin, dx, grads, o_fin, o_dx, o_qkv, o_out, o_in, o_back, v_fin, v_dx, v_grads, sem_in, sem_out):
    own = o_out.shape[1]
    heads = own // HEAD_DIM
    sources = (
        (dx, v_dx), (grads.at[2], v_grads.at[2]), (grads.at[1], v_grads.at[1]),
        (fin, v_fin), (grads.at[0], v_grads.at[0]),
    )
    pieces = [
        (v_grads.at[0, :, pl.ds((3 * hd + i) * HEAD_DIM, HEAD_DIM)], o_qkv.at[i, :, pl.ds(hd * HEAD_DIM, HEAD_DIM)])
        for i in range(3) for hd in range(heads)
    ]
    pieces.append((v_grads.at[0, :, pl.ds(3 * own, own)], o_out))
    targets = (
        [(v_dx, o_dx.at[0])], [(v_grads.at[2], o_back)], [(v_grads.at[1], o_in.at[0])],
        [(v_fin, o_fin.at[0])], pieces,
    )
    loads = [pltpu.make_async_copy(a, b, sem_in.at[i]) for i, (a, b) in enumerate(sources)]
    for load in loads:
        load.start()
    stores = []
    for load, pairs in zip(loads, targets):
        load.wait()
        for a, b in pairs:
            store = pltpu.make_async_copy(a, b, sem_out.at[len(stores)])
            store.start()
            stores.append(store)
    for store in stores:
        store.wait()


def step(dims, tokens, modulation, w_qkv, w_out, w_in, w_back, out_grad):
    nz, ny, nh = dims
    count, width = tokens.shape[1:]
    rows, own, ff = w_qkv.shape[1], w_qkv.shape[3], w_in.shape[2]
    assert ff == width and 4 * own == width
    seq = 4 * count
    heads = own // HEAD_DIM
    big = (nz, ny, nh * rows)
    half = width // 2
    vmem = pltpu.VMEM
    dma = pltpu.SemaphoreType.DMA
    tokens_buf = vmem((2, 2, count, width), BF)
    scratch = [
        vmem((3, *big, width), BF),
        vmem((2, *big, width), BF),
        vmem((3, 3, 4, nh * rows, half), BF),
        vmem((3, 3, 4, nh * rows, half), BF),
        vmem((3, 3, nh * rows, half), BF),
        vmem((3, 3, nh * rows, half), BF),
        vmem((3, rows, width), BF),
        vmem((3, 4, rows, 256), BF),
        vmem((3, rows, 256), BF),
        vmem((nz, ny, rows, 256), BF),
        vmem((1 + heads, nz, ny, rows, own // 3), BF),
        *[tokens_buf] * 6,
        vmem((seq, 3 * own), BF),
        vmem((seq, 3 * own), BF),
        vmem((seq, own), BF),
        vmem((seq, own), BF),
        vmem((heads, seq, seq), BF),
        tokens_buf,
        vmem((2, 3, count, width), BF),
        vmem((count, width), BF),
        vmem((count, width), F32),
        vmem((count, width), F32),
        vmem((nz, ny * nh * rows, seq), BF),
        vmem((count, width), BF),
        vmem((6, 1, width), F32),
        vmem((count, width), BF),
        vmem((count, width), BF),
        vmem((count, width), F32),
        vmem((3, rows, width), F32),
        dma((6 + 3 * heads,)),
        dma((5,)),
        dma((3, 5)), dma((3, 2)), dma((3, 3, 2)), dma((3, 3, 2)), dma((3, 2)), dma((3, 2)),
        dma((3 + heads, 6)), dma((3 + heads, 3, 3)), dma((3 + heads, 3)), dma((3 + heads,)), dma((3 + heads,)),
        dma((2, 2, 3)),
        dma((4,)), dma((4, 3)), dma((4,)), dma((4, 3)),
    ]
    whole = pl.BlockSpec(memory_space=pl.ANY)
    final, dx, grads = pl.pallas_call(
        functools.partial(kernel, dims),
        out_shape=(
            jax.ShapeDtypeStruct((count, width), BF),
            jax.ShapeDtypeStruct((count, width), F32),
            jax.ShapeDtypeStruct((3, rows, width), F32),
        ),
        in_specs=[whole] * 7,
        out_specs=(whole,) * 3,
        scratch_shapes=scratch,
        compiler_params=pltpu.CompilerParams(
            collective_id=0, has_side_effects=True, vmem_limit_bytes=67043328
        ),
    )(
        tokens[0], modulation[0].transpose(1, 0, 2), w_qkv[0].transpose(1, 0, 2), w_out[0].T,
        w_in[0], w_back[0].T, out_grad[0],
    )
    final, dx, qkv, out, inner, back = pl.pallas_call(
        place,
        out_shape=(
            jax.ShapeDtypeStruct((1, count, width), BF),
            jax.ShapeDtypeStruct((1, count, width), F32),
            jax.ShapeDtypeStruct((3, rows, own), F32),
            jax.ShapeDtypeStruct((rows, own), F32),
            jax.ShapeDtypeStruct((1, rows, width), F32),
            jax.ShapeDtypeStruct((rows, width), F32),
        ),
        in_specs=[whole] * 3,
        out_specs=(whole,) * 6,
        scratch_shapes=[
            vmem((count, width), BF), vmem((count, width), F32), vmem((3, rows, width), F32),
            dma((5,)), dma((5 + 3 * heads,)),
        ],
    )(final, dx, grads)
    return final, dx, qkv.transpose(1, 0, 2)[None], out.T[None], inner, back.T[None]


def solution(mesh):
    dims = (4, 4, 2)
    assert mesh.shape["fsdp"] == 32 and mesh.shape["sp"] == 4
    torus = Mesh(mesh.devices.reshape(*dims, 2, 2), AXES)
    fsdp, sp = AXES[:3], AXES[3:]
    placed = (
        P(fsdp, sp, None),
        P(fsdp, None, None, None),
        P(None, fsdp, None, sp),
        P(None, sp, fsdp),
        P(None, fsdp, sp),
        P(None, sp, fsdp),
        P(fsdp, sp, None),
    )
    return jax.shard_map(
        functools.partial(step, dims),
        mesh=torus,
        in_specs=placed,
        out_specs=(placed[0], *placed[:1], *placed[2:6]),
        check_vma=False,
    )
```

```python
import functools
import math

import jax
import jax.numpy as jnp
from jax import lax
from jax.experimental import pallas as pl
from jax.experimental.pallas import tpu as pltpu
from jax.sharding import Mesh
from jax.sharding import PartitionSpec as P

HEAD_DIM = 128
LN_EPS = 1e-06
TEMPER = 2.5
BF = jnp.bfloat16
F32 = jnp.float32
AXES = ("z", "y", "h", "l", "c")


def bf(x):
    return x.astype(BF)


def f32(x):
    return x.astype(F32)


def dot(a, b, ca=1, cb=0):
    return lax.dot_general(a, b, (((ca,), (cb,)), ((), ())), preferred_element_type=F32)


def normalize(x):
    d = x - jnp.mean(x, axis=-1, keepdims=True)
    r = lax.rsqrt(jnp.mean(d * d, axis=-1, keepdims=True) + LN_EPS)
    return d * r, r


def norm_back(n, r, e):
    return r * (e - jnp.mean(e, axis=-1, keepdims=True) - n * jnp.mean(e * n, axis=-1, keepdims=True))


def gelu_pair(u):
    k0 = math.sqrt(2.0 / math.pi)
    s = u * u
    t = jnp.tanh(k0 * u * (1.0 + 0.044715 * s))
    g = 0.5 * u * (1.0 + t)
    d = 0.5 * (1.0 + t) + 0.5 * k0 * u * (1.0 - t * t) * (1.0 + 3.0 * 0.044715 * s)
    return g, d


class copy:
    def __init__(self, src, dst, ssem, rsem, dev):
        self.src, self.rest = src, (dst, ssem, rsem, dev)

    def made(self):
        dst, ssem, rsem, dev = self.rest
        return pltpu.make_async_remote_copy(
            src_ref=self.src, dst_ref=dst, send_sem=ssem, recv_sem=rsem,
            device_id=dev, device_id_type=pl.DeviceIdType.MESH,
        )

    def start(self):
        self.made().start()

    def wait_send(self):
        self.made().wait_send()

    def wait_recv(self):
        self.made().wait_recv()


def kernel(
    dims, tok_in, mod_in, wq_in, wo_in, wi_in, wb_in, og_in, fin_out, dx_out, grads_out,
    W, G, R1A, R1B, R2A, R2B, R3, R1C, R2C, R4, R4H, A1, A2, DM, DA, GG, DU, QKV, DQKV, O, DO, PR, PS, RX, SX, MID, DX, AT,
    tok, mod, og, fin, dxin, grads, in_sem, out_sem, ags, a1r, a2r, a3r, a4r, a5r, rss, r1r, r2r, r3r, r4r, r5r, gs, gr, ss, sr,
):
    nz, ny, nh = dims
    z, y, h, l, c = (lax.axis_index(a) for a in AXES)
    ol, oc = 1 - l, 1 - c
    rows, width = wi_in.shape
    half = width // 2
    seq = QKV.shape[0]
    pair = seq // 2
    own = QKV.shape[1] // 3
    heads = own // HEAD_DIM
    slab = ny * nh * rows
    scale = TEMPER / math.sqrt(HEAD_DIM)
    q_s = 1.0 / math.sqrt(seq * nz * ny * nh)
    cols = (pl.ds(0, half), pl.ds(half, half))

    def drain(sem, moves):
        units = sum(math.prod(move.src.shape) for move in moves) // (rows * 128)
        for q, height in ((1, rows), (1, nh * rows), (3, nh * rows)):
            for i in range(1, nz + 1):
                for j in range(1, ny + 1):
                    n, rest = divmod(units * rows, q * height * i * j)
                    if rest == 0 and n <= width // 128:
                        view = W.at[pl.ds(0, q), pl.ds(0, i), pl.ds(0, j), pl.ds(0, height), pl.ds(0, n * 128)]
                        pltpu.make_async_copy(view, view, sem).wait()
                        return
        raise ValueError(units)

    def zz(k):
        return lax.rem(z + k + nz, nz)

    def yy(k):
        return lax.rem(y + k + ny, ny)

    def hh(k):
        return lax.rem(h + k + nh, nh)

    def at_rows(i):
        return pl.ds(pl.multiple_of(i * rows, 16), rows)

    core_peer = {"c": oc}
    line_peer = {"l": ol}
    pair_peer = {"h": 1 - h}
    halves = (pl.ds(0, 2), pl.ds(2, 2))

    def last(color, k):
        return {"z": zz(k)} if color == 0 else {"y": yy(k)}

    def mid_dev(color, k):
        return last(1 - color, k)

    strip = 256
    side = (width - strip) // 2
    ag_cols = ((pl.ds(0, side), pl.ds(side, side), pl.ds(2 * side, strip)),) * 2 + (cols,)
    every = slice(None)

    def slab_at(buf, color, k, at, part=every, row=every):
        return buf.at[zz(k), part, row, at] if color == 0 else buf.at[part, yy(k), row, at]

    def line_at(buf, color, k, at, row=every):
        return buf.at[z, yy(k), row, at] if color == 0 else buf.at[zz(k), y, row, at]

    def line_of(s, color):
        return color if color < 2 else s % 2

    def row_of(color):
        return every if color < 2 else at_rows(h)

    def direct(s, color):
        return s == 0 or color == 2

    def ag_pair(s, recv):
        piece = W.at[s, z, y, at_rows(1 - h if recv else h), pl.ds(0, 2 * side if s < 2 else width)]
        return copy(piece, piece, ags.at[s, 0], a1r.at[s, 0], pair_peer)

    def ag_final(s, recv):
        piece = W.at[s, :, :, at_rows(1 - h if recv else h), ag_cols[s][2]]
        return copy(piece, piece, ags.at[s, 1], a1r.at[s, 1], pair_peer)

    def ag_mid(s, color, k, which, recv):
        line = line_of(s, color)
        piece = line_at(W.at[s], line, -k if recv else 0, ag_cols[s][color], at_rows(h if which == 0 else 1 - h))
        side_of = 0 if direct(s, color) else (k - 1) // 2
        return copy(piece, piece, ags.at[s, 2 + 2 * (color // 2)], a2r.at[s, color, side_of], mid_dev(line, k))

    def ag_hop(s, color, d, recv):
        k = 1 - 2 * d
        piece = line_at(W.at[s], color, 2 if recv else -k, ag_cols[s][color], at_rows(d))
        return copy(piece, piece, ags.at[s, 2], a5r.at[s, color], mid_dev(color, k))

    def ag_last(s, color, d, j, recv):
        k, line = 1 - 2 * d, line_of(s, color)
        part = halves[d if j == 0 else 1 - d]
        piece = slab_at(W.at[s], line, -k if recv else 0, ag_cols[s][color], part, row_of(color))
        arrived = a3r.at[s, color] if j == 0 else a4r.at[s, color // 2]
        return copy(piece, piece, ags.at[s, 3 + color // 2], arrived, last(line, k))

    def ag_relay(s, color, d, recv):
        k, line = 1 - 2 * d, line_of(s, color)
        piece = slab_at(W.at[s], line, 2 if recv else -k, ag_cols[s][color], halves[d], row_of(color))
        return copy(piece, piece, ags.at[s, 3 + color // 2], a4r.at[s, color // 2], last(line, k))

    def ag_mid_start(s, which, colors=(0, 1)):
        if which:
            ag_pair(s, True).wait_recv()
        for k in (1, 3, 2) if direct(s, colors[0]) else (1, 3):
            for color in colors:
                ag_mid(s, color, k, which, False).start()

    def ag_hop_start(s):
        for color in (0, 1):
            for d in (0, 1):
                drain(a2r.at[s, color, d], [ag_mid(s, color, 1 + 2 * d, which, True) for which in (0, 1)])
                ag_hop(s, color, d, False).start()

    def ag_last_start(s, colors=(0, 1)):
        for color in colors:
            if direct(s, color):
                sides = (0, 1) if color < 2 else (0,)
                drain(a2r.at[s, color, 0], [ag_mid(s, color, k, which, True) for which in sides for k in (1, 2, 3)])
            else:
                drain(a5r.at[s, color], [ag_hop(s, color, d, True) for d in (0, 1)])
        for j in (0, 1):
            for color in colors:
                for d in (0, 1):
                    ag_last(s, color, d, j, False).start()

    def ag_relay_start(s, colors=(0, 1)):
        for color in colors:
            drain(a3r.at[s, color], [ag_last(s, color, d, 0, True) for d in (0, 1)])
            for d in (0, 1):
                ag_relay(s, color, d, False).start()

    def late(s, colors):
        return [move for color in colors for d in (0, 1)
                for move in (ag_last(s, color, d, 1, True), ag_relay(s, color, d, True))]

    def ag_final_start(s):
        drain(a4r.at[s, 1], late(s, (2,)))
        ag_final(s, False).start()

    def ag_wait(s):
        drain(a4r.at[s, 0], late(s, (0, 1)))

    def ag_sent(s):
        ag_pair(s, False).wait_send()
        middle = [ag_mid(s, color, k, which, False) for color in (0, 1) for which in (0, 1)
                  for k in ((1, 2, 3) if direct(s, 0) else (1, 3))]
        if not direct(s, 0):
            middle += [ag_hop(s, color, d, False) for color in (0, 1) for d in (0, 1)]
        drain(ags.at[s, 2], middle)

        def ends(colors):
            return [ag_last(s, color, d, j, False) for color in colors for d in (0, 1) for j in (0, 1)] + [
                ag_relay(s, color, d, False) for color in colors for d in (0, 1)]

        drain(ags.at[s, 3], ends((0, 1)))
        if s < 2:
            ag_final(s, False).wait_send()
            drain(ags.at[s, 4], [ag_mid(s, 2, k, 0, False) for k in (1, 2, 3)] + ends((2,)))

    R1 = (R1A, R1B)
    R2 = (R2A, R2B)
    full = 3 * own
    sections = 3 + heads
    parts = (G.at[0], G.at[1]) + (W.at[1],) * (1 + heads)
    slots = (2, 1) + (0,) * (1 + heads)
    lead = pl.ds(0, side)
    local_cols = [(lead, lead), (cols[0], cols[0])]
    grad_cols = [ag_cols[0], cols]
    pair_cols = [pl.ds(0, 2 * side), pl.ds(0, width)]
    third = own // 3
    for i, start in enumerate([full] + [hd * own for hd in range(heads)]):
        at = pl.ds(i * third, third)
        local_cols.append((at, at))
        grad_cols.append(tuple(pl.ds(start + j * third, third) for j in range(3)))
        pair_cols.append(pl.ds(start, 2 * third))

    spare = {2: (1, 4), 3: (1, 5), 4: (0, 4), 5: (0, 5)}

    def rs_line(s, color):
        return color if color < 2 else (0, None, 1, 1, 0, 1)[s]

    def spare_at(s):
        return pl.ds(spare[s][1] * third, third)

    def r1_at(s, color):
        if color < 2:
            return R1[color].at[slots[s], :, :, :, local_cols[s][color]]
        return R1C if s == 0 else R1[spare[s][0]].at[0, :, :, pl.ds(0, rows), spare_at(s)]

    def r2_at(s, color):
        if color < 2:
            return R2[color].at[slots[s], :, :, local_cols[s][color]]
        return R2C if s == 0 else R2[spare[s][0]].at[0, :, pl.ds(0, rows), spare_at(s)]

    def r4_at(s):
        return R4 if s == 0 else R4H.at[s - 2]

    def rs_first(s):
        src = parts[s].at[:, :, at_rows(1 - h), grad_cols[s][2]]
        return copy(src, r4_at(s), rss.at[1], r4r.at[s], pair_peer)

    def rs_ring(s, color, d, kind):
        k, line = 1 - 2 * d, rs_line(s, color)
        part = halves[1 - d if kind == 1 else d]
        src = slab_at(parts[s], line, 2 if kind == 0 else k, grad_cols[s][color], part, row_of(color))
        dst = r1_at(s, color).at[2 if kind == 0 else d, part]
        arrived = r1r.at[s, color, min(kind, 1)]
        return copy(src, dst, rss.at[0], arrived, last(line, k))

    def rs_mid(s, color, k):
        line = rs_line(s, color)
        return copy(
            line_at(parts[s], line, k, grad_cols[s][color], row_of(color)), r2_at(s, color).at[k - 1],
            rss.at[1], r2r.at[s, color], mid_dev(line, k),
        )

    def ringed(s, color):
        return s < 2 and color < 2

    def rs_hop(s, color, d, kind):
        k = 1 - 2 * d
        row = at_rows(1 - d if kind == 1 else d)
        src = line_at(parts[s], color, 2 if kind == 0 else k, grad_cols[s][color], row)
        dst = r2_at(s, color).at[2 if kind == 0 else d, row]
        arrived = r5r.at[s, color, d if kind == 0 else 2]
        return copy(src, dst, rss.at[1], arrived, mid_dev(color, k))

    def rs_hop_combine(s):
        for color in (0, 1):
            for d in (0, 1):
                rs_hop(s, color, d, 0).wait_recv()
                k = 1 - 2 * d
                at = (z, yy(k)) if color == 0 else (zz(k), y)
                at = (*at, at_rows(d), grad_cols[s][color])
                parts[s][at] = bf(f32(parts[s][at]) + f32(r2_at(s, color)[2, d * rows : (d + 1) * rows]))
                rs_hop(s, color, d, 2).start()

    def rs_pair(s):
        return copy(
            parts[s].at[z, y, at_rows(1 - h), pair_cols[s]], R3.at[slots[s], :, pair_cols[s]],
            rss.at[1], r3r.at[s], pair_peer,
        )

    def rs_second(s):
        rs_first(s).wait_recv()

        @pl.loop(0, nz)
        def _(i):
            at = (i, every, at_rows(h), grad_cols[s][2])
            parts[s][at] = bf(f32(parts[s][at]) + f32(r4_at(s)[i]))

        rs_start(s, (2,))

    def rs_start(s, colors=(0, 1)):
        for kind in (0, 1):
            for color in colors:
                for d in (0, 1):
                    rs_ring(s, color, d, kind).start()

    def rs_combine(s, colors=(0, 1)):
        for color in colors:
            line = rs_line(s, color)
            drain(r1r.at[s, color, 0], [rs_ring(s, color, d, 0) for d in (0, 1)])
            for d in (0, 1):
                k = 1 - 2 * d

                @pl.loop(2 * d, 2 * d + 2)
                def _(i):
                    at = (zz(k), i) if line == 0 else (i, yy(k))
                    at = (*at, row_of(color), grad_cols[s][color])
                    parts[s][at] = bf(f32(parts[s][at]) + f32(r1_at(s, color)[2, i]))

                rs_ring(s, color, d, 2).start()

    def rs_mid_start(s, colors=(0, 1)):
        for color in colors:
            line = rs_line(s, color)
            drain(r1r.at[s, color, 1], [rs_ring(s, color, d, kind) for d in (0, 1) for kind in (1, 2)])

            @pl.loop(0, 4)
            def _(i):
                at = (z, i) if line == 0 else (i, y)
                at = (*at, row_of(color), grad_cols[s][color])
                total = f32(parts[s][at])
                for d in (0, 1):
                    total = total + f32(r1_at(s, color)[d, i])
                parts[s][at] = bf(total)

            if ringed(s, color):
                for kind in (0, 1):
                    for d in (0, 1):
                        rs_hop(s, color, d, kind).start()
            else:
                for k in (1, 3, 2):
                    rs_mid(s, color, k).start()

    def rs_total(s, color):
        if ringed(s, color):
            drain(r5r.at[s, color, 2], [rs_hop(s, color, d, kind) for d in (0, 1) for kind in (1, 2)])
        else:
            drain(r2r.at[s, color], [rs_mid(s, color, k) for k in (1, 2, 3)])
        total = f32(parts[s][z, y, row_of(color), grad_cols[s][color]])
        for k in range(2 if ringed(s, color) else 3):
            total = total + f32(r2_at(s, color)[k])
        return total

    def rs_pair_start(s):
        for color in (0, 1):
            parts[s][z, y, every, grad_cols[s][color]] = bf(rs_total(s, color))
        rs_pair(s).start()

    def rs_finish(s):
        rs_pair(s).wait_recv()
        at = pair_cols[s]
        grads[slots[s], :, at] = f32(parts[s][z, y, at_rows(h), at]) + f32(R3[slots[s], :, at])

    def rs_finish_third(s):
        grads[slots[s], :, grad_cols[s][2]] = rs_total(s, 2)

    def rs_sent():
        rings, others = [], []
        for s in range(sections):
            for color in (0, 1) if s == 1 else (0, 1, 2):
                rings += [rs_ring(s, color, d, kind) for d in (0, 1) for kind in (0, 1, 2)]
                if ringed(s, color):
                    others += [rs_hop(s, color, d, kind) for d in (0, 1) for kind in (0, 1, 2)]
                else:
                    others += [rs_mid(s, color, k) for k in (1, 2, 3)]
            others += [rs_pair(s)] if s == 1 else [rs_pair(s), rs_first(s)]
        drain(rss.at[0], rings)
        drain(rss.at[1], others)

    def g_copy(i, buf, step, recv):
        if step == 0:
            piece, dev = buf.at[l, oc if recv else c], core_peer
        elif step == 1:
            piece, dev = buf.at[ol if recv else l, c], line_peer
        else:
            piece, dev = buf.at[ol, oc if recv else c], core_peer
        return copy(piece, piece, gs.at[i], gr.at[i, step], dev)

    def gather_start(i, buf):
        g_copy(i, buf, 1, False).start()
        g_copy(i, buf, 0, False).start()

    def gather_relay(i, buf):
        g_copy(i, buf, 1, True).wait_recv()
        g_copy(i, buf, 2, False).start()

    def gather_wait(i, buf, step):
        g_copy(i, buf, step, True).wait_recv()

    def gather_sent(i, buf):
        drain(gs.at[i], [g_copy(i, buf, step, False) for step in range(3)])

    def s_copy(i, step):
        src, dev = (
            (PS.at[ol, oc], core_peer),
            (SX, line_peer),
            (PS.at[l, oc], core_peer),
        )[step]
        return copy(src, RX.at[i % 2, step], ss.at[i], sr.at[i, step], dev)

    def scatter_far(i, compute):
        compute(ol)
        s_copy(i, 0).start()
        s_copy(i, 0).wait_recv()
        SX[...] = bf(f32(PS[ol, c]) + f32(RX[i % 2, 0]))
        s_copy(i, 1).start()

    def scatter_near(i, compute):
        compute(l)
        s_copy(i, 2).start()

    def scatter_result(i):
        s_copy(i, 2).wait_recv()
        s_copy(i, 1).wait_recv()
        total = f32(PS[l, c]) + f32(RX[i % 2, 2]) + f32(RX[i % 2, 1])
        drain(ss.at[i], [s_copy(i, step) for step in range(3)])
        return total

    def pair_rows(i):
        return pl.ds(pl.multiple_of(i * pair, 128), pair)

    def back_product(left, s, lo, n):
        def compute(i):
            @pl.loop(0, nz)
            def _(b):
                w = W[s, b, :, :, pl.ds(lo, n)].reshape(slab, n)
                at = pl.ds(pl.multiple_of(b * slab, 128), slab)
                PS[i, :, :, at] = bf(dot(left(i), w, 1, 1)).reshape(2, pair // 2, slab)
        return compute

    def two(buf, i):
        return buf[i].reshape(pair, buf.shape[-1])

    def all_rows(buf, at):
        return buf[:, :, :, at].reshape(seq, -1)

    def turn(buf):
        @pl.loop(0, nz)
        def _(b):
            AT[b] = all_rows(buf, pl.ds(pl.multiple_of(b * slab, 128), slab)).T

    def grad_turned(s, right, start, stop, tile):
        @pl.loop(0, (stop - start) // tile)
        def _(t):
            at = pl.ds(pl.multiple_of(start + t * tile, 128), tile)
            value = dot(AT[...].reshape(width, seq), right(at)) * q_s
            parts[s][:, :, :, at] = bf(value).reshape(nz, ny, nh * rows, tile)

    def grad_product(s, left, right, n, lo):
        @pl.loop(0, nz)
        def _(b):
            a = all_rows(left, pl.ds(pl.multiple_of(b * slab, 128), slab)).T
            value = dot(a, right) * q_s
            parts[s][b, :, :, pl.ds(lo, n)] = bf(value).reshape(ny, nh * rows, n)

    peers = [{"z": zz(k)} for k in range(1, 4)] + [{"y": yy(k)} for k in range(1, 4)]
    peers += [pair_peer, core_peer, line_peer, {"l": ol, "c": oc}]
    barrier = pltpu.get_barrier_semaphore()
    for dev in peers:
        pl.semaphore_signal(barrier, inc=1, device_id=dev, device_id_type=pl.DeviceIdType.MESH)
    outs = [(fin, fin_out), (dxin, dx_out)] + [(grads.at[i], grads_out.at[i]) for i in range(3)]
    results = [pltpu.make_async_copy(src, dst, out_sem.at[i]) for i, (src, dst) in enumerate(outs)]
    mine = at_rows(h)
    moves = [
        (wq_in.at[i, :, pl.ds(hd * HEAD_DIM, HEAD_DIM)], W.at[0, z, y, mine, pl.ds((3 * hd + i) * HEAD_DIM, HEAD_DIM)])
        for i in range(3) for hd in range(heads)
    ]
    moves += [(wo_in, W.at[0, z, y, mine, pl.ds(3 * own, own)])]
    moves += [(wi_in, W.at[1, z, y, mine]), (wb_in, W.at[2, z, y, mine])]
    moves += [(tok_in, tok), (og_in, og), (mod_in, mod)]
    count = len(moves) - 3
    loads = [pltpu.make_async_copy(src, dst, in_sem.at[max(i - count + 1, 0)]) for i, (src, dst) in enumerate(moves)]
    for load in loads:
        load.start()
    drain(in_sem.at[0], [copy(src, dst, None, None, None) for src, dst in moves[:count]])
    pl.semaphore_wait(barrier, len(peers))

    for s in range(3):
        ag_pair(s, False).start()
    for s in (0, 1):
        ag_mid_start(s, 0, (2,))
        ag_mid_start(s, 0)
    for load in loads[count:]:
        load.wait()
    m = [mod[i] for i in range(6)]
    n1, r1 = normalize(f32(tok[...]))
    A1[l, c] = bf(n1 * (1.0 + m[1]) + m[0])
    DM[l, c] = bf(m[5] * f32(og[...]))
    gather_start(0, A1)
    ag_last_start(0, (2,))
    ag_mid_start(0, 1)
    ag_mid_start(1, 1)
    ag_last_start(1, (2,))
    ag_relay_start(0, (2,))
    ag_hop_start(1)
    ag_last_start(0)
    ag_relay_start(1, (2,))
    ag_final_start(0)
    gather_relay(0, A1)
    gather_start(1, DM)
    ag_relay_start(0)
    ag_mid_start(2, 0)
    ag_mid_start(2, 1)
    ag_last_start(1)
    ag_final_start(1)
    gather_wait(0, A1, 0)
    gather_wait(0, A1, 2)

    ag_wait(0)

    @pl.loop(0, 3)
    def _(t):
        at = pl.ds(pl.multiple_of(t * own, 128), own)
        w = W[0, :, :, :, at].reshape(width, own)
        QKV[:, at] = bf(dot(A1[...].reshape(seq, width), w))

    ag_hop_start(2)

    def head(hd, i):
        return pl.ds(pl.multiple_of((3 * hd + i) * HEAD_DIM, 128), HEAD_DIM)

    def wide(hd):
        return pl.ds(pl.multiple_of(hd * HEAD_DIM, 128), HEAD_DIM)

    @pl.loop(0, heads)
    def _(hd):
        s = dot(QKV[:, head(hd, 0)], QKV[:, head(hd, 1)], 1, 1) * scale
        e = jnp.exp(s - jnp.max(s, axis=-1, keepdims=True))
        p = bf(e * (1.0 / jnp.sum(e, axis=-1, keepdims=True)))
        PR[hd] = p
        O[:, wide(hd)] = bf(dot(p, QKV[:, head(hd, 2)]))

    out_product = back_product(lambda i: O[pair_rows(i), :], 0, 3 * own, own)
    ag_final(0, True).wait_recv()
    scatter_far(0, out_product)
    scatter_near(0, out_product)
    ag_relay_start(1)
    ag_last_start(2)
    mid = f32(tok[...]) + m[2] * scatter_result(0)
    MID[...] = mid
    n2, r2 = normalize(mid)
    A2[l, c] = bf(n2 * (1.0 + m[4]) + m[3])
    gather_start(2, A2)

    tile = 256

    def hidden(i):
        @pl.loop(0, width // (2 * tile))
        def _(t):
            for j in (0, 1):
                at = pl.ds(pl.multiple_of((2 * t + j) * tile, 128), tile)
                g, d = gelu_pair(dot(two(A2, i), W[1, :, :, :, at].reshape(width, tile)))
                GG[i, :, :, at] = bf(g).reshape(2, pair // 2, tile)
                DU[i, :, :, at] = bf(d).reshape(2, pair // 2, tile)

    gather_relay(1, DM)
    gather_wait(1, DM, 0)
    gather_wait(1, DM, 2)
    turn(DM)
    ag_wait(1)
    ag_final(1, True).wait_recv()
    gather_wait(2, A2, 0)
    hidden(l)
    ag_relay_start(2)
    gather_relay(2, A2)
    gather_wait(2, A2, 2)
    hidden(ol)
    for lo, hi in ((2 * side, width), (0, half), (half, 2 * side)):
        grad_turned(0, lambda at: all_rows(GG, at), lo, hi, tile)
        if lo == 2 * side:
            rs_first(0).start()
        else:
            rs_start(0, (0,) if lo == 0 else (1,))
    ag_wait(2)

    @pl.loop(0, width // tile)
    def _(t):
        at = pl.ds(pl.multiple_of(t * tile, 128), tile)
        dg = dot(DM[...].reshape(seq, width), W[2, :, :, :, at].reshape(width, tile))
        DU[:, :, :, at] = bf(f32(DU[:, :, :, at]) * dg.reshape(2, 2, pair // 2, tile))

    in_back = back_product(lambda i: two(DU, i), 1, 0, width)
    scatter_far(1, in_back)
    rs_combine(0)
    turn(A2)
    grad_turned(1, lambda at: all_rows(DU, at), 0, half, tile)
    rs_second(0)
    rs_start(1, (0,))
    grad_turned(1, lambda at: all_rows(DU, at), half, width, tile)
    rs_start(1, (1,))
    scatter_near(1, in_back)
    e2 = scatter_result(1) * (1.0 + m[4])
    n2, r2 = normalize(MID[...])
    dmid = f32(og[...]) + norm_back(n2, r2, e2)
    DX[...] = dmid
    DA[l, c] = bf(m[2] * dmid)
    gather_start(3, DA)

    ff_back = back_product(lambda i: two(GG, i), 2, 0, width)
    scatter_far(2, ff_back)
    rs_combine(0, (2,))
    rs_combine(1)
    scatter_near(2, ff_back)
    turn(A1)
    rs_mid_start(0)
    gather_relay(3, DA)
    gather_wait(3, DA, 0)
    gather_wait(3, DA, 2)

    DO[...] = bf(dot(DA[...].reshape(seq, width), W[0, :, :, :, pl.ds(3 * own, own)].reshape(width, own)))
    ag_sent(1)
    grad_product(2, DA, O[...], own, full)
    rs_first(2).start()
    rs_start(2)

    for hd in range(heads):
        do = DO[:, wide(hd)]
        p = PR[hd]
        t = f32(p) * dot(do, QKV[:, head(hd, 2)], 1, 1)
        ds = bf(scale * (t - f32(p) * jnp.sum(t, axis=-1, keepdims=True)))
        DQKV[:, head(hd, 0)] = bf(dot(ds, QKV[:, head(hd, 1)]))
        DQKV[:, head(hd, 1)] = bf(dot(ds.T, QKV[:, head(hd, 0)]))
        DQKV[:, head(hd, 2)] = bf(dot(p.T, do))
        grad_turned(3 + hd, lambda at: DQKV[:, at], hd * own, (hd + 1) * own, own)
        rs_first(3 + hd).start()
        rs_start(3 + hd)

    qkv_back = back_product(lambda i: DQKV[pair_rows(i), :], 0, 0, 3 * own)
    fin[...] = bf(MID[...] + m[5] * scatter_result(2))
    results[0].start()
    rs_hop_combine(0)
    rs_combine(2)
    rs_mid_start(1)
    rs_combine(3)
    qkv_back = back_product(lambda i: DQKV[pair_rows(i), :], 0, 0, 3 * own)
    scatter_far(3, qkv_back)
    rs_second(2)
    rs_combine(4)
    scatter_near(3, qkv_back)
    rs_second(3)
    rs_mid_start(0, (2,))
    rs_pair_start(0)
    rs_combine(5)
    rs_second(4)
    rs_mid_start(2)
    rs_combine(2, (2,))
    rs_hop_combine(1)
    rs_second(5)
    rs_combine(3, (2,))
    rs_mid_start(3)
    rs_combine(4, (2,))
    rs_mid_start(4)
    rs_mid_start(2, (2,))
    rs_mid_start(3, (2,))
    rs_mid_start(5)
    rs_combine(5, (2,))
    rs_pair_start(2)
    rs_pair_start(1)
    rs_finish_third(0)
    rs_mid_start(4, (2,))
    rs_pair_start(3)
    rs_finish(0)
    results[4].start()
    e1 = scatter_result(3) * (1.0 + m[1])
    n1, r1 = normalize(f32(tok[...]))
    dxin[...] = DX[...] + norm_back(n1, r1, e1)
    results[1].start()
    rs_pair_start(4)
    rs_mid_start(5, (2,))
    rs_pair_start(5)
    rs_finish(1)
    results[3].start()
    for s in range(2, sections):
        rs_finish_third(s)
    for s in range(2, sections):
        rs_finish(s)
    results[2].start()
    rs_sent()
    ag_sent(0)
    ag_sent(2)
    for i, buf in enumerate((A1, DM, A2, DA)):
        gather_sent(i, buf)
    for result in results:
        result.wait()


def place(fin, dx, grads, o_fin, o_dx, o_qkv, o_out, o_in, o_back, v_fin, v_dx, v_grads, sem_in, sem_out):
    own = o_out.shape[1]
    heads = own // HEAD_DIM
    sources = (
        (dx, v_dx), (grads.at[2], v_grads.at[2]), (grads.at[1], v_grads.at[1]),
        (fin, v_fin), (grads.at[0], v_grads.at[0]),
    )
    pieces = [
        (v_grads.at[0, :, pl.ds((3 * hd + i) * HEAD_DIM, HEAD_DIM)], o_qkv.at[i, :, pl.ds(hd * HEAD_DIM, HEAD_DIM)])
        for i in range(3) for hd in range(heads)
    ]
    pieces.append((v_grads.at[0, :, pl.ds(3 * own, own)], o_out))
    targets = (
        [(v_dx, o_dx.at[0])], [(v_grads.at[2], o_back)], [(v_grads.at[1], o_in.at[0])],
        [(v_fin, o_fin.at[0])], pieces,
    )
    loads = [pltpu.make_async_copy(a, b, sem_in.at[i]) for i, (a, b) in enumerate(sources)]
    for load in loads:
        load.start()
    stores = []
    for load, pairs in zip(loads, targets):
        load.wait()
        for a, b in pairs:
            store = pltpu.make_async_copy(a, b, sem_out.at[len(stores)])
            store.start()
            stores.append(store)
    for store in stores:
        store.wait()


def step(dims, tokens, modulation, w_qkv, w_out, w_in, w_back, out_grad):
    nz, ny, nh = dims
    count, width = tokens.shape[1:]
    rows, own, ff = w_qkv.shape[1], w_qkv.shape[3], w_in.shape[2]
    assert ff == width and 4 * own == width
    seq = 4 * count
    heads = own // HEAD_DIM
    big = (nz, ny, nh * rows)
    half = width // 2
    vmem = pltpu.VMEM
    dma = pltpu.SemaphoreType.DMA
    tokens_buf = vmem((2, 2, count, width), BF)
    scratch = [
        vmem((3, *big, width), BF),
        vmem((2, *big, width), BF),
        vmem((3, 3, 4, nh * rows, half), BF),
        vmem((3, 3, 4, nh * rows, half), BF),
        vmem((3, 3, nh * rows, half), BF),
        vmem((3, 3, nh * rows, half), BF),
        vmem((3, rows, width), BF),
        vmem((3, 4, rows, 256), BF),
        vmem((3, rows, 256), BF),
        vmem((nz, ny, rows, 256), BF),
        vmem((1 + heads, nz, ny, rows, own // 3), BF),
        *[tokens_buf] * 6,
        vmem((seq, 3 * own), BF),
        vmem((seq, 3 * own), BF),
        vmem((seq, own), BF),
        vmem((seq, own), BF),
        vmem((heads, seq, seq), BF),
        tokens_buf,
        vmem((2, 3, count, width), BF),
        vmem((count, width), BF),
        vmem((count, width), F32),
        vmem((count, width), F32),
        vmem((nz, ny * nh * rows, seq), BF),
        vmem((count, width), BF),
        vmem((6, 1, width), F32),
        vmem((count, width), BF),
        vmem((count, width), BF),
        vmem((count, width), F32),
        vmem((3, rows, width), F32),
        dma((4,)),
        dma((5,)),
        dma((3, 5)), dma((3, 2)), dma((3, 3, 2)), dma((3, 3)), dma((3, 2)), dma((3, 2)),
        dma((2,)), dma((3 + heads, 3, 2)), dma((3 + heads, 3)), dma((3 + heads,)), dma((3 + heads,)),
        dma((2, 2, 3)),
        dma((4,)), dma((4, 3)), dma((4,)), dma((4, 3)),
    ]
    whole = pl.BlockSpec(memory_space=pl.ANY)
    final, dx, grads = pl.pallas_call(
        functools.partial(kernel, dims),
        out_shape=(
            jax.ShapeDtypeStruct((count, width), BF),
            jax.ShapeDtypeStruct((count, width), F32),
            jax.ShapeDtypeStruct((3, rows, width), F32),
        ),
        in_specs=[whole] * 7,
        out_specs=(whole,) * 3,
        scratch_shapes=scratch,
        compiler_params=pltpu.CompilerParams(
            collective_id=0, has_side_effects=True, vmem_limit_bytes=67043328
        ),
    )(
        tokens[0], modulation[0].transpose(1, 0, 2), w_qkv[0].transpose(1, 0, 2), w_out[0].T,
        w_in[0], w_back[0].T, out_grad[0],
    )
    final, dx, qkv, out, inner, back = pl.pallas_call(
        place,
        out_shape=(
            jax.ShapeDtypeStruct((1, count, width), BF),
            jax.ShapeDtypeStruct((1, count, width), F32),
            jax.ShapeDtypeStruct((3, rows, own), F32),
            jax.ShapeDtypeStruct((rows, own), F32),
            jax.ShapeDtypeStruct((1, rows, width), F32),
            jax.ShapeDtypeStruct((rows, width), F32),
        ),
        in_specs=[whole] * 3,
        out_specs=(whole,) * 6,
        scratch_shapes=[
            vmem((count, width), BF), vmem((count, width), F32), vmem((3, rows, width), F32),
            dma((5,)), dma((5 + 3 * heads,)),
        ],
    )(final, dx, grads)
    return final, dx, qkv.transpose(1, 0, 2)[None], out.T[None], inner, back.T[None]


def solution(mesh):
    dims = (4, 4, 2)
    assert mesh.shape["fsdp"] == 32 and mesh.shape["sp"] == 4
    torus = Mesh(mesh.devices.reshape(*dims, 2, 2), AXES)
    fsdp, sp = AXES[:3], AXES[3:]
    placed = (
        P(fsdp, sp, None),
        P(fsdp, None, None, None),
        P(None, fsdp, None, sp),
        P(None, sp, fsdp),
        P(None, fsdp, sp),
        P(None, sp, fsdp),
        P(fsdp, sp, None),
    )
    return jax.shard_map(
        functools.partial(step, dims),
        mesh=torus,
        in_specs=placed,
        out_specs=(placed[0], *placed[:1], *placed[2:6]),
        check_vma=False,
    )
```

```python
import functools
import math

import jax
import jax.numpy as jnp
from jax import lax
from jax.experimental import pallas as pl
from jax.experimental.pallas import tpu as pltpu
from jax.sharding import Mesh
from jax.sharding import PartitionSpec as P

HEAD_DIM = 128
LN_EPS = 1e-06
TEMPER = 2.5
BF = jnp.bfloat16
F32 = jnp.float32
AXES = ("z", "y", "h", "l", "c")


def bf(x):
    return x.astype(BF)


def f32(x):
    return x.astype(F32)


def dot(a, b, ca=1, cb=0):
    return lax.dot_general(a, b, (((ca,), (cb,)), ((), ())), preferred_element_type=F32)


def normalize(x):
    d = x - jnp.mean(x, axis=-1, keepdims=True)
    r = lax.rsqrt(jnp.mean(d * d, axis=-1, keepdims=True) + LN_EPS)
    return d * r, r


def norm_back(n, r, e):
    return r * (e - jnp.mean(e, axis=-1, keepdims=True) - n * jnp.mean(e * n, axis=-1, keepdims=True))


def gelu_pair(u):
    k0 = math.sqrt(2.0 / math.pi)
    s = u * u
    t = jnp.tanh(k0 * u * (1.0 + 0.044715 * s))
    g = 0.5 * u * (1.0 + t)
    d = 0.5 * (1.0 + t) + 0.5 * k0 * u * (1.0 - t * t) * (1.0 + 3.0 * 0.044715 * s)
    return g, d


class copy:
    def __init__(self, src, dst, ssem, rsem, dev):
        self.src, self.rest = src, (dst, ssem, rsem, dev)

    def made(self):
        dst, ssem, rsem, dev = self.rest
        return pltpu.make_async_remote_copy(
            src_ref=self.src, dst_ref=dst, send_sem=ssem, recv_sem=rsem,
            device_id=dev, device_id_type=pl.DeviceIdType.MESH,
        )

    def start(self):
        self.made().start()

    def wait_send(self):
        self.made().wait_send()

    def wait_recv(self):
        self.made().wait_recv()


def kernel(
    dims, tok_in, mod_in, wq_in, wo_in, wi_in, wb_in, og_in, fin_out, dx_out, grads_out,
    W, G, R1A, R1B, R2A, R2B, R3, R1C, R2C, R4, R4H, A1, A2, DM, DA, GG, DU, QKV, DQKV, O, DO, PR, PS, RX, SX, MID, DX, AT,
    tok, mod, og, fin, dxin, grads, in_sem, out_sem, ags, a1r, a2r, a3r, a4r, a5r, rss, r1r, r2r, r3r, r4r, r5r, gs, gr, ss, sr,
):
    nz, ny, nh = dims
    z, y, h, l, c = (lax.axis_index(a) for a in AXES)
    ol, oc = 1 - l, 1 - c
    rows, width = wi_in.shape
    half = width // 2
    seq = QKV.shape[0]
    pair = seq // 2
    own = QKV.shape[1] // 3
    heads = own // HEAD_DIM
    slab = ny * nh * rows
    scale = TEMPER / math.sqrt(HEAD_DIM)
    q_s = 1.0 / math.sqrt(seq * nz * ny * nh)
    cols = (pl.ds(0, half), pl.ds(half, half))

    def drain(sem, moves):
        units = sum(math.prod(move.src.shape) for move in moves) // (rows * 128)
        for q, height in ((1, rows), (1, nh * rows), (3, nh * rows)):
            for i in range(1, nz + 1):
                for j in range(1, ny + 1):
                    n, rest = divmod(units * rows, q * height * i * j)
                    if rest == 0 and n <= width // 128:
                        view = W.at[pl.ds(0, q), pl.ds(0, i), pl.ds(0, j), pl.ds(0, height), pl.ds(0, n * 128)]
                        pltpu.make_async_copy(view, view, sem).wait()
                        return
        raise ValueError(units)

    def zz(k):
        return lax.rem(z + k + nz, nz)

    def yy(k):
        return lax.rem(y + k + ny, ny)

    def hh(k):
        return lax.rem(h + k + nh, nh)

    def at_rows(i):
        return pl.ds(pl.multiple_of(i * rows, 16), rows)

    core_peer = {"c": oc}
    line_peer = {"l": ol}
    pair_peer = {"h": 1 - h}
    halves = (pl.ds(0, 2), pl.ds(2, 2))

    def last(color, k):
        return {"z": zz(k)} if color == 0 else {"y": yy(k)}

    def mid_dev(color, k):
        return last(1 - color, k)

    strip = 256
    side = (width - strip) // 2
    ag_cols = ((pl.ds(0, side), pl.ds(side, side), pl.ds(2 * side, strip)),) * 2 + (cols,)
    every = slice(None)

    def slab_at(buf, color, k, at, part=every, row=every):
        return buf.at[zz(k), part, row, at] if color == 0 else buf.at[part, yy(k), row, at]

    def line_at(buf, color, k, at, row=every):
        return buf.at[z, yy(k), row, at] if color == 0 else buf.at[zz(k), y, row, at]

    def line_of(s, color):
        return color if color < 2 else s % 2

    def row_of(color):
        return every if color < 2 else at_rows(h)

    def direct(s, color):
        return s == 0 or color == 2

    def ag_pair(s, recv):
        piece = W.at[s, z, y, at_rows(1 - h if recv else h), pl.ds(0, 2 * side if s < 2 else width)]
        return copy(piece, piece, ags.at[s, 0], a1r.at[s, 0], pair_peer)

    def ag_final(s, recv):
        piece = W.at[s, :, :, at_rows(1 - h if recv else h), ag_cols[s][2]]
        return copy(piece, piece, ags.at[s, 1], a1r.at[s, 1], pair_peer)

    def ag_mid(s, color, k, which, recv):
        line = line_of(s, color)
        piece = line_at(W.at[s], line, -k if recv else 0, ag_cols[s][color], at_rows(h if which == 0 else 1 - h))
        side_of = 0 if direct(s, color) else (k - 1) // 2
        return copy(piece, piece, ags.at[s, 2 + 2 * (color // 2)], a2r.at[s, color, side_of], mid_dev(line, k))

    def ag_hop(s, color, d, recv):
        k = 1 - 2 * d
        piece = line_at(W.at[s], color, 2 if recv else -k, ag_cols[s][color], at_rows(d))
        return copy(piece, piece, ags.at[s, 2], a5r.at[s, color], mid_dev(color, k))

    def ag_last(s, color, d, j, recv):
        k, line = 1 - 2 * d, line_of(s, color)
        part = halves[d if j == 0 else 1 - d]
        piece = slab_at(W.at[s], line, -k if recv else 0, ag_cols[s][color], part, row_of(color))
        arrived = a3r.at[s, color] if j == 0 else a4r.at[s, color // 2]
        return copy(piece, piece, ags.at[s, 3 + color // 2], arrived, last(line, k))

    def ag_relay(s, color, d, recv):
        k, line = 1 - 2 * d, line_of(s, color)
        piece = slab_at(W.at[s], line, 2 if recv else -k, ag_cols[s][color], halves[d], row_of(color))
        return copy(piece, piece, ags.at[s, 3 + color // 2], a4r.at[s, color // 2], last(line, k))

    def ag_mid_start(s, which, colors=(0, 1)):
        if which:
            ag_pair(s, True).wait_recv()
        for k in (1, 3, 2) if direct(s, colors[0]) else (1, 3):
            for color in colors:
                ag_mid(s, color, k, which, False).start()

    def ag_hop_start(s):
        for color in (0, 1):
            for d in (0, 1):
                drain(a2r.at[s, color, d], [ag_mid(s, color, 1 + 2 * d, which, True) for which in (0, 1)])
                ag_hop(s, color, d, False).start()

    def ag_last_start(s, colors=(0, 1)):
        for color in colors:
            if direct(s, color):
                sides = (0, 1) if color < 2 else (0,)
                drain(a2r.at[s, color, 0], [ag_mid(s, color, k, which, True) for which in sides for k in (1, 2, 3)])
            else:
                drain(a5r.at[s, color], [ag_hop(s, color, d, True) for d in (0, 1)])
        for j in (0, 1):
            for color in colors:
                for d in (0, 1):
                    ag_last(s, color, d, j, False).start()

    def ag_relay_start(s, colors=(0, 1)):
        for color in colors:
            drain(a3r.at[s, color], [ag_last(s, color, d, 0, True) for d in (0, 1)])
            for d in (0, 1):
                ag_relay(s, color, d, False).start()

    def late(s, colors):
        return [move for color in colors for d in (0, 1)
                for move in (ag_last(s, color, d, 1, True), ag_relay(s, color, d, True))]

    def ag_final_start(s):
        drain(a4r.at[s, 1], late(s, (2,)))
        ag_final(s, False).start()

    def ag_wait(s):
        drain(a4r.at[s, 0], late(s, (0, 1)))

    def ag_sent(s):
        ag_pair(s, False).wait_send()
        middle = [ag_mid(s, color, k, which, False) for color in (0, 1) for which in (0, 1)
                  for k in ((1, 2, 3) if direct(s, 0) else (1, 3))]
        if not direct(s, 0):
            middle += [ag_hop(s, color, d, False) for color in (0, 1) for d in (0, 1)]
        drain(ags.at[s, 2], middle)

        def ends(colors):
            return [ag_last(s, color, d, j, False) for color in colors for d in (0, 1) for j in (0, 1)] + [
                ag_relay(s, color, d, False) for color in colors for d in (0, 1)]

        drain(ags.at[s, 3], ends((0, 1)))
        if s < 2:
            ag_final(s, False).wait_send()
            drain(ags.at[s, 4], [ag_mid(s, 2, k, 0, False) for k in (1, 2, 3)] + ends((2,)))

    R1 = (R1A, R1B)
    R2 = (R2A, R2B)
    full = 3 * own
    sections = 3 + heads
    parts = (G.at[0], G.at[1]) + (W.at[1],) * (1 + heads)
    slots = (2, 1) + (0,) * (1 + heads)
    lead = pl.ds(0, side)
    local_cols = [(lead, lead), (cols[0], cols[0])]
    grad_cols = [ag_cols[0], cols]
    pair_cols = [pl.ds(0, 2 * side), pl.ds(0, width)]
    third = own // 3
    for i, start in enumerate([full] + [hd * own for hd in range(heads)]):
        at = pl.ds(i * third, third)
        local_cols.append((at, at))
        grad_cols.append(tuple(pl.ds(start + j * third, third) for j in range(3)))
        pair_cols.append(pl.ds(start, 2 * third))

    spare = {2: (1, 4), 3: (1, 5), 4: (0, 4), 5: (0, 5)}

    def rs_line(s, color):
        return color if color < 2 else (0, None, 0, 1, 0, 1)[s]

    def spare_at(s):
        return pl.ds(spare[s][1] * third, third)

    def r1_at(s, color):
        if color < 2:
            return R1[color].at[slots[s], :, :, :, local_cols[s][color]]
        return R1C if s == 0 else R1[spare[s][0]].at[0, :, :, pl.ds(0, rows), spare_at(s)]

    def r2_at(s, color):
        if color < 2:
            return R2[color].at[slots[s], :, :, local_cols[s][color]]
        return R2C if s == 0 else R2[spare[s][0]].at[0, :, pl.ds(0, rows), spare_at(s)]

    def r4_at(s):
        return R4 if s == 0 else R4H.at[s - 2]

    def rs_first(s):
        src = parts[s].at[:, :, at_rows(1 - h), grad_cols[s][2]]
        return copy(src, r4_at(s), rss.at[1], r4r.at[s], pair_peer)

    def rs_ring(s, color, d, kind):
        k, line = 1 - 2 * d, rs_line(s, color)
        part = halves[1 - d if kind == 1 else d]
        src = slab_at(parts[s], line, 2 if kind == 0 else k, grad_cols[s][color], part, row_of(color))
        dst = r1_at(s, color).at[2 if kind == 0 else d, part]
        arrived = r1r.at[s, color, min(kind, 1)]
        return copy(src, dst, rss.at[0], arrived, last(line, k))

    def rs_mid(s, color, k):
        line = rs_line(s, color)
        return copy(
            line_at(parts[s], line, k, grad_cols[s][color], row_of(color)), r2_at(s, color).at[k - 1],
            rss.at[1], r2r.at[s, color], mid_dev(line, k),
        )

    def ringed(s, color):
        return s < 2 and color < 2

    def rs_hop(s, color, d, kind):
        k = 1 - 2 * d
        row = at_rows(1 - d if kind == 1 else d)
        src = line_at(parts[s], color, 2 if kind == 0 else k, grad_cols[s][color], row)
        dst = r2_at(s, color).at[2 if kind == 0 else d, row]
        arrived = r5r.at[s, color, d if kind == 0 else 2]
        return copy(src, dst, rss.at[1], arrived, mid_dev(color, k))

    def rs_hop_combine(s):
        for color in (0, 1):
            for d in (0, 1):
                rs_hop(s, color, d, 0).wait_recv()
                k = 1 - 2 * d
                at = (z, yy(k)) if color == 0 else (zz(k), y)
                at = (*at, at_rows(d), grad_cols[s][color])
                parts[s][at] = bf(f32(parts[s][at]) + f32(r2_at(s, color)[2, d * rows : (d + 1) * rows]))
                rs_hop(s, color, d, 2).start()

    def rs_pair(s):
        return copy(
            parts[s].at[z, y, at_rows(1 - h), pair_cols[s]], R3.at[slots[s], :, pair_cols[s]],
            rss.at[1], r3r.at[s], pair_peer,
        )

    def rs_second(s):
        rs_first(s).wait_recv()

        @pl.loop(0, nz)
        def _(i):
            at = (i, every, at_rows(h), grad_cols[s][2])
            parts[s][at] = bf(f32(parts[s][at]) + f32(r4_at(s)[i]))

        rs_start(s, (2,))

    def rs_start(s, colors=(0, 1)):
        for kind in (0, 1):
            for color in colors:
                for d in (0, 1):
                    rs_ring(s, color, d, kind).start()

    def rs_combine(s, colors=(0, 1)):
        for color in colors:
            line = rs_line(s, color)
            drain(r1r.at[s, color, 0], [rs_ring(s, color, d, 0) for d in (0, 1)])
            for d in (0, 1):
                k = 1 - 2 * d

                @pl.loop(2 * d, 2 * d + 2)
                def _(i):
                    at = (zz(k), i) if line == 0 else (i, yy(k))
                    at = (*at, row_of(color), grad_cols[s][color])
                    parts[s][at] = bf(f32(parts[s][at]) + f32(r1_at(s, color)[2, i]))

                rs_ring(s, color, d, 2).start()

    def rs_mid_start(s, colors=(0, 1)):
        for color in colors:
            line = rs_line(s, color)
            drain(r1r.at[s, color, 1], [rs_ring(s, color, d, kind) for d in (0, 1) for kind in (1, 2)])

            @pl.loop(0, 4)
            def _(i):
                at = (z, i) if line == 0 else (i, y)
                at = (*at, row_of(color), grad_cols[s][color])
                total = f32(parts[s][at])
                for d in (0, 1):
                    total = total + f32(r1_at(s, color)[d, i])
                parts[s][at] = bf(total)

            if ringed(s, color):
                for kind in (0, 1):
                    for d in (0, 1):
                        rs_hop(s, color, d, kind).start()
            else:
                for k in (1, 3, 2):
                    rs_mid(s, color, k).start()

    def rs_total(s, color):
        if ringed(s, color):
            drain(r5r.at[s, color, 2], [rs_hop(s, color, d, kind) for d in (0, 1) for kind in (1, 2)])
        else:
            drain(r2r.at[s, color], [rs_mid(s, color, k) for k in (1, 2, 3)])
        total = f32(parts[s][z, y, row_of(color), grad_cols[s][color]])
        for k in range(2 if ringed(s, color) else 3):
            total = total + f32(r2_at(s, color)[k])
        return total

    def rs_pair_start(s):
        for color in (0, 1):
            parts[s][z, y, every, grad_cols[s][color]] = bf(rs_total(s, color))
        rs_pair(s).start()

    def rs_finish(s):
        rs_pair(s).wait_recv()
        at = pair_cols[s]
        grads[slots[s], :, at] = f32(parts[s][z, y, at_rows(h), at]) + f32(R3[slots[s], :, at])

    def rs_finish_third(s):
        grads[slots[s], :, grad_cols[s][2]] = rs_total(s, 2)

    def rs_sent():
        rings, others = [], []
        for s in range(sections):
            for color in (0, 1) if s == 1 else (0, 1, 2):
                rings += [rs_ring(s, color, d, kind) for d in (0, 1) for kind in (0, 1, 2)]
                if ringed(s, color):
                    others += [rs_hop(s, color, d, kind) for d in (0, 1) for kind in (0, 1, 2)]
                else:
                    others += [rs_mid(s, color, k) for k in (1, 2, 3)]
            others += [rs_pair(s)] if s == 1 else [rs_pair(s), rs_first(s)]
        drain(rss.at[0], rings)
        drain(rss.at[1], others)

    def g_copy(i, buf, step, recv):
        if step == 0:
            piece, dev = buf.at[l, oc if recv else c], core_peer
        elif step == 1:
            piece, dev = buf.at[ol if recv else l, c], line_peer
        else:
            piece, dev = buf.at[ol, oc if recv else c], core_peer
        return copy(piece, piece, gs.at[i], gr.at[i, step], dev)

    def gather_start(i, buf):
        g_copy(i, buf, 1, False).start()
        g_copy(i, buf, 0, False).start()

    def gather_relay(i, buf):
        g_copy(i, buf, 1, True).wait_recv()
        g_copy(i, buf, 2, False).start()

    def gather_wait(i, buf, step):
        g_copy(i, buf, step, True).wait_recv()

    def gather_sent(i, buf):
        drain(gs.at[i], [g_copy(i, buf, step, False) for step in range(3)])

    def s_copy(i, step):
        src, dev = (
            (PS.at[ol, oc], core_peer),
            (SX, line_peer),
            (PS.at[l, oc], core_peer),
        )[step]
        return copy(src, RX.at[i % 2, step], ss.at[i], sr.at[i, step], dev)

    def scatter_far(i, compute):
        compute(ol)
        s_copy(i, 0).start()
        s_copy(i, 0).wait_recv()
        SX[...] = bf(f32(PS[ol, c]) + f32(RX[i % 2, 0]))
        s_copy(i, 1).start()

    def scatter_near(i, compute):
        compute(l)
        s_copy(i, 2).start()

    def scatter_result(i):
        s_copy(i, 2).wait_recv()
        s_copy(i, 1).wait_recv()
        total = f32(PS[l, c]) + f32(RX[i % 2, 2]) + f32(RX[i % 2, 1])
        drain(ss.at[i], [s_copy(i, step) for step in range(3)])
        return total

    def pair_rows(i):
        return pl.ds(pl.multiple_of(i * pair, 128), pair)

    def back_product(left, s, lo, n):
        def compute(i):
            @pl.loop(0, nz)
            def _(b):
                w = W[s, b, :, :, pl.ds(lo, n)].reshape(slab, n)
                at = pl.ds(pl.multiple_of(b * slab, 128), slab)
                PS[i, :, :, at] = bf(dot(left(i), w, 1, 1)).reshape(2, pair // 2, slab)
        return compute

    def two(buf, i):
        return buf[i].reshape(pair, buf.shape[-1])

    def all_rows(buf, at):
        return buf[:, :, :, at].reshape(seq, -1)

    def turn(buf):
        @pl.loop(0, nz)
        def _(b):
            AT[b] = all_rows(buf, pl.ds(pl.multiple_of(b * slab, 128), slab)).T

    def grad_turned(s, right, start, stop, tile):
        @pl.loop(0, (stop - start) // tile)
        def _(t):
            at = pl.ds(pl.multiple_of(start + t * tile, 128), tile)
            value = dot(AT[...].reshape(width, seq), right(at)) * q_s
            parts[s][:, :, :, at] = bf(value).reshape(nz, ny, nh * rows, tile)

    def grad_product(s, left, right, n, lo):
        @pl.loop(0, nz)
        def _(b):
            a = all_rows(left, pl.ds(pl.multiple_of(b * slab, 128), slab)).T
            value = dot(a, right) * q_s
            parts[s][b, :, :, pl.ds(lo, n)] = bf(value).reshape(ny, nh * rows, n)

    peers = [{"z": zz(k)} for k in range(1, 4)] + [{"y": yy(k)} for k in range(1, 4)]
    peers += [pair_peer, core_peer, line_peer, {"l": ol, "c": oc}]
    barrier = pltpu.get_barrier_semaphore()
    for dev in peers:
        pl.semaphore_signal(barrier, inc=1, device_id=dev, device_id_type=pl.DeviceIdType.MESH)
    outs = [(fin, fin_out), (dxin, dx_out)] + [(grads.at[i], grads_out.at[i]) for i in range(3)]
    results = [pltpu.make_async_copy(src, dst, out_sem.at[i]) for i, (src, dst) in enumerate(outs)]
    mine = at_rows(h)
    moves = [
        (wq_in.at[i, :, pl.ds(hd * HEAD_DIM, HEAD_DIM)], W.at[0, z, y, mine, pl.ds((3 * hd + i) * HEAD_DIM, HEAD_DIM)])
        for i in range(3) for hd in range(heads)
    ]
    moves += [(wo_in, W.at[0, z, y, mine, pl.ds(3 * own, own)])]
    moves += [(wi_in, W.at[1, z, y, mine]), (wb_in, W.at[2, z, y, mine])]
    moves += [(tok_in, tok), (og_in, og), (mod_in, mod)]
    count = len(moves) - 3
    loads = [pltpu.make_async_copy(src, dst, in_sem.at[max(i - count + 1, 0)]) for i, (src, dst) in enumerate(moves)]
    for load in loads:
        load.start()
    drain(in_sem.at[0], [copy(src, dst, None, None, None) for src, dst in moves[:count]])
    pl.semaphore_wait(barrier, len(peers))

    for s in range(3):
        ag_pair(s, False).start()
    for s in (0, 1):
        ag_mid_start(s, 0, (2,))
        ag_mid_start(s, 0)
    for load in loads[count:]:
        load.wait()
    m = [mod[i] for i in range(6)]
    n1, r1 = normalize(f32(tok[...]))
    A1[l, c] = bf(n1 * (1.0 + m[1]) + m[0])
    DM[l, c] = bf(m[5] * f32(og[...]))
    gather_start(0, A1)
    ag_last_start(0, (2,))
    ag_mid_start(0, 1)
    ag_mid_start(1, 1)
    ag_last_start(1, (2,))
    ag_relay_start(0, (2,))
    ag_hop_start(1)
    ag_last_start(0)
    ag_relay_start(1, (2,))
    ag_final_start(0)
    gather_relay(0, A1)
    gather_start(1, DM)
    ag_relay_start(0)
    ag_mid_start(2, 0)
    ag_mid_start(2, 1)
    ag_last_start(1)
    ag_final_start(1)
    gather_wait(0, A1, 0)
    gather_wait(0, A1, 2)

    ag_wait(0)

    @pl.loop(0, 3)
    def _(t):
        at = pl.ds(pl.multiple_of(t * own, 128), own)
        w = W[0, :, :, :, at].reshape(width, own)
        QKV[:, at] = bf(dot(A1[...].reshape(seq, width), w))

    ag_hop_start(2)

    def head(hd, i):
        return pl.ds(pl.multiple_of((3 * hd + i) * HEAD_DIM, 128), HEAD_DIM)

    def wide(hd):
        return pl.ds(pl.multiple_of(hd * HEAD_DIM, 128), HEAD_DIM)

    @pl.loop(0, heads)
    def _(hd):
        s = dot(QKV[:, head(hd, 0)], QKV[:, head(hd, 1)], 1, 1) * scale
        e = jnp.exp(s - jnp.max(s, axis=-1, keepdims=True))
        p = bf(e * (1.0 / jnp.sum(e, axis=-1, keepdims=True)))
        PR[hd] = p
        O[:, wide(hd)] = bf(dot(p, QKV[:, head(hd, 2)]))

    out_product = back_product(lambda i: O[pair_rows(i), :], 0, 3 * own, own)
    ag_final(0, True).wait_recv()
    scatter_far(0, out_product)
    scatter_near(0, out_product)
    ag_relay_start(1)
    ag_last_start(2)
    mid = f32(tok[...]) + m[2] * scatter_result(0)
    MID[...] = mid
    n2, r2 = normalize(mid)
    A2[l, c] = bf(n2 * (1.0 + m[4]) + m[3])
    gather_start(2, A2)

    tile = 256

    def hidden(i):
        @pl.loop(0, width // (2 * tile))
        def _(t):
            for j in (0, 1):
                at = pl.ds(pl.multiple_of((2 * t + j) * tile, 128), tile)
                g, d = gelu_pair(dot(two(A2, i), W[1, :, :, :, at].reshape(width, tile)))
                GG[i, :, :, at] = bf(g).reshape(2, pair // 2, tile)
                DU[i, :, :, at] = bf(d).reshape(2, pair // 2, tile)

    gather_relay(1, DM)
    gather_wait(1, DM, 0)
    gather_wait(1, DM, 2)
    turn(DM)
    ag_wait(1)
    ag_final(1, True).wait_recv()
    gather_wait(2, A2, 0)
    hidden(l)
    ag_relay_start(2)
    gather_relay(2, A2)
    gather_wait(2, A2, 2)
    hidden(ol)
    for lo, hi in ((2 * side, width), (0, half), (half, 2 * side)):
        grad_turned(0, lambda at: all_rows(GG, at), lo, hi, tile)
        if lo == 2 * side:
            rs_first(0).start()
        else:
            rs_start(0, (0,) if lo == 0 else (1,))
    ag_wait(2)

    @pl.loop(0, width // tile)
    def _(t):
        at = pl.ds(pl.multiple_of(t * tile, 128), tile)
        dg = dot(DM[...].reshape(seq, width), W[2, :, :, :, at].reshape(width, tile))
        DU[:, :, :, at] = bf(f32(DU[:, :, :, at]) * dg.reshape(2, 2, pair // 2, tile))

    in_back = back_product(lambda i: two(DU, i), 1, 0, width)
    scatter_far(1, in_back)
    rs_combine(0)
    turn(A2)
    grad_turned(1, lambda at: all_rows(DU, at), 0, half, tile)
    rs_second(0)
    rs_start(1, (0,))
    grad_turned(1, lambda at: all_rows(DU, at), half, width, tile)
    rs_start(1, (1,))
    scatter_near(1, in_back)
    e2 = scatter_result(1) * (1.0 + m[4])
    n2, r2 = normalize(MID[...])
    dmid = f32(og[...]) + norm_back(n2, r2, e2)
    DX[...] = dmid
    DA[l, c] = bf(m[2] * dmid)
    gather_start(3, DA)

    ff_back = back_product(lambda i: two(GG, i), 2, 0, width)
    scatter_far(2, ff_back)
    rs_combine(0, (2,))
    rs_combine(1)
    scatter_near(2, ff_back)
    turn(A1)
    rs_mid_start(0)
    gather_relay(3, DA)
    gather_wait(3, DA, 0)
    gather_wait(3, DA, 2)

    DO[...] = bf(dot(DA[...].reshape(seq, width), W[0, :, :, :, pl.ds(3 * own, own)].reshape(width, own)))
    ag_sent(1)
    grad_product(2, DA, O[...], own, full)
    rs_first(2).start()
    rs_start(2)

    for hd in range(heads):
        do = DO[:, wide(hd)]
        p = PR[hd]
        t = f32(p) * dot(do, QKV[:, head(hd, 2)], 1, 1)
        ds = bf(scale * (t - f32(p) * jnp.sum(t, axis=-1, keepdims=True)))
        DQKV[:, head(hd, 0)] = bf(dot(ds, QKV[:, head(hd, 1)]))
        DQKV[:, head(hd, 1)] = bf(dot(ds.T, QKV[:, head(hd, 0)]))
        DQKV[:, head(hd, 2)] = bf(dot(p.T, do))
        grad_turned(3 + hd, lambda at: DQKV[:, at], hd * own, (hd + 1) * own, own)
        rs_first(3 + hd).start()
        rs_start(3 + hd)

    qkv_back = back_product(lambda i: DQKV[pair_rows(i), :], 0, 0, 3 * own)
    fin[...] = bf(MID[...] + m[5] * scatter_result(2))
    results[0].start()
    rs_hop_combine(0)
    rs_combine(2)
    rs_mid_start(1)
    rs_combine(3)
    qkv_back = back_product(lambda i: DQKV[pair_rows(i), :], 0, 0, 3 * own)
    scatter_far(3, qkv_back)
    rs_second(2)
    rs_combine(4)
    scatter_near(3, qkv_back)
    rs_second(3)
    rs_mid_start(0, (2,))
    rs_pair_start(0)
    rs_combine(5)
    rs_second(4)
    rs_mid_start(2)
    rs_combine(2, (2,))
    rs_hop_combine(1)
    rs_second(5)
    rs_combine(3, (2,))
    rs_mid_start(3)
    rs_combine(4, (2,))
    rs_mid_start(4)
    rs_mid_start(2, (2,))
    rs_mid_start(3, (2,))
    rs_mid_start(5)
    rs_combine(5, (2,))
    rs_pair_start(2)
    rs_pair_start(1)
    rs_finish_third(0)
    rs_mid_start(4, (2,))
    rs_pair_start(3)
    rs_finish(0)
    results[4].start()
    e1 = scatter_result(3) * (1.0 + m[1])
    n1, r1 = normalize(f32(tok[...]))
    dxin[...] = DX[...] + norm_back(n1, r1, e1)
    results[1].start()
    rs_pair_start(4)
    rs_mid_start(5, (2,))
    rs_pair_start(5)
    rs_finish(1)
    results[3].start()
    for s in range(2, sections):
        rs_finish_third(s)
    for s in range(2, sections):
        rs_finish(s)
    results[2].start()
    rs_sent()
    ag_sent(0)
    ag_sent(2)
    for i, buf in enumerate((A1, DM, A2, DA)):
        gather_sent(i, buf)
    for result in results:
        result.wait()


def place(fin, dx, grads, o_fin, o_dx, o_qkv, o_out, o_in, o_back, v_fin, v_dx, v_grads, sem_in, sem_out):
    own = o_out.shape[1]
    heads = own // HEAD_DIM
    sources = (
        (dx, v_dx), (grads.at[2], v_grads.at[2]), (grads.at[1], v_grads.at[1]),
        (fin, v_fin), (grads.at[0], v_grads.at[0]),
    )
    pieces = [
        (v_grads.at[0, :, pl.ds((3 * hd + i) * HEAD_DIM, HEAD_DIM)], o_qkv.at[i, :, pl.ds(hd * HEAD_DIM, HEAD_DIM)])
        for i in range(3) for hd in range(heads)
    ]
    pieces.append((v_grads.at[0, :, pl.ds(3 * own, own)], o_out))
    targets = (
        [(v_dx, o_dx.at[0])], [(v_grads.at[2], o_back)], [(v_grads.at[1], o_in.at[0])],
        [(v_fin, o_fin.at[0])], pieces,
    )
    loads = [pltpu.make_async_copy(a, b, sem_in.at[i]) for i, (a, b) in enumerate(sources)]
    for load in loads:
        load.start()
    stores = []
    for load, pairs in zip(loads, targets):
        load.wait()
        for a, b in pairs:
            store = pltpu.make_async_copy(a, b, sem_out.at[len(stores)])
            store.start()
            stores.append(store)
    for store in stores:
        store.wait()


def step(dims, tokens, modulation, w_qkv, w_out, w_in, w_back, out_grad):
    nz, ny, nh = dims
    count, width = tokens.shape[1:]
    rows, own, ff = w_qkv.shape[1], w_qkv.shape[3], w_in.shape[2]
    assert ff == width and 4 * own == width
    seq = 4 * count
    heads = own // HEAD_DIM
    big = (nz, ny, nh * rows)
    half = width // 2
    vmem = pltpu.VMEM
    dma = pltpu.SemaphoreType.DMA
    tokens_buf = vmem((2, 2, count, width), BF)
    scratch = [
        vmem((3, *big, width), BF),
        vmem((2, *big, width), BF),
        vmem((3, 3, 4, nh * rows, half), BF),
        vmem((3, 3, 4, nh * rows, half), BF),
        vmem((3, 3, nh * rows, half), BF),
        vmem((3, 3, nh * rows, half), BF),
        vmem((3, rows, width), BF),
        vmem((3, 4, rows, 256), BF),
        vmem((3, rows, 256), BF),
        vmem((nz, ny, rows, 256), BF),
        vmem((1 + heads, nz, ny, rows, own // 3), BF),
        *[tokens_buf] * 6,
        vmem((seq, 3 * own), BF),
        vmem((seq, 3 * own), BF),
        vmem((seq, own), BF),
        vmem((seq, own), BF),
        vmem((heads, seq, seq), BF),
        tokens_buf,
        vmem((2, 3, count, width), BF),
        vmem((count, width), BF),
        vmem((count, width), F32),
        vmem((count, width), F32),
        vmem((nz, ny * nh * rows, seq), BF),
        vmem((count, width), BF),
        vmem((6, 1, width), F32),
        vmem((count, width), BF),
        vmem((count, width), BF),
        vmem((count, width), F32),
        vmem((3, rows, width), F32),
        dma((4,)),
        dma((5,)),
        dma((3, 5)), dma((3, 2)), dma((3, 3, 2)), dma((3, 3)), dma((3, 2)), dma((3, 2)),
        dma((2,)), dma((3 + heads, 3, 2)), dma((3 + heads, 3)), dma((3 + heads,)), dma((3 + heads,)),
        dma((2, 2, 3)),
        dma((4,)), dma((4, 3)), dma((4,)), dma((4, 3)),
    ]
    whole = pl.BlockSpec(memory_space=pl.ANY)
    final, dx, grads = pl.pallas_call(
        functools.partial(kernel, dims),
        out_shape=(
            jax.ShapeDtypeStruct((count, width), BF),
            jax.ShapeDtypeStruct((count, width), F32),
            jax.ShapeDtypeStruct((3, rows, width), F32),
        ),
        in_specs=[whole] * 7,
        out_specs=(whole,) * 3,
        scratch_shapes=scratch,
        compiler_params=pltpu.CompilerParams(
            collective_id=0, has_side_effects=True, vmem_limit_bytes=67043328
        ),
    )(
        tokens[0], modulation[0].transpose(1, 0, 2), w_qkv[0].transpose(1, 0, 2), w_out[0].T,
        w_in[0], w_back[0].T, out_grad[0],
    )
    final, dx, qkv, out, inner, back = pl.pallas_call(
        place,
        out_shape=(
            jax.ShapeDtypeStruct((1, count, width), BF),
            jax.ShapeDtypeStruct((1, count, width), F32),
            jax.ShapeDtypeStruct((3, rows, own), F32),
            jax.ShapeDtypeStruct((rows, own), F32),
            jax.ShapeDtypeStruct((1, rows, width), F32),
            jax.ShapeDtypeStruct((rows, width), F32),
        ),
        in_specs=[whole] * 3,
        out_specs=(whole,) * 6,
        scratch_shapes=[
            vmem((count, width), BF), vmem((count, width), F32), vmem((3, rows, width), F32),
            dma((5,)), dma((5 + 3 * heads,)),
        ],
    )(final, dx, grads)
    return final, dx, qkv.transpose(1, 0, 2)[None], out.T[None], inner, back.T[None]


def solution(mesh):
    dims = (4, 4, 2)
    assert mesh.shape["fsdp"] == 32 and mesh.shape["sp"] == 4
    torus = Mesh(mesh.devices.reshape(*dims, 2, 2), AXES)
    fsdp, sp = AXES[:3], AXES[3:]
    placed = (
        P(fsdp, sp, None),
        P(fsdp, None, None, None),
        P(None, fsdp, None, sp),
        P(None, sp, fsdp),
        P(None, fsdp, sp),
        P(None, sp, fsdp),
        P(fsdp, sp, None),
    )
    return jax.shard_map(
        functools.partial(step, dims),
        mesh=torus,
        in_specs=placed,
        out_specs=(placed[0], *placed[:1], *placed[2:6]),
        check_vma=False,
    )
```

```python
import functools
import math

import jax
import jax.numpy as jnp
from jax import lax
from jax.experimental import pallas as pl
from jax.experimental.pallas import tpu as pltpu
from jax.sharding import Mesh
from jax.sharding import PartitionSpec as P

HEAD_DIM = 128
LN_EPS = 1e-06
TEMPER = 2.5
BF = jnp.bfloat16
F32 = jnp.float32
AXES = ("z", "y", "h", "l", "c")


def bf(x):
    return x.astype(BF)


def f32(x):
    return x.astype(F32)


def dot(a, b, ca=1, cb=0):
    return lax.dot_general(a, b, (((ca,), (cb,)), ((), ())), preferred_element_type=F32)


def normalize(x):
    d = x - jnp.mean(x, axis=-1, keepdims=True)
    r = lax.rsqrt(jnp.mean(d * d, axis=-1, keepdims=True) + LN_EPS)
    return d * r, r


def norm_back(n, r, e):
    return r * (e - jnp.mean(e, axis=-1, keepdims=True) - n * jnp.mean(e * n, axis=-1, keepdims=True))


def gelu_pair(u):
    k0 = math.sqrt(2.0 / math.pi)
    s = u * u
    t = jnp.tanh(k0 * u * (1.0 + 0.044715 * s))
    g = 0.5 * u * (1.0 + t)
    d = 0.5 * (1.0 + t) + 0.5 * k0 * u * (1.0 - t * t) * (1.0 + 3.0 * 0.044715 * s)
    return g, d


class copy:
    def __init__(self, src, dst, ssem, rsem, dev):
        self.src, self.rest = src, (dst, ssem, rsem, dev)

    def made(self):
        dst, ssem, rsem, dev = self.rest
        return pltpu.make_async_remote_copy(
            src_ref=self.src, dst_ref=dst, send_sem=ssem, recv_sem=rsem,
            device_id=dev, device_id_type=pl.DeviceIdType.MESH,
        )

    def start(self):
        self.made().start()

    def wait_send(self):
        self.made().wait_send()

    def wait_recv(self):
        self.made().wait_recv()


def kernel(
    dims, tok_in, mod_in, wq_in, wo_in, wi_in, wb_in, og_in, fin_out, dx_out, grads_out,
    W, G, R1A, R1B, R2A, R2B, R3, R1C, R2C, R4, R4H, A1, A2, DM, DA, GG, DU, QKV, DQKV, O, DO, PR, PS, RX, SX, MID, DX, AT,
    tok, mod, og, fin, dxin, grads, in_sem, out_sem, ags, a1r, a2r, a3r, a4r, a5r, rss, r1r, r2r, r3r, r4r, r5r, gs, gr, ss, sr,
):
    nz, ny, nh = dims
    z, y, h, l, c = (lax.axis_index(a) for a in AXES)
    ol, oc = 1 - l, 1 - c
    rows, width = wi_in.shape
    half = width // 2
    seq = QKV.shape[0]
    pair = seq // 2
    own = QKV.shape[1] // 3
    heads = own // HEAD_DIM
    slab = ny * nh * rows
    scale = TEMPER / math.sqrt(HEAD_DIM)
    q_s = 1.0 / math.sqrt(seq * nz * ny * nh)
    cols = (pl.ds(0, half), pl.ds(half, half))

    def drain(sem, moves):
        units = sum(math.prod(move.src.shape) for move in moves) // (rows * 128)
        for q, height in ((1, rows), (1, nh * rows), (3, nh * rows)):
            for i in range(1, nz + 1):
                for j in range(1, ny + 1):
                    n, rest = divmod(units * rows, q * height * i * j)
                    if rest == 0 and n <= width // 128:
                        view = W.at[pl.ds(0, q), pl.ds(0, i), pl.ds(0, j), pl.ds(0, height), pl.ds(0, n * 128)]
                        pltpu.make_async_copy(view, view, sem).wait()
                        return
        raise ValueError(units)

    def zz(k):
        return lax.rem(z + k + nz, nz)

    def yy(k):
        return lax.rem(y + k + ny, ny)

    def hh(k):
        return lax.rem(h + k + nh, nh)

    def at_rows(i):
        return pl.ds(pl.multiple_of(i * rows, 16), rows)

    core_peer = {"c": oc}
    line_peer = {"l": ol}
    pair_peer = {"h": 1 - h}
    halves = (pl.ds(0, 2), pl.ds(2, 2))

    def last(color, k):
        return {"z": zz(k)} if color == 0 else {"y": yy(k)}

    def mid_dev(color, k):
        return last(1 - color, k)

    strip = 256
    side = (width - strip) // 2
    ag_cols = ((pl.ds(0, side), pl.ds(side, side), pl.ds(2 * side, strip)),) * 2 + (cols,)
    every = slice(None)

    def slab_at(buf, color, k, at, part=every, row=every):
        return buf.at[zz(k), part, row, at] if color == 0 else buf.at[part, yy(k), row, at]

    def line_at(buf, color, k, at, row=every):
        return buf.at[z, yy(k), row, at] if color == 0 else buf.at[zz(k), y, row, at]

    def line_of(s, color):
        return color if color < 2 else s % 2

    def row_of(color):
        return every if color < 2 else at_rows(h)

    def direct(s, color):
        return s == 0 or color == 2

    def ag_pair(s, recv):
        piece = W.at[s, z, y, at_rows(1 - h if recv else h), pl.ds(0, 2 * side if s < 2 else width)]
        return copy(piece, piece, ags.at[s, 0], a1r.at[s, 0], pair_peer)

    def ag_final(s, recv):
        piece = W.at[s, :, :, at_rows(1 - h if recv else h), ag_cols[s][2]]
        return copy(piece, piece, ags.at[s, 1], a1r.at[s, 1], pair_peer)

    def ag_mid(s, color, k, which, recv):
        line = line_of(s, color)
        piece = line_at(W.at[s], line, -k if recv else 0, ag_cols[s][color], at_rows(h if which == 0 else 1 - h))
        side_of = 0 if direct(s, color) else (k - 1) // 2
        return copy(piece, piece, ags.at[s, 2 + 2 * (color // 2)], a2r.at[s, color, side_of], mid_dev(line, k))

    def ag_hop(s, color, d, recv):
        k = 1 - 2 * d
        piece = line_at(W.at[s], color, 2 if recv else -k, ag_cols[s][color], at_rows(d))
        return copy(piece, piece, ags.at[s, 2], a5r.at[s, color], mid_dev(color, k))

    def ag_last(s, color, d, j, recv):
        k, line = 1 - 2 * d, line_of(s, color)
        part = halves[d if j == 0 else 1 - d]
        piece = slab_at(W.at[s], line, -k if recv else 0, ag_cols[s][color], part, row_of(color))
        arrived = a3r.at[s, color] if j == 0 else a4r.at[s, color // 2]
        return copy(piece, piece, ags.at[s, 3 + color // 2], arrived, last(line, k))

    def ag_relay(s, color, d, recv):
        k, line = 1 - 2 * d, line_of(s, color)
        piece = slab_at(W.at[s], line, 2 if recv else -k, ag_cols[s][color], halves[d], row_of(color))
        return copy(piece, piece, ags.at[s, 3 + color // 2], a4r.at[s, color // 2], last(line, k))

    def ag_mid_start(s, which, colors=(0, 1)):
        if which:
            ag_pair(s, True).wait_recv()
        for k in (1, 3, 2) if direct(s, colors[0]) else (1, 3):
            for color in colors:
                ag_mid(s, color, k, which, False).start()

    def ag_hop_start(s):
        for color in (0, 1):
            for d in (0, 1):
                drain(a2r.at[s, color, d], [ag_mid(s, color, 1 + 2 * d, which, True) for which in (0, 1)])
                ag_hop(s, color, d, False).start()

    def ag_last_start(s, colors=(0, 1)):
        for color in colors:
            if direct(s, color):
                sides = (0, 1) if color < 2 else (0,)
                drain(a2r.at[s, color, 0], [ag_mid(s, color, k, which, True) for which in sides for k in (1, 2, 3)])
            else:
                drain(a5r.at[s, color], [ag_hop(s, color, d, True) for d in (0, 1)])
        for j in (0, 1):
            for color in colors:
                for d in (0, 1):
                    ag_last(s, color, d, j, False).start()

    def ag_relay_start(s, colors=(0, 1)):
        for color in colors:
            drain(a3r.at[s, color], [ag_last(s, color, d, 0, True) for d in (0, 1)])
            for d in (0, 1):
                ag_relay(s, color, d, False).start()

    def late(s, colors):
        return [move for color in colors for d in (0, 1)
                for move in (ag_last(s, color, d, 1, True), ag_relay(s, color, d, True))]

    def ag_final_start(s):
        drain(a4r.at[s, 1], late(s, (2,)))
        ag_final(s, False).start()

    def ag_wait(s):
        drain(a4r.at[s, 0], late(s, (0, 1)))

    def ag_sent(s):
        ag_pair(s, False).wait_send()
        middle = [ag_mid(s, color, k, which, False) for color in (0, 1) for which in (0, 1)
                  for k in ((1, 2, 3) if direct(s, 0) else (1, 3))]
        if not direct(s, 0):
            middle += [ag_hop(s, color, d, False) for color in (0, 1) for d in (0, 1)]
        drain(ags.at[s, 2], middle)

        def ends(colors):
            return [ag_last(s, color, d, j, False) for color in colors for d in (0, 1) for j in (0, 1)] + [
                ag_relay(s, color, d, False) for color in colors for d in (0, 1)]

        drain(ags.at[s, 3], ends((0, 1)))
        if s < 2:
            ag_final(s, False).wait_send()
            drain(ags.at[s, 4], [ag_mid(s, 2, k, 0, False) for k in (1, 2, 3)] + ends((2,)))

    R1 = (R1A, R1B)
    R2 = (R2A, R2B)
    full = 3 * own
    sections = 3 + heads
    parts = (G.at[0], G.at[1]) + (W.at[1],) * (1 + heads)
    slots = (2, 1) + (0,) * (1 + heads)
    lead = pl.ds(0, side)
    local_cols = [(lead, lead), (cols[0], cols[0])]
    grad_cols = [ag_cols[0], cols]
    pair_cols = [pl.ds(0, 2 * side), pl.ds(0, width)]
    third = own // 3
    for i, start in enumerate([full] + [hd * own for hd in range(heads)]):
        at = pl.ds(i * third, third)
        local_cols.append((at, at))
        grad_cols.append(tuple(pl.ds(start + j * third, third) for j in range(3)))
        pair_cols.append(pl.ds(start, 2 * third))

    spare = {2: (1, 4), 3: (1, 5), 4: (0, 4), 5: (0, 5)}

    def rs_line(s, color):
        return color if color < 2 else (0, None, 0, 1, 0, 1)[s]

    def spare_at(s):
        return pl.ds(spare[s][1] * third, third)

    def r1_at(s, color):
        if color < 2:
            return R1[color].at[slots[s], :, :, :, local_cols[s][color]]
        return R1C if s == 0 else R1[spare[s][0]].at[0, :, :, pl.ds(0, rows), spare_at(s)]

    def r2_at(s, color):
        if color < 2:
            return R2[color].at[slots[s], :, :, local_cols[s][color]]
        return R2C if s == 0 else R2[spare[s][0]].at[0, :, pl.ds(0, rows), spare_at(s)]

    def r4_at(s):
        return R4 if s == 0 else R4H.at[s - 2]

    def rs_first(s):
        src = parts[s].at[:, :, at_rows(1 - h), grad_cols[s][2]]
        return copy(src, r4_at(s), rss.at[1], r4r.at[s], pair_peer)

    def rs_ring(s, color, d, kind):
        k, line = 1 - 2 * d, rs_line(s, color)
        part = halves[1 - d if kind == 1 else d]
        src = slab_at(parts[s], line, 2 if kind == 0 else k, grad_cols[s][color], part, row_of(color))
        dst = r1_at(s, color).at[2 if kind == 0 else d, part]
        arrived = r1r.at[s, color, min(kind, 1)]
        return copy(src, dst, rss.at[0], arrived, last(line, k))

    def rs_mid(s, color, k):
        line = rs_line(s, color)
        return copy(
            line_at(parts[s], line, k, grad_cols[s][color], row_of(color)), r2_at(s, color).at[k - 1],
            rss.at[1], r2r.at[s, color], mid_dev(line, k),
        )

    def ringed(s, color):
        return s < 2 and color < 2

    def rs_hop(s, color, d, kind):
        k = 1 - 2 * d
        row = at_rows(1 - d if kind == 1 else d)
        src = line_at(parts[s], color, 2 if kind == 0 else k, grad_cols[s][color], row)
        dst = r2_at(s, color).at[2 if kind == 0 else d, row]
        arrived = r5r.at[s, color, d if kind == 0 else 2]
        return copy(src, dst, rss.at[1], arrived, mid_dev(color, k))

    def rs_hop_combine(s):
        for color in (0, 1):
            for d in (0, 1):
                rs_hop(s, color, d, 0).wait_recv()
                k = 1 - 2 * d
                at = (z, yy(k)) if color == 0 else (zz(k), y)
                at = (*at, at_rows(d), grad_cols[s][color])
                parts[s][at] = bf(f32(parts[s][at]) + f32(r2_at(s, color)[2, d * rows : (d + 1) * rows]))
                rs_hop(s, color, d, 2).start()

    def rs_pair(s):
        return copy(
            parts[s].at[z, y, at_rows(1 - h), pair_cols[s]], R3.at[slots[s], :, pair_cols[s]],
            rss.at[1], r3r.at[s], pair_peer,
        )

    def rs_second(s):
        rs_first(s).wait_recv()

        @pl.loop(0, nz)
        def _(i):
            at = (i, every, at_rows(h), grad_cols[s][2])
            parts[s][at] = bf(f32(parts[s][at]) + f32(r4_at(s)[i]))

        rs_start(s, (2,))

    def rs_start(s, colors=(0, 1)):
        for kind in (0, 1):
            for color in colors:
                for d in (0, 1):
                    rs_ring(s, color, d, kind).start()

    def rs_combine(s, colors=(0, 1)):
        for color in colors:
            line = rs_line(s, color)
            drain(r1r.at[s, color, 0], [rs_ring(s, color, d, 0) for d in (0, 1)])
            for d in (0, 1):
                k = 1 - 2 * d

                @pl.loop(2 * d, 2 * d + 2)
                def _(i):
                    at = (zz(k), i) if line == 0 else (i, yy(k))
                    at = (*at, row_of(color), grad_cols[s][color])
                    parts[s][at] = bf(f32(parts[s][at]) + f32(r1_at(s, color)[2, i]))

                rs_ring(s, color, d, 2).start()

    def rs_mid_start(s, colors=(0, 1)):
        for color in colors:
            line = rs_line(s, color)
            drain(r1r.at[s, color, 1], [rs_ring(s, color, d, kind) for d in (0, 1) for kind in (1, 2)])

            @pl.loop(0, 4)
            def _(i):
                at = (z, i) if line == 0 else (i, y)
                at = (*at, row_of(color), grad_cols[s][color])
                total = f32(parts[s][at])
                for d in (0, 1):
                    total = total + f32(r1_at(s, color)[d, i])
                parts[s][at] = bf(total)

            if ringed(s, color):
                for kind in (0, 1):
                    for d in (0, 1):
                        rs_hop(s, color, d, kind).start()
            else:
                for k in (1, 3, 2):
                    rs_mid(s, color, k).start()

    def rs_total(s, color):
        if ringed(s, color):
            drain(r5r.at[s, color, 2], [rs_hop(s, color, d, kind) for d in (0, 1) for kind in (1, 2)])
        else:
            drain(r2r.at[s, color], [rs_mid(s, color, k) for k in (1, 2, 3)])
        total = f32(parts[s][z, y, row_of(color), grad_cols[s][color]])
        for k in range(2 if ringed(s, color) else 3):
            total = total + f32(r2_at(s, color)[k])
        return total

    def rs_pair_start(s):
        for color in (0, 1):
            parts[s][z, y, every, grad_cols[s][color]] = bf(rs_total(s, color))
        rs_pair(s).start()

    def rs_finish(s):
        rs_pair(s).wait_recv()
        at = pair_cols[s]
        grads[slots[s], :, at] = f32(parts[s][z, y, at_rows(h), at]) + f32(R3[slots[s], :, at])

    def rs_finish_third(s):
        grads[slots[s], :, grad_cols[s][2]] = rs_total(s, 2)

    def rs_sent():
        rings, others = [], []
        for s in range(sections):
            for color in (0, 1) if s == 1 else (0, 1, 2):
                rings += [rs_ring(s, color, d, kind) for d in (0, 1) for kind in (0, 1, 2)]
                if ringed(s, color):
                    others += [rs_hop(s, color, d, kind) for d in (0, 1) for kind in (0, 1, 2)]
                else:
                    others += [rs_mid(s, color, k) for k in (1, 2, 3)]
            others += [rs_pair(s)] if s == 1 else [rs_pair(s), rs_first(s)]
        drain(rss.at[0], rings)
        drain(rss.at[1], others)

    def g_copy(i, buf, step, recv):
        if step == 0:
            piece, dev = buf.at[l, oc if recv else c], core_peer
        elif step == 1:
            piece, dev = buf.at[ol if recv else l, c], line_peer
        else:
            piece, dev = buf.at[ol, oc if recv else c], core_peer
        return copy(piece, piece, gs.at[i], gr.at[i, step], dev)

    def gather_start(i, buf):
        g_copy(i, buf, 1, False).start()
        g_copy(i, buf, 0, False).start()

    def gather_relay(i, buf):
        g_copy(i, buf, 1, True).wait_recv()
        g_copy(i, buf, 2, False).start()

    def gather_wait(i, buf, step):
        g_copy(i, buf, step, True).wait_recv()

    def gather_sent(i, buf):
        drain(gs.at[i], [g_copy(i, buf, step, False) for step in range(3)])

    def s_copy(i, step):
        src, dev = (
            (PS.at[ol, oc], core_peer),
            (SX, line_peer),
            (PS.at[l, oc], core_peer),
        )[step]
        return copy(src, RX.at[i % 2, step], ss.at[i], sr.at[i, step], dev)

    def scatter_far(i, compute):
        compute(ol)
        s_copy(i, 0).start()
        s_copy(i, 0).wait_recv()
        SX[...] = bf(f32(PS[ol, c]) + f32(RX[i % 2, 0]))
        s_copy(i, 1).start()

    def scatter_near(i, compute):
        compute(l)
        s_copy(i, 2).start()

    def scatter_result(i):
        s_copy(i, 2).wait_recv()
        s_copy(i, 1).wait_recv()
        total = f32(PS[l, c]) + f32(RX[i % 2, 2]) + f32(RX[i % 2, 1])
        drain(ss.at[i], [s_copy(i, step) for step in range(3)])
        return total

    def pair_rows(i):
        return pl.ds(pl.multiple_of(i * pair, 128), pair)

    def back_product(left, s, lo, n):
        def compute(i):
            @pl.loop(0, nz)
            def _(b):
                w = W[s, b, :, :, pl.ds(lo, n)].reshape(slab, n)
                at = pl.ds(pl.multiple_of(b * slab, 128), slab)
                PS[i, :, :, at] = bf(dot(left(i), w, 1, 1)).reshape(2, pair // 2, slab)
        return compute

    def two(buf, i):
        return buf[i].reshape(pair, buf.shape[-1])

    def all_rows(buf, at):
        return buf[:, :, :, at].reshape(seq, -1)

    def turn(buf):
        @pl.loop(0, nz)
        def _(b):
            AT[b] = all_rows(buf, pl.ds(pl.multiple_of(b * slab, 128), slab)).T

    def grad_turned(s, right, start, stop, tile):
        @pl.loop(0, (stop - start) // tile)
        def _(t):
            at = pl.ds(pl.multiple_of(start + t * tile, 128), tile)
            value = dot(AT[...].reshape(width, seq), right(at)) * q_s
            parts[s][:, :, :, at] = bf(value).reshape(nz, ny, nh * rows, tile)

    def grad_product(s, left, right, n, lo):
        @pl.loop(0, nz)
        def _(b):
            a = all_rows(left, pl.ds(pl.multiple_of(b * slab, 128), slab)).T
            value = dot(a, right) * q_s
            parts[s][b, :, :, pl.ds(lo, n)] = bf(value).reshape(ny, nh * rows, n)

    peers = [{"z": zz(k)} for k in range(1, 4)] + [{"y": yy(k)} for k in range(1, 4)]
    peers += [pair_peer, core_peer, line_peer, {"l": ol, "c": oc}]
    barrier = pltpu.get_barrier_semaphore()
    for dev in peers:
        pl.semaphore_signal(barrier, inc=1, device_id=dev, device_id_type=pl.DeviceIdType.MESH)
    outs = [(fin, fin_out), (dxin, dx_out)] + [(grads.at[i], grads_out.at[i]) for i in range(3)]
    results = [pltpu.make_async_copy(src, dst, out_sem.at[i]) for i, (src, dst) in enumerate(outs)]
    mine = at_rows(h)
    moves = [
        (wq_in.at[i, :, pl.ds(hd * HEAD_DIM, HEAD_DIM)], W.at[0, z, y, mine, pl.ds((3 * hd + i) * HEAD_DIM, HEAD_DIM)])
        for i in range(3) for hd in range(heads)
    ]
    moves += [(wo_in, W.at[0, z, y, mine, pl.ds(3 * own, own)])]
    moves += [(wi_in, W.at[1, z, y, mine]), (wb_in, W.at[2, z, y, mine])]
    moves += [(tok_in, tok), (og_in, og), (mod_in, mod)]
    count = len(moves) - 3
    loads = [pltpu.make_async_copy(src, dst, in_sem.at[max(i - count + 1, 0)]) for i, (src, dst) in enumerate(moves)]
    for load in loads:
        load.start()
    drain(in_sem.at[0], [copy(src, dst, None, None, None) for src, dst in moves[:count]])
    pl.semaphore_wait(barrier, len(peers))

    for s in range(3):
        ag_pair(s, False).start()
    for s in (0, 1):
        ag_mid_start(s, 0, (2,))
        ag_mid_start(s, 0)
    for load in loads[count:]:
        load.wait()
    m = [mod[i] for i in range(6)]
    n1, r1 = normalize(f32(tok[...]))
    A1[l, c] = bf(n1 * (1.0 + m[1]) + m[0])
    DM[l, c] = bf(m[5] * f32(og[...]))
    gather_start(0, A1)
    ag_last_start(0, (2,))
    ag_mid_start(0, 1)
    ag_mid_start(1, 1)
    ag_last_start(1, (2,))
    ag_relay_start(0, (2,))
    ag_hop_start(1)
    ag_last_start(0)
    ag_relay_start(1, (2,))
    ag_final_start(0)
    gather_relay(0, A1)
    gather_start(1, DM)
    ag_relay_start(0)
    ag_mid_start(2, 0)
    ag_mid_start(2, 1)
    ag_last_start(1)
    ag_final_start(1)
    gather_wait(0, A1, 0)
    gather_wait(0, A1, 2)

    ag_wait(0)

    @pl.loop(0, 3)
    def _(t):
        at = pl.ds(pl.multiple_of(t * own, 128), own)
        w = W[0, :, :, :, at].reshape(width, own)
        QKV[:, at] = bf(dot(A1[...].reshape(seq, width), w))

    ag_hop_start(2)

    def head(hd, i):
        return pl.ds(pl.multiple_of((3 * hd + i) * HEAD_DIM, 128), HEAD_DIM)

    def wide(hd):
        return pl.ds(pl.multiple_of(hd * HEAD_DIM, 128), HEAD_DIM)

    @pl.loop(0, heads)
    def _(hd):
        s = dot(QKV[:, head(hd, 0)], QKV[:, head(hd, 1)], 1, 1) * scale
        e = jnp.exp(s - jnp.max(s, axis=-1, keepdims=True))
        p = bf(e * (1.0 / jnp.sum(e, axis=-1, keepdims=True)))
        PR[hd] = p
        O[:, wide(hd)] = bf(dot(p, QKV[:, head(hd, 2)]))

    out_product = back_product(lambda i: O[pair_rows(i), :], 0, 3 * own, own)
    ag_final(0, True).wait_recv()
    scatter_far(0, out_product)
    scatter_near(0, out_product)
    ag_relay_start(1)
    ag_last_start(2)
    mid = f32(tok[...]) + m[2] * scatter_result(0)
    MID[...] = mid
    n2, r2 = normalize(mid)
    A2[l, c] = bf(n2 * (1.0 + m[4]) + m[3])
    gather_start(2, A2)

    tile = 256

    def hidden(i):
        @pl.loop(0, width // (2 * tile))
        def _(t):
            for j in (0, 1):
                at = pl.ds(pl.multiple_of((2 * t + j) * tile, 128), tile)
                g, d = gelu_pair(dot(two(A2, i), W[1, :, :, :, at].reshape(width, tile)))
                GG[i, :, :, at] = bf(g).reshape(2, pair // 2, tile)
                DU[i, :, :, at] = bf(d).reshape(2, pair // 2, tile)

    gather_relay(1, DM)
    gather_wait(1, DM, 0)
    gather_wait(1, DM, 2)
    turn(DM)
    ag_wait(1)
    ag_final(1, True).wait_recv()
    gather_wait(2, A2, 0)
    hidden(l)
    ag_relay_start(2)
    gather_relay(2, A2)
    gather_wait(2, A2, 2)
    hidden(ol)
    for lo, hi in ((2 * side, width), (0, half), (half, 2 * side)):
        grad_turned(0, lambda at: all_rows(GG, at), lo, hi, tile)
        if lo == 2 * side:
            rs_first(0).start()
        else:
            rs_start(0, (0,) if lo == 0 else (1,))
    ag_wait(2)

    @pl.loop(0, width // tile)
    def _(t):
        at = pl.ds(pl.multiple_of(t * tile, 128), tile)
        dg = dot(DM[...].reshape(seq, width), W[2, :, :, :, at].reshape(width, tile))
        DU[:, :, :, at] = bf(f32(DU[:, :, :, at]) * dg.reshape(2, 2, pair // 2, tile))

    in_back = back_product(lambda i: two(DU, i), 1, 0, width)
    scatter_far(1, in_back)
    rs_combine(0)
    turn(A2)
    grad_turned(1, lambda at: all_rows(DU, at), 0, half, tile)
    rs_second(0)
    rs_start(1, (0,))
    grad_turned(1, lambda at: all_rows(DU, at), half, width, tile)
    rs_start(1, (1,))
    scatter_near(1, in_back)
    e2 = scatter_result(1) * (1.0 + m[4])
    n2, r2 = normalize(MID[...])
    dmid = f32(og[...]) + norm_back(n2, r2, e2)
    DX[...] = dmid
    DA[l, c] = bf(m[2] * dmid)
    gather_start(3, DA)

    ff_back = back_product(lambda i: two(GG, i), 2, 0, width)
    scatter_far(2, ff_back)
    rs_combine(0, (2,))
    rs_combine(1)
    scatter_near(2, ff_back)
    turn(A1)
    rs_mid_start(0)
    gather_relay(3, DA)
    gather_wait(3, DA, 0)
    gather_wait(3, DA, 2)

    DO[...] = bf(dot(DA[...].reshape(seq, width), W[0, :, :, :, pl.ds(3 * own, own)].reshape(width, own)))
    ag_sent(1)
    grad_product(2, DA, O[...], own, full)
    rs_first(2).start()
    rs_start(2)

    for hd in range(heads):
        do = DO[:, wide(hd)]
        p = PR[hd]
        t = f32(p) * dot(do, QKV[:, head(hd, 2)], 1, 1)
        ds = bf(scale * (t - f32(p) * jnp.sum(t, axis=-1, keepdims=True)))
        DQKV[:, head(hd, 0)] = bf(dot(ds, QKV[:, head(hd, 1)]))
        DQKV[:, head(hd, 1)] = bf(dot(ds.T, QKV[:, head(hd, 0)]))
        DQKV[:, head(hd, 2)] = bf(dot(p.T, do))
        grad_turned(3 + hd, lambda at: DQKV[:, at], hd * own, (hd + 1) * own, own)
        rs_first(3 + hd).start()
        rs_start(3 + hd)

    qkv_back = back_product(lambda i: DQKV[pair_rows(i), :], 0, 0, 3 * own)
    fin[...] = bf(MID[...] + m[5] * scatter_result(2))
    results[0].start()
    rs_hop_combine(0)
    rs_combine(2)
    rs_mid_start(1)
    rs_combine(3)
    qkv_back = back_product(lambda i: DQKV[pair_rows(i), :], 0, 0, 3 * own)
    rs_second(2)
    scatter_far(3, qkv_back)
    rs_combine(4)
    scatter_near(3, qkv_back)
    rs_second(3)
    rs_mid_start(0, (2,))
    rs_pair_start(0)
    rs_combine(5)
    rs_second(4)
    rs_mid_start(2)
    rs_combine(2, (2,))
    rs_hop_combine(1)
    rs_second(5)
    rs_combine(3, (2,))
    rs_mid_start(3)
    rs_combine(4, (2,))
    rs_mid_start(4)
    rs_mid_start(2, (2,))
    rs_mid_start(3, (2,))
    rs_mid_start(5)
    rs_combine(5, (2,))
    rs_pair_start(2)
    rs_pair_start(1)
    rs_finish_third(0)
    rs_mid_start(4, (2,))
    rs_pair_start(3)
    rs_finish(0)
    results[4].start()
    e1 = scatter_result(3) * (1.0 + m[1])
    n1, r1 = normalize(f32(tok[...]))
    dxin[...] = DX[...] + norm_back(n1, r1, e1)
    results[1].start()
    rs_pair_start(4)
    rs_mid_start(5, (2,))
    rs_pair_start(5)
    rs_finish(1)
    results[3].start()
    for s in range(2, sections):
        rs_finish_third(s)
    for s in range(2, sections):
        rs_finish(s)
    results[2].start()
    rs_sent()
    ag_sent(0)
    ag_sent(2)
    for i, buf in enumerate((A1, DM, A2, DA)):
        gather_sent(i, buf)
    for result in results:
        result.wait()


def place(fin, dx, grads, o_fin, o_dx, o_qkv, o_out, o_in, o_back, v_fin, v_dx, v_grads, sem_in, sem_out):
    own = o_out.shape[1]
    heads = own // HEAD_DIM
    sources = (
        (dx, v_dx), (grads.at[2], v_grads.at[2]), (grads.at[1], v_grads.at[1]),
        (fin, v_fin), (grads.at[0], v_grads.at[0]),
    )
    pieces = [
        (v_grads.at[0, :, pl.ds((3 * hd + i) * HEAD_DIM, HEAD_DIM)], o_qkv.at[i, :, pl.ds(hd * HEAD_DIM, HEAD_DIM)])
        for i in range(3) for hd in range(heads)
    ]
    pieces.append((v_grads.at[0, :, pl.ds(3 * own, own)], o_out))
    targets = (
        [(v_dx, o_dx.at[0])], [(v_grads.at[2], o_back)], [(v_grads.at[1], o_in.at[0])],
        [(v_fin, o_fin.at[0])], pieces,
    )
    loads = [pltpu.make_async_copy(a, b, sem_in.at[i]) for i, (a, b) in enumerate(sources)]
    for load in loads:
        load.start()
    stores = []
    for load, pairs in zip(loads, targets):
        load.wait()
        for a, b in pairs:
            store = pltpu.make_async_copy(a, b, sem_out.at[len(stores)])
            store.start()
            stores.append(store)
    for store in stores:
        store.wait()


def step(dims, tokens, modulation, w_qkv, w_out, w_in, w_back, out_grad):
    nz, ny, nh = dims
    count, width = tokens.shape[1:]
    rows, own, ff = w_qkv.shape[1], w_qkv.shape[3], w_in.shape[2]
    assert ff == width and 4 * own == width
    seq = 4 * count
    heads = own // HEAD_DIM
    big = (nz, ny, nh * rows)
    half = width // 2
    vmem = pltpu.VMEM
    dma = pltpu.SemaphoreType.DMA
    tokens_buf = vmem((2, 2, count, width), BF)
    scratch = [
        vmem((3, *big, width), BF),
        vmem((2, *big, width), BF),
        vmem((3, 3, 4, nh * rows, half), BF),
        vmem((3, 3, 4, nh * rows, half), BF),
        vmem((3, 3, nh * rows, half), BF),
        vmem((3, 3, nh * rows, half), BF),
        vmem((3, rows, width), BF),
        vmem((3, 4, rows, 256), BF),
        vmem((3, rows, 256), BF),
        vmem((nz, ny, rows, 256), BF),
        vmem((1 + heads, nz, ny, rows, own // 3), BF),
        *[tokens_buf] * 6,
        vmem((seq, 3 * own), BF),
        vmem((seq, 3 * own), BF),
        vmem((seq, own), BF),
        vmem((seq, own), BF),
        vmem((heads, seq, seq), BF),
        tokens_buf,
        vmem((2, 3, count, width), BF),
        vmem((count, width), BF),
        vmem((count, width), F32),
        vmem((count, width), F32),
        vmem((nz, ny * nh * rows, seq), BF),
        vmem((count, width), BF),
        vmem((6, 1, width), F32),
        vmem((count, width), BF),
        vmem((count, width), BF),
        vmem((count, width), F32),
        vmem((3, rows, width), F32),
        dma((4,)),
        dma((5,)),
        dma((3, 5)), dma((3, 2)), dma((3, 3, 2)), dma((3, 3)), dma((3, 2)), dma((3, 2)),
        dma((2,)), dma((3 + heads, 3, 2)), dma((3 + heads, 3)), dma((3 + heads,)), dma((3 + heads,)),
        dma((2, 2, 3)),
        dma((4,)), dma((4, 3)), dma((4,)), dma((4, 3)),
    ]
    whole = pl.BlockSpec(memory_space=pl.ANY)
    final, dx, grads = pl.pallas_call(
        functools.partial(kernel, dims),
        out_shape=(
            jax.ShapeDtypeStruct((count, width), BF),
            jax.ShapeDtypeStruct((count, width), F32),
            jax.ShapeDtypeStruct((3, rows, width), F32),
        ),
        in_specs=[whole] * 7,
        out_specs=(whole,) * 3,
        scratch_shapes=scratch,
        compiler_params=pltpu.CompilerParams(
            collective_id=0, has_side_effects=True, vmem_limit_bytes=67043328
        ),
    )(
        tokens[0], modulation[0].transpose(1, 0, 2), w_qkv[0].transpose(1, 0, 2), w_out[0].T,
        w_in[0], w_back[0].T, out_grad[0],
    )
    final, dx, qkv, out, inner, back = pl.pallas_call(
        place,
        out_shape=(
            jax.ShapeDtypeStruct((1, count, width), BF),
            jax.ShapeDtypeStruct((1, count, width), F32),
            jax.ShapeDtypeStruct((3, rows, own), F32),
            jax.ShapeDtypeStruct((rows, own), F32),
            jax.ShapeDtypeStruct((1, rows, width), F32),
            jax.ShapeDtypeStruct((rows, width), F32),
        ),
        in_specs=[whole] * 3,
        out_specs=(whole,) * 6,
        scratch_shapes=[
            vmem((count, width), BF), vmem((count, width), F32), vmem((3, rows, width), F32),
            dma((5,)), dma((5 + 3 * heads,)),
        ],
    )(final, dx, grads)
    return final, dx, qkv.transpose(1, 0, 2)[None], out.T[None], inner, back.T[None]


def solution(mesh):
    dims = (4, 4, 2)
    assert mesh.shape["fsdp"] == 32 and mesh.shape["sp"] == 4
    torus = Mesh(mesh.devices.reshape(*dims, 2, 2), AXES)
    fsdp, sp = AXES[:3], AXES[3:]
    placed = (
        P(fsdp, sp, None),
        P(fsdp, None, None, None),
        P(None, fsdp, None, sp),
        P(None, sp, fsdp),
        P(None, fsdp, sp),
        P(None, sp, fsdp),
        P(fsdp, sp, None),
    )
    return jax.shard_map(
        functools.partial(step, dims),
        mesh=torus,
        in_specs=placed,
        out_specs=(placed[0], *placed[:1], *placed[2:6]),
        check_vma=False,
    )
```

```python
import functools
import math

import jax
import jax.numpy as jnp
from jax import lax
from jax.experimental import pallas as pl
from jax.experimental.pallas import tpu as pltpu
from jax.sharding import Mesh
from jax.sharding import PartitionSpec as P

HEAD_DIM = 128
LN_EPS = 1e-06
TEMPER = 2.5
BF = jnp.bfloat16
F32 = jnp.float32
AXES = ("z", "y", "h", "l", "c")


def bf(x):
    return x.astype(BF)


def f32(x):
    return x.astype(F32)


def dot(a, b, ca=1, cb=0):
    return lax.dot_general(a, b, (((ca,), (cb,)), ((), ())), preferred_element_type=F32)


def normalize(x):
    d = x - jnp.mean(x, axis=-1, keepdims=True)
    r = lax.rsqrt(jnp.mean(d * d, axis=-1, keepdims=True) + LN_EPS)
    return d * r, r


def norm_back(n, r, e):
    return r * (e - jnp.mean(e, axis=-1, keepdims=True) - n * jnp.mean(e * n, axis=-1, keepdims=True))


def gelu_pair(u):
    k0 = math.sqrt(2.0 / math.pi)
    s = u * u
    t = jnp.tanh(k0 * u * (1.0 + 0.044715 * s))
    g = 0.5 * u * (1.0 + t)
    d = 0.5 * (1.0 + t) + 0.5 * k0 * u * (1.0 - t * t) * (1.0 + 3.0 * 0.044715 * s)
    return g, d


class copy:
    def __init__(self, src, dst, ssem, rsem, dev):
        self.src, self.rest = src, (dst, ssem, rsem, dev)

    def made(self):
        dst, ssem, rsem, dev = self.rest
        return pltpu.make_async_remote_copy(
            src_ref=self.src, dst_ref=dst, send_sem=ssem, recv_sem=rsem,
            device_id=dev, device_id_type=pl.DeviceIdType.MESH,
        )

    def start(self):
        self.made().start()

    def wait_send(self):
        self.made().wait_send()

    def wait_recv(self):
        self.made().wait_recv()


def kernel(
    dims, tok_in, mod_in, wq_in, wo_in, wi_in, wb_in, og_in, fin_out, dx_out, grads_out,
    W, G, R1A, R1B, R2A, R2B, R3, R1C, R2C, R4, R4H, A1, A2, DM, DA, GG, DU, QKV, DQKV, O, DO, PR, PS, RX, SX, MID, DX, AT,
    tok, mod, og, fin, dxin, grads, in_sem, out_sem, ags, a1r, a2r, a3r, a4r, a5r, rss, r1r, r2r, r3r, r4r, r5r, gs, gr, ss, sr,
):
    nz, ny, nh = dims
    z, y, h, l, c = (lax.axis_index(a) for a in AXES)
    ol, oc = 1 - l, 1 - c
    rows, width = wi_in.shape
    half = width // 2
    seq = QKV.shape[0]
    pair = seq // 2
    own = QKV.shape[1] // 3
    heads = own // HEAD_DIM
    slab = ny * nh * rows
    scale = TEMPER / math.sqrt(HEAD_DIM)
    q_s = 1.0 / math.sqrt(seq * nz * ny * nh)
    cols = (pl.ds(0, half), pl.ds(half, half))

    def drain(sem, moves):
        units = sum(math.prod(move.src.shape) for move in moves) // (rows * 128)
        for q, height in ((1, rows), (1, nh * rows), (3, nh * rows)):
            for i in range(1, nz + 1):
                for j in range(1, ny + 1):
                    n, rest = divmod(units * rows, q * height * i * j)
                    if rest == 0 and n <= width // 128:
                        view = W.at[pl.ds(0, q), pl.ds(0, i), pl.ds(0, j), pl.ds(0, height), pl.ds(0, n * 128)]
                        pltpu.make_async_copy(view, view, sem).wait()
                        return
        raise ValueError(units)

    def zz(k):
        return lax.rem(z + k + nz, nz)

    def yy(k):
        return lax.rem(y + k + ny, ny)

    def hh(k):
        return lax.rem(h + k + nh, nh)

    def at_rows(i):
        return pl.ds(pl.multiple_of(i * rows, 16), rows)

    core_peer = {"c": oc}
    line_peer = {"l": ol}
    pair_peer = {"h": 1 - h}
    halves = (pl.ds(0, 2), pl.ds(2, 2))

    def last(color, k):
        return {"z": zz(k)} if color == 0 else {"y": yy(k)}

    def mid_dev(color, k):
        return last(1 - color, k)

    strip = 256
    side = (width - strip) // 2
    ag_cols = ((pl.ds(0, side), pl.ds(side, side), pl.ds(2 * side, strip)),) * 2 + (cols,)
    every = slice(None)

    def slab_at(buf, color, k, at, part=every, row=every):
        return buf.at[zz(k), part, row, at] if color == 0 else buf.at[part, yy(k), row, at]

    def line_at(buf, color, k, at, row=every):
        return buf.at[z, yy(k), row, at] if color == 0 else buf.at[zz(k), y, row, at]

    def line_of(s, color):
        return color if color < 2 else s % 2

    def row_of(color):
        return every if color < 2 else at_rows(h)

    def direct(s, color):
        return s == 0 or color == 2

    def ag_pair(s, recv):
        piece = W.at[s, z, y, at_rows(1 - h if recv else h), pl.ds(0, 2 * side if s < 2 else width)]
        return copy(piece, piece, ags.at[s, 0], a1r.at[s, 0], pair_peer)

    def ag_final(s, recv):
        piece = W.at[s, :, :, at_rows(1 - h if recv else h), ag_cols[s][2]]
        return copy(piece, piece, ags.at[s, 1], a1r.at[s, 1], pair_peer)

    def ag_mid(s, color, k, which, recv):
        line = line_of(s, color)
        piece = line_at(W.at[s], line, -k if recv else 0, ag_cols[s][color], at_rows(h if which == 0 else 1 - h))
        side_of = 0 if direct(s, color) else (k - 1) // 2
        return copy(piece, piece, ags.at[s, 2 + 2 * (color // 2)], a2r.at[s, color, side_of], mid_dev(line, k))

    def ag_hop(s, color, d, recv):
        k = 1 - 2 * d
        piece = line_at(W.at[s], color, 2 if recv else -k, ag_cols[s][color], at_rows(d))
        return copy(piece, piece, ags.at[s, 2], a5r.at[s, color], mid_dev(color, k))

    def ag_last(s, color, d, j, recv):
        k, line = 1 - 2 * d, line_of(s, color)
        part = halves[d if j == 0 else 1 - d]
        piece = slab_at(W.at[s], line, -k if recv else 0, ag_cols[s][color], part, row_of(color))
        arrived = a3r.at[s, color] if j == 0 else a4r.at[s, color // 2]
        return copy(piece, piece, ags.at[s, 3 + color // 2], arrived, last(line, k))

    def ag_relay(s, color, d, recv):
        k, line = 1 - 2 * d, line_of(s, color)
        piece = slab_at(W.at[s], line, 2 if recv else -k, ag_cols[s][color], halves[d], row_of(color))
        return copy(piece, piece, ags.at[s, 3 + color // 2], a4r.at[s, color // 2], last(line, k))

    def ag_mid_start(s, which, colors=(0, 1)):
        if which:
            ag_pair(s, True).wait_recv()
        for k in (1, 3, 2) if direct(s, colors[0]) else (1, 3):
            for color in colors:
                ag_mid(s, color, k, which, False).start()

    def ag_hop_start(s):
        for color in (0, 1):
            for d in (0, 1):
                drain(a2r.at[s, color, d], [ag_mid(s, color, 1 + 2 * d, which, True) for which in (0, 1)])
                ag_hop(s, color, d, False).start()

    def ag_last_start(s, colors=(0, 1)):
        for color in colors:
            if direct(s, color):
                sides = (0, 1) if color < 2 else (0,)
                drain(a2r.at[s, color, 0], [ag_mid(s, color, k, which, True) for which in sides for k in (1, 2, 3)])
            else:
                drain(a5r.at[s, color], [ag_hop(s, color, d, True) for d in (0, 1)])
        for j in (0, 1):
            for color in colors:
                for d in (0, 1):
                    ag_last(s, color, d, j, False).start()

    def ag_relay_start(s, colors=(0, 1)):
        for color in colors:
            drain(a3r.at[s, color], [ag_last(s, color, d, 0, True) for d in (0, 1)])
            for d in (0, 1):
                ag_relay(s, color, d, False).start()

    def late(s, colors):
        return [move for color in colors for d in (0, 1)
                for move in (ag_last(s, color, d, 1, True), ag_relay(s, color, d, True))]

    def ag_final_start(s):
        drain(a4r.at[s, 1], late(s, (2,)))
        ag_final(s, False).start()

    def ag_wait(s):
        drain(a4r.at[s, 0], late(s, (0, 1)))

    def ag_sent(s):
        ag_pair(s, False).wait_send()
        middle = [ag_mid(s, color, k, which, False) for color in (0, 1) for which in (0, 1)
                  for k in ((1, 2, 3) if direct(s, 0) else (1, 3))]
        if not direct(s, 0):
            middle += [ag_hop(s, color, d, False) for color in (0, 1) for d in (0, 1)]
        drain(ags.at[s, 2], middle)

        def ends(colors):
            return [ag_last(s, color, d, j, False) for color in colors for d in (0, 1) for j in (0, 1)] + [
                ag_relay(s, color, d, False) for color in colors for d in (0, 1)]

        drain(ags.at[s, 3], ends((0, 1)))
        if s < 2:
            ag_final(s, False).wait_send()
            drain(ags.at[s, 4], [ag_mid(s, 2, k, 0, False) for k in (1, 2, 3)] + ends((2,)))

    R1 = (R1A, R1B)
    R2 = (R2A, R2B)
    full = 3 * own
    sections = 3 + heads
    parts = (G.at[0], G.at[1]) + (W.at[1],) * (1 + heads)
    slots = (2, 1) + (0,) * (1 + heads)
    lead = pl.ds(0, side)
    local_cols = [(lead, lead), (cols[0], cols[0])]
    grad_cols = [ag_cols[0], cols]
    pair_cols = [pl.ds(0, 2 * side), pl.ds(0, width)]
    third = own // 3
    for i, start in enumerate([full] + [hd * own for hd in range(heads)]):
        at = pl.ds(i * third, third)
        local_cols.append((at, at))
        grad_cols.append(tuple(pl.ds(start + j * third, third) for j in range(3)))
        pair_cols.append(pl.ds(start, 2 * third))

    spare = {2: (1, 4), 3: (1, 5), 4: (0, 4), 5: (0, 5)}

    def rs_line(s, color):
        return color if color < 2 else (0, None, 0, 1, 0, 1)[s]

    def spare_at(s):
        return pl.ds(spare[s][1] * third, third)

    def r1_at(s, color):
        if color < 2:
            return R1[color].at[slots[s], :, :, :, local_cols[s][color]]
        return R1C if s == 0 else R1[spare[s][0]].at[0, :, :, pl.ds(0, rows), spare_at(s)]

    def r2_at(s, color):
        if color < 2:
            return R2[color].at[slots[s], :, :, local_cols[s][color]]
        return R2C if s == 0 else R2[spare[s][0]].at[0, :, pl.ds(0, rows), spare_at(s)]

    def r4_at(s):
        return R4 if s == 0 else R4H.at[s - 2]

    def rs_first(s):
        src = parts[s].at[:, :, at_rows(1 - h), grad_cols[s][2]]
        return copy(src, r4_at(s), rss.at[1], r4r.at[s], pair_peer)

    def rs_ring(s, color, d, kind):
        k, line = 1 - 2 * d, rs_line(s, color)
        part = halves[1 - d if kind == 1 else d]
        src = slab_at(parts[s], line, 2 if kind == 0 else k, grad_cols[s][color], part, row_of(color))
        dst = r1_at(s, color).at[2 if kind == 0 else d, part]
        arrived = r1r.at[s, color, min(kind, 1)]
        return copy(src, dst, rss.at[0], arrived, last(line, k))

    def rs_mid(s, color, k):
        line = rs_line(s, color)
        return copy(
            line_at(parts[s], line, k, grad_cols[s][color], row_of(color)), r2_at(s, color).at[k - 1],
            rss.at[1], r2r.at[s, color], mid_dev(line, k),
        )

    def ringed(s, color):
        return s < 2 and color < 2

    def rs_hop(s, color, d, kind):
        k = 1 - 2 * d
        row = at_rows(1 - d if kind == 1 else d)
        src = line_at(parts[s], color, 2 if kind == 0 else k, grad_cols[s][color], row)
        dst = r2_at(s, color).at[2 if kind == 0 else d, row]
        arrived = r5r.at[s, color, d if kind == 0 else 2]
        return copy(src, dst, rss.at[1], arrived, mid_dev(color, k))

    def rs_hop_combine(s):
        for color in (0, 1):
            for d in (0, 1):
                rs_hop(s, color, d, 0).wait_recv()
                k = 1 - 2 * d
                at = (z, yy(k)) if color == 0 else (zz(k), y)
                at = (*at, at_rows(d), grad_cols[s][color])
                parts[s][at] = bf(f32(parts[s][at]) + f32(r2_at(s, color)[2, d * rows : (d + 1) * rows]))
                rs_hop(s, color, d, 2).start()

    def rs_pair(s):
        return copy(
            parts[s].at[z, y, at_rows(1 - h), pair_cols[s]], R3.at[slots[s], :, pair_cols[s]],
            rss.at[1], r3r.at[s], pair_peer,
        )

    def rs_second(s):
        rs_first(s).wait_recv()

        @pl.loop(0, nz)
        def _(i):
            at = (i, every, at_rows(h), grad_cols[s][2])
            parts[s][at] = bf(f32(parts[s][at]) + f32(r4_at(s)[i]))

        rs_start(s, (2,))

    def rs_start(s, colors=(0, 1)):
        for kind in (0, 1):
            for color in colors:
                for d in (0, 1):
                    rs_ring(s, color, d, kind).start()

    def rs_combine(s, colors=(0, 1)):
        for color in colors:
            line = rs_line(s, color)
            drain(r1r.at[s, color, 0], [rs_ring(s, color, d, 0) for d in (0, 1)])
            for d in (0, 1):
                k = 1 - 2 * d

                @pl.loop(2 * d, 2 * d + 2)
                def _(i):
                    at = (zz(k), i) if line == 0 else (i, yy(k))
                    at = (*at, row_of(color), grad_cols[s][color])
                    parts[s][at] = bf(f32(parts[s][at]) + f32(r1_at(s, color)[2, i]))

                rs_ring(s, color, d, 2).start()

    def rs_mid_start(s, colors=(0, 1)):
        for color in colors:
            line = rs_line(s, color)
            drain(r1r.at[s, color, 1], [rs_ring(s, color, d, kind) for d in (0, 1) for kind in (1, 2)])

            @pl.loop(0, 4)
            def _(i):
                at = (z, i) if line == 0 else (i, y)
                at = (*at, row_of(color), grad_cols[s][color])
                total = f32(parts[s][at])
                for d in (0, 1):
                    total = total + f32(r1_at(s, color)[d, i])
                parts[s][at] = bf(total)

            if ringed(s, color):
                for kind in (0, 1):
                    for d in (0, 1):
                        rs_hop(s, color, d, kind).start()
            else:
                for k in (1, 3, 2):
                    rs_mid(s, color, k).start()

    def rs_total(s, color):
        if ringed(s, color):
            drain(r5r.at[s, color, 2], [rs_hop(s, color, d, kind) for d in (0, 1) for kind in (1, 2)])
        else:
            drain(r2r.at[s, color], [rs_mid(s, color, k) for k in (1, 2, 3)])
        total = f32(parts[s][z, y, row_of(color), grad_cols[s][color]])
        for k in range(2 if ringed(s, color) else 3):
            total = total + f32(r2_at(s, color)[k])
        return total

    def rs_pair_start(s):
        for color in (0, 1):
            parts[s][z, y, every, grad_cols[s][color]] = bf(rs_total(s, color))
        rs_pair(s).start()

    def rs_finish(s):
        rs_pair(s).wait_recv()
        at = pair_cols[s]
        grads[slots[s], :, at] = f32(parts[s][z, y, at_rows(h), at]) + f32(R3[slots[s], :, at])

    def rs_finish_third(s):
        grads[slots[s], :, grad_cols[s][2]] = rs_total(s, 2)

    def rs_sent():
        rings, others = [], []
        for s in range(sections):
            for color in (0, 1) if s == 1 else (0, 1, 2):
                rings += [rs_ring(s, color, d, kind) for d in (0, 1) for kind in (0, 1, 2)]
                if ringed(s, color):
                    others += [rs_hop(s, color, d, kind) for d in (0, 1) for kind in (0, 1, 2)]
                else:
                    others += [rs_mid(s, color, k) for k in (1, 2, 3)]
            others += [rs_pair(s)] if s == 1 else [rs_pair(s), rs_first(s)]
        drain(rss.at[0], rings)
        drain(rss.at[1], others)

    def g_copy(i, buf, step, recv):
        if step == 0:
            piece, dev = buf.at[l, oc if recv else c], core_peer
        elif step == 1:
            piece, dev = buf.at[ol if recv else l, c], line_peer
        else:
            piece, dev = buf.at[ol, oc if recv else c], core_peer
        return copy(piece, piece, gs.at[i], gr.at[i, step], dev)

    def gather_start(i, buf):
        g_copy(i, buf, 1, False).start()
        g_copy(i, buf, 0, False).start()

    def gather_relay(i, buf):
        g_copy(i, buf, 1, True).wait_recv()
        g_copy(i, buf, 2, False).start()

    def gather_wait(i, buf, step):
        g_copy(i, buf, step, True).wait_recv()

    def gather_sent(i, buf):
        drain(gs.at[i], [g_copy(i, buf, step, False) for step in range(3)])

    def s_copy(i, step):
        src, dev = (
            (PS.at[ol, oc], core_peer),
            (SX, line_peer),
            (PS.at[l, oc], core_peer),
        )[step]
        return copy(src, RX.at[i % 2, step], ss.at[i], sr.at[i, step], dev)

    def scatter_far(i, compute):
        compute(ol)
        s_copy(i, 0).start()
        s_copy(i, 0).wait_recv()
        SX[...] = bf(f32(PS[ol, c]) + f32(RX[i % 2, 0]))
        s_copy(i, 1).start()

    def scatter_near(i, compute):
        compute(l)
        s_copy(i, 2).start()

    def scatter_result(i):
        s_copy(i, 2).wait_recv()
        s_copy(i, 1).wait_recv()
        total = f32(PS[l, c]) + f32(RX[i % 2, 2]) + f32(RX[i % 2, 1])
        drain(ss.at[i], [s_copy(i, step) for step in range(3)])
        return total

    def pair_rows(i):
        return pl.ds(pl.multiple_of(i * pair, 128), pair)

    def back_product(left, s, lo, n):
        def compute(i):
            @pl.loop(0, nz)
            def _(b):
                w = W[s, b, :, :, pl.ds(lo, n)].reshape(slab, n)
                at = pl.ds(pl.multiple_of(b * slab, 128), slab)
                PS[i, :, :, at] = bf(dot(left(i), w, 1, 1)).reshape(2, pair // 2, slab)
        return compute

    def two(buf, i):
        return buf[i].reshape(pair, buf.shape[-1])

    def all_rows(buf, at):
        return buf[:, :, :, at].reshape(seq, -1)

    def turn(buf):
        @pl.loop(0, nz)
        def _(b):
            AT[b] = all_rows(buf, pl.ds(pl.multiple_of(b * slab, 128), slab)).T

    def grad_turned(s, right, start, stop, tile):
        @pl.loop(0, (stop - start) // tile)
        def _(t):
            at = pl.ds(pl.multiple_of(start + t * tile, 128), tile)
            value = dot(AT[...].reshape(width, seq), right(at)) * q_s
            parts[s][:, :, :, at] = bf(value).reshape(nz, ny, nh * rows, tile)

    def grad_product(s, left, right, n, lo):
        @pl.loop(0, nz)
        def _(b):
            a = all_rows(left, pl.ds(pl.multiple_of(b * slab, 128), slab)).T
            value = dot(a, right) * q_s
            parts[s][b, :, :, pl.ds(lo, n)] = bf(value).reshape(ny, nh * rows, n)

    peers = [{"z": zz(k)} for k in range(1, 4)] + [{"y": yy(k)} for k in range(1, 4)]
    peers += [pair_peer, core_peer, line_peer, {"l": ol, "c": oc}]
    barrier = pltpu.get_barrier_semaphore()
    for dev in peers:
        pl.semaphore_signal(barrier, inc=1, device_id=dev, device_id_type=pl.DeviceIdType.MESH)
    outs = [(fin, fin_out), (dxin, dx_out)] + [(grads.at[i], grads_out.at[i]) for i in range(3)]
    results = [pltpu.make_async_copy(src, dst, out_sem.at[i]) for i, (src, dst) in enumerate(outs)]
    mine = at_rows(h)
    moves = [
        (wq_in.at[i, :, pl.ds(hd * HEAD_DIM, HEAD_DIM)], W.at[0, z, y, mine, pl.ds((3 * hd + i) * HEAD_DIM, HEAD_DIM)])
        for i in range(3) for hd in range(heads)
    ]
    moves += [(wo_in, W.at[0, z, y, mine, pl.ds(3 * own, own)])]
    moves += [(wi_in, W.at[1, z, y, mine]), (wb_in, W.at[2, z, y, mine])]
    moves += [(tok_in, tok), (og_in, og), (mod_in, mod)]
    count = len(moves) - 3
    loads = [pltpu.make_async_copy(src, dst, in_sem.at[max(i - count + 1, 0)]) for i, (src, dst) in enumerate(moves)]
    for load in loads:
        load.start()
    drain(in_sem.at[0], [copy(src, dst, None, None, None) for src, dst in moves[:count]])
    pl.semaphore_wait(barrier, len(peers))

    for s in range(3):
        ag_pair(s, False).start()
    for s in (0, 1):
        ag_mid_start(s, 0, (2,))
        ag_mid_start(s, 0)
    for load in loads[count:]:
        load.wait()
    m = [mod[i] for i in range(6)]
    n1, r1 = normalize(f32(tok[...]))
    A1[l, c] = bf(n1 * (1.0 + m[1]) + m[0])
    DM[l, c] = bf(m[5] * f32(og[...]))
    gather_start(0, A1)
    ag_last_start(0, (2,))
    ag_mid_start(0, 1)
    ag_mid_start(1, 1)
    ag_last_start(1, (2,))
    ag_relay_start(0, (2,))
    ag_hop_start(1)
    ag_last_start(0)
    ag_relay_start(1, (2,))
    ag_final_start(0)
    gather_relay(0, A1)
    gather_start(1, DM)
    ag_relay_start(0)
    ag_mid_start(2, 0)
    ag_mid_start(2, 1)
    ag_last_start(1)
    ag_final_start(1)
    gather_wait(0, A1, 0)
    gather_wait(0, A1, 2)

    ag_wait(0)

    @pl.loop(0, 3)
    def _(t):
        at = pl.ds(pl.multiple_of(t * own, 128), own)
        w = W[0, :, :, :, at].reshape(width, own)
        QKV[:, at] = bf(dot(A1[...].reshape(seq, width), w))

    ag_hop_start(2)

    def head(hd, i):
        return pl.ds(pl.multiple_of((3 * hd + i) * HEAD_DIM, 128), HEAD_DIM)

    def wide(hd):
        return pl.ds(pl.multiple_of(hd * HEAD_DIM, 128), HEAD_DIM)

    @pl.loop(0, heads)
    def _(hd):
        s = dot(QKV[:, head(hd, 0)], QKV[:, head(hd, 1)], 1, 1) * scale
        e = jnp.exp(s - jnp.max(s, axis=-1, keepdims=True))
        p = bf(e * (1.0 / jnp.sum(e, axis=-1, keepdims=True)))
        PR[hd] = p
        O[:, wide(hd)] = bf(dot(p, QKV[:, head(hd, 2)]))

    out_product = back_product(lambda i: O[pair_rows(i), :], 0, 3 * own, own)
    ag_final(0, True).wait_recv()
    scatter_far(0, out_product)
    scatter_near(0, out_product)
    ag_relay_start(1)
    ag_last_start(2)
    mid = f32(tok[...]) + m[2] * scatter_result(0)
    MID[...] = mid
    n2, r2 = normalize(mid)
    A2[l, c] = bf(n2 * (1.0 + m[4]) + m[3])
    gather_start(2, A2)

    tile = 256

    def hidden(i):
        @pl.loop(0, width // (2 * tile))
        def _(t):
            for j in (0, 1):
                at = pl.ds(pl.multiple_of((2 * t + j) * tile, 128), tile)
                g, d = gelu_pair(dot(two(A2, i), W[1, :, :, :, at].reshape(width, tile)))
                GG[i, :, :, at] = bf(g).reshape(2, pair // 2, tile)
                DU[i, :, :, at] = bf(d).reshape(2, pair // 2, tile)

    gather_relay(1, DM)
    gather_wait(1, DM, 0)
    gather_wait(1, DM, 2)
    turn(DM)
    ag_wait(1)
    ag_final(1, True).wait_recv()
    gather_wait(2, A2, 0)
    hidden(l)
    ag_relay_start(2)
    gather_relay(2, A2)
    gather_wait(2, A2, 2)
    hidden(ol)
    for lo, hi in ((2 * side, width), (0, half), (half, 2 * side)):
        grad_turned(0, lambda at: all_rows(GG, at), lo, hi, tile)
        if lo == 2 * side:
            rs_first(0).start()
        else:
            rs_start(0, (0,) if lo == 0 else (1,))
    ag_wait(2)

    @pl.loop(0, width // tile)
    def _(t):
        at = pl.ds(pl.multiple_of(t * tile, 128), tile)
        dg = dot(DM[...].reshape(seq, width), W[2, :, :, :, at].reshape(width, tile))
        DU[:, :, :, at] = bf(f32(DU[:, :, :, at]) * dg.reshape(2, 2, pair // 2, tile))

    in_back = back_product(lambda i: two(DU, i), 1, 0, width)
    scatter_far(1, in_back)
    rs_combine(0)
    turn(A2)
    grad_turned(1, lambda at: all_rows(DU, at), 0, half, tile)
    rs_second(0)
    rs_start(1, (0,))
    grad_turned(1, lambda at: all_rows(DU, at), half, width, tile)
    rs_start(1, (1,))
    scatter_near(1, in_back)
    e2 = scatter_result(1) * (1.0 + m[4])
    n2, r2 = normalize(MID[...])
    dmid = f32(og[...]) + norm_back(n2, r2, e2)
    DX[...] = dmid
    DA[l, c] = bf(m[2] * dmid)
    gather_start(3, DA)

    ff_back = back_product(lambda i: two(GG, i), 2, 0, width)
    scatter_far(2, ff_back)
    rs_combine(0, (2,))
    rs_combine(1)
    scatter_near(2, ff_back)
    turn(A1)
    rs_mid_start(0)
    gather_relay(3, DA)
    gather_wait(3, DA, 0)
    gather_wait(3, DA, 2)

    DO[...] = bf(dot(DA[...].reshape(seq, width), W[0, :, :, :, pl.ds(3 * own, own)].reshape(width, own)))
    ag_sent(1)
    grad_product(2, DA, O[...], own, full)
    rs_first(2).start()
    rs_start(2)

    for hd in range(heads):
        do = DO[:, wide(hd)]
        p = PR[hd]
        t = f32(p) * dot(do, QKV[:, head(hd, 2)], 1, 1)
        ds = bf(scale * (t - f32(p) * jnp.sum(t, axis=-1, keepdims=True)))
        DQKV[:, head(hd, 0)] = bf(dot(ds, QKV[:, head(hd, 1)]))
        DQKV[:, head(hd, 1)] = bf(dot(ds.T, QKV[:, head(hd, 0)]))
        DQKV[:, head(hd, 2)] = bf(dot(p.T, do))
        grad_turned(3 + hd, lambda at: DQKV[:, at], hd * own, (hd + 1) * own, own)
        rs_first(3 + hd).start()
        rs_start(3 + hd)

    qkv_back = back_product(lambda i: DQKV[pair_rows(i), :], 0, 0, 3 * own)
    fin[...] = bf(MID[...] + m[5] * scatter_result(2))
    results[0].start()
    rs_hop_combine(0)
    rs_combine(2)
    rs_mid_start(1)
    rs_combine(3)
    qkv_back = back_product(lambda i: DQKV[pair_rows(i), :], 0, 0, 3 * own)
    rs_second(2)
    scatter_far(3, qkv_back)
    rs_combine(4)
    rs_second(3)
    scatter_near(3, qkv_back)
    rs_mid_start(0, (2,))
    rs_pair_start(0)
    rs_combine(5)
    rs_second(4)
    rs_mid_start(2)
    rs_combine(2, (2,))
    rs_hop_combine(1)
    rs_second(5)
    rs_combine(3, (2,))
    rs_mid_start(3)
    rs_combine(4, (2,))
    rs_mid_start(4)
    rs_mid_start(2, (2,))
    rs_mid_start(3, (2,))
    rs_mid_start(5)
    rs_combine(5, (2,))
    rs_pair_start(2)
    rs_pair_start(1)
    rs_finish_third(0)
    rs_mid_start(4, (2,))
    rs_pair_start(3)
    rs_finish(0)
    results[4].start()
    e1 = scatter_result(3) * (1.0 + m[1])
    n1, r1 = normalize(f32(tok[...]))
    dxin[...] = DX[...] + norm_back(n1, r1, e1)
    results[1].start()
    rs_pair_start(4)
    rs_mid_start(5, (2,))
    rs_pair_start(5)
    rs_finish(1)
    results[3].start()
    for s in range(2, sections):
        rs_finish_third(s)
    for s in range(2, sections):
        rs_finish(s)
    results[2].start()
    rs_sent()
    ag_sent(0)
    ag_sent(2)
    for i, buf in enumerate((A1, DM, A2, DA)):
        gather_sent(i, buf)
    for result in results:
        result.wait()


def place(fin, dx, grads, o_fin, o_dx, o_qkv, o_out, o_in, o_back, v_fin, v_dx, v_grads, sem_in, sem_out):
    own = o_out.shape[1]
    heads = own // HEAD_DIM
    sources = (
        (dx, v_dx), (grads.at[2], v_grads.at[2]), (grads.at[1], v_grads.at[1]),
        (fin, v_fin), (grads.at[0], v_grads.at[0]),
    )
    pieces = [
        (v_grads.at[0, :, pl.ds((3 * hd + i) * HEAD_DIM, HEAD_DIM)], o_qkv.at[i, :, pl.ds(hd * HEAD_DIM, HEAD_DIM)])
        for i in range(3) for hd in range(heads)
    ]
    pieces.append((v_grads.at[0, :, pl.ds(3 * own, own)], o_out))
    targets = (
        [(v_dx, o_dx.at[0])], [(v_grads.at[2], o_back)], [(v_grads.at[1], o_in.at[0])],
        [(v_fin, o_fin.at[0])], pieces,
    )
    loads = [pltpu.make_async_copy(a, b, sem_in.at[i]) for i, (a, b) in enumerate(sources)]
    for load in loads:
        load.start()
    stores = []
    for load, pairs in zip(loads, targets):
        load.wait()
        for a, b in pairs:
            store = pltpu.make_async_copy(a, b, sem_out.at[len(stores)])
            store.start()
            stores.append(store)
    for store in stores:
        store.wait()


def step(dims, tokens, modulation, w_qkv, w_out, w_in, w_back, out_grad):
    nz, ny, nh = dims
    count, width = tokens.shape[1:]
    rows, own, ff = w_qkv.shape[1], w_qkv.shape[3], w_in.shape[2]
    assert ff == width and 4 * own == width
    seq = 4 * count
    heads = own // HEAD_DIM
    big = (nz, ny, nh * rows)
    half = width // 2
    vmem = pltpu.VMEM
    dma = pltpu.SemaphoreType.DMA
    tokens_buf = vmem((2, 2, count, width), BF)
    scratch = [
        vmem((3, *big, width), BF),
        vmem((2, *big, width), BF),
        vmem((3, 3, 4, nh * rows, half), BF),
        vmem((3, 3, 4, nh * rows, half), BF),
        vmem((3, 3, nh * rows, half), BF),
        vmem((3, 3, nh * rows, half), BF),
        vmem((3, rows, width), BF),
        vmem((3, 4, rows, 256), BF),
        vmem((3, rows, 256), BF),
        vmem((nz, ny, rows, 256), BF),
        vmem((1 + heads, nz, ny, rows, own // 3), BF),
        *[tokens_buf] * 6,
        vmem((seq, 3 * own), BF),
        vmem((seq, 3 * own), BF),
        vmem((seq, own), BF),
        vmem((seq, own), BF),
        vmem((heads, seq, seq), BF),
        tokens_buf,
        vmem((2, 3, count, width), BF),
        vmem((count, width), BF),
        vmem((count, width), F32),
        vmem((count, width), F32),
        vmem((nz, ny * nh * rows, seq), BF),
        vmem((count, width), BF),
        vmem((6, 1, width), F32),
        vmem((count, width), BF),
        vmem((count, width), BF),
        vmem((count, width), F32),
        vmem((3, rows, width), F32),
        dma((4,)),
        dma((5,)),
        dma((3, 5)), dma((3, 2)), dma((3, 3, 2)), dma((3, 3)), dma((3, 2)), dma((3, 2)),
        dma((2,)), dma((3 + heads, 3, 2)), dma((3 + heads, 3)), dma((3 + heads,)), dma((3 + heads,)),
        dma((2, 2, 3)),
        dma((4,)), dma((4, 3)), dma((4,)), dma((4, 3)),
    ]
    whole = pl.BlockSpec(memory_space=pl.ANY)
    final, dx, grads = pl.pallas_call(
        functools.partial(kernel, dims),
        out_shape=(
            jax.ShapeDtypeStruct((count, width), BF),
            jax.ShapeDtypeStruct((count, width), F32),
            jax.ShapeDtypeStruct((3, rows, width), F32),
        ),
        in_specs=[whole] * 7,
        out_specs=(whole,) * 3,
        scratch_shapes=scratch,
        compiler_params=pltpu.CompilerParams(
            collective_id=0, has_side_effects=True, vmem_limit_bytes=67043328
        ),
    )(
        tokens[0], modulation[0].transpose(1, 0, 2), w_qkv[0].transpose(1, 0, 2), w_out[0].T,
        w_in[0], w_back[0].T, out_grad[0],
    )
    final, dx, qkv, out, inner, back = pl.pallas_call(
        place,
        out_shape=(
            jax.ShapeDtypeStruct((1, count, width), BF),
            jax.ShapeDtypeStruct((1, count, width), F32),
            jax.ShapeDtypeStruct((3, rows, own), F32),
            jax.ShapeDtypeStruct((rows, own), F32),
            jax.ShapeDtypeStruct((1, rows, width), F32),
            jax.ShapeDtypeStruct((rows, width), F32),
        ),
        in_specs=[whole] * 3,
        out_specs=(whole,) * 6,
        scratch_shapes=[
            vmem((count, width), BF), vmem((count, width), F32), vmem((3, rows, width), F32),
            dma((5,)), dma((5 + 3 * heads,)),
        ],
    )(final, dx, grads)
    return final, dx, qkv.transpose(1, 0, 2)[None], out.T[None], inner, back.T[None]


def solution(mesh):
    dims = (4, 4, 2)
    assert mesh.shape["fsdp"] == 32 and mesh.shape["sp"] == 4
    torus = Mesh(mesh.devices.reshape(*dims, 2, 2), AXES)
    fsdp, sp = AXES[:3], AXES[3:]
    placed = (
        P(fsdp, sp, None),
        P(fsdp, None, None, None),
        P(None, fsdp, None, sp),
        P(None, sp, fsdp),
        P(None, fsdp, sp),
        P(None, sp, fsdp),
        P(fsdp, sp, None),
    )
    return jax.shard_map(
        functools.partial(step, dims),
        mesh=torus,
        in_specs=placed,
        out_specs=(placed[0], *placed[:1], *placed[2:6]),
        check_vma=False,
    )
```
